32 devices in a mesh: dp: 16 (over z, y, core), tensor: 2 (over x).
Axes of the slice: x: 2, y: 2, z: 4, core: 2. Of those that a mesh axis runs over, the one named last changes fastest.
Arguments:
- block_in: float32 [4096, 2048], P(('dp', 'tensor')), may hold values from -6 to 6
- positions: int32 [16, 256], P('dp'), may hold values from 0 to 255, each once within a row
- out_grad: float32 [4096, 2048], P(('dp', 'tensor')), may hold values from -6 to 6
- attn_weight: float32 [2048, 4, 2048], P('dp', None, 'tensor'), may hold values from -3 to 3
- mlp_weight: float32 [2048, 2, 8192], P('dp', None, 'tensor'), may hold values from -0.125 to 0.125
- small_params: float32 [12, 2048], P(None, ('dp', 'tensor')), may hold values from -1 to 2, as said below
- attn_first: float32 [2048, 4, 2048], P('dp', None, 'tensor'), may hold values from -12 to 12
- attn_second: float32 [2048, 4, 2048], P('dp', None, 'tensor'), may hold values from 1 to 100
- mlp_first: float32 [2048, 2, 8192], P('dp', None, 'tensor'), may hold values from -12 to 12
- mlp_second: float32 [2048, 2, 8192], P('dp', None, 'tensor'), may hold values from 1 to 100
- small_first: float32 [12, 2048], P(None, ('dp', 'tensor')), may hold values from -12 to 12
- small_second: float32 [12, 2048], P(None, ('dp', 'tensor')), may hold values from 1 to 100
Outputs:
- block_out: float32 [4096, 2048], P(('dp', 'tensor'))
- input_grad: float32 [4096, 2048], P(('dp', 'tensor'))
- attn_grad: float32 [2048, 4, 2048], P('dp', None, 'tensor')
- mlp_grad: float32 [2048, 2, 8192], P('dp', None, 'tensor')
- small_grad: float32 [12, 2048], P(None, ('dp', 'tensor'))
- attn_new: float32 [2048, 4, 2048], P('dp', None, 'tensor')
- attn_first_new: float32 [2048, 4, 2048], P('dp', None, 'tensor')
- attn_second_new: float32 [2048, 4, 2048], P('dp', None, 'tensor')
- mlp_new: float32 [2048, 2, 8192], P('dp', None, 'tensor')
- mlp_first_new: float32 [2048, 2, 8192], P('dp', None, 'tensor')
- mlp_second_new: float32 [2048, 2, 8192], P('dp', None, 'tensor')
- small_new: float32 [12, 2048], P(None, ('dp', 'tensor'))
- small_first_new: float32 [12, 2048], P(None, ('dp', 'tensor'))
- small_second_new: float32 [12, 2048], P(None, ('dp', 'tensor'))
The draws below stay inside these ranges and needn't reach their ends.
Inputs may be any that keep to these rules, and one draw needn't show every extreme that they name: Each row of positions holds every position once. `small_params`: rows 0 and 2 are positive.
All inputs are finite; a program needn't handle non-finite values.
Results may differ from the reference program's by a relative error of at most 0.0092.
Values may be sent and summed in bfloat16 or wider, within the bound.
A program may use at most 448 MiB of HBM per device.

```python
import math
import jax
import jax.numpy as jnp
from jax import lax

D = 2048
HEADS = 8
FF = 8192
ROT = 64
SEQ = 256
ADAM_STEP = 3
HEAD_DIM = 256
SEQS = 16
TOKENS = 4096


def draw_attn_weight(key, part):
    base_draw = jnp.clip(jax.random.normal(key, (D, 4, D), jnp.float32), -6.0, 6.0)
    slot_scales = jnp.array([1.0, 1.0, 1.0, 4.0], jnp.float32) * D ** (-0.5)
    base_draw = base_draw * slot_scales[None, :, None]
    return base_draw


def draw_small_params(key, part):
    gain_key, bias_key = jax.random.split(key)
    gain_draw = jax.random.uniform(gain_key, (12, D), jnp.float32, 0.5, 1.5)
    biases = jnp.clip(jax.random.normal(bias_key, (12, D), jnp.float32), -3.0, 3.0) * 0.3
    row_ids = jnp.arange(12)[:, None]
    return jnp.where((row_ids == 0) | (row_ids == 2), gain_draw, biases)


def block_levels(own_key, extent, cuts, smallest, largest):
    def one(position, shards_of):
        heights = jax.random.uniform(jax.random.fold_in(jax.random.fold_in(own_key, 6), position), (shards_of,), jnp.float32, smallest / len(cuts), largest / len(cuts))
        return jnp.repeat(jnp.exp(heights), extent[position] // shards_of).reshape((-1,) + (1,) * (len(extent) - position - 1))

    gain = one(*cuts[0])
    for cut in cuts[1:]:
        gain = gain * one(*cut)
    return gain


def normal_values(rng, extent, deviation, limit, pieces=(), dtype=jnp.bfloat16):
    loudness = block_levels(rng, extent, pieces, -0.22, 0.18) if pieces else 1.0
    drawn = jax.random.normal(rng, extent, jnp.float32) * deviation * loudness
    return jnp.minimum(jnp.maximum(drawn, -limit), limit).astype(dtype)


def setup_inputs(seed: int = 0) -> dict:
    seeds = jax.random.split(jax.random.key(seed), 13)
    block_in = normal_values(seeds[0], (TOKENS, D), 1.0, 6.0, ((0, 32),), jnp.float32)
    positions = jax.vmap(lambda own: jax.random.permutation(own, SEQ))(jax.random.split(seeds[1], SEQS)).reshape((SEQS, SEQ)).astype(jnp.int32)
    out_grad = normal_values(seeds[2], (TOKENS, D), 1.0, 6.0, ((0, 32),), jnp.float32)
    attn_weight = draw_attn_weight(jax.random.fold_in(seeds[12], 71), 0)
    mlp_weight = normal_values(seeds[4], (D, 2, FF), D ** -0.5, 0.125, ((0, 16), (2, 2)), jnp.float32)
    small_params = draw_small_params(jax.random.fold_in(seeds[12], 71), 0)
    attn_first = normal_values(seeds[6], (D, 4, D), 2.0, 12.0, ((0, 16), (2, 2)), jnp.float32)
    attn_second = jnp.clip(jnp.exp(math.log(100.0) - 4.6051702 * jax.random.uniform(seeds[7], (D, 4, D), jnp.float32) ** block_levels(seeds[7], (D, 4, D), ((0, 16), (2, 2)), -0.2, 0.2)), 1.0, 100.0)
    mlp_first = normal_values(seeds[8], (D, 2, FF), 2.0, 12.0, ((0, 16), (2, 2)), jnp.float32)
    mlp_second = jnp.clip(jnp.exp(math.log(100.0) - 4.6051702 * jax.random.uniform(seeds[9], (D, 2, FF), jnp.float32) ** block_levels(seeds[9], (D, 2, FF), ((0, 16), (2, 2)), -0.2, 0.2)), 1.0, 100.0)
    small_first = normal_values(seeds[10], (12, D), 2.0, 12.0, ((1, 32),), jnp.float32)
    small_second = jnp.clip(jnp.exp(math.log(100.0) - 4.6051702 * jax.random.uniform(seeds[11], (12, D), jnp.float32) ** block_levels(seeds[11], (12, D), ((1, 32),), -0.2, 0.2)), 1.0, 100.0)
    return {"block_in": block_in, "positions": positions, "out_grad": out_grad, "attn_weight": attn_weight, "mlp_weight": mlp_weight, "small_params": small_params, "attn_first": attn_first, "attn_second": attn_second, "mlp_first": mlp_first, "mlp_second": mlp_second, "small_first": small_first, "small_second": small_second}


norm_epsilon = 1e-05
learn_rate = 0.006
beta_first = 0.9
beta_second = 0.95
adam_epsilon = 1e-08
weight_decay = 0.1

def layer_stats(row_data):
    center = row_data - lax.optimization_barrier(jnp.mean(row_data, axis=-1, keepdims=True))
    inverse = lax.rsqrt(lax.optimization_barrier(jnp.mean(center * center, axis=-1, keepdims=True)) + norm_epsilon)
    return (center * inverse, inverse)

def norm_back(grad_rows, gain_row, normed, inverse):
    scaled = grad_rows * gain_row
    return inverse * (scaled - lax.optimization_barrier(jnp.mean(scaled, axis=-1, keepdims=True)) - normed * lax.optimization_barrier(jnp.mean(scaled * normed, axis=-1, keepdims=True)))

def angle_tables(places):
    half_dims = ROT // 2
    frequency = 10000.0 ** (-(jnp.arange(half_dims).astype(jnp.float32) * (2.0 / ROT)))
    angles = places.astype(jnp.float32)[:, None] * frequency[None, :]
    return (jnp.cos(angles)[:, None, :], jnp.sin(angles)[:, None, :])

def rotate(values, cos_table, sin_table):
    half_dims = ROT // 2
    low_half = values[..., :half_dims]
    high_half = values[..., half_dims:ROT]
    return jnp.concatenate([low_half * cos_table - high_half * sin_table, high_half * cos_table + low_half * sin_table, values[..., ROT:]], axis=-1)

def rotate_back(grad_rows, cos_table, sin_table):
    half_dims = ROT // 2
    low_half = grad_rows[..., :half_dims]
    high_half = grad_rows[..., half_dims:ROT]
    return jnp.concatenate([low_half * cos_table + high_half * sin_table, high_half * cos_table - low_half * sin_table, grad_rows[..., ROT:]], axis=-1)

def gelu_exact(pre_act):
    return 0.5 * pre_act * (1.0 + lax.erf(pre_act * 0.7071067811865476))

def gelu_slope(pre_act):
    return 0.5 * (1.0 + lax.erf(pre_act * 0.7071067811865476)) + pre_act * jnp.exp(-0.5 * pre_act * pre_act) * 0.3989422804014327

def adam_step(weight, gradient, moment_one, moment_two):
    one_new = beta_first * moment_one + (1.0 - beta_first) * gradient
    two_new = beta_second * moment_two + (1.0 - beta_second) * gradient * gradient
    corrected = one_new / (1.0 - beta_first ** ADAM_STEP) / (jnp.sqrt(two_new / (1.0 - beta_second ** ADAM_STEP)) + adam_epsilon)
    return (weight - learn_rate * (corrected + weight_decay * weight), one_new, two_new)

def reference(block_in, positions, out_grad, attn_weight, mlp_weight, small_params, attn_first, attn_second, mlp_first, mlp_second, small_first, small_second):
    attn_low = attn_weight.astype(jnp.bfloat16)
    mlp_low = mlp_weight.astype(jnp.bfloat16)
    up_bias = small_params[8:12].reshape(-1)
    score_scale = HEAD_DIM ** (-0.5)
    f32 = jnp.float32
    bf16_type = jnp.bfloat16

    def one_sequence(totals, inputs):
        row_data, places, grad_data = inputs
        seq_rows = row_data.shape[0]
        normed, inverse = layer_stats(row_data)
        norm_one = (normed * small_params[0] + small_params[1]).astype(bf16_type)
        norm_two = (normed * small_params[2] + small_params[3]).astype(bf16_type)
        cos_table, sin_table = angle_tables(places)
        query_pre = jnp.dot(norm_one, attn_low[:, 0, :], preferred_element_type=f32) + small_params[4]
        key_pre = jnp.dot(norm_one, attn_low[:, 1, :], preferred_element_type=f32)
        values_low = (jnp.dot(norm_one, attn_low[:, 2, :], preferred_element_type=f32) + small_params[5]).astype(bf16_type).reshape(seq_rows, HEADS, HEAD_DIM)
        queries = rotate(query_pre.reshape(seq_rows, HEADS, HEAD_DIM), cos_table, sin_table).astype(bf16_type)
        key_rows = rotate(key_pre.reshape(seq_rows, HEADS, HEAD_DIM), cos_table, sin_table).astype(bf16_type)
        visible = places[None, :] <= places[:, None]
        scores = jnp.einsum('qhd,khd->hqk', queries.astype(f32), key_rows.astype(f32)) * score_scale
        scores = jnp.where(visible[None], scores, -jnp.inf)
        row_max = lax.optimization_barrier(jnp.max(scores, axis=-1, keepdims=True))
        log_total = row_max + jnp.log(lax.optimization_barrier(jnp.sum(jnp.exp(scores - row_max), axis=-1, keepdims=True)))
        attn_probs = jnp.exp(scores - log_total)
        probs_low = attn_probs.astype(bf16_type)
        attended = jnp.einsum('hqk,khd->qhd', probs_low.astype(f32), values_low.astype(f32)).astype(bf16_type).reshape(seq_rows, D)
        attn_branch = jnp.dot(attended, attn_low[:, 3, :].T, preferred_element_type=f32)
        pre_act = jnp.dot(norm_two, mlp_low[:, 0, :], preferred_element_type=f32) + up_bias
        activation = gelu_exact(pre_act).astype(bf16_type)
        mlp_branch = jnp.dot(activation, mlp_low[:, 1, :].T, preferred_element_type=f32)
        block_rows = row_data + attn_branch + mlp_branch + small_params[6] + small_params[7]
        grad_low = grad_data.astype(bf16_type)
        d_attended = jnp.dot(grad_low, attn_low[:, 3, :], preferred_element_type=f32).astype(bf16_type).reshape(seq_rows, HEADS, HEAD_DIM)
        d_probs = jnp.einsum('qhd,khd->hqk', d_attended.astype(f32), values_low.astype(f32))
        d_scores = (attn_probs * (d_probs - lax.optimization_barrier(jnp.sum(attn_probs * d_probs, axis=-1, keepdims=True))) * score_scale).astype(bf16_type)
        d_query = rotate_back(jnp.einsum('hqk,khd->qhd', d_scores.astype(f32), key_rows.astype(f32)), cos_table, sin_table).reshape(seq_rows, D)
        d_key = rotate_back(jnp.einsum('hqk,qhd->khd', d_scores.astype(f32), queries.astype(f32)), cos_table, sin_table).reshape(seq_rows, D)
        d_value = jnp.einsum('hqk,qhd->khd', probs_low.astype(f32), d_attended.astype(f32)).reshape(seq_rows, D)
        dq_low = d_query.astype(bf16_type)
        dk_low = d_key.astype(bf16_type)
        dv_low = d_value.astype(bf16_type)
        d_norm_one = jnp.dot(dq_low, attn_low[:, 0, :].T, preferred_element_type=f32) + jnp.dot(dk_low, attn_low[:, 1, :].T, preferred_element_type=f32) + jnp.dot(dv_low, attn_low[:, 2, :].T, preferred_element_type=f32)
        d_pre = jnp.dot(grad_low, mlp_low[:, 1, :], preferred_element_type=f32) * gelu_slope(pre_act)
        d_pre_low = d_pre.astype(bf16_type)
        d_norm_two = jnp.dot(d_pre_low, mlp_low[:, 0, :].T, preferred_element_type=f32)
        input_rows = grad_data + norm_back(d_norm_one, small_params[0], normed, inverse) + norm_back(d_norm_two, small_params[2], normed, inverse)
        attn_terms = jnp.stack([jnp.dot(norm_one.T, dq_low, preferred_element_type=f32), jnp.dot(norm_one.T, dk_low, preferred_element_type=f32), jnp.dot(norm_one.T, dv_low, preferred_element_type=f32), jnp.dot(grad_low.T, attended, preferred_element_type=f32)], axis=1)
        mlp_terms = jnp.stack([jnp.dot(norm_two.T, d_pre_low, preferred_element_type=f32), jnp.dot(grad_low.T, activation, preferred_element_type=f32)], axis=1)
        out_sum = lax.optimization_barrier(jnp.sum(grad_data, axis=0))
        small_terms = jnp.concatenate([jnp.stack([lax.optimization_barrier(jnp.sum(d_norm_one * normed, axis=0)), lax.optimization_barrier(jnp.sum(d_norm_one, axis=0)), lax.optimization_barrier(jnp.sum(d_norm_two * normed, axis=0)), lax.optimization_barrier(jnp.sum(d_norm_two, axis=0)), lax.optimization_barrier(jnp.sum(d_query, axis=0)), lax.optimization_barrier(jnp.sum(d_value, axis=0)), out_sum, out_sum]), lax.optimization_barrier(jnp.sum(d_pre, axis=0)).reshape(4, D)], axis=0)
        return ((totals[0] + attn_terms, totals[1] + mlp_terms, totals[2] + small_terms), (block_rows, input_rows))
    initial = (jnp.zeros((D, 4, D), jnp.float32), jnp.zeros((D, 2, FF), jnp.float32), jnp.zeros((12, D), jnp.float32))
    totals, (block_rows, input_rows) = lax.scan(one_sequence, initial, (block_in.reshape(-1, SEQ, D), positions, out_grad.reshape(-1, SEQ, D)))
    attn_grad, mlp_grad, small_grad = totals
    attn_new, attn_first_new, attn_second_new = adam_step(attn_weight, attn_grad, attn_first, attn_second)
    mlp_new, mlp_first_new, mlp_second_new = adam_step(mlp_weight, mlp_grad, mlp_first, mlp_second)
    small_new, small_first_new, small_second_new = adam_step(small_params, small_grad, small_first, small_second)
    return (block_rows.reshape(-1, D), input_rows.reshape(-1, D), attn_grad, mlp_grad, small_grad, attn_new, attn_first_new, attn_second_new, mlp_new, mlp_first_new, mlp_second_new, small_new, small_first_new, small_second_new)
```

```python
import functools

import jax
import jax.numpy as jnp
from jax import lax
from jax.experimental import pallas as pl
from jax.experimental.pallas import tpu as pltpu
from jax.sharding import PartitionSpec as P

ROT = 64
ADAM_STEP = 3
HEAD_DIM = 256
Z = 4

norm_epsilon = 1e-05
learn_rate = 0.006
beta_first = 0.9
beta_second = 0.95
adam_epsilon = 1e-08
weight_decay = 0.1

f32 = jnp.float32
bf16 = jnp.bfloat16


def layer_stats(row_data):
    center = row_data - jnp.mean(row_data, axis=-1, keepdims=True)
    inverse = lax.rsqrt(jnp.mean(center * center, axis=-1, keepdims=True) + norm_epsilon)
    return (center * inverse, inverse)


def angle_tables(places):
    half_dims = ROT // 2
    frequency = 10000.0 ** (-(jnp.arange(half_dims).astype(f32) * (2.0 / ROT)))
    angles = places[..., None] * frequency
    return (jnp.cos(angles), jnp.sin(angles))


def rotate(values, cos_table, sin_table):
    half_dims = ROT // 2
    low_half = values[..., :half_dims]
    high_half = values[..., half_dims:ROT]
    return jnp.concatenate(
        [
            low_half * cos_table - high_half * sin_table,
            high_half * cos_table + low_half * sin_table,
            values[..., ROT:],
        ],
        axis=-1,
    )


def gelu_exact(pre_act):
    return 0.5 * pre_act * (1.0 + lax.erf(pre_act * 0.7071067811865476))


def gelu_slope(pre_act):
    return (
        0.5 * (1.0 + lax.erf(pre_act * 0.7071067811865476))
        + pre_act * jnp.exp(-0.5 * pre_act * pre_act) * 0.3989422804014327
    )


def adam_step(weight, gradient, moment_one, moment_two):
    one_new = beta_first * moment_one + (1.0 - beta_first) * gradient
    two_new = beta_second * moment_two + (1.0 - beta_second) * gradient * gradient
    corrected = (
        one_new
        / (1.0 - beta_first**ADAM_STEP)
        / (jnp.sqrt(two_new / (1.0 - beta_second**ADAM_STEP)) + adam_epsilon)
    )
    return (weight - learn_rate * (corrected + weight_decay * weight), one_new, two_new)


class Grid:
    def __init__(self, dp, tensor):
        assert tensor == 2 and dp % (2 * Z) == 0
        self.dp, self.m = dp, dp // (2 * Z)
        index = lax.axis_index("dp")
        self.index = index * 2 + lax.axis_index("tensor")
        self.z_now = index // (2 * self.m)
        self.m_now = (index // 2) % self.m
        self.c_now = index % 2
        self.t_now = lax.axis_index("tensor")
        self.diag = self.c_now == self.t_now


def split_kernel(attn, mlp, qk, vo, up, dn):
    quarter_a = attn.shape[2] // Z
    quarter_m = mlp.shape[2] // Z
    for q in range(Z):
        for j in range(4):
            block = attn[:, j, q * quarter_a : (q + 1) * quarter_a].astype(bf16)
            (qk, qk, vo, vo)[j][q, :, (j % 2) * quarter_a : (j % 2 + 1) * quarter_a] = block
        for j in range(2):
            (up, dn)[j][q] = mlp[:, j, q * quarter_m : (q + 1) * quarter_m].astype(bf16)


def split_weights(attn_weight, mlp_weight):
    rows, _, width = attn_weight.shape
    hidden = mlp_weight.shape[2]
    step = min(rows, 32)
    shapes = [2 * width // Z] * 2 + [hidden // Z] * 2
    return pl.pallas_call(
        split_kernel,
        grid=(rows // step,),
        in_specs=[
            pl.BlockSpec((step, 4, width), lambda i: (i, 0, 0)),
            pl.BlockSpec((step, 2, hidden), lambda i: (i, 0, 0)),
        ],
        out_specs=[pl.BlockSpec((Z, step, n), lambda i: (0, i, 0)) for n in shapes],
        out_shape=[jax.ShapeDtypeStruct((Z, rows, n), bf16) for n in shapes],
        name="split_weights",
    )(attn_weight, mlp_weight)


MESH = pl.DeviceIdType.MESH
M_FIRST = (True, False, True, False)


class Links:
    def __init__(self, m_size):
        self.m_size = m_size
        index = lax.axis_index("dp")
        self.z, self.m, self.c = index // (2 * m_size), (index // 2) % m_size, index % 2
        self.t = lax.axis_index("tensor")
        self.sends = []

    def to(self, z=None, m=None, c=None, t=None):
        z, m, c = (own if v is None else v for v, own in ((z, self.z), (m, self.m), (c, self.c)))
        return ((z * self.m_size + m) * 2 + c, self.t if t is None else t)

    def copy(self, src, dst, send_sem, recv_sem, target):
        return pltpu.make_async_remote_copy(
            src_ref=src, dst_ref=dst, send_sem=send_sem, recv_sem=recv_sem, device_id=target, device_id_type=MESH
        )

    def send(self, src, dst, send_sem, recv_sem, target):
        one = self.copy(src, dst, send_sem, recv_sem, target)
        one.start()
        self.sends.append(one)

    def landed(self, dst, recv_sem):
        self.copy(dst, dst, recv_sem, recv_sem, self.to(c=1 - self.c)).wait_recv()

    def drain(self):
        for one in self.sends:
            one.wait_send()

    def partners(self):
        other = 1 - self.t
        out = [self.to(z=self.z ^ k) for k in range(1, Z)]
        out += [self.to(m=self.m ^ j) for j in range(1, self.m_size)]
        out += [self.to(c=1 - self.c), self.to(t=other), self.to(c=1 - self.c, t=other)]
        return out

    def meet(self):
        barrier = pltpu.get_barrier_semaphore()
        everyone = self.partners()
        for target in everyone:
            pl.semaphore_signal(barrier, inc=1, device_id=target, device_id_type=MESH)
        pl.semaphore_wait(barrier, len(everyone))


def gather_kernel(m_size, *refs):
    pieces, low, mine_small = refs[:4], refs[4], refs[5]
    full, act, table = refs[6:10], refs[10], refs[11]
    stage, stage_m = refs[12:16], refs[16:20]
    (zs, zr, ps, pr, ms, mr, near_s, far_s, xr, as_, ar, ws, wr, ss, sr) = refs[20:35]
    bounce, bounce_low, lin, lout = refs[35:39], refs[39], refs[40], refs[41]
    net = Links(m_size)
    z, m, c, t = net.z, net.m, net.c, net.t
    rows = pieces[0].shape[1]
    half = low.shape[1]
    role = lax.rem(c + t, 2)

    def by_role(do):
        @pl.when(role == 0)
        def _():
            do(True)

        @pl.when(role == 1)
        def _():
            do(False)

    def block(zz, mm, cc, count=1):
        start = ((zz * m_size + mm) * 2 + cc) * rows
        return pl.ds(pl.multiple_of(start, rows), count * rows)

    own_place = pl.ds(pl.multiple_of(z * 2 * half + t * half, half), half)
    place = lambda zz, h: pl.ds(pl.multiple_of(zz * 2 * half + (t ^ h) * half, half), half)

    loads = [pltpu.make_async_copy(pieces[ch].at[z], bounce[ch], lin.at[ch]) for ch in range(4)]
    loads.append(pltpu.make_async_copy(low.at[0], bounce_low, lin.at[4]))
    stores = [pltpu.make_async_copy(bounce[ch], full[ch].at[block(z, m, c)], lout.at[ch]) for ch in range(4)]
    stores.append(pltpu.make_async_copy(bounce_low, act.at[0, own_place], lout.at[4]))

    def load_own(diag):
        if diag:
            for one in loads:
                one.start()

    by_role(load_own)
    net.meet()

    near = net.copy(low.at[1], act.at[1, own_place], near_s, xr.at[0], net.to(c=1 - c))
    far = [
        net.copy(low.at[0], act.at[0, own_place], near_s, xr.at[1], net.to(t=1 - t)),
        net.copy(low.at[1], act.at[1, own_place], far_s, xr.at[1], net.to(c=1 - c, t=1 - t)),
    ]

    def rows_out(diag):
        if diag:
            near.start()
        else:
            for one in far:
                one.start()

    by_role(rows_out)

    steps = [(1, net.to(t=1 - t)), (2, net.to(c=1 - c))]
    j = 1
    while j < m_size:
        steps.append((4 * j, net.to(m=m ^ j)))
        j *= 2
    steps += [(4 * m_size, net.to(z=z ^ 1)), (8 * m_size, net.to(z=z ^ 3))]
    flat = ((z * m_size + m) * 2 + c) * 2 + t
    small_own = pltpu.make_async_copy(mine_small, table.at[flat], ss.at[len(steps)])
    small_own.start()
    state = {"small": 0}

    def small_send():
        i = state["small"]
        if i < len(steps):
            size, target = steps[i]
            span = table.at[pl.ds(flat // size * size, size)]
            net.send(span, span, ss.at[i], sr.at[i], target)

    def small_next():
        i = state["small"]
        if i < len(steps):
            size = steps[i][0]
            net.landed(table.at[pl.ds((flat // size ^ 1) * size, size)], sr.at[i])
            state["small"] += 1
            small_send()

    def spot(diag, ch, zz, j):
        if diag:
            return full[ch].at[block(zz, m ^ j, c)]
        return stage_m[ch].at[m ^ j, zz] if j else stage[ch].at[zz]

    order = [(ch, k) for ch in range(4) for k in (0, 1, 3, 2)]

    def quarters_out(diag):
        for ch, k in order:
            if k:
                net.copy(
                    pieces[ch].at[z ^ k], spot(diag, ch, z, 0), zs.at[ch, k], zr.at[ch, k], net.to(z=z ^ k)
                ).start()

    by_role(quarters_out)
    small_own.wait()
    small_send()

    def store_own(diag):
        if diag:
            for load, store in zip(loads, stores):
                load.wait()
                store.start()

    by_role(store_own)

    def source(diag, ch, k, j):
        return pieces[ch].at[z] if k == 0 and j == 0 else spot(diag, ch, z ^ k, j)

    def spread(diag, ch, k, j):
        src = source(diag, ch, k, j)
        dst = full[ch].at[block(z ^ k, m ^ j, c)]
        net.copy(src, dst, ps.at[ch, j, k, 1], pr.at[ch, j, k, c], net.to(c=t, t=1 - t)).start()
        if not diag:
            net.copy(src, dst, ps.at[ch, j, k, 0], pr.at[ch, j, k, c], net.to(c=1 - c)).start()

    def spread_landed(diag, ch, k, j):
        for cc in (1 - c,) if diag else (1 - c, c):
            net.landed(full[ch].at[block(z ^ k, m ^ j, cc)], pr.at[ch, j, k, cc])

    def first(ch, k):
        def do(diag):
            if k:
                net.landed(spot(diag, ch, z ^ k, 0), zr.at[ch, k])
            if M_FIRST[ch]:
                for j in range(1, m_size):
                    dst = full[ch].at[block(z ^ k, m, c)] if diag else stage_m[ch].at[m, z ^ k]
                    net.copy(
                        source(diag, ch, k, 0), dst, ms.at[ch, j, k], mr.at[ch, j, k], net.to(m=m ^ j)
                    ).start()
            spread(diag, ch, k, 0)

        by_role(do)

    def second(ch, k):
        def do(diag):
            if M_FIRST[ch]:
                for j in range(1, m_size):
                    net.landed(spot(diag, ch, z ^ k, j), mr.at[ch, j, k])
                    spread(diag, ch, k, j)
            else:
                if diag and k == 0:
                    stores[ch].wait()
                spread_landed(diag, ch, k, 0)
                both = full[ch].at[block(z ^ k, m, 0, 2)]
                for j in range(1, m_size):
                    net.copy(both, both, ms.at[ch, j, k], mr.at[ch, j, k], net.to(m=m ^ j)).start()

        by_role(do)

    def third(ch, k):
        def do(diag):
            if M_FIRST[ch]:
                for j in range(m_size):
                    spread_landed(diag, ch, k, j)
                if diag and k == 0:
                    stores[ch].wait()
            else:
                for j in range(1, m_size):
                    net.landed(full[ch].at[block(z ^ k, m ^ j, 0, 2)], mr.at[ch, j, k])

        by_role(do)

    def drain(ch, k):
        def do(diag):
            if k:
                src = pieces[ch].at[z ^ k]
                net.copy(src, src, zs.at[ch, k], zr.at[ch, k], net.to(z=z ^ k)).wait_send()
            if M_FIRST[ch]:
                src = source(diag, ch, k, 0)
            else:
                src = full[ch].at[block(z ^ k, m, 0, 2)]
            for j in range(1, m_size):
                net.copy(src, src, ms.at[ch, j, k], mr.at[ch, j, k], net.to(m=m ^ j)).wait_send()
            for j in range(m_size if M_FIRST[ch] else 1):
                src = source(diag, ch, k, j)
                for side in (1,) if diag else (1, 0):
                    net.copy(src, src, ps.at[ch, j, k, side], pr.at[ch, j, k, 0], net.to(c=1 - c)).wait_send()

        by_role(do)

    own_first = [p for p in order if p[1] == 0] + [p for p in order if p[1]]

    def rows_start(h):
        def do(diag):
            if h:
                net.landed(act.at[0 if diag else 1, place(z, 1)], xr.at[1])
            elif diag:
                stores[4].wait()
            else:
                net.landed(act.at[1, place(z, 0)], xr.at[0])

        by_role(do)
        src = act.at[role, place(z, h)]
        net.send(src, src, as_.at[h, 0], ar.at[h, 0], net.to(z=z ^ 3))
        net.send(src, src, as_.at[h, 1], ar.at[h, 1], net.to(z=z ^ 1))
        net.send(src, src, ws.at[0, h], wr.at[0, h], net.to(c=1 - c))

    def rows_far(h):
        src = act.at[role, place(z ^ 3, h)]
        net.landed(src, ar.at[h, 0])
        net.send(src, src, as_.at[h, 2], ar.at[h, 2], net.to(z=z ^ 1))
        net.send(src, src, ws.at[3, h], wr.at[3, h], net.to(c=1 - c))

    def rows_last(h, k):
        src = act.at[role, place(z ^ k, h)]
        net.landed(src, ar.at[h, k])
        net.send(src, src, ws.at[k, h], wr.at[k, h], net.to(c=1 - c))

    for ch, k in own_first[:4]:
        first(ch, k)
    small_next()
    rows_start(0)
    small_next()
    rows_start(1)
    small_next()
    pending = list(own_first[:4])
    for i, (ch, k) in enumerate(own_first[4:]):
        first(ch, k)
        pending.append((ch, k))
        if len(pending) > 3:
            second(*pending.pop(0))
        if i % 3 == 2:
            small_next()
    rows_far(0)
    while pending:
        second(*pending.pop(0))
    while state["small"] < len(steps):
        small_next()
    rows_far(1)
    for h in range(2):
        rows_last(h, 1)
    for ch, k in own_first:
        third(ch, k)
    for h in range(2):
        rows_last(h, 2)
    for k in (0, 3, 1, 2):
        for h in range(2):
            net.landed(act.at[1 - role, place(z ^ k, h)], wr.at[k, h])
    net.drain()
    for ch, k in order:
        drain(ch, k)

    def rows_drain(diag):
        if diag:
            near.wait_send()
        else:
            for one in far:
                one.wait_send()

    by_role(rows_drain)


def gather(pieces, low, small, m_size):
    rows = pieces[0].shape[1]
    width = low.shape[2]
    devices = m_size * 4 * Z
    cols = [p.shape[2] for p in pieces]
    stages = [jax.ShapeDtypeStruct((Z, rows, n), bf16) for n in cols]
    stages_m = [jax.ShapeDtypeStruct((m_size, Z, rows, n), bf16) for n in cols]
    sem = pltpu.SemaphoreType.DMA
    doubling = m_size.bit_length() - 1 + 4
    outs = pl.pallas_call(
        functools.partial(gather_kernel, m_size),
        out_shape=[jax.ShapeDtypeStruct((width, n), bf16) for n in cols]
        + [
            jax.ShapeDtypeStruct((2, Z * 2 * low.shape[1], width), bf16),
            jax.ShapeDtypeStruct((devices,) + small.shape, f32),
        ]
        + stages
        + stages_m,
        in_specs=[pl.BlockSpec(memory_space=pl.ANY)] * 6,
        out_specs=[pl.BlockSpec(memory_space=pl.ANY)] * 14,
        scratch_shapes=[
            sem((4, Z)),
            sem((4, Z)),
            sem((4, m_size, Z, 2)),
            sem((4, m_size, Z, 2)),
            sem((4, m_size, Z)),
            sem((4, m_size, Z)),
            sem,
            sem,
            sem((2,)),
            sem((2, 3)),
            sem((2, 3)),
            sem((Z, 2)),
            sem((Z, 2)),
            sem((doubling + 1,)),
            sem((doubling,)),
        ]
        + [pltpu.VMEM((rows, n), bf16) for n in cols]
        + [pltpu.VMEM(low.shape[1:], bf16), sem((5,)), sem((5,))],
        compiler_params=pltpu.CompilerParams(collective_id=0, has_side_effects=True),
        name="gather_all",
    )(*pieces, low, small)
    return outs[:4], outs[4], outs[5]


def out_kernel(blocks, scalar, y_ref, one, two, plain, par, keep, send, sums):
    diag = scalar[blocks] == 1

    @pl.when(pl.program_id(0) == 0)
    def _():
        sums[...] = jnp.zeros_like(sums)

    for p in range(blocks):
        dst = pl.ds(pl.multiple_of(scalar[p] * 128, 128), 128)
        src = slice(p * 128, (p + 1) * 128)
        y, d_one, d_two = y_ref[:, src], one[:, src], two[:, src]
        x = plain[:, src].astype(f32)
        u = d_one * par[0:1, dst] + d_two * par[2:3, dst]
        keep[:, dst] = jnp.where(diag, y, u).astype(bf16)
        send[:, dst] = jnp.where(diag, u, y).astype(bf16)
        rows = [jnp.sum(v, axis=0, keepdims=True) for v in (d_one * x, d_one, d_two * x, d_two)]
        for i, row in enumerate(rows):
            sums[i : i + 1, dst] += row


def place_outs(y, d_one, d_two, plain, par, order, diag):
    rows, width = y.shape
    blocks = order.shape[0]
    if (width // blocks) % 128:
        back = jnp.argsort(order)
        take = lambda v: jnp.take(v.reshape(v.shape[0], blocks, -1), back, axis=1).reshape(v.shape)
        y, d_one, d_two, x = take(y), take(d_one), take(d_two), take(plain).astype(f32)
        u = d_one * par[0] + d_two * par[2]
        sums = jnp.stack([jnp.sum(v, axis=0) for v in (d_one * x, d_one, d_two * x, d_two)])
        return jnp.where(diag, y, u).astype(bf16), jnp.where(diag, u, y).astype(bf16), sums
    per = width // 128 // blocks
    order = (order[:, None] * per + jnp.arange(per)[None]).reshape(-1)
    blocks = blocks * per
    step = 256
    spec = pl.BlockSpec((step, width), lambda i, s: (i, 0))
    whole = pl.BlockSpec((4, width), lambda i, s: (0, 0))
    return pl.pallas_call(
        functools.partial(out_kernel, blocks),
        grid_spec=pltpu.PrefetchScalarGridSpec(
            num_scalar_prefetch=1,
            grid=(rows // step,),
            in_specs=[spec] * 4 + [whole],
            out_specs=[spec, spec, whole],
        ),
        out_shape=[jax.ShapeDtypeStruct((rows, width), bf16)] * 2
        + [jax.ShapeDtypeStruct((4, width), f32)],
        name="place_outs",
    )(
        jnp.concatenate([order, diag.astype(jnp.int32).reshape(1)]).astype(jnp.int32),
        y,
        d_one,
        d_two,
        plain,
        par,
    )


def add_rows(dst, sources):
    step = min(dst.shape[0], 32)

    @pl.loop(0, dst.shape[0] // step)
    def _(i):
        span = pl.ds(pl.multiple_of(i * step, step), step)
        total = sources[0][span, :].astype(f32)
        for one in sources[1:]:
            total = total + one[span, :].astype(f32)
        dst[span, :] = total.astype(dst.dtype)


def scatter_kernel(m_size, *refs):
    grads, keep, give, terms = refs[:4], refs[4], refs[5], refs[6]
    own, rows_out, small_out = refs[7:11], refs[11], refs[12]
    home_first, x_first, mid_first, far_first, sum_first = (refs[13 + 2 * i : 15 + 2 * i] for i in range(5))
    own_last, far_last, sum_last, home_last, x_last, sum_far = (refs[23 + 2 * i : 25 + 2 * i] for i in range(6))
    got, kept, total, got_z, three, final, current, got_small = refs[35:43]
    (cl, cs, cr, fs, fr, zs, zr, zl, dl, ds_, dr, es, er, kl, gs, gr, ys, yr, rs, rr, rl, ss, sr) = refs[43:]
    net = Links(m_size)
    z, m, c, t = net.z, net.m, net.c, net.t
    half = rows_out.shape[1]
    role = lax.rem(c + t, 2)
    first_chunks = [ch for ch in range(4) if M_FIRST[ch]]
    last_chunks = [ch for ch in range(4) if not M_FIRST[ch]]
    pairs_first = [(i, ch) for i, ch in enumerate(first_chunks)]
    pairs_last = [(i, ch) for i, ch in enumerate(last_chunks)]
    ks = (3, 2, 1, 0)

    def by_role(do):
        @pl.when(role == 0)
        def _():
            do(True)

        @pl.when(role == 1)
        def _():
            do(False)

    loads_keep = [pltpu.make_async_copy(keep.at[z ^ k], kept.at[k], kl.at[k]) for k in range(Z)]
    loads_last = {
        (i, k): pltpu.make_async_copy(grads[ch].at[z ^ k, m], own_last[i].at[k], dl.at[i, k])
        for i, ch in pairs_last
        for k in ks
    }
    loads_first = {
        (i, j, k): pltpu.make_async_copy(grads[ch].at[z ^ k, m ^ j, c], home_first[i].at[j, k], cl.at[i, j, k])
        for i, ch in pairs_first
        for j in range(m_size)
        for k in ks
    }
    for one in loads_keep:
        one.start()
    for one in loads_last.values():
        one.start()

    def load_first(diag):
        if diag:
            for one in loads_first.values():
                one.start()

    by_role(load_first)
    current[...] = terms[...]
    net.meet()

    flat = ((z * m_size + m) * 2 + c) * 2 + t
    steps = [(1, net.to(t=1 - t)), (2, net.to(c=1 - c))]
    j = 1
    while j < m_size:
        steps.append((4 * j, net.to(m=m ^ j)))
        j *= 2
    steps += [(4 * m_size, net.to(z=z ^ 1)), (8 * m_size, net.to(z=z ^ 3))]
    steps = steps[::-1]
    state = {"small": 0}

    def small_send():
        i = state["small"]
        if i < len(steps):
            size, target = steps[i]
            net.send(
                current.at[pl.ds((flat // size ^ 1) * size, size)],
                got_small.at[pl.ds(size, size)],
                ss.at[i],
                sr.at[i],
                target,
            )

    def small_next():
        i = state["small"]
        if i < len(steps):
            size = steps[i][0]
            net.landed(got_small.at[pl.ds(size, size)], sr.at[i])
            span = pl.ds(flat // size * size, size)
            current[span] = current[span] + got_small[pl.ds(size, size)]
            state["small"] += 1
            small_send()

    for k in (1, 2, 3, 0):
        net.send(give.at[z ^ k], got.at[k], gs.at[k], gr.at[k], net.to(c=1 - c))
    small_send()

    def to_owner(diag, source, home, far, sems, i, jk):
        send_sem, recv_sem = sems
        if diag:
            net.copy(source(1 - c), home, send_sem.at[i, *jk, 0], recv_sem.at[i, *jk, 0], net.to(c=1 - c)).start()
        else:
            net.copy(source(c), far, send_sem.at[i, *jk, 0], recv_sem.at[i, *jk, 1], net.to(t=1 - t)).start()
            net.copy(
                source(1 - c), far, send_sem.at[i, *jk, 1], recv_sem.at[i, *jk, 1], net.to(c=1 - c, t=1 - t)
            ).start()

    def collect_first(i, ch, j, k):
        def do(diag):
            to_owner(
                diag,
                lambda cc: grads[ch].at[z ^ k, m ^ j, cc],
                home_first[i].at[j, k],
                x_first[i].at[j, k],
                (cs, cr),
                i,
                (j, k),
            )

        by_role(do)

    for k in ks:
        for i, ch in pairs_last:
            for j in range(1, m_size):
                net.send(grads[ch].at[z ^ k, m ^ j], far_last[i].at[j - 1, k], ds_.at[i, j, k], dr.at[i, j, k], net.to(m=m ^ j))
        for i, ch in pairs_first:
            for j in range(1, m_size):
                collect_first(i, ch, j, k)
    for k in ks:
        for i, ch in pairs_first:
            collect_first(i, ch, 0, k)

    def collected_first(i, j, k):
        def do(diag):
            if diag:
                loads_first[i, j, k].wait()
            else:
                net.landed(home_first[i].at[j, k], cr.at[i, j, k, 0])

        by_role(do)
        net.landed(x_first[i].at[j, k], cr.at[i, j, k, 1])

    for one in loads_keep:
        one.wait()
    for k in (1, 2, 3, 0):
        net.landed(got.at[k], gr.at[k])
        add_rows(total.at[k], [kept.at[k], got.at[k]])
        if k in (1, 2):
            net.send(total.at[k], got_z.at[k - 1], ys.at[k], yr.at[k], net.to(z=z ^ 1))
    small_next()

    def to_z(ch, tile, k):
        if k:
            net.send(tile, own[ch].at[z], zs.at[ch, k], zr.at[ch, k], net.to(z=z ^ k))
        else:
            pltpu.make_async_copy(tile, own[ch].at[z], zl.at[ch]).start()

    def middle(k):
        for i, ch in pairs_first:
            for j in range(1, m_size):
                collected_first(i, j, k)
                add_rows(mid_first[i].at[j - 1, k], [home_first[i].at[j, k], x_first[i].at[j, k]])
                net.send(mid_first[i].at[j - 1, k], far_first[i].at[j - 1, k], fs.at[i, j, k], fr.at[i, j, k], net.to(m=m ^ j))
        for i, ch in pairs_last:
            loads_last[i, k].wait()
            for j in range(1, m_size):
                net.landed(far_last[i].at[j - 1, k], dr.at[i, j, k])
            for cc in range(2):
                add_rows(
                    sum_last[i].at[k, cc],
                    [own_last[i].at[k, cc]] + [far_last[i].at[j - 1, k, cc] for j in range(1, m_size)],
                )

            def do(diag):
                to_owner(
                    diag,
                    lambda cc: sum_last[i].at[k, cc],
                    home_last[i].at[k],
                    x_last[i].at[k],
                    (es, er),
                    i,
                    (k,),
                )

            by_role(do)

    def finish(k):
        for i, ch in pairs_first:
            collected_first(i, 0, k)
            for j in range(1, m_size):
                net.landed(far_first[i].at[j - 1, k], fr.at[i, j, k])
            add_rows(
                sum_first[i].at[k],
                [home_first[i].at[0, k], x_first[i].at[0, k]] + [far_first[i].at[j - 1, k] for j in range(1, m_size)],
            )
            to_z(ch, sum_first[i].at[k], k)
        for i, ch in pairs_last:

            def do(diag):
                net.landed(x_last[i].at[k], er.at[i, k, 1])
                if diag:
                    add_rows(sum_far[i].at[k], [sum_last[i].at[k, c], x_last[i].at[k]])
                else:
                    net.landed(home_last[i].at[k], er.at[i, k, 0])
                    add_rows(sum_far[i].at[k], [home_last[i].at[k], x_last[i].at[k]])

            by_role(do)
            to_z(ch, sum_far[i].at[k], k)

    middle(3)
    small_next()
    middle(2)
    net.landed(got_z.at[1], yr.at[2])
    add_rows(three, [total.at[3], got_z.at[1]])
    net.send(three, got_z.at[2], ys.at[3], yr.at[3], net.to(z=z ^ 3))
    small_next()
    middle(1)
    finish(3)
    small_next()
    middle(0)
    finish(2)
    while state["small"] < len(steps):
        small_next()
    small_out[...] = current[flat]
    finish(1)
    net.landed(got_z.at[0], yr.at[1])
    net.landed(got_z.at[2], yr.at[3])
    add_rows(final, [total.at[0], got_z.at[0], got_z.at[2]])
    mine = final.at[pl.ds(pl.multiple_of(t * half, half), half)]
    other = final.at[pl.ds(pl.multiple_of((1 - t) * half, half), half)]
    keep_rows = pltpu.make_async_copy(mine, rows_out.at[0], rl)

    def rows_back(diag):
        if diag:
            keep_rows.start()
            net.copy(other, rows_out.at[0], rs.at[0], rr.at[0], net.to(t=1 - t)).start()
        else:
            net.copy(mine, rows_out.at[1], rs.at[0], rr.at[1], net.to(c=1 - c)).start()
            net.copy(other, rows_out.at[1], rs.at[1], rr.at[1], net.to(c=1 - c, t=1 - t)).start()

    by_role(rows_back)
    finish(0)
    for ch in range(4):
        for k in range(1, Z):
            net.landed(own[ch].at[z ^ k], zr.at[ch, k])
        pltpu.make_async_copy(own[ch].at[z], own[ch].at[z], zl.at[ch]).wait()

    def rows_done(diag):
        net.landed(rows_out.at[1], rr.at[1])
        if diag:
            keep_rows.wait()
            net.copy(other, rows_out.at[0], rs.at[0], rr.at[0], net.to(t=1 - t)).wait_send()
        else:
            net.landed(rows_out.at[0], rr.at[0])
            net.copy(mine, rows_out.at[1], rs.at[0], rr.at[1], net.to(c=1 - c)).wait_send()
            net.copy(other, rows_out.at[1], rs.at[1], rr.at[1], net.to(c=1 - c, t=1 - t)).wait_send()

    by_role(rows_done)

    def owners_done(diag):
        for k in ks:
            for side in range(1 if diag else 2):
                for i, ch in pairs_first:
                    for j in range(m_size):
                        src = grads[ch].at[z ^ k, m ^ j, 0]
                        net.copy(src, src, cs.at[i, j, k, side], cr.at[i, j, k, 0], net.to(c=1 - c)).wait_send()
                for i, ch in pairs_last:
                    src = sum_last[i].at[k, 0]
                    net.copy(src, src, es.at[i, k, side], er.at[i, k, 0], net.to(c=1 - c)).wait_send()

    by_role(owners_done)
    net.drain()


def scatter(grads, keep, give, terms, m_size, rows):
    cols = [g.shape[1] for g in grads]
    width = keep.shape[1]
    block = width // (2 * Z * m_size)
    seq = keep.shape[0] // Z
    first = [n for ch, n in enumerate(cols) if M_FIRST[ch]]
    last = [n for ch, n in enumerate(cols) if not M_FIRST[ch]]
    nf, nl = len(first), len(last)
    sem = pltpu.SemaphoreType.DMA
    vmem = lambda *shape: pltpu.VMEM(shape, bf16)
    doubling = m_size.bit_length() - 1 + 4
    any_spec = pl.BlockSpec(memory_space=pl.ANY)
    in_vmem = pl.BlockSpec(memory_space=pltpu.VMEM)
    far = m_size - 1
    outs = pl.pallas_call(
        functools.partial(scatter_kernel, m_size),
        out_shape=[jax.ShapeDtypeStruct((Z, block, n), bf16) for n in cols]
        + [jax.ShapeDtypeStruct((2, rows, width), bf16), jax.ShapeDtypeStruct(terms.shape[1:], f32)],
        in_specs=[any_spec] * 6 + [in_vmem],
        out_specs=[any_spec] * 5 + [in_vmem],
        scratch_shapes=[vmem(m_size, Z, block, n) for n in first] * 2
        + [vmem(far, Z, block, n) for n in first] * 2
        + [vmem(Z, block, n) for n in first]
        + [vmem(Z, 2, block, n) for n in last]
        + [vmem(far, Z, 2, block, n) for n in last]
        + [vmem(Z, 2, block, n) for n in last]
        + [vmem(Z, block, n) for n in last] * 3
        + [vmem(Z, seq, width)] * 3
        + [vmem(3, seq, width), vmem(seq, width), vmem(seq, width)]
        + [pltpu.VMEM(terms.shape, f32)] * 2
        + [
            sem((nf, m_size, Z)),
            sem((nf, m_size, Z, 2)),
            sem((nf, m_size, Z, 2)),
            sem((nf, m_size, Z)),
            sem((nf, m_size, Z)),
            sem((4, Z)),
            sem((4, Z)),
            sem((4,)),
            sem((nl, Z)),
            sem((nl, m_size, Z)),
            sem((nl, m_size, Z)),
            sem((nl, Z, 2)),
            sem((nl, Z, 2)),
            sem((Z,)),
            sem((Z,)),
            sem((Z,)),
            sem((Z,)),
            sem((Z,)),
            sem((2,)),
            sem((2,)),
            sem,
            sem((doubling,)),
            sem((doubling,)),
        ],
        compiler_params=pltpu.CompilerParams(
            collective_id=1, has_side_effects=True, vmem_limit_bytes=60 * 1024 * 1024
        ),
        name="scatter_all",
    )(
        *[g.reshape(Z, m_size, 2, block, -1) for g in grads],
        keep.reshape(Z, seq, width),
        give.reshape(Z, seq, width),
        terms,
    )
    return outs[:4], outs[4], outs[5]


def adam_kernel(per, *refs):
    count = len(refs) - 7
    grads, (weight, one, two), outs = refs[:count], refs[count : count + 3], refs[count + 3 :]
    cols = weight.shape[2]
    for j in range(weight.shape[1]):
        g = grads[j // per][0, :, (j % per) * cols : (j % per + 1) * cols].astype(f32)
        w_new, one_new, two_new = adam_step(weight[:, j, :], g, one[:, j, :], two[:, j, :])
        for ref, value in zip(outs, (g, w_new, one_new, two_new)):
            ref[:, j, :] = value


def adam_update(grads, per, weight, one, two):
    rows, kinds, width = weight.shape
    cols = width // Z
    spec = pl.BlockSpec((rows, kinds, cols), lambda q: (0, 0, q))
    return pl.pallas_call(
        functools.partial(adam_kernel, per),
        grid=(Z,),
        in_specs=[pl.BlockSpec((1, rows, per * cols), lambda q: (q, 0, 0))] * len(grads) + [spec] * 3,
        out_specs=[spec] * 4,
        out_shape=[jax.ShapeDtypeStruct(weight.shape, f32)] * 4,
        name="adam_update",
    )(*grads, weight, one, two)


def body(
    block_in,
    positions,
    out_grad,
    attn_weight,
    mlp_weight,
    small_params,
    attn_first,
    attn_second,
    mlp_first,
    mlp_second,
    small_first,
    small_second,
):
    grid = Grid(lax.axis_size("dp"), lax.axis_size("tensor"))
    z, m, c, t, diag = grid.z_now, grid.m_now, grid.c_now, grid.t_now, grid.diag
    devices = grid.dp * 2
    rows, width = block_in.shape
    seq = 2 * rows
    part = small_params.shape[1]

    normed, inverse = layer_stats(block_in)
    x_low, g_low = normed.astype(bf16), out_grad.astype(bf16)

    pieces = split_weights(attn_weight, mlp_weight)
    tile = -(-12 * part // 1024) * 1024
    small_tile = jnp.concatenate(
        [small_params.reshape(-1), jnp.zeros((tile - 12 * part,), f32), positions[0].astype(f32)]
        + [jnp.zeros((1024 - seq,), f32)]
    ).reshape(-1, 128)
    weights, acts, table = gather(pieces, jnp.stack([x_low, g_low]), small_tile, grid.m)
    w_qk, w_vo, w_up, w_dn = weights
    everyone = table.reshape(devices, -1)
    small_all = jnp.transpose(everyone[:, : 12 * part].reshape(devices, 12, part), (1, 0, 2)).reshape(12, width)
    group = (jnp.arange(Z) * grid.m + m) * 4 + t * 2
    places = jnp.take(everyone[:, tile : tile + seq], group, axis=0)
    plain, grads = acts[0], acts[1]
    x_group = plain.astype(f32)
    one_low = (x_group * small_all[0] + small_all[1]).astype(bf16)
    two_low = (x_group * small_all[2] + small_all[3]).astype(bf16)
    order = jnp.arange(grid.dp)

    head = c * Z + z
    hidden = w_up.shape[1]
    query_bias = lax.dynamic_slice_in_dim(small_all[4], head * HEAD_DIM, HEAD_DIM)
    value_bias = lax.dynamic_slice_in_dim(small_all[5], head * HEAD_DIM, HEAD_DIM)
    up_bias = lax.dynamic_slice_in_dim(small_all[8:12].reshape(-1), head * hidden, hidden)

    dot = functools.partial(jnp.einsum, preferred_element_type=f32)

    cos_table, sin_table = angle_tables(places)
    score_scale = HEAD_DIM ** (-0.5)
    visible = places[:, None, :] <= places[:, :, None]
    qk = dot("sd,dn->sn", one_low, w_qk)
    w_v, w_o = w_vo[:, :HEAD_DIM], w_vo[:, HEAD_DIM:]
    per_seq = lambda v: v.reshape(Z, seq, HEAD_DIM)
    queries = rotate(per_seq(qk[:, :HEAD_DIM] + query_bias), cos_table, sin_table).astype(bf16)
    key_rows = rotate(per_seq(qk[:, HEAD_DIM:]), cos_table, sin_table).astype(bf16)
    values = per_seq((dot("sd,dn->sn", one_low, w_v) + value_bias).astype(bf16))
    scores = dot("nqd,nkd->nqk", queries, key_rows) * score_scale
    scores = jnp.where(visible, scores, -jnp.inf)
    row_max = jnp.max(scores, axis=-1, keepdims=True)
    log_total = row_max + jnp.log(jnp.sum(jnp.exp(scores - row_max), axis=-1, keepdims=True))
    probs = jnp.exp(scores - log_total)
    probs_low = probs.astype(bf16)
    attended = dot("nqk,nkd->nqd", probs_low, values).astype(bf16)
    d_attended = per_seq(dot("sd,dn->sn", grads, w_o).astype(bf16))
    d_probs = dot("nqd,nkd->nqk", d_attended, values)
    d_scores = (probs * (d_probs - jnp.sum(probs * d_probs, axis=-1, keepdims=True)) * score_scale).astype(bf16)
    d_query = rotate(dot("nqk,nkd->nqd", d_scores, key_rows), cos_table, -sin_table)
    d_key = rotate(dot("nqk,nqd->nkd", d_scores, queries), cos_table, -sin_table)
    d_value = dot("nqk,nqd->nkd", probs_low, d_attended)
    flat = lambda v: v.reshape(Z * seq, HEAD_DIM)
    attended, d_query, d_key, d_value = flat(attended), flat(d_query), flat(d_key), flat(d_value)
    dqk_low = jnp.concatenate([d_query, d_key], axis=1).astype(bf16)
    dv_low = d_value.astype(bf16)
    d_one = dot("sn,dn->sd", dqk_low, w_qk) + dot("sn,dn->sd", dv_low, w_v)
    y_attn = dot("sn,dn->sd", attended, w_o)
    grad_qk = dot("sd,sn->dn", one_low, dqk_low).astype(bf16)
    grad_vo = jnp.concatenate(
        [dot("sd,sn->dn", one_low, dv_low).astype(bf16), dot("sd,sn->dn", grads, attended).astype(bf16)], axis=1
    )

    pre_act = dot("sd,dn->sn", two_low, w_up) + up_bias
    activation = gelu_exact(pre_act).astype(bf16)
    d_pre = dot("sd,dn->sn", grads, w_dn) * gelu_slope(pre_act)
    d_pre_low = d_pre.astype(bf16)
    y_part = dot("sn,dn->sd", activation, w_dn) + y_attn
    d_two = dot("sn,dn->sd", d_pre_low, w_up)
    grad_up = dot("sd,sn->dn", two_low, d_pre_low).astype(bf16)
    grad_dn = dot("sd,sn->dn", grads, activation).astype(bf16)

    keep, give, norm_sums = place_outs(y_part, d_one, d_two, plain, small_all[:4], order, diag)
    spread_cols = lambda v, n: lax.dynamic_update_slice_in_dim(
        jnp.zeros((n,), f32), v, head * v.shape[0], 0
    )
    out_sum = jnp.sum(out_grad, axis=0)
    small_terms = jnp.concatenate(
        [
            norm_sums,
            spread_cols(jnp.sum(d_query, axis=0), width)[None],
            spread_cols(jnp.sum(d_value, axis=0), width)[None],
            out_sum[None],
            out_sum[None],
            spread_cols(jnp.sum(d_pre, axis=0), 4 * width).reshape(4, width),
        ],
        axis=0,
    )
    terms = jnp.transpose(small_terms.reshape(12, devices, part), (1, 0, 2)).reshape(devices, 12 * part)
    terms = jnp.pad(terms, ((0, 0), (0, tile - 12 * part))).reshape(devices, -1, 128)
    own, own_rows, own_small = scatter([grad_qk, grad_vo, grad_up, grad_dn], keep, give, terms, grid.m, rows)
    y_rows, u_rows = own_rows[0].astype(f32), own_rows[1].astype(f32)
    block_out = block_in + y_rows + small_all[6] + small_all[7]
    input_grad = out_grad + inverse * (
        u_rows
        - jnp.mean(u_rows, axis=-1, keepdims=True)
        - normed * jnp.mean(u_rows * normed, axis=-1, keepdims=True)
    )
    attn_out = adam_update(own[:2], 2, attn_weight, attn_first, attn_second)
    mlp_out = adam_update(own[2:], 1, mlp_weight, mlp_first, mlp_second)
    small_grad = own_small.reshape(-1)[: 12 * part].reshape(12, part)
    small_new, small_first_new, small_second_new = adam_step(small_params, small_grad, small_first, small_second)

    attn_grad, attn_new, attn_first_new, attn_second_new = attn_out
    mlp_grad, mlp_new, mlp_first_new, mlp_second_new = mlp_out
    return (
        block_out,
        input_grad,
        attn_grad,
        mlp_grad,
        small_grad,
        attn_new,
        attn_first_new,
        attn_second_new,
        mlp_new,
        mlp_first_new,
        mlp_second_new,
        small_new,
        small_first_new,
        small_second_new,
    )


def solution(mesh):
    rows = P(("dp", "tensor"), None)
    weights = P("dp", None, "tensor")
    small = P(None, ("dp", "tensor"))
    return jax.shard_map(
        body,
        mesh=mesh,
        in_specs=(rows, P("dp", None), rows, weights, weights, small, weights, weights, weights, weights, small, small),
        out_specs=(rows, rows) + (weights,) * 2 + (small,) + (weights,) * 6 + (small,) * 3,
        check_vma=False,
    )
```

```python
import functools

import jax
import jax.numpy as jnp
from jax import lax
from jax.experimental import pallas as pl
from jax.experimental.pallas import tpu as pltpu
from jax.sharding import PartitionSpec as P

ROT = 64
ADAM_STEP = 3
HEAD_DIM = 256
Z = 4

norm_epsilon = 1e-05
learn_rate = 0.006
beta_first = 0.9
beta_second = 0.95
adam_epsilon = 1e-08
weight_decay = 0.1

f32 = jnp.float32
bf16 = jnp.bfloat16


def layer_stats(row_data):
    center = row_data - jnp.mean(row_data, axis=-1, keepdims=True)
    inverse = lax.rsqrt(jnp.mean(center * center, axis=-1, keepdims=True) + norm_epsilon)
    return (center * inverse, inverse)


def adam_step(weight, gradient, moment_one, moment_two):
    one_new = beta_first * moment_one + (1.0 - beta_first) * gradient
    two_new = beta_second * moment_two + (1.0 - beta_second) * gradient * gradient
    corrected = (
        one_new
        / (1.0 - beta_first**ADAM_STEP)
        / (jnp.sqrt(two_new / (1.0 - beta_second**ADAM_STEP)) + adam_epsilon)
    )
    return (weight - learn_rate * (corrected + weight_decay * weight), one_new, two_new)


class Grid:
    def __init__(self, dp, tensor):
        assert tensor == 2 and dp % (2 * Z) == 0
        self.dp, self.m = dp, dp // (2 * Z)
        index = lax.axis_index("dp")
        self.index = index * 2 + lax.axis_index("tensor")
        self.z_now = index // (2 * self.m)
        self.m_now = (index // 2) % self.m
        self.c_now = index % 2
        self.t_now = lax.axis_index("tensor")
        self.diag = self.c_now == self.t_now


def split_kernel(attn, mlp, qk, vo, up, dn):
    quarter_a = attn.shape[2] // Z
    quarter_m = mlp.shape[2] // Z
    for q in range(Z):
        for j in range(4):
            block = attn[:, j, q * quarter_a : (q + 1) * quarter_a].astype(bf16)
            (qk, qk, vo, vo)[j][q, :, (j % 2) * quarter_a : (j % 2 + 1) * quarter_a] = block
        for j in range(2):
            (up, dn)[j][q] = mlp[:, j, q * quarter_m : (q + 1) * quarter_m].astype(bf16)


def split_weights(attn_weight, mlp_weight):
    rows, _, width = attn_weight.shape
    hidden = mlp_weight.shape[2]
    step = min(rows, 32)
    shapes = [2 * width // Z] * 2 + [hidden // Z] * 2
    return pl.pallas_call(
        split_kernel,
        grid=(rows // step,),
        in_specs=[
            pl.BlockSpec((step, 4, width), lambda i: (i, 0, 0)),
            pl.BlockSpec((step, 2, hidden), lambda i: (i, 0, 0)),
        ],
        out_specs=[pl.BlockSpec((Z, step, n), lambda i: (0, i, 0)) for n in shapes],
        out_shape=[jax.ShapeDtypeStruct((Z, rows, n), bf16) for n in shapes],
        name="split_weights",
    )(attn_weight, mlp_weight)


MESH = pl.DeviceIdType.MESH
PARTS = (1, 1, 2, 2)
CHUNKS = ((0, 0, True), (1, 0, False), (2, 0, True), (2, 1, False), (3, 0, True), (3, 1, False))
GATHER_ORDER = {
    (False, False): (
        0, 10, 500, 510, 520, 530, 540, 550, 700, 600, 501, 900, 620, 511, 910, 640, 601, 801, 502, 710, 20, 30, 40,
        50, 512, 602, 610, 920, 630, 811, 521, 650, 531, 621, 541, 551, 641, 611, 930, 802, 940, 503, 612, 513, 603,
        631, 651, 812, 522, 532, 622, 542, 552, 632, 642, 613, 652, 803, 813, 523, 533, 623, 543, 553, 633, 643, 653,
    ),
    (False, True): (
        0, 10, 700, 500, 510, 520, 530, 540, 550, 610, 630, 650, 600, 501, 900, 620, 511, 611, 640, 710, 20, 30, 40,
        50, 801, 910, 601, 502, 602, 811, 521, 930, 531, 621, 541, 940, 551, 641, 631, 512, 612, 651, 920, 802, 503,
        603, 812, 522, 532, 622, 542, 552, 642, 632, 513, 613, 652, 803, 813, 523, 533, 623, 543, 633, 553, 643, 653,
    ),
    (True, False): (
        0, 10, 500, 510, 520, 530, 540, 550, 900, 700, 600, 200, 503, 620, 100, 300, 640, 501, 513, 603, 210, 310,
        601, 110, 511, 710, 20, 30, 40, 50, 803, 400, 610, 801, 502, 910, 410, 630, 512, 602, 650, 811, 220, 813,
        120, 920, 523, 521, 320, 230, 623, 533, 130, 613, 621, 330, 531, 543, 240, 340, 140, 611, 553, 541, 643, 350,
        250, 930, 150, 551, 641, 940, 802, 612, 633, 631, 812, 653, 420, 651, 522, 430, 532, 622, 440, 542, 632, 450,
        642, 552, 652,
    ),
    (True, True): (
        0, 10, 700, 500, 510, 520, 530, 540, 550, 900, 610, 630, 650, 600, 200, 503, 620, 100, 300, 640, 501, 513,
        613, 710, 20, 30, 40, 50, 210, 310, 110, 511, 611, 603, 601, 803, 400, 801, 502, 910, 602, 813, 811, 523,
        220, 320, 120, 623, 533, 930, 521, 330, 230, 940, 543, 130, 621, 633, 340, 531, 643, 631, 553, 240, 350, 140,
        410, 541, 653, 512, 612, 250, 920, 641, 150, 551, 651, 802, 812, 420, 522, 430, 622, 532, 632, 440, 542, 450,
        642, 552, 652,
    ),
}


class Links:
    def __init__(self, m_size):
        self.m_size = m_size
        index = lax.axis_index("dp")
        self.z, self.m, self.c = index // (2 * m_size), (index // 2) % m_size, index % 2
        self.t = lax.axis_index("tensor")
        self.sends = []

    def to(self, z=None, m=None, c=None, t=None):
        z, m, c = (own if v is None else v for v, own in ((z, self.z), (m, self.m), (c, self.c)))
        return ((z * self.m_size + m) * 2 + c, self.t if t is None else t)

    def copy(self, src, dst, send_sem, recv_sem, target):
        return pltpu.make_async_remote_copy(
            src_ref=src, dst_ref=dst, send_sem=send_sem, recv_sem=recv_sem, device_id=target, device_id_type=MESH
        )

    def send(self, src, dst, send_sem, recv_sem, target):
        one = self.copy(src, dst, send_sem, recv_sem, target)
        one.start()
        self.sends.append(one)

    def landed(self, dst, recv_sem):
        self.copy(dst, dst, recv_sem, recv_sem, self.to(c=1 - self.c)).wait_recv()

    def drain(self):
        for one in self.sends:
            one.wait_send()
        self.sends = []

    def partners(self):
        other = 1 - self.t
        out = [self.to(z=self.z ^ k) for k in range(1, Z)]
        out += [self.to(m=self.m ^ j) for j in range(1, self.m_size)]
        out += [self.to(c=1 - self.c), self.to(t=other), self.to(c=1 - self.c, t=other)]
        return out

    def doubling(self):
        high = self.z // 2
        place = ((self.m * 2 + self.c) * 2 + self.t) * 4 + lax.rem(self.z + high, 2) * 2 + high
        steps = [(1, self.to(z=self.z ^ 3)), (2, self.to(z=self.z ^ 1)), (4, self.to(t=1 - self.t))]
        steps.append((8, self.to(c=1 - self.c)))
        j = 1
        while j < self.m_size:
            steps.append((16 * j, self.to(m=self.m ^ j)))
            j *= 2
        return place, steps

    def meet(self):
        barrier = pltpu.get_barrier_semaphore()
        everyone = self.partners()
        for target in everyone:
            pl.semaphore_signal(barrier, inc=1, device_id=target, device_id_type=MESH)
        pl.semaphore_wait(barrier, len(everyone))


def gather_kernel(m_size, *refs):
    pieces, low, mine_small = refs[:4], refs[4], refs[5]
    full, act, table = refs[6:10], refs[10], refs[11]
    count = len(CHUNKS)
    stage, stage_m, relay = (refs[12 + i * count : 12 + (i + 1) * count] for i in range(3))
    refs = refs[12 + 3 * count :]
    (zs, zr, gs, gr, ps, pr, ms, mr, near_s, far_s, xr, as_, ar, ws, wr, ss, sr, lin, lout) = refs[:19]
    bounce, bounce_low = refs[19 : 19 + count], refs[19 + count]
    net = Links(m_size)
    z, m, c, t = net.z, net.m, net.c, net.t
    rows = pieces[0].shape[1]
    half = low.shape[1]
    role = lax.rem(c + t, 2)
    inner_z = lax.rem(z + z // 2, 2)

    def columns(ch):
        array, part, _ = CHUNKS[ch]
        wide = pieces[array].shape[2] // PARTS[array]
        return array, slice(part * wide, (part + 1) * wide)

    def piece(ch, zz):
        array, cols = columns(ch)
        return pieces[array].at[zz, :, cols]

    def whole(ch, zz, mm, cc, size=1):
        array, cols = columns(ch)
        start = ((zz * m_size + mm) * 2 + cc) * rows
        return full[array].at[pl.ds(pl.multiple_of(start, rows), size * rows), cols]

    own_place = pl.ds(pl.multiple_of(z * 2 * half + t * half, half), half)
    place = lambda zz, h: pl.ds(pl.multiple_of(zz * 2 * half + (t ^ h) * half, half), half)

    loads = [pltpu.make_async_copy(piece(ch, z), bounce[ch], lin.at[ch]) for ch in range(count)]
    loads.append(pltpu.make_async_copy(low.at[0], bounce_low, lin.at[count]))
    stores = [pltpu.make_async_copy(bounce[ch], whole(ch, z, m, c), lout.at[ch]) for ch in range(count)]
    stores.append(pltpu.make_async_copy(bounce_low, act.at[0, own_place], lout.at[count]))

    @pl.when(role == 0)
    def _():
        for one in loads:
            one.start()

    net.meet()
    flat, steps = net.doubling()
    small_own = pltpu.make_async_copy(mine_small, table.at[flat], ss.at[len(steps)])
    small_own.start()

    def program(inner, diag):
        state = {"small": 0}

        def small_send():
            i = state["small"]
            if i < len(steps):
                size, target = steps[i]
                span = table.at[pl.ds(flat // size * size, size)]
                net.send(span, span, ss.at[i], sr.at[i], target)

        def small_next():
            i = state["small"]
            if i < len(steps):
                size = steps[i][0]
                net.landed(table.at[pl.ds((flat // size ^ 1) * size, size)], sr.at[i])
                state["small"] += 1
                small_send()

        def spot(ch, zz, j):
            if diag:
                return whole(ch, zz, m ^ j, c)
            return stage_m[ch].at[m ^ j, zz] if j else stage[ch].at[zz]

        def source(ch, k, j):
            return piece(ch, z) if k == 0 and j == 0 else spot(ch, z ^ k, j)

        def spread(ch, k, j):
            src, dst = source(ch, k, j), whole(ch, z ^ k, m ^ j, c)
            net.send(src, dst, ps.at[ch, j, k, 1], pr.at[ch, j, k, c], net.to(c=t, t=1 - t))
            if not diag:
                net.send(src, dst, ps.at[ch, j, k, 0], pr.at[ch, j, k, c], net.to(c=1 - c))

        def spread_landed(ch, k, j):
            for cc in (1 - c,) if diag else (1 - c, c):
                net.landed(whole(ch, z ^ k, m ^ j, cc), pr.at[ch, j, k, cc])

        def swap(h, k):
            src = act.at[role, place(z ^ k, h)]
            net.send(src, src, ws.at[k, h], wr.at[k, h], net.to(c=1 - c))

        def rows_on(h, block, i, hop, k):
            src = act.at[role, place(block, h)]
            net.send(src, src, as_.at[h, i], ar.at[h, k], net.to(z=z ^ hop))

        def quarters(ch, _):
            for i, (k, hop, through) in enumerate(
                ((3, 3, None), (2, 3, 2), (1, 1, None)) if inner else ((3, 1, 1), (2, 1, 0), (1, 1, None))
            ):
                target = net.to(z=z ^ hop)
                if through is None:
                    net.send(piece(ch, z ^ k), spot(ch, z, 0), zs.at[ch, i], zr.at[ch, k], target)
                else:
                    net.send(piece(ch, z ^ k), relay[ch].at[through], zs.at[ch, i], gr.at[ch, through], target)

        def pass_on(through):
            hop, k = ((3, 2), (3, None), (1, 2), (1, 3))[through]

            def run(ch, _):
                src = relay[ch].at[through]
                net.landed(src, gr.at[ch, through])
                if k is None:
                    net.send(src, relay[ch].at[3], gs.at[ch, through], gr.at[ch, 3], net.to(z=z ^ hop))
                else:
                    dst = spot(ch, z ^ hop ^ k, 0)
                    net.send(src, dst, gs.at[ch, through], zr.at[ch, k], net.to(z=z ^ hop))

            return run

        def first(ch, k):
            if k:
                net.landed(spot(ch, z ^ k, 0), zr.at[ch, k])
            if CHUNKS[ch][2]:
                for j in range(1, m_size):
                    dst = whole(ch, z ^ k, m, c) if diag else stage_m[ch].at[m, z ^ k]
                    net.send(source(ch, k, 0), dst, ms.at[ch, j, k], mr.at[ch, j, k], net.to(m=m ^ j))
            spread(ch, k, 0)

        def second(ch, k):
            if CHUNKS[ch][2]:
                for j in range(1, m_size):
                    net.landed(spot(ch, z ^ k, j), mr.at[ch, j, k])
                    spread(ch, k, j)
            else:
                if diag and k == 0:
                    stores[ch].wait()
                spread_landed(ch, k, 0)
                both = whole(ch, z ^ k, m, 0, 2)
                for j in range(1, m_size):
                    net.send(both, both, ms.at[ch, j, k], mr.at[ch, j, k], net.to(m=m ^ j))

        def rows_start(h, _):
            if h:
                net.landed(act.at[0 if diag else 1, place(z, 1)], xr.at[1])
            elif diag:
                stores[count].wait()
            else:
                net.landed(act.at[1, place(z, 0)], xr.at[0])
            if inner:
                rows_on(h, z, 0, 3, 3)
            rows_on(h, z, 1, 1, 1)
            swap(h, 0)

        def rows_next(h, k):
            net.landed(act.at[role, place(z ^ k, h)], ar.at[h, k])
            if inner:
                hop, there = {1: (3, 2), 3: (1, 2), 2: (1, 3)}[k]
                rows_on(h, z ^ k, 1 + k, hop, there)
            swap(h, k)

        small_own.wait()
        small_send()
        if diag:
            net.send(low.at[1], act.at[1, own_place], near_s, xr.at[0], net.to(c=1 - c))
        else:
            net.send(low.at[0], act.at[0, own_place], near_s, xr.at[1], net.to(t=1 - t))
            net.send(low.at[1], act.at[1, own_place], far_s, xr.at[1], net.to(c=1 - c, t=1 - t))
        if diag:
            for load, store in zip(loads, stores):
                load.wait()
                store.start()
        runs = [quarters] + [pass_on(i) for i in range(4)] + [first, second, rows_start, rows_next]
        runs.append(lambda *_: small_next())
        for code in GATHER_ORDER[inner, diag]:
            runs[code // 100](code // 10 % 10, code % 10)
        while state["small"] < len(steps):
            small_next()
        for ch in range(count):
            for k in range(Z):
                if CHUNKS[ch][2]:
                    for j in range(m_size):
                        spread_landed(ch, k, j)
                    if diag and k == 0:
                        stores[ch].wait()
                else:
                    for j in range(1, m_size):
                        net.landed(whole(ch, z ^ k, m ^ j, 0, 2), mr.at[ch, j, k])
        for k in range(Z):
            for h in range(2):
                net.landed(act.at[1 - role, place(z ^ k, h)], wr.at[k, h])
        net.drain()

    by_class(inner_z, role, program)


def table_order(m_size):
    order = []
    for z in range(Z):
        for rest in range(4 * m_size):
            order.append(rest * 4 + (z + z // 2) % 2 * 2 + z // 2)
    return order


def by_class(inner_z, role, program):
    for inner in (False, True):
        for diag in (False, True):

            @pl.when((inner_z == int(inner)) & (role == int(not diag)))
            def _(inner=inner, diag=diag):
                program(inner, diag)


def gather(pieces, low, small, m_size):
    rows = pieces[0].shape[1]
    width = low.shape[2]
    devices = m_size * 4 * Z
    cols = [p.shape[2] for p in pieces]
    count = len(CHUNKS)
    parts = [cols[array] // PARTS[array] for array, _, _ in CHUNKS]
    sem = pltpu.SemaphoreType.DMA
    doubling = m_size.bit_length() - 1 + 4
    in_place = pl.BlockSpec(memory_space=pl.ANY)
    shape = lambda *dims: jax.ShapeDtypeStruct(dims, bf16)
    outs = pl.pallas_call(
        functools.partial(gather_kernel, m_size),
        out_shape=[shape(width, n) for n in cols]
        + [shape(2, Z * 2 * low.shape[1], width), jax.ShapeDtypeStruct((devices,) + small.shape, f32)]
        + [shape(Z, rows, n) for n in parts]
        + [shape(m_size, Z, rows, n) for n in parts]
        + [shape(4, rows, n) for n in parts],
        in_specs=[in_place] * 6,
        out_specs=[in_place] * (6 + 3 * count),
        scratch_shapes=[
            sem((count, 3)),
            sem((count, Z)),
            sem((count, 4)),
            sem((count, 4)),
            sem((count, m_size, Z, 2)),
            sem((count, m_size, Z, 2)),
            sem((count, m_size, Z)),
            sem((count, m_size, Z)),
            sem,
            sem,
            sem((2,)),
            sem((2, 5)),
            sem((2, Z)),
            sem((Z, 2)),
            sem((Z, 2)),
            sem((doubling + 1,)),
            sem((doubling,)),
            sem((count + 1,)),
            sem((count + 1,)),
        ]
        + [pltpu.VMEM((rows, n), bf16) for n in parts]
        + [pltpu.VMEM(low.shape[1:], bf16)],
        compiler_params=pltpu.CompilerParams(collective_id=0, has_side_effects=True),
        name="gather_all",
    )(*pieces, low, small)
    return outs[:4], outs[4], outs[5]


VMEM_BYTES = 60 * 1024 * 1024


def dot(a, b, over_a=1, over_b=0):
    return lax.dot_general(a, b, (((over_a,), (over_b,)), ((), ())), preferred_element_type=f32)


def turn(value, tables, sign):
    cos, low, high = (table[...] for table in tables)
    part = value[:, :128]
    turned = part * cos + sign * (
        pltpu.roll(part, 128 - ROT // 2, 1) * low + pltpu.roll(part, ROT // 2, 1) * high
    )
    return jnp.concatenate([turned, value[:, 128:]], axis=1)


def turn_tables(places):
    half = ROT // 2
    column = jnp.arange(128)
    frequency = 10000.0 ** (-((column % half).astype(f32) * (2.0 / ROT)))
    angles = places.reshape(-1, 1) * frequency
    cos = jnp.where(column < ROT, jnp.cos(angles), 1.0)
    sin = jnp.sin(angles)
    return cos, jnp.where(column < half, -sin, 0.0), jnp.where((column >= half) & (column < ROT), sin, 0.0)


def attn_kernel(x, g, w_qk, w_vo, par, bias, cos, low, high, across, down, one_out, att_out, d_out, sums):
    tables = (cos, low, high)
    n = HEAD_DIM
    scale = HEAD_DIM ** (-0.5)
    one = (x[...].astype(f32) * par[0:1, :] + par[1:2, :]).astype(bf16)
    one_out[...] = one
    qk = dot(one, w_qk[...])
    q = turn(qk[:, :n] + bias[0:1, :], tables, 1.0).astype(bf16)
    k = turn(qk[:, n:], tables, 1.0).astype(bf16)
    v = (dot(one, w_vo[:, :n]) + bias[1:2, :]).astype(bf16)
    d_att = dot(g[...], w_vo[:, n:]).astype(bf16)
    scores = jnp.where(across[0] <= down[0], dot(q, k, 1, 1) * scale, -jnp.inf)
    top = jnp.max(scores, axis=-1, keepdims=True)
    log_total = top + jnp.log(jnp.sum(jnp.exp(scores - top), axis=-1, keepdims=True))
    probs = jnp.exp(scores - log_total)
    low_probs = probs.astype(bf16)
    att_out[...] = dot(low_probs, v).astype(bf16)
    d_probs = dot(d_att, v, 1, 1)
    d_scores = (probs * (d_probs - jnp.sum(probs * d_probs, axis=-1, keepdims=True)) * scale).astype(bf16)
    d_q = turn(dot(d_scores, k), tables, -1.0)
    d_k = turn(dot(d_scores, q, 0, 0), tables, -1.0)
    d_v = dot(low_probs, d_att, 0, 0)
    d_out[:, :n] = d_q.astype(bf16)
    d_out[:, n : 2 * n] = d_k.astype(bf16)
    d_out[:, 2 * n :] = d_v.astype(bf16)

    @pl.when(pl.program_id(0) == 0)
    def _():
        sums[...] = jnp.zeros_like(sums)

    sums[0:1, :] += jnp.sum(d_q, axis=0, keepdims=True)
    sums[1:2, :] += jnp.sum(d_v, axis=0, keepdims=True)


def fixed(*shape):
    return pl.BlockSpec(shape, lambda i: (0,) * len(shape))


def run_attention(acts, w_qk, w_vo, par, bias, places):
    _, rows, width = acts.shape
    seq, n = rows // Z, HEAD_DIM
    by_rows = lambda cols: pl.BlockSpec((seq, cols), lambda i: (i, 0))
    act = lambda which: pl.BlockSpec((None, seq, width), lambda i: (which, i, 0))
    return pl.pallas_call(
        attn_kernel,
        grid=(Z,),
        in_specs=[act(0), act(1), fixed(width, 2 * n), fixed(width, 2 * n), fixed(*par.shape), fixed(2, n)]
        + [by_rows(128)] * 3
        + [pl.BlockSpec((1, 1, seq), lambda i: (i, 0, 0)), pl.BlockSpec((1, seq, 1), lambda i: (i, 0, 0))],
        out_specs=[by_rows(width), by_rows(n), by_rows(3 * n), fixed(2, n)],
        out_shape=[jax.ShapeDtypeStruct((rows, cols), bf16) for cols in (width, n, 3 * n)]
        + [jax.ShapeDtypeStruct((2, n), f32)],
        compiler_params=pltpu.CompilerParams(vmem_limit_bytes=VMEM_BYTES),
        name="attention",
    )(acts, acts, w_qk, w_vo, par, bias, *turn_tables(places), places[:, None, :], places[:, :, None])


def hidden_kernel(x, g, up, down, par, bias, two_out, act_out, d_out, sums):
    @pl.when(pl.program_id(0) == 0)
    def _():
        two_out[...] = (x[...].astype(f32) * par[2:3, :] + par[3:4, :]).astype(bf16)

    pre = dot(two_out[...], up[...]) + bias[...]
    erf = 1.0 + lax.erf(pre * 0.7071067811865476)
    act_out[...] = (0.5 * pre * erf).astype(bf16)
    slope = 0.5 * erf + pre * jnp.exp(-0.5 * pre * pre) * 0.3989422804014327
    d_pre = dot(g[...], down[...]) * slope
    d_out[...] = d_pre.astype(bf16)
    sums[...] = jnp.sum(d_pre, axis=0, keepdims=True)


def run_hidden(acts, w_up, w_dn, par, bias):
    _, rows, width = acts.shape
    hidden = w_up.shape[1]
    step = 256
    act = lambda which: pl.BlockSpec((None, rows, width), lambda i: (which, 0, 0), pipeline_mode=pl.Buffered(1))
    tile = lambda height: pl.BlockSpec((height, step), lambda i: (0, i))
    return pl.pallas_call(
        hidden_kernel,
        grid=(hidden // step,),
        in_specs=[act(0), act(1), tile(width), tile(width), fixed(*par.shape), tile(1)],
        out_specs=[fixed(rows, width), tile(rows), tile(rows), tile(1)],
        out_shape=[jax.ShapeDtypeStruct((rows, n), bf16) for n in (width, hidden, hidden)]
        + [jax.ShapeDtypeStruct((1, hidden), f32)],
        compiler_params=pltpu.CompilerParams(vmem_limit_bytes=VMEM_BYTES),
        name="hidden_units",
    )(acts, acts, w_up, w_dn, par, bias)


def outs_kernel(flag, att, d_attn, act, d_pre, x, w_qk, w_vo, w_up, w_dn, par, keep, give, sums):
    diag = flag[0] == 1
    n = HEAD_DIM
    y = dot(att[...], w_vo[:, n:], 1, 1) + dot(act[...], w_dn[...], 1, 1)
    d_one = dot(d_attn[:, : 2 * n], w_qk[...], 1, 1) + dot(d_attn[:, 2 * n :], w_vo[:, :n], 1, 1)
    d_two = dot(d_pre[...], w_up[...], 1, 1)
    u = d_one * par[0:1, :] + d_two * par[2:3, :]
    keep[...] = jnp.where(diag, y, u).astype(bf16)
    give[...] = jnp.where(diag, u, y).astype(bf16)
    plain = x[...].astype(f32)
    for i, value in enumerate((d_one * plain, d_one, d_two * plain, d_two)):
        sums[i : i + 1, :] = jnp.sum(value, axis=0, keepdims=True)


def run_outs(diag, att, d_attn, act, d_pre, acts, weights, par):
    _, rows, width = acts.shape
    step = 256
    fix = lambda v: pl.BlockSpec(v.shape, lambda i, s: (0, 0), pipeline_mode=pl.Buffered(1))
    tile = lambda height: pl.BlockSpec((height, step), lambda i, s: (0, i))
    return pl.pallas_call(
        outs_kernel,
        grid_spec=pltpu.PrefetchScalarGridSpec(
            num_scalar_prefetch=1,
            grid=(width // step,),
            in_specs=[fix(v) for v in (att, d_attn, act, d_pre)]
            + [pl.BlockSpec((None, rows, step), lambda i, s: (0, 0, i))]
            + [pl.BlockSpec((step, v.shape[1]), lambda i, s: (i, 0)) for v in weights]
            + [tile(4)],
            out_specs=[tile(rows), tile(rows), tile(4)],
        ),
        out_shape=[jax.ShapeDtypeStruct((rows, width), bf16)] * 2 + [jax.ShapeDtypeStruct((4, width), f32)],
        compiler_params=pltpu.CompilerParams(vmem_limit_bytes=VMEM_BYTES),
        name="outputs",
    )(diag.astype(jnp.int32).reshape(1), att, d_attn, act, d_pre, acts, *weights, par)


def grads_kernel(one, two, g, att, d_attn, act, d_pre, qk, vo, up, dn):
    n = HEAD_DIM
    first = dot(one[...], d_attn[...], 0, 0)
    qk[...] = first[:, : 2 * n].astype(bf16)
    vo[:, :n] = first[:, 2 * n :].astype(bf16)
    vo[:, n:] = dot(g[...], att[...], 0, 0).astype(bf16)
    up[...] = dot(two[...], d_pre[...], 0, 0).astype(bf16)
    dn[...] = dot(g[...], act[...], 0, 0).astype(bf16)


def run_grads(one, two, acts, att, d_attn, act, d_pre):
    rows, width = one.shape
    step = 256
    tile = pl.BlockSpec((rows, step), lambda i: (0, i))
    fix = lambda v: pl.BlockSpec(v.shape, lambda i: (0, 0), pipeline_mode=pl.Buffered(1))
    cols = [2 * HEAD_DIM, 2 * HEAD_DIM, act.shape[1], act.shape[1]]
    return pl.pallas_call(
        grads_kernel,
        grid=(width // step,),
        in_specs=[tile, tile, pl.BlockSpec((None, rows, step), lambda i: (1, 0, i))]
        + [fix(v) for v in (att, d_attn, act, d_pre)],
        out_specs=[pl.BlockSpec((step, n), lambda i: (i, 0)) for n in cols],
        out_shape=[jax.ShapeDtypeStruct((width, n), bf16) for n in cols],
        compiler_params=pltpu.CompilerParams(vmem_limit_bytes=VMEM_BYTES),
        name="weight_grads",
    )(one, two, acts, att, d_attn, act, d_pre)


M_FIRST = (True, False, True, False)


def add_rows(dst, sources):
    step = min(dst.shape[0], 32)

    @pl.loop(0, dst.shape[0] // step)
    def _(i):
        span = pl.ds(pl.multiple_of(i * step, step), step)
        total = sources[0][span, :].astype(f32)
        for one in sources[1:]:
            total = total + one[span, :].astype(f32)
        dst[span, :] = total.astype(dst.dtype)


def scatter_kernel(m_size, *refs):
    grads, keep, give, terms = refs[:4], refs[4], refs[5], refs[6]
    own, rows_out, small_out = refs[7:11], refs[11], refs[12]
    home_first, x_first, mid_first, far_first, sum_first = (refs[13 + 2 * i : 15 + 2 * i] for i in range(5))
    own_last, far_last, sum_last, home_last, x_last, sum_far = (refs[23 + 2 * i : 25 + 2 * i] for i in range(6))
    got, kept, total, got_z, three, final, current, got_small = refs[35:43]
    (cl, cs, cr, fs, fr, zs, zr, zl, dl, ds_, dr, es, er, kl, gs, gr, ys, yr, rs, rr, rl, ss, sr) = refs[43:]
    net = Links(m_size)
    z, m, c, t = net.z, net.m, net.c, net.t
    half = rows_out.shape[1]
    role = lax.rem(c + t, 2)
    first_chunks = [ch for ch in range(4) if M_FIRST[ch]]
    last_chunks = [ch for ch in range(4) if not M_FIRST[ch]]
    pairs_first = [(i, ch) for i, ch in enumerate(first_chunks)]
    pairs_last = [(i, ch) for i, ch in enumerate(last_chunks)]
    ks = (3, 2, 1, 0)

    def by_role(do):
        @pl.when(role == 0)
        def _():
            do(True)

        @pl.when(role == 1)
        def _():
            do(False)

    loads_keep = [pltpu.make_async_copy(keep.at[z ^ k], kept.at[k], kl.at[k]) for k in range(Z)]
    loads_last = {
        (i, k): pltpu.make_async_copy(grads[ch].at[z ^ k, m], own_last[i].at[k], dl.at[i, k])
        for i, ch in pairs_last
        for k in ks
    }
    loads_first = {
        (i, j, k): pltpu.make_async_copy(grads[ch].at[z ^ k, m ^ j, c], home_first[i].at[j, k], cl.at[i, j, k])
        for i, ch in pairs_first
        for j in range(m_size)
        for k in ks
    }
    for one in loads_keep:
        one.start()
    for one in loads_last.values():
        one.start()

    def load_first(diag):
        if diag:
            for one in loads_first.values():
                one.start()

    by_role(load_first)
    current[...] = terms[...]
    net.meet()

    flat, steps = net.doubling()
    steps = steps[::-1]
    state = {"small": 0}

    def small_send():
        i = state["small"]
        if i < len(steps):
            size, target = steps[i]
            net.send(
                current.at[pl.ds((flat // size ^ 1) * size, size)],
                got_small.at[pl.ds(size, size)],
                ss.at[i],
                sr.at[i],
                target,
            )

    def small_next():
        i = state["small"]
        if i < len(steps):
            size = steps[i][0]
            net.landed(got_small.at[pl.ds(size, size)], sr.at[i])
            span = pl.ds(flat // size * size, size)
            current[span] = current[span] + got_small[pl.ds(size, size)]
            state["small"] += 1
            small_send()

    for k in (1, 2, 3, 0):
        net.send(give.at[z ^ k], got.at[k], gs.at[k], gr.at[k], net.to(c=1 - c))
    small_send()

    def to_owner(diag, source, home, far, sems, i, jk):
        send_sem, recv_sem = sems
        if diag:
            net.copy(source(1 - c), home, send_sem.at[i, *jk, 0], recv_sem.at[i, *jk, 0], net.to(c=1 - c)).start()
        else:
            net.copy(source(c), far, send_sem.at[i, *jk, 0], recv_sem.at[i, *jk, 1], net.to(t=1 - t)).start()
            net.copy(
                source(1 - c), far, send_sem.at[i, *jk, 1], recv_sem.at[i, *jk, 1], net.to(c=1 - c, t=1 - t)
            ).start()

    def collect_first(i, ch, j, k):
        def do(diag):
            to_owner(
                diag,
                lambda cc: grads[ch].at[z ^ k, m ^ j, cc],
                home_first[i].at[j, k],
                x_first[i].at[j, k],
                (cs, cr),
                i,
                (j, k),
            )

        by_role(do)

    for k in ks:
        for i, ch in pairs_last:
            for j in range(1, m_size):
                net.send(grads[ch].at[z ^ k, m ^ j], far_last[i].at[j - 1, k], ds_.at[i, j, k], dr.at[i, j, k], net.to(m=m ^ j))
        for i, ch in pairs_first:
            for j in range(1, m_size):
                collect_first(i, ch, j, k)
    for k in ks:
        for i, ch in pairs_first:
            collect_first(i, ch, 0, k)

    def collected_first(i, j, k):
        def do(diag):
            if diag:
                loads_first[i, j, k].wait()
            else:
                net.landed(home_first[i].at[j, k], cr.at[i, j, k, 0])

        by_role(do)
        net.landed(x_first[i].at[j, k], cr.at[i, j, k, 1])

    for one in loads_keep:
        one.wait()
    for k in (1, 2, 3, 0):
        net.landed(got.at[k], gr.at[k])
        add_rows(total.at[k], [kept.at[k], got.at[k]])
        if k in (1, 2):
            net.send(total.at[k], got_z.at[k - 1], ys.at[k], yr.at[k], net.to(z=z ^ 1))
    small_next()

    def to_z(ch, tile, k):
        if k:
            net.send(tile, own[ch].at[z], zs.at[ch, k], zr.at[ch, k], net.to(z=z ^ k))
        else:
            pltpu.make_async_copy(tile, own[ch].at[z], zl.at[ch]).start()

    def middle(k):
        for i, ch in pairs_first:
            for j in range(1, m_size):
                collected_first(i, j, k)
                add_rows(mid_first[i].at[j - 1, k], [home_first[i].at[j, k], x_first[i].at[j, k]])
                net.send(mid_first[i].at[j - 1, k], far_first[i].at[j - 1, k], fs.at[i, j, k], fr.at[i, j, k], net.to(m=m ^ j))
        for i, ch in pairs_last:
            loads_last[i, k].wait()
            for j in range(1, m_size):
                net.landed(far_last[i].at[j - 1, k], dr.at[i, j, k])
            for cc in range(2):
                add_rows(
                    sum_last[i].at[k, cc],
                    [own_last[i].at[k, cc]] + [far_last[i].at[j - 1, k, cc] for j in range(1, m_size)],
                )

            def do(diag):
                to_owner(
                    diag,
                    lambda cc: sum_last[i].at[k, cc],
                    home_last[i].at[k],
                    x_last[i].at[k],
                    (es, er),
                    i,
                    (k,),
                )

            by_role(do)

    def finish(k):
        for i, ch in pairs_first:
            collected_first(i, 0, k)
            for j in range(1, m_size):
                net.landed(far_first[i].at[j - 1, k], fr.at[i, j, k])
            add_rows(
                sum_first[i].at[k],
                [home_first[i].at[0, k], x_first[i].at[0, k]] + [far_first[i].at[j - 1, k] for j in range(1, m_size)],
            )
            to_z(ch, sum_first[i].at[k], k)
        for i, ch in pairs_last:

            def do(diag):
                net.landed(x_last[i].at[k], er.at[i, k, 1])
                if diag:
                    add_rows(sum_far[i].at[k], [sum_last[i].at[k, c], x_last[i].at[k]])
                else:
                    net.landed(home_last[i].at[k], er.at[i, k, 0])
                    add_rows(sum_far[i].at[k], [home_last[i].at[k], x_last[i].at[k]])

            by_role(do)
            to_z(ch, sum_far[i].at[k], k)

    middle(3)
    small_next()
    middle(2)
    net.landed(got_z.at[1], yr.at[2])
    add_rows(three, [total.at[3], got_z.at[1]])
    net.send(three, got_z.at[2], ys.at[3], yr.at[3], net.to(z=z ^ 3))
    small_next()
    middle(1)
    finish(3)
    small_next()
    middle(0)
    finish(2)
    while state["small"] < len(steps):
        small_next()
    small_out[...] = current[flat]
    finish(1)
    net.landed(got_z.at[0], yr.at[1])
    net.landed(got_z.at[2], yr.at[3])
    add_rows(final, [total.at[0], got_z.at[0], got_z.at[2]])
    mine = final.at[pl.ds(pl.multiple_of(t * half, half), half)]
    other = final.at[pl.ds(pl.multiple_of((1 - t) * half, half), half)]
    keep_rows = pltpu.make_async_copy(mine, rows_out.at[0], rl)

    def rows_back(diag):
        if diag:
            keep_rows.start()
            net.copy(other, rows_out.at[0], rs.at[0], rr.at[0], net.to(t=1 - t)).start()
        else:
            net.copy(mine, rows_out.at[1], rs.at[0], rr.at[1], net.to(c=1 - c)).start()
            net.copy(other, rows_out.at[1], rs.at[1], rr.at[1], net.to(c=1 - c, t=1 - t)).start()

    by_role(rows_back)
    finish(0)
    for ch in range(4):
        for k in range(1, Z):
            net.landed(own[ch].at[z ^ k], zr.at[ch, k])
        pltpu.make_async_copy(own[ch].at[z], own[ch].at[z], zl.at[ch]).wait()

    def rows_done(diag):
        net.landed(rows_out.at[1], rr.at[1])
        if diag:
            keep_rows.wait()
            net.copy(other, rows_out.at[0], rs.at[0], rr.at[0], net.to(t=1 - t)).wait_send()
        else:
            net.landed(rows_out.at[0], rr.at[0])
            net.copy(mine, rows_out.at[1], rs.at[0], rr.at[1], net.to(c=1 - c)).wait_send()
            net.copy(other, rows_out.at[1], rs.at[1], rr.at[1], net.to(c=1 - c, t=1 - t)).wait_send()

    by_role(rows_done)

    def owners_done(diag):
        for k in ks:
            for side in range(1 if diag else 2):
                for i, ch in pairs_first:
                    for j in range(m_size):
                        src = grads[ch].at[z ^ k, m ^ j, 0]
                        net.copy(src, src, cs.at[i, j, k, side], cr.at[i, j, k, 0], net.to(c=1 - c)).wait_send()
                for i, ch in pairs_last:
                    src = sum_last[i].at[k, 0]
                    net.copy(src, src, es.at[i, k, side], er.at[i, k, 0], net.to(c=1 - c)).wait_send()

    by_role(owners_done)
    net.drain()


def scatter(grads, keep, give, terms, m_size, rows):
    cols = [g.shape[1] for g in grads]
    width = keep.shape[1]
    block = width // (2 * Z * m_size)
    seq = keep.shape[0] // Z
    first = [n for ch, n in enumerate(cols) if M_FIRST[ch]]
    last = [n for ch, n in enumerate(cols) if not M_FIRST[ch]]
    nf, nl = len(first), len(last)
    sem = pltpu.SemaphoreType.DMA
    vmem = lambda *shape: pltpu.VMEM(shape, bf16)
    doubling = m_size.bit_length() - 1 + 4
    any_spec = pl.BlockSpec(memory_space=pl.ANY)
    in_vmem = pl.BlockSpec(memory_space=pltpu.VMEM)
    far = m_size - 1
    outs = pl.pallas_call(
        functools.partial(scatter_kernel, m_size),
        out_shape=[jax.ShapeDtypeStruct((Z, block, n), bf16) for n in cols]
        + [jax.ShapeDtypeStruct((2, rows, width), bf16), jax.ShapeDtypeStruct(terms.shape[1:], f32)],
        in_specs=[any_spec] * 6 + [in_vmem],
        out_specs=[any_spec] * 5 + [in_vmem],
        scratch_shapes=[vmem(m_size, Z, block, n) for n in first] * 2
        + [vmem(far, Z, block, n) for n in first] * 2
        + [vmem(Z, block, n) for n in first]
        + [vmem(Z, 2, block, n) for n in last]
        + [vmem(far, Z, 2, block, n) for n in last]
        + [vmem(Z, 2, block, n) for n in last]
        + [vmem(Z, block, n) for n in last] * 3
        + [vmem(Z, seq, width)] * 3
        + [vmem(3, seq, width), vmem(seq, width), vmem(seq, width)]
        + [pltpu.VMEM(terms.shape, f32)] * 2
        + [
            sem((nf, m_size, Z)),
            sem((nf, m_size, Z, 2)),
            sem((nf, m_size, Z, 2)),
            sem((nf, m_size, Z)),
            sem((nf, m_size, Z)),
            sem((4, Z)),
            sem((4, Z)),
            sem((4,)),
            sem((nl, Z)),
            sem((nl, m_size, Z)),
            sem((nl, m_size, Z)),
            sem((nl, Z, 2)),
            sem((nl, Z, 2)),
            sem((Z,)),
            sem((Z,)),
            sem((Z,)),
            sem((Z,)),
            sem((Z,)),
            sem((2,)),
            sem((2,)),
            sem,
            sem((doubling,)),
            sem((doubling,)),
        ],
        compiler_params=pltpu.CompilerParams(
            collective_id=1, has_side_effects=True, vmem_limit_bytes=60 * 1024 * 1024
        ),
        name="scatter_all",
    )(
        *[g.reshape(Z, m_size, 2, block, -1) for g in grads],
        keep.reshape(Z, seq, width),
        give.reshape(Z, seq, width),
        terms,
    )
    return outs[:4], outs[4], outs[5]


def adam_kernel(per, *refs):
    count = len(refs) - 7
    grads, (weight, one, two), outs = refs[:count], refs[count : count + 3], refs[count + 3 :]
    cols = weight.shape[2]
    for j in range(weight.shape[1]):
        g = grads[j // per][0, :, (j % per) * cols : (j % per + 1) * cols].astype(f32)
        w_new, one_new, two_new = adam_step(weight[:, j, :], g, one[:, j, :], two[:, j, :])
        for ref, value in zip(outs, (g, w_new, one_new, two_new)):
            ref[:, j, :] = value


def adam_update(grads, per, weight, one, two):
    rows, kinds, width = weight.shape
    cols = width // Z
    spec = pl.BlockSpec((rows, kinds, cols), lambda q: (0, 0, q))
    return pl.pallas_call(
        functools.partial(adam_kernel, per),
        grid=(Z,),
        in_specs=[pl.BlockSpec((1, rows, per * cols), lambda q: (q, 0, 0))] * len(grads) + [spec] * 3,
        out_specs=[spec] * 4,
        out_shape=[jax.ShapeDtypeStruct(weight.shape, f32)] * 4,
        name="adam_update",
    )(*grads, weight, one, two)


def body(
    block_in,
    positions,
    out_grad,
    attn_weight,
    mlp_weight,
    small_params,
    attn_first,
    attn_second,
    mlp_first,
    mlp_second,
    small_first,
    small_second,
):
    grid = Grid(lax.axis_size("dp"), lax.axis_size("tensor"))
    z, m, c, t, diag = grid.z_now, grid.m_now, grid.c_now, grid.t_now, grid.diag
    devices = grid.dp * 2
    rows, width = block_in.shape
    seq = 2 * rows
    part = small_params.shape[1]

    normed, inverse = layer_stats(block_in)
    x_low, g_low = normed.astype(bf16), out_grad.astype(bf16)

    pieces = split_weights(attn_weight, mlp_weight)
    tile = -(-12 * part // 1024) * 1024
    small_tile = jnp.concatenate(
        [small_params.reshape(-1), jnp.zeros((tile - 12 * part,), f32), positions[0].astype(f32)]
        + [jnp.zeros((1024 - seq,), f32)]
    ).reshape(-1, 128)
    weights, acts, table = gather(pieces, jnp.stack([x_low, g_low]), small_tile, grid.m)
    w_qk, w_vo, w_up, w_dn = weights
    everyone = jnp.take(table.reshape(devices, -1), jnp.array(table_order(grid.m)), axis=0)
    small_all = jnp.transpose(everyone[:, : 12 * part].reshape(devices, 12, part), (1, 0, 2)).reshape(12, width)
    group = (jnp.arange(Z) * grid.m + m) * 4 + t * 2
    places = jnp.take(everyone[:, tile : tile + seq], group, axis=0)
    par = small_all[:4]
    head = c * Z + z
    hidden = w_up.shape[1]
    head_bias = lax.dynamic_slice_in_dim(small_all[4:6], head * HEAD_DIM, HEAD_DIM, axis=1)
    up_bias = lax.dynamic_slice_in_dim(small_all[8:12].reshape(1, -1), head * hidden, hidden, axis=1)

    one_low, attended, d_attn, head_sums = run_attention(acts, w_qk, w_vo, par, head_bias, places)
    two_low, activation, d_pre, up_sums = run_hidden(acts, w_up, w_dn, par, up_bias)
    keep, give, norm_sums = run_outs(diag, attended, d_attn, activation, d_pre, acts, weights, par)
    weight_grads = run_grads(one_low, two_low, acts, attended, d_attn, activation, d_pre)

    spread_cols = lambda v, n: lax.dynamic_update_slice_in_dim(
        jnp.zeros((n,), f32), v, head * v.shape[0], 0
    )
    out_sum = jnp.sum(out_grad, axis=0)
    small_terms = jnp.concatenate(
        [
            norm_sums,
            spread_cols(head_sums[0], width)[None],
            spread_cols(head_sums[1], width)[None],
            out_sum[None],
            out_sum[None],
            spread_cols(up_sums[0], 4 * width).reshape(4, width),
        ],
        axis=0,
    )
    terms = jnp.transpose(small_terms.reshape(12, devices, part), (1, 0, 2)).reshape(devices, 12 * part)
    places_of = table_order(grid.m)
    terms = jnp.take(terms, jnp.array([places_of.index(i) for i in range(devices)]), axis=0)
    terms = jnp.pad(terms, ((0, 0), (0, tile - 12 * part))).reshape(devices, -1, 128)
    own, own_rows, own_small = scatter(weight_grads, keep, give, terms, grid.m, rows)
    y_rows, u_rows = own_rows[0].astype(f32), own_rows[1].astype(f32)
    block_out = block_in + y_rows + small_all[6] + small_all[7]
    input_grad = out_grad + inverse * (
        u_rows
        - jnp.mean(u_rows, axis=-1, keepdims=True)
        - normed * jnp.mean(u_rows * normed, axis=-1, keepdims=True)
    )
    attn_out = adam_update(own[:2], 2, attn_weight, attn_first, attn_second)
    mlp_out = adam_update(own[2:], 1, mlp_weight, mlp_first, mlp_second)
    small_grad = own_small.reshape(-1)[: 12 * part].reshape(12, part)
    small_new, small_first_new, small_second_new = adam_step(small_params, small_grad, small_first, small_second)

    attn_grad, attn_new, attn_first_new, attn_second_new = attn_out
    mlp_grad, mlp_new, mlp_first_new, mlp_second_new = mlp_out
    return (
        block_out,
        input_grad,
        attn_grad,
        mlp_grad,
        small_grad,
        attn_new,
        attn_first_new,
        attn_second_new,
        mlp_new,
        mlp_first_new,
        mlp_second_new,
        small_new,
        small_first_new,
        small_second_new,
    )


def solution(mesh):
    rows = P(("dp", "tensor"), None)
    weights = P("dp", None, "tensor")
    small = P(None, ("dp", "tensor"))
    return jax.shard_map(
        body,
        mesh=mesh,
        in_specs=(rows, P("dp", None), rows, weights, weights, small, weights, weights, weights, weights, small, small),
        out_specs=(rows, rows) + (weights,) * 2 + (small,) + (weights,) * 6 + (small,) * 3,
        check_vma=False,
    )
```

```python
import functools

import jax
import jax.numpy as jnp
from jax import lax
from jax.experimental import pallas as pl
from jax.experimental.pallas import tpu as pltpu
from jax.sharding import PartitionSpec as P

ROT = 64
ADAM_STEP = 3
HEAD_DIM = 256
Z = 4

norm_epsilon = 1e-05
learn_rate = 0.006
beta_first = 0.9
beta_second = 0.95
adam_epsilon = 1e-08
weight_decay = 0.1

f32 = jnp.float32
bf16 = jnp.bfloat16


def layer_stats(row_data):
    center = row_data - jnp.mean(row_data, axis=-1, keepdims=True)
    inverse = lax.rsqrt(jnp.mean(center * center, axis=-1, keepdims=True) + norm_epsilon)
    return (center * inverse, inverse)


def adam_step(weight, gradient, moment_one, moment_two):
    one_new = beta_first * moment_one + (1.0 - beta_first) * gradient
    two_new = beta_second * moment_two + (1.0 - beta_second) * gradient * gradient
    corrected = (
        one_new
        / (1.0 - beta_first**ADAM_STEP)
        / (jnp.sqrt(two_new / (1.0 - beta_second**ADAM_STEP)) + adam_epsilon)
    )
    return (weight - learn_rate * (corrected + weight_decay * weight), one_new, two_new)


class Grid:
    def __init__(self, dp, tensor):
        assert tensor == 2 and dp % (2 * Z) == 0
        self.dp, self.m = dp, dp // (2 * Z)
        index = lax.axis_index("dp")
        self.index = index * 2 + lax.axis_index("tensor")
        self.z_now = index // (2 * self.m)
        self.m_now = (index // 2) % self.m
        self.c_now = index % 2
        self.t_now = lax.axis_index("tensor")
        self.diag = self.c_now == self.t_now


def split_kernel(attn, mlp, qk, vo, up, dn):
    quarter_a = attn.shape[2] // Z
    quarter_m = mlp.shape[2] // Z
    for q in range(Z):
        for j in range(4):
            block = attn[:, j, q * quarter_a : (q + 1) * quarter_a].astype(bf16)
            (qk, qk, vo, vo)[j][q, :, (j % 2) * quarter_a : (j % 2 + 1) * quarter_a] = block
        for j in range(2):
            (up, dn)[j][q] = mlp[:, j, q * quarter_m : (q + 1) * quarter_m].astype(bf16)


def split_weights(attn_weight, mlp_weight):
    rows, _, width = attn_weight.shape
    hidden = mlp_weight.shape[2]
    step = min(rows, 32)
    shapes = [2 * width // Z] * 2 + [hidden // Z] * 2
    return pl.pallas_call(
        split_kernel,
        grid=(rows // step,),
        in_specs=[
            pl.BlockSpec((step, 4, width), lambda i: (i, 0, 0)),
            pl.BlockSpec((step, 2, hidden), lambda i: (i, 0, 0)),
        ],
        out_specs=[pl.BlockSpec((Z, step, n), lambda i: (0, i, 0)) for n in shapes],
        out_shape=[jax.ShapeDtypeStruct((Z, rows, n), bf16) for n in shapes],
        name="split_weights",
    )(attn_weight, mlp_weight)


MESH = pl.DeviceIdType.MESH
PARTS = (1, 1, 2, 2)
CHUNKS = ((0, 0, True), (1, 0, False), (2, 0, True), (2, 1, False), (3, 0, True), (3, 1, False))
GATHER_ORDER = {
    (False, False): (
        0, 10, 500, 510, 520, 530, 540, 550, 700, 600, 501, 900, 620, 511, 910, 640, 601, 801, 502, 710, 20, 30, 40,
        50, 512, 602, 610, 920, 630, 811, 521, 650, 531, 621, 541, 551, 641, 611, 930, 802, 940, 503, 612, 513, 603,
        631, 651, 812, 522, 532, 622, 542, 552, 632, 642, 613, 652, 803, 813, 523, 533, 623, 543, 553, 633, 643, 653,
    ),
    (False, True): (
        0, 10, 700, 500, 510, 520, 530, 540, 550, 610, 630, 650, 600, 501, 900, 620, 511, 611, 640, 710, 20, 30, 40,
        50, 801, 910, 601, 502, 602, 811, 521, 930, 531, 621, 541, 940, 551, 641, 631, 512, 612, 651, 920, 802, 503,
        603, 812, 522, 532, 622, 542, 552, 642, 632, 513, 613, 652, 803, 813, 523, 533, 623, 543, 633, 553, 643, 653,
    ),
    (True, False): (
        0, 10, 500, 510, 520, 530, 540, 550, 900, 700, 600, 200, 503, 620, 100, 300, 640, 501, 513, 603, 210, 310,
        601, 110, 511, 710, 20, 30, 40, 50, 803, 400, 610, 801, 502, 910, 410, 630, 512, 602, 650, 811, 220, 813,
        120, 920, 523, 521, 320, 230, 623, 533, 130, 613, 621, 330, 531, 543, 240, 340, 140, 611, 553, 541, 643, 350,
        250, 930, 150, 551, 641, 940, 802, 612, 633, 631, 812, 653, 420, 651, 522, 430, 532, 622, 440, 542, 632, 450,
        642, 552, 652,
    ),
    (True, True): (
        0, 10, 700, 500, 510, 520, 530, 540, 550, 900, 610, 630, 650, 600, 200, 503, 620, 100, 300, 640, 501, 513,
        613, 710, 20, 30, 40, 50, 210, 310, 110, 511, 611, 603, 601, 803, 400, 801, 502, 910, 602, 813, 811, 523,
        220, 320, 120, 623, 533, 930, 521, 330, 230, 940, 543, 130, 621, 633, 340, 531, 643, 631, 553, 240, 350, 140,
        410, 541, 653, 512, 612, 250, 920, 641, 150, 551, 651, 802, 812, 420, 522, 430, 622, 532, 632, 440, 542, 450,
        642, 552, 652,
    ),
}
SCATTER_ORDER = {
    (False, False): (
        30, 31, 20, 21, 10, 11, 0, 1, 131, 530, 531, 520, 521, 510, 511, 500, 501, 1600, 203, 413, 223, 433, 243,
        453, 121, 1610, 202, 412, 222, 432, 242, 452, 111, 903, 1620, 201, 411, 221, 431, 241, 451, 101, 923, 943,
        1630, 200, 410, 220, 430, 240, 450, 130, 902, 1013, 1033, 303, 323, 922, 343, 120, 942, 1053, 302, 322, 342,
        110, 901, 1012, 921, 301, 321, 341, 100, 941, 300, 320, 340, 1032, 900, 920, 800, 1052, 940, 1113, 1133,
        1011, 1103, 810, 1031, 1051, 1153, 1123, 1143, 1640, 1010, 1112, 1030, 1050, 1102, 1122, 1142, 1101, 1132,
        1121, 1152, 1141, 1111, 1100, 1120, 1140, 1131, 1151, 1110, 1130, 1150,
    ),
    (False, True): (
        30, 31, 20, 21, 10, 11, 0, 1, 131, 530, 531, 520, 521, 510, 511, 500, 501, 1600, 203, 413, 223, 433, 243,
        453, 121, 1610, 903, 202, 412, 222, 432, 242, 452, 111, 923, 201, 411, 221, 431, 241, 451, 101, 943, 1620,
        200, 410, 220, 430, 240, 450, 130, 902, 1013, 922, 1033, 1630, 303, 323, 343, 120, 942, 1053, 901, 302, 322,
        342, 110, 921, 301, 321, 341, 100, 1012, 941, 300, 320, 340, 900, 920, 1032, 940, 800, 1113, 1052, 1133,
        1103, 1123, 810, 1011, 1031, 1153, 1051, 1143, 1640, 1010, 1112, 1030, 1050, 1102, 1122, 1142, 1132, 1101,
        1152, 1121, 1111, 1141, 1100, 1120, 1131, 1140, 1151, 1110, 1130, 1150,
    ),
    (True, False): (
        30, 31, 20, 21, 10, 11, 0, 1, 131, 530, 531, 520, 521, 510, 511, 500, 501, 1600, 203, 413, 223, 433, 243,
        453, 121, 1610, 202, 412, 222, 432, 242, 452, 111, 620, 903, 923, 1620, 201, 411, 221, 431, 241, 451, 101,
        943, 200, 410, 220, 430, 240, 450, 130, 902, 1013, 621, 922, 1033, 303, 323, 343, 1053, 120, 700, 901, 942,
        302, 322, 342, 110, 1012, 630, 921, 941, 301, 321, 341, 100, 710, 900, 920, 1032, 300, 320, 340, 1052, 940,
        631, 1113, 1133, 1103, 1011, 1123, 800, 1031, 1153, 1051, 1143, 810, 1630, 1310, 1112, 1010, 1330, 1300,
        1640, 1030, 1350, 1510, 1320, 1410, 1050, 1340, 1530, 1102, 1132, 1210, 1500, 1122, 1550, 1200, 1101, 1520,
        1220, 1142, 1540, 1240, 1121, 1152, 1400, 1141, 1111, 1430, 1230, 1100, 1131, 1120, 1151, 1420, 1250, 1140,
        1110, 1440, 1130, 1150, 1450,
    ),
    (True, True): (
        30, 31, 20, 21, 10, 11, 0, 1, 131, 530, 531, 520, 521, 510, 511, 500, 501, 1600, 203, 413, 223, 433, 243,
        453, 121, 1610, 903, 202, 412, 222, 432, 242, 452, 111, 620, 923, 201, 411, 221, 431, 241, 451, 101, 943,
        1620, 902, 200, 410, 220, 430, 240, 450, 130, 1013, 621, 922, 1033, 942, 1053, 303, 323, 343, 120, 700, 901,
        921, 302, 322, 342, 110, 630, 1012, 941, 900, 301, 321, 341, 100, 710, 920, 1032, 940, 300, 320, 340, 1113,
        1052, 631, 1133, 1103, 1123, 1011, 800, 1153, 1031, 1051, 1143, 810, 1630, 1112, 1102, 1310, 1330, 1010,
        1300, 1640, 1320, 1410, 1030, 1350, 1400, 1340, 1510, 1132, 1050, 1210, 1530, 1122, 1500, 1200, 1142, 1520,
        1220, 1101, 1550, 1240, 1152, 1121, 1540, 1230, 1111, 1141, 1430, 1131, 1100, 1250, 1151, 1120, 1420, 1140,
        1440, 1110, 1130, 1150, 1450,
    ),
}


class Links:
    def __init__(self, m_size):
        self.m_size = m_size
        index = lax.axis_index("dp")
        self.z, self.m, self.c = index // (2 * m_size), (index // 2) % m_size, index % 2
        self.t = lax.axis_index("tensor")
        self.sends = []

    def to(self, z=None, m=None, c=None, t=None):
        z, m, c = (own if v is None else v for v, own in ((z, self.z), (m, self.m), (c, self.c)))
        return ((z * self.m_size + m) * 2 + c, self.t if t is None else t)

    def copy(self, src, dst, send_sem, recv_sem, target):
        return pltpu.make_async_remote_copy(
            src_ref=src, dst_ref=dst, send_sem=send_sem, recv_sem=recv_sem, device_id=target, device_id_type=MESH
        )

    def send(self, src, dst, send_sem, recv_sem, target):
        one = self.copy(src, dst, send_sem, recv_sem, target)
        one.start()
        self.sends.append(one)

    def landed(self, dst, recv_sem):
        self.copy(dst, dst, recv_sem, recv_sem, self.to(c=1 - self.c)).wait_recv()

    def drain(self):
        for one in self.sends:
            one.wait_send()
        self.sends = []

    def partners(self):
        other = 1 - self.t
        out = [self.to(z=self.z ^ k) for k in range(1, Z)]
        out += [self.to(m=self.m ^ j) for j in range(1, self.m_size)]
        out += [self.to(c=1 - self.c), self.to(t=other), self.to(c=1 - self.c, t=other)]
        return out

    def doubling(self):
        high = self.z // 2
        place = ((self.m * 2 + self.c) * 2 + self.t) * 4 + lax.rem(self.z + high, 2) * 2 + high
        steps = [(1, self.to(z=self.z ^ 3)), (2, self.to(z=self.z ^ 1)), (4, self.to(t=1 - self.t))]
        steps.append((8, self.to(c=1 - self.c)))
        j = 1
        while j < self.m_size:
            steps.append((16 * j, self.to(m=self.m ^ j)))
            j *= 2
        return place, steps

    def meet(self):
        barrier = pltpu.get_barrier_semaphore()
        everyone = self.partners()
        for target in everyone:
            pl.semaphore_signal(barrier, inc=1, device_id=target, device_id_type=MESH)
        pl.semaphore_wait(barrier, len(everyone))


def gather_kernel(m_size, *refs):
    pieces, low, mine_small = refs[:4], refs[4], refs[5]
    full, act, table = refs[6:10], refs[10], refs[11]
    count = len(CHUNKS)
    stage, stage_m, relay = (refs[12 + i * count : 12 + (i + 1) * count] for i in range(3))
    refs = refs[12 + 3 * count :]
    (zs, zr, gs, gr, ps, pr, ms, mr, near_s, far_s, xr, as_, ar, ws, wr, ss, sr, lin, lout) = refs[:19]
    bounce, bounce_low = refs[19 : 19 + count], refs[19 + count]
    net = Links(m_size)
    z, m, c, t = net.z, net.m, net.c, net.t
    rows = pieces[0].shape[1]
    half = low.shape[1]
    role = lax.rem(c + t, 2)
    inner_z = lax.rem(z + z // 2, 2)

    def columns(ch):
        array, part, _ = CHUNKS[ch]
        wide = pieces[array].shape[2] // PARTS[array]
        return array, slice(part * wide, (part + 1) * wide)

    def piece(ch, zz):
        array, cols = columns(ch)
        return pieces[array].at[zz, :, cols]

    def whole(ch, zz, mm, cc, size=1):
        array, cols = columns(ch)
        start = ((zz * m_size + mm) * 2 + cc) * rows
        return full[array].at[pl.ds(pl.multiple_of(start, rows), size * rows), cols]

    own_place = pl.ds(pl.multiple_of(z * 2 * half + t * half, half), half)
    place = lambda zz, h: pl.ds(pl.multiple_of(zz * 2 * half + (t ^ h) * half, half), half)

    loads = [pltpu.make_async_copy(piece(ch, z), bounce[ch], lin.at[ch]) for ch in range(count)]
    loads.append(pltpu.make_async_copy(low.at[0], bounce_low, lin.at[count]))
    stores = [pltpu.make_async_copy(bounce[ch], whole(ch, z, m, c), lout.at[ch]) for ch in range(count)]
    stores.append(pltpu.make_async_copy(bounce_low, act.at[0, own_place], lout.at[count]))

    @pl.when(role == 0)
    def _():
        for one in loads:
            one.start()

    net.meet()
    flat, steps = net.doubling()
    small_own = pltpu.make_async_copy(mine_small, table.at[flat], ss.at[len(steps)])
    small_own.start()

    def program(inner, diag):
        state = {"small": 0}

        def small_send():
            i = state["small"]
            if i < len(steps):
                size, target = steps[i]
                span = table.at[pl.ds(flat // size * size, size)]
                net.send(span, span, ss.at[i], sr.at[i], target)

        def small_next():
            i = state["small"]
            if i < len(steps):
                size = steps[i][0]
                net.landed(table.at[pl.ds((flat // size ^ 1) * size, size)], sr.at[i])
                state["small"] += 1
                small_send()

        def spot(ch, zz, j):
            if diag:
                return whole(ch, zz, m ^ j, c)
            return stage_m[ch].at[m ^ j, zz] if j else stage[ch].at[zz]

        def source(ch, k, j):
            return piece(ch, z) if k == 0 and j == 0 else spot(ch, z ^ k, j)

        def spread(ch, k, j):
            src, dst = source(ch, k, j), whole(ch, z ^ k, m ^ j, c)
            net.send(src, dst, ps.at[ch, j, k, 1], pr.at[ch, j, k, c], net.to(c=t, t=1 - t))
            if not diag:
                net.send(src, dst, ps.at[ch, j, k, 0], pr.at[ch, j, k, c], net.to(c=1 - c))

        def spread_landed(ch, k, j):
            for cc in (1 - c,) if diag else (1 - c, c):
                net.landed(whole(ch, z ^ k, m ^ j, cc), pr.at[ch, j, k, cc])

        def swap(h, k):
            src = act.at[role, place(z ^ k, h)]
            net.send(src, src, ws.at[k, h], wr.at[k, h], net.to(c=1 - c))

        def rows_on(h, block, i, hop, k):
            src = act.at[role, place(block, h)]
            net.send(src, src, as_.at[h, i], ar.at[h, k], net.to(z=z ^ hop))

        def quarters(ch, _):
            for i, (k, hop, through) in enumerate(
                ((3, 3, None), (2, 3, 2), (1, 1, None)) if inner else ((3, 1, 1), (2, 1, 0), (1, 1, None))
            ):
                target = net.to(z=z ^ hop)
                if through is None:
                    net.send(piece(ch, z ^ k), spot(ch, z, 0), zs.at[ch, i], zr.at[ch, k], target)
                else:
                    net.send(piece(ch, z ^ k), relay[ch].at[through], zs.at[ch, i], gr.at[ch, through], target)

        def pass_on(through):
            hop, k = ((3, 2), (3, None), (1, 2), (1, 3))[through]

            def run(ch, _):
                src = relay[ch].at[through]
                net.landed(src, gr.at[ch, through])
                if k is None:
                    net.send(src, relay[ch].at[3], gs.at[ch, through], gr.at[ch, 3], net.to(z=z ^ hop))
                else:
                    dst = spot(ch, z ^ hop ^ k, 0)
                    net.send(src, dst, gs.at[ch, through], zr.at[ch, k], net.to(z=z ^ hop))

            return run

        def first(ch, k):
            if k:
                net.landed(spot(ch, z ^ k, 0), zr.at[ch, k])
            if CHUNKS[ch][2]:
                for j in range(1, m_size):
                    dst = whole(ch, z ^ k, m, c) if diag else stage_m[ch].at[m, z ^ k]
                    net.send(source(ch, k, 0), dst, ms.at[ch, j, k], mr.at[ch, j, k], net.to(m=m ^ j))
            spread(ch, k, 0)

        def second(ch, k):
            if CHUNKS[ch][2]:
                for j in range(1, m_size):
                    net.landed(spot(ch, z ^ k, j), mr.at[ch, j, k])
                    spread(ch, k, j)
            else:
                if diag and k == 0:
                    stores[ch].wait()
                spread_landed(ch, k, 0)
                both = whole(ch, z ^ k, m, 0, 2)
                for j in range(1, m_size):
                    net.send(both, both, ms.at[ch, j, k], mr.at[ch, j, k], net.to(m=m ^ j))

        def rows_start(h, _):
            if h:
                net.landed(act.at[0 if diag else 1, place(z, 1)], xr.at[1])
            elif diag:
                stores[count].wait()
            else:
                net.landed(act.at[1, place(z, 0)], xr.at[0])
            if inner:
                rows_on(h, z, 0, 3, 3)
            rows_on(h, z, 1, 1, 1)
            swap(h, 0)

        def rows_next(h, k):
            net.landed(act.at[role, place(z ^ k, h)], ar.at[h, k])
            if inner:
                hop, there = {1: (3, 2), 3: (1, 2), 2: (1, 3)}[k]
                rows_on(h, z ^ k, 1 + k, hop, there)
            swap(h, k)

        small_own.wait()
        small_send()
        if diag:
            net.send(low.at[1], act.at[1, own_place], near_s, xr.at[0], net.to(c=1 - c))
        else:
            net.send(low.at[0], act.at[0, own_place], near_s, xr.at[1], net.to(t=1 - t))
            net.send(low.at[1], act.at[1, own_place], far_s, xr.at[1], net.to(c=1 - c, t=1 - t))
        if diag:
            for load, store in zip(loads, stores):
                load.wait()
                store.start()
        runs = [quarters] + [pass_on(i) for i in range(4)] + [first, second, rows_start, rows_next]
        runs.append(lambda *_: small_next())
        for code in GATHER_ORDER[inner, diag]:
            runs[code // 100](code // 10 % 10, code % 10)
        while state["small"] < len(steps):
            small_next()
        for ch in range(count):
            for k in range(Z):
                if CHUNKS[ch][2]:
                    for j in range(m_size):
                        spread_landed(ch, k, j)
                    if diag and k == 0:
                        stores[ch].wait()
                else:
                    for j in range(1, m_size):
                        net.landed(whole(ch, z ^ k, m ^ j, 0, 2), mr.at[ch, j, k])
        for k in range(Z):
            for h in range(2):
                net.landed(act.at[1 - role, place(z ^ k, h)], wr.at[k, h])
        net.drain()

    by_class(inner_z, role, program)


def table_order(m_size):
    order = []
    for z in range(Z):
        for rest in range(4 * m_size):
            order.append(rest * 4 + (z + z // 2) % 2 * 2 + z // 2)
    return order


def by_class(inner_z, role, program):
    for inner in (False, True):
        for diag in (False, True):

            @pl.when((inner_z == int(inner)) & (role == int(not diag)))
            def _(inner=inner, diag=diag):
                program(inner, diag)


def gather(pieces, low, small, m_size):
    rows = pieces[0].shape[1]
    width = low.shape[2]
    devices = m_size * 4 * Z
    cols = [p.shape[2] for p in pieces]
    count = len(CHUNKS)
    parts = [cols[array] // PARTS[array] for array, _, _ in CHUNKS]
    sem = pltpu.SemaphoreType.DMA
    doubling = m_size.bit_length() - 1 + 4
    in_place = pl.BlockSpec(memory_space=pl.ANY)
    shape = lambda *dims: jax.ShapeDtypeStruct(dims, bf16)
    outs = pl.pallas_call(
        functools.partial(gather_kernel, m_size),
        out_shape=[shape(width, n) for n in cols]
        + [shape(2, Z * 2 * low.shape[1], width), jax.ShapeDtypeStruct((devices,) + small.shape, f32)]
        + [shape(Z, rows, n) for n in parts]
        + [shape(m_size, Z, rows, n) for n in parts]
        + [shape(4, rows, n) for n in parts],
        in_specs=[in_place] * 6,
        out_specs=[in_place] * (6 + 3 * count),
        scratch_shapes=[
            sem((count, 3)),
            sem((count, Z)),
            sem((count, 4)),
            sem((count, 4)),
            sem((count, m_size, Z, 2)),
            sem((count, m_size, Z, 2)),
            sem((count, m_size, Z)),
            sem((count, m_size, Z)),
            sem,
            sem,
            sem((2,)),
            sem((2, 5)),
            sem((2, Z)),
            sem((Z, 2)),
            sem((Z, 2)),
            sem((doubling + 1,)),
            sem((doubling,)),
            sem((count + 1,)),
            sem((count + 1,)),
        ]
        + [pltpu.VMEM((rows, n), bf16) for n in parts]
        + [pltpu.VMEM(low.shape[1:], bf16)],
        compiler_params=pltpu.CompilerParams(collective_id=0, has_side_effects=True),
        name="gather_all",
    )(*pieces, low, small)
    return outs[:4], outs[4], outs[5]


VMEM_BYTES = 60 * 1024 * 1024


def dot(a, b, over_a=1, over_b=0):
    return lax.dot_general(a, b, (((over_a,), (over_b,)), ((), ())), preferred_element_type=f32)


def turn(value, tables, sign):
    cos, low, high = (table[...] for table in tables)
    part = value[:, :128]
    turned = part * cos + sign * (
        pltpu.roll(part, 128 - ROT // 2, 1) * low + pltpu.roll(part, ROT // 2, 1) * high
    )
    return jnp.concatenate([turned, value[:, 128:]], axis=1)


def turn_tables(places):
    half = ROT // 2
    column = jnp.arange(128)
    frequency = 10000.0 ** (-((column % half).astype(f32) * (2.0 / ROT)))
    angles = places.reshape(-1, 1) * frequency
    cos = jnp.where(column < ROT, jnp.cos(angles), 1.0)
    sin = jnp.sin(angles)
    return cos, jnp.where(column < half, -sin, 0.0), jnp.where((column >= half) & (column < ROT), sin, 0.0)


def attn_kernel(x, g, w_qk, w_vo, par, bias, cos, low, high, across, down, one_out, att_out, d_out, sums):
    tables = (cos, low, high)
    n = HEAD_DIM
    scale = HEAD_DIM ** (-0.5)
    one = (x[...].astype(f32) * par[0:1, :] + par[1:2, :]).astype(bf16)
    one_out[...] = one
    qk = dot(one, w_qk[...])
    q = turn(qk[:, :n] + bias[0:1, :], tables, 1.0).astype(bf16)
    k = turn(qk[:, n:], tables, 1.0).astype(bf16)
    v = (dot(one, w_vo[:, :n]) + bias[1:2, :]).astype(bf16)
    d_att = dot(g[...], w_vo[:, n:]).astype(bf16)
    scores = jnp.where(across[0] <= down[0], dot(q, k, 1, 1) * scale, -jnp.inf)
    top = jnp.max(scores, axis=-1, keepdims=True)
    log_total = top + jnp.log(jnp.sum(jnp.exp(scores - top), axis=-1, keepdims=True))
    probs = jnp.exp(scores - log_total)
    low_probs = probs.astype(bf16)
    att_out[...] = dot(low_probs, v).astype(bf16)
    d_probs = dot(d_att, v, 1, 1)
    d_scores = (probs * (d_probs - jnp.sum(probs * d_probs, axis=-1, keepdims=True)) * scale).astype(bf16)
    d_q = turn(dot(d_scores, k), tables, -1.0)
    d_k = turn(dot(d_scores, q, 0, 0), tables, -1.0)
    d_v = dot(low_probs, d_att, 0, 0)
    d_out[:, :n] = d_q.astype(bf16)
    d_out[:, n : 2 * n] = d_k.astype(bf16)
    d_out[:, 2 * n :] = d_v.astype(bf16)

    @pl.when(pl.program_id(0) == 0)
    def _():
        sums[...] = jnp.zeros_like(sums)

    sums[0:1, :] += jnp.sum(d_q, axis=0, keepdims=True)
    sums[1:2, :] += jnp.sum(d_v, axis=0, keepdims=True)


def fixed(*shape):
    return pl.BlockSpec(shape, lambda i: (0,) * len(shape))


def run_attention(acts, w_qk, w_vo, par, bias, places):
    _, rows, width = acts.shape
    seq, n = rows // Z, HEAD_DIM
    by_rows = lambda cols: pl.BlockSpec((seq, cols), lambda i: (i, 0))
    act = lambda which: pl.BlockSpec((None, seq, width), lambda i: (which, i, 0))
    return pl.pallas_call(
        attn_kernel,
        grid=(Z,),
        in_specs=[act(0), act(1), fixed(width, 2 * n), fixed(width, 2 * n), fixed(*par.shape), fixed(2, n)]
        + [by_rows(128)] * 3
        + [pl.BlockSpec((1, 1, seq), lambda i: (i, 0, 0)), pl.BlockSpec((1, seq, 1), lambda i: (i, 0, 0))],
        out_specs=[by_rows(width), by_rows(n), by_rows(3 * n), fixed(2, n)],
        out_shape=[jax.ShapeDtypeStruct((rows, cols), bf16) for cols in (width, n, 3 * n)]
        + [jax.ShapeDtypeStruct((2, n), f32)],
        compiler_params=pltpu.CompilerParams(vmem_limit_bytes=VMEM_BYTES),
        name="attention",
    )(acts, acts, w_qk, w_vo, par, bias, *turn_tables(places), places[:, None, :], places[:, :, None])


def hidden_kernel(x, g, up, down, par, bias, two_out, act_out, d_out, sums):
    @pl.when(pl.program_id(0) == 0)
    def _():
        two_out[...] = (x[...].astype(f32) * par[2:3, :] + par[3:4, :]).astype(bf16)

    pre = dot(two_out[...], up[...]) + bias[...]
    erf = 1.0 + lax.erf(pre * 0.7071067811865476)
    act_out[...] = (0.5 * pre * erf).astype(bf16)
    slope = 0.5 * erf + pre * jnp.exp(-0.5 * pre * pre) * 0.3989422804014327
    d_pre = dot(g[...], down[...]) * slope
    d_out[...] = d_pre.astype(bf16)
    sums[...] = jnp.sum(d_pre, axis=0, keepdims=True)


def run_hidden(acts, w_up, w_dn, par, bias):
    _, rows, width = acts.shape
    hidden = w_up.shape[1]
    step = 256
    act = lambda which: pl.BlockSpec((None, rows, width), lambda i: (which, 0, 0), pipeline_mode=pl.Buffered(1))
    tile = lambda height: pl.BlockSpec((height, step), lambda i: (0, i))
    return pl.pallas_call(
        hidden_kernel,
        grid=(hidden // step,),
        in_specs=[act(0), act(1), tile(width), tile(width), fixed(*par.shape), tile(1)],
        out_specs=[fixed(rows, width), tile(rows), tile(rows), tile(1)],
        out_shape=[jax.ShapeDtypeStruct((rows, n), bf16) for n in (width, hidden, hidden)]
        + [jax.ShapeDtypeStruct((1, hidden), f32)],
        compiler_params=pltpu.CompilerParams(vmem_limit_bytes=VMEM_BYTES),
        name="hidden_units",
    )(acts, acts, w_up, w_dn, par, bias)


def outs_kernel(flag, att, d_attn, act, d_pre, x, w_qk, w_vo, w_up, w_dn, par, keep, give, sums):
    diag = flag[0] == 1
    n = HEAD_DIM
    y = dot(att[...], w_vo[:, n:], 1, 1) + dot(act[...], w_dn[...], 1, 1)
    d_one = dot(d_attn[:, : 2 * n], w_qk[...], 1, 1) + dot(d_attn[:, 2 * n :], w_vo[:, :n], 1, 1)
    d_two = dot(d_pre[...], w_up[...], 1, 1)
    u = d_one * par[0:1, :] + d_two * par[2:3, :]
    keep[...] = jnp.where(diag, y, u).astype(bf16)
    give[...] = jnp.where(diag, u, y).astype(bf16)
    plain = x[...].astype(f32)
    for i, value in enumerate((d_one * plain, d_one, d_two * plain, d_two)):
        sums[i : i + 1, :] = jnp.sum(value, axis=0, keepdims=True)


def run_outs(diag, att, d_attn, act, d_pre, acts, weights, par):
    _, rows, width = acts.shape
    step = 256
    fix = lambda v: pl.BlockSpec(v.shape, lambda i, s: (0, 0), pipeline_mode=pl.Buffered(1))
    tile = lambda height: pl.BlockSpec((height, step), lambda i, s: (0, i))
    return pl.pallas_call(
        outs_kernel,
        grid_spec=pltpu.PrefetchScalarGridSpec(
            num_scalar_prefetch=1,
            grid=(width // step,),
            in_specs=[fix(v) for v in (att, d_attn, act, d_pre)]
            + [pl.BlockSpec((None, rows, step), lambda i, s: (0, 0, i))]
            + [pl.BlockSpec((step, v.shape[1]), lambda i, s: (i, 0)) for v in weights]
            + [tile(4)],
            out_specs=[tile(rows), tile(rows), tile(4)],
        ),
        out_shape=[jax.ShapeDtypeStruct((rows, width), bf16)] * 2 + [jax.ShapeDtypeStruct((4, width), f32)],
        compiler_params=pltpu.CompilerParams(vmem_limit_bytes=VMEM_BYTES),
        name="outputs",
    )(diag.astype(jnp.int32).reshape(1), att, d_attn, act, d_pre, acts, *weights, par)


def grads_kernel(one, two, g, att, d_attn, act, d_pre, qk, vo, up, dn):
    n = HEAD_DIM
    first = dot(one[...], d_attn[...], 0, 0)
    qk[...] = first[:, : 2 * n].astype(bf16)
    vo[:, :n] = first[:, 2 * n :].astype(bf16)
    vo[:, n:] = dot(g[...], att[...], 0, 0).astype(bf16)
    up[...] = dot(two[...], d_pre[...], 0, 0).astype(bf16)
    dn[...] = dot(g[...], act[...], 0, 0).astype(bf16)


def run_grads(one, two, acts, att, d_attn, act, d_pre):
    rows, width = one.shape
    step = 256
    tile = pl.BlockSpec((rows, step), lambda i: (0, i))
    fix = lambda v: pl.BlockSpec(v.shape, lambda i: (0, 0), pipeline_mode=pl.Buffered(1))
    cols = [2 * HEAD_DIM, 2 * HEAD_DIM, act.shape[1], act.shape[1]]
    return pl.pallas_call(
        grads_kernel,
        grid=(width // step,),
        in_specs=[tile, tile, pl.BlockSpec((None, rows, step), lambda i: (1, 0, i))]
        + [fix(v) for v in (att, d_attn, act, d_pre)],
        out_specs=[pl.BlockSpec((step, n), lambda i: (i, 0)) for n in cols],
        out_shape=[jax.ShapeDtypeStruct((width, n), bf16) for n in cols],
        compiler_params=pltpu.CompilerParams(vmem_limit_bytes=VMEM_BYTES),
        name="weight_grads",
    )(one, two, acts, att, d_attn, act, d_pre)


def add_rows(dst, sources):
    step = min(dst.shape[0], 32)

    @pl.loop(0, dst.shape[0] // step)
    def _(i):
        span = pl.ds(pl.multiple_of(i * step, step), step)
        total = sources[0][span, :].astype(f32)
        for one in sources[1:]:
            total = total + one[span, :].astype(f32)
        dst[span, :] = total.astype(dst.dtype)


def scatter_kernel(m_size, fused, *refs):
    if fused:
        ones, twos, acts, att, d_attn, act, d_pre = refs[:7]
        keep, give, terms = refs[7:10]
        grads, refs = refs[10:14], refs[14:]
    else:
        grads, (keep, give, terms), refs = refs[:4], refs[4:7], refs[7:]
    own, rows_out, small_out, refs = refs[:4], refs[4], refs[5], refs[6:]
    count = len(CHUNKS)
    buffers = []
    for _, _, m_first in CHUNKS:
        size = 5 if m_first else 6
        buffers.append(refs[:size])
        refs = refs[size:]
    relay, refs = refs[:count], refs[count:]
    got, kept, got_z, final, current, got_small = refs[:6]
    (gs, gr, kl, as_, ar, ys, yr, yl, ws, wr, wl, fs, fr, xs, xr, zs, zr, zl, ps, pr, ss, sr) = refs[6:28]
    if fused:
        tiles, made, tl, ml = refs[28:]
    net = Links(m_size)
    z, m, c, t = net.z, net.m, net.c, net.t
    half = rows_out.shape[1]
    role = lax.rem(c + t, 2)
    inner_z = lax.rem(z + z // 2, 2)
    flat, steps = net.doubling()
    steps = steps[::-1]

    def columns(ch):
        array, part, _ = CHUNKS[ch]
        wide = own[array].shape[2] // PARTS[array]
        return array, slice(part * wide, (part + 1) * wide)

    def rows_of(ch, k, j, cc=None):
        array, cols = columns(ch)
        if cc is None:
            return grads[array].at[z ^ k, m ^ j, :, :, cols]
        return grads[array].at[z ^ k, m ^ j, cc, :, cols]

    def owned(ch, zz):
        array, cols = columns(ch)
        return own[array].at[zz, :, cols]

    span = lambda h: pl.ds(pl.multiple_of((t ^ h) * half, half), half)
    loads_keep = [pltpu.make_async_copy(keep.at[z ^ k], kept.at[k], kl.at[k]) for k in range(Z)]
    for one in loads_keep:
        one.start()
    current[...] = terms[...]

    def tile_loads(i, slot):
        block = (z ^ (Z - 1 - lax.rem(i, Z))) * m_size + (m ^ (1 - i // Z))
        wide = tiles.shape[3]
        cols = pl.ds(pl.multiple_of(block * wide, wide), wide)
        sources = (ones.at[:, cols], twos.at[:, cols], acts.at[1, :, cols])
        return [pltpu.make_async_copy(src, tiles.at[slot, n], tl.at[slot, n]) for n, src in enumerate(sources)]

    def make(i):
        slot = lax.rem(i, 2)

        @pl.when(i < 2 * Z - 1)
        def _():
            for one in tile_loads(i + 1, 1 - slot):
                one.start()

        for one in tile_loads(i, slot):
            one.wait()
        n = HEAD_DIM
        high = made[0].shape[1]
        for array, at, left, right, lo, hi in (
            (0, 0, 0, d_attn, 0, 2 * n),
            (1, 0, 0, d_attn, 2 * n, 3 * n),
            (1, n, 2, att, 0, n),
            (2, 0, 1, d_pre, 0, d_pre.shape[1]),
            (3, 0, 2, act, 0, act.shape[1]),
        ):
            value = dot(tiles[slot, left], right[:, lo:hi], 0, 0).astype(bf16)
            for cc in range(2):
                made[array][cc, :, at : at + hi - lo] = value[cc * high : (cc + 1) * high]
        stores = [
            pltpu.make_async_copy(
                made[array], grads[array].at[z ^ (Z - 1 - lax.rem(i, Z)), m ^ (1 - i // Z)], ml.at[array]
            )
            for array in range(4)
        ]
        for one in stores:
            one.start()
        for one in stores:
            one.wait()

    if fused:
        for one in tile_loads(0, 0):
            one.start()
    net.meet()

    def program(inner, diag):
        state = {"small": 0}
        sent = []

        def send(*parts):
            (parts,) = parts
            net.copy(*parts()).start()
            sent.append(parts)

        def small_send():
            i = state["small"]
            if i < len(steps):
                size, target = steps[i]
                send(
                    lambda: (
                        current.at[pl.ds((flat // size ^ 1) * size, size)],
                        got_small.at[pl.ds(size, size)],
                        ss.at[i],
                        sr.at[i],
                        target,
                    )
                )

        def small_next(*_):
            i = state["small"]
            if i < len(steps):
                size = steps[i][0]
                net.landed(got_small.at[pl.ds(size, size)], sr.at[i])
                block = pl.ds(flat // size * size, size)
                current[block] = current[block] + got_small[pl.ds(size, size)]
                state["small"] += 1
                small_send()

        def swap(k, h):
            send(
                lambda: (give.at[z ^ k, span(h)], got.at[k, span(h)], gs.at[k, h], gr.at[k, h], net.to(c=1 - c))
            )

        def load_mine(ch, j, k):
            if CHUNKS[ch][2]:
                return pltpu.make_async_copy(rows_of(ch, k, j, c), buffers[ch][0].at[j, k], wl.at[ch, j, k])
            return pltpu.make_async_copy(rows_of(ch, k, 0), buffers[ch][0].at[k], wl.at[ch, 0, k])

        def load_made(k, own_m):
            for j in (0,) if own_m == 0 else range(1, m_size):
                for ch in range(count):
                    if (diag and CHUNKS[ch][2]) or (j == 0 and not CHUNKS[ch][2]):
                        load_mine(ch, j, k).start()

        def to_owner(source, home, far, ch, j, k):
            if diag:
                send(lambda: (source(1 - c), home(), ws.at[ch, j, k, 0], wr.at[ch, j, k, 0], net.to(c=1 - c)))
            else:
                send(lambda: (source(c), far(), ws.at[ch, j, k, 0], wr.at[ch, j, k, 1], net.to(t=1 - t)))
                send(
                    lambda: (source(1 - c), far(), ws.at[ch, j, k, 1], wr.at[ch, j, k, 1], net.to(c=1 - c, t=1 - t))
                )

        def owners_part(ch, j, k):
            home, far = buffers[ch][0], buffers[ch][1]
            to_owner(lambda cc: rows_of(ch, k, j, cc), lambda: home.at[j, k], lambda: far.at[j, k], ch, j, k)

        def others(ch, k):
            for j in range(1, m_size):
                owners_part(ch, j, k)

        def same(ch, k):
            owners_part(ch, 0, k)

        def across(ch, k):
            for j in range(1, m_size):
                send(
                    lambda j=j: (
                        rows_of(ch, k, j),
                        buffers[ch][1].at[j - 1, k],
                        fs.at[ch, j, k],
                        fr.at[ch, j, k],
                        net.to(m=m ^ j),
                    )
                )

        def collected(home, far, ch, j, k):
            if not diag:
                net.landed(home, wr.at[ch, j, k, 0])
            elif CHUNKS[ch][2]:
                load_mine(ch, j, k).wait()
            net.landed(far, wr.at[ch, j, k, 1])

        def middle(ch, k):
            home, far, mid, far_m, _ = buffers[ch]
            for j in range(1, m_size):
                collected(home.at[j, k], far.at[j, k], ch, j, k)
                add_rows(mid.at[j - 1, k], [home.at[j, k], far.at[j, k]])
                send(
                    lambda j=j: (
                        mid.at[j - 1, k],
                        far_m.at[j - 1, k],
                        xs.at[ch, j, k],
                        xr.at[ch, j, k],
                        net.to(m=m ^ j),
                    )
                )

        def summed(ch, k):
            mine, far_m, both, home, far, _ = buffers[ch]
            load_mine(ch, 0, k).wait()
            for j in range(1, m_size):
                net.landed(far_m.at[j - 1, k], fr.at[ch, j, k])
            for cc in range(2):
                add_rows(both.at[k, cc], [mine.at[k, cc]] + [far_m.at[j - 1, k, cc] for j in range(1, m_size)])
            to_owner(lambda cc: both.at[k, cc], lambda: home.at[k], lambda: far.at[k], ch, 0, k)

        def finish(ch, k):
            if CHUNKS[ch][2]:
                home, far, _, far_m, result = buffers[ch]
                collected(home.at[0, k], far.at[0, k], ch, 0, k)
                for j in range(1, m_size):
                    net.landed(far_m.at[j - 1, k], xr.at[ch, j, k])
                sources = [home.at[0, k], far.at[0, k]] + [far_m.at[j - 1, k] for j in range(1, m_size)]
            else:
                _, _, both, home, far, result = buffers[ch]
                collected(home.at[k], far.at[k], ch, 0, k)
                sources = [both.at[k, c] if diag else home.at[k], far.at[k]]
            add_rows(result.at[k], sources)
            if k == 0:
                pltpu.make_async_copy(result.at[k], owned(ch, z), zl.at[ch]).start()
                return
            hop, through = {1: (1, None), 2: (3, 2), 3: (3, None)}[k] if inner else {1: (1, None), 2: (1, 0), 3: (1, 1)}[k]
            if through is None:
                send(lambda: (result.at[k], owned(ch, z), zs.at[ch, k], zr.at[ch, k], net.to(z=z ^ hop)))
            else:
                send(
                    lambda: (
                        result.at[k],
                        relay[ch].at[through],
                        zs.at[ch, k],
                        pr.at[ch, through],
                        net.to(z=z ^ hop),
                    )
                )

        def pass_on(through):
            hop, k = ((3, 2), (3, None), (1, 2), (1, 3))[through]

            def run(ch, _):
                net.landed(relay[ch].at[through], pr.at[ch, through])

                def parts():
                    if k is None:
                        dst, recv_sem = relay[ch].at[3], pr.at[ch, 3]
                    else:
                        dst, recv_sem = owned(ch, z ^ hop ^ k), zr.at[ch, k]
                    return relay[ch].at[through], dst, ps.at[ch, through], recv_sem, net.to(z=z ^ hop)

                send(parts)

            return run

        def rows_first(k, h):
            if h == 0:
                pltpu.make_async_copy(keep.at[z ^ k], kept.at[k], kl.at[k]).wait()
            net.landed(got.at[k, span(h)], gr.at[k, h])
            add_rows(kept.at[k, span(h)], [kept.at[k, span(h)], got.at[k, span(h)]])
            if k and not inner:
                slot = {1: 0, 2: 1, 3: 2}[k]
                send(
                    lambda: (
                        kept.at[k, span(h)],
                        got_z.at[slot, span(h)],
                        as_.at[k, h],
                        ar.at[slot, h],
                        net.to(z=z ^ 1),
                    )
                )

        def rows_through(k, h, slot, there, hop):
            net.landed(got_z.at[slot, span(h)], ar.at[slot, h])
            add_rows(kept.at[k, span(h)], [kept.at[k, span(h)], got_z.at[slot, span(h)]])
            send(
                lambda: (
                    kept.at[k, span(h)],
                    got_z.at[there, span(h)],
                    as_.at[k, h],
                    ar.at[there, h],
                    net.to(z=z ^ hop),
                )
            )

        def rows_inner(k, h):
            rows_through(k, h, {3: 1, 2: 2}[k], {3: 3, 2: 4}[k], 3)

        def rows_outer(h, _):
            rows_through(1, h, 4, 0, 1)

        def rows_back(h, _):
            slots = (0, 3) if inner else (0,)
            for slot in slots:
                net.landed(got_z.at[slot, span(h)], ar.at[slot, h])
            add_rows(final.at[h], [kept.at[0, span(h)]] + [got_z.at[slot, span(h)] for slot in slots])
            if diag and h == 0:
                pltpu.make_async_copy(final.at[h], rows_out.at[0], yl).start()
            elif diag:
                send(lambda: (final.at[h], rows_out.at[0], ys.at[h], yr.at[0], net.to(t=1 - t)))
            elif h == 0:
                send(lambda: (final.at[h], rows_out.at[1], ys.at[h], yr.at[1], net.to(c=1 - c)))
            else:
                send(lambda: (final.at[h], rows_out.at[1], ys.at[h], yr.at[1], net.to(c=1 - c, t=1 - t)))

        runs = [swap, load_made, others, same, across, rows_first, rows_inner, rows_outer, rows_back]
        runs += [middle, summed, finish] + [pass_on(i) for i in range(4)] + [small_next]

        def run(codes):
            for code in codes:
                runs[code // 100](code // 10 % 10, code % 10)

        def end():
            while state["small"] < len(steps):
                small_next()
            small_out[...] = current[flat]
            for ch in range(count):
                for k in range(1, Z):
                    net.landed(owned(ch, z ^ k), zr.at[ch, k])
                pltpu.make_async_copy(owned(ch, z), owned(ch, z), zl.at[ch]).wait()
            net.landed(rows_out.at[1], yr.at[1])
            if diag:
                pltpu.make_async_copy(final.at[0], rows_out.at[0], yl).wait()
            else:
                net.landed(rows_out.at[0], yr.at[0])
            for parts in sent:
                net.copy(*parts()).wait_send()

        return small_send, run, end

    programs = {key: program(*key) for key in SCATTER_ORDER}
    cuts = {
        key: [i for i, code in enumerate(codes) if code // 100 == 1] + [len(codes)]
        for key, codes in SCATTER_ORDER.items()
    }

    def begin(inner, diag):
        small_send, run, _ = programs[inner, diag]
        small_send()
        run(SCATTER_ORDER[inner, diag][: cuts[inner, diag][0]])

    def part(i, inner, diag):
        lo, hi = cuts[inner, diag][i : i + 2]
        programs[inner, diag][1](SCATTER_ORDER[inner, diag][lo:hi])

    by_class(inner_z, role, begin)
    if fused:

        @pl.loop(0, 2 * Z)
        def _(i):
            make(i)
            for n in range(2 * Z):

                @pl.when(i == n)
                def _(n=n):
                    by_class(inner_z, role, functools.partial(part, n))

    else:
        for n in range(2 * Z):
            by_class(inner_z, role, functools.partial(part, n))
    by_class(inner_z, role, lambda inner, diag: programs[inner, diag][2]())


def scatter(factors, keep, give, terms, m_size, rows):
    one, two, acts, att, d_attn, act, d_pre = factors
    width = keep.shape[1]
    block = width // (2 * Z * m_size)
    seq = keep.shape[0] // Z
    cols = [2 * HEAD_DIM, 2 * HEAD_DIM, act.shape[1], act.shape[1]]
    parts = [cols[array] // PARTS[array] for array, _, _ in CHUNKS]
    count = len(CHUNKS)
    fused = m_size == 2 and 2 * block % 256 == 0
    sem = pltpu.SemaphoreType.DMA
    vmem = lambda *shape: pltpu.VMEM(shape, bf16)
    doubling = m_size.bit_length() - 1 + 4
    in_place = pl.BlockSpec(memory_space=pl.ANY)
    in_vmem = pl.BlockSpec(memory_space=pltpu.VMEM)
    far = m_size - 1
    term_shapes = [jax.ShapeDtypeStruct((Z, m_size, 2, block, n), bf16) for n in cols]
    out_shape = [jax.ShapeDtypeStruct((Z, block, n), bf16) for n in cols]
    out_shape += [jax.ShapeDtypeStruct((2, rows, width), bf16), jax.ShapeDtypeStruct(terms.shape[1:], f32)]
    out_specs = [in_place] * 5 + [in_vmem]
    if fused:
        inputs = [one, two, acts, att, d_attn, act, d_pre]
        in_specs = [in_place] * 3 + [in_vmem] * 4
        out_shape, out_specs = term_shapes + out_shape, [in_place] * 4 + out_specs
    else:
        inputs = [g.reshape(s.shape) for g, s in zip(run_grads(*factors), term_shapes)]
        in_specs = [in_place] * 4
    scratch = []
    for n, (_, _, m_first) in zip(parts, CHUNKS):
        if m_first:
            scratch += [vmem(m_size, Z, block, n)] * 2 + [vmem(far, Z, block, n)] * 2 + [vmem(Z, block, n)]
        else:
            scratch += [vmem(Z, 2, block, n), vmem(far, Z, 2, block, n), vmem(Z, 2, block, n)]
            scratch += [vmem(Z, block, n)] * 3
    scratch += [vmem(4, block, n) for n in parts]
    scratch += [vmem(Z, seq, width)] * 2 + [vmem(5, seq, width), vmem(2, rows, width)]
    scratch += [pltpu.VMEM(terms.shape, f32)] * 2
    scratch += [
        sem((Z, 2)),
        sem((Z, 2)),
        sem((Z,)),
        sem((Z, 2)),
        sem((5, 2)),
        sem((2,)),
        sem((2,)),
        sem,
        sem((count, m_size, Z, 2)),
        sem((count, m_size, Z, 2)),
        sem((count, m_size, Z)),
        sem((count, m_size, Z)),
        sem((count, m_size, Z)),
        sem((count, m_size, Z)),
        sem((count, m_size, Z)),
        sem((count, Z)),
        sem((count, Z)),
        sem((count,)),
        sem((count, 4)),
        sem((count, 4)),
        sem((doubling,)),
        sem((doubling,)),
    ]
    if fused:
        scratch.append(vmem(2, 3, keep.shape[0], 2 * block))
        made = [vmem(2, block, n) for n in cols]
        scratch_made = [sem((2, 3)), sem((4,))]
    outs = pl.pallas_call(
        functools.partial(scatter_entry, m_size, fused),
        out_shape=out_shape,
        in_specs=in_specs + [in_place] * 2 + [in_vmem],
        out_specs=out_specs,
        scratch_shapes=scratch + (made + scratch_made if fused else []),
        compiler_params=pltpu.CompilerParams(collective_id=1, has_side_effects=True, vmem_limit_bytes=67043328),
        name="scatter_all",
    )(*inputs, keep.reshape(Z, seq, width), give.reshape(Z, seq, width), terms)
    outs = outs[4:] if fused else outs
    return outs[:4], outs[4], outs[5]


def scatter_entry(m_size, fused, *refs):
    if fused:
        refs = refs[:-6] + (refs[-6:-2],) + refs[-2:]
    scatter_kernel(m_size, fused, *refs)


def adam_kernel(per, *refs):
    count = len(refs) - 7
    grads, (weight, one, two), outs = refs[:count], refs[count : count + 3], refs[count + 3 :]
    cols = weight.shape[2]
    for j in range(weight.shape[1]):
        g = grads[j // per][0, :, (j % per) * cols : (j % per + 1) * cols].astype(f32)
        w_new, one_new, two_new = adam_step(weight[:, j, :], g, one[:, j, :], two[:, j, :])
        for ref, value in zip(outs, (g, w_new, one_new, two_new)):
            ref[:, j, :] = value


def adam_update(grads, per, weight, one, two):
    rows, kinds, width = weight.shape
    cols = width // Z
    spec = pl.BlockSpec((rows, kinds, cols), lambda q: (0, 0, q))
    return pl.pallas_call(
        functools.partial(adam_kernel, per),
        grid=(Z,),
        in_specs=[pl.BlockSpec((1, rows, per * cols), lambda q: (q, 0, 0))] * len(grads) + [spec] * 3,
        out_specs=[spec] * 4,
        out_shape=[jax.ShapeDtypeStruct(weight.shape, f32)] * 4,
        name="adam_update",
    )(*grads, weight, one, two)


def body(
    block_in,
    positions,
    out_grad,
    attn_weight,
    mlp_weight,
    small_params,
    attn_first,
    attn_second,
    mlp_first,
    mlp_second,
    small_first,
    small_second,
):
    grid = Grid(lax.axis_size("dp"), lax.axis_size("tensor"))
    z, m, c, t, diag = grid.z_now, grid.m_now, grid.c_now, grid.t_now, grid.diag
    devices = grid.dp * 2
    rows, width = block_in.shape
    seq = 2 * rows
    part = small_params.shape[1]

    normed, inverse = layer_stats(block_in)
    x_low, g_low = normed.astype(bf16), out_grad.astype(bf16)

    pieces = split_weights(attn_weight, mlp_weight)
    tile = -(-12 * part // 1024) * 1024
    small_tile = jnp.concatenate(
        [small_params.reshape(-1), jnp.zeros((tile - 12 * part,), f32), positions[0].astype(f32)]
        + [jnp.zeros((1024 - seq,), f32)]
    ).reshape(-1, 128)
    weights, acts, table = gather(pieces, jnp.stack([x_low, g_low]), small_tile, grid.m)
    w_qk, w_vo, w_up, w_dn = weights
    everyone = jnp.take(table.reshape(devices, -1), jnp.array(table_order(grid.m)), axis=0)
    small_all = jnp.transpose(everyone[:, : 12 * part].reshape(devices, 12, part), (1, 0, 2)).reshape(12, width)
    group = (jnp.arange(Z) * grid.m + m) * 4 + t * 2
    places = jnp.take(everyone[:, tile : tile + seq], group, axis=0)
    par = small_all[:4]
    head = c * Z + z
    hidden = w_up.shape[1]
    head_bias = lax.dynamic_slice_in_dim(small_all[4:6], head * HEAD_DIM, HEAD_DIM, axis=1)
    up_bias = lax.dynamic_slice_in_dim(small_all[8:12].reshape(1, -1), head * hidden, hidden, axis=1)

    one_low, attended, d_attn, head_sums = run_attention(acts, w_qk, w_vo, par, head_bias, places)
    two_low, activation, d_pre, up_sums = run_hidden(acts, w_up, w_dn, par, up_bias)
    keep, give, norm_sums = run_outs(diag, attended, d_attn, activation, d_pre, acts, weights, par)
    factors = (one_low, two_low, acts, attended, d_attn, activation, d_pre)

    spread_cols = lambda v, n: lax.dynamic_update_slice_in_dim(
        jnp.zeros((n,), f32), v, head * v.shape[0], 0
    )
    out_sum = jnp.sum(out_grad, axis=0)
    small_terms = jnp.concatenate(
        [
            norm_sums,
            spread_cols(head_sums[0], width)[None],
            spread_cols(head_sums[1], width)[None],
            out_sum[None],
            out_sum[None],
            spread_cols(up_sums[0], 4 * width).reshape(4, width),
        ],
        axis=0,
    )
    terms = jnp.transpose(small_terms.reshape(12, devices, part), (1, 0, 2)).reshape(devices, 12 * part)
    places_of = table_order(grid.m)
    terms = jnp.take(terms, jnp.array([places_of.index(i) for i in range(devices)]), axis=0)
    terms = jnp.pad(terms, ((0, 0), (0, tile - 12 * part))).reshape(devices, -1, 128)
    own, own_rows, own_small = scatter(factors, keep, give, terms, grid.m, rows)
    y_rows, u_rows = own_rows[0].astype(f32), own_rows[1].astype(f32)
    block_out = block_in + y_rows + small_all[6] + small_all[7]
    input_grad = out_grad + inverse * (
        u_rows
        - jnp.mean(u_rows, axis=-1, keepdims=True)
        - normed * jnp.mean(u_rows * normed, axis=-1, keepdims=True)
    )
    attn_out = adam_update(own[:2], 2, attn_weight, attn_first, attn_second)
    mlp_out = adam_update(own[2:], 1, mlp_weight, mlp_first, mlp_second)
    small_grad = own_small.reshape(-1)[: 12 * part].reshape(12, part)
    small_new, small_first_new, small_second_new = adam_step(small_params, small_grad, small_first, small_second)

    attn_grad, attn_new, attn_first_new, attn_second_new = attn_out
    mlp_grad, mlp_new, mlp_first_new, mlp_second_new = mlp_out
    return (
        block_out,
        input_grad,
        attn_grad,
        mlp_grad,
        small_grad,
        attn_new,
        attn_first_new,
        attn_second_new,
        mlp_new,
        mlp_first_new,
        mlp_second_new,
        small_new,
        small_first_new,
        small_second_new,
    )


def solution(mesh):
    rows = P(("dp", "tensor"), None)
    weights = P("dp", None, "tensor")
    small = P(None, ("dp", "tensor"))
    return jax.shard_map(
        body,
        mesh=mesh,
        in_specs=(rows, P("dp", None), rows, weights, weights, small, weights, weights, weights, weights, small, small),
        out_specs=(rows, rows) + (weights,) * 2 + (small,) + (weights,) * 6 + (small,) * 3,
        check_vma=False,
    )
```

```python
import functools

import jax
import jax.numpy as jnp
from jax import lax
from jax.experimental import pallas as pl
from jax.experimental.pallas import tpu as pltpu
from jax.sharding import PartitionSpec as P

ROT = 64
ADAM_STEP = 3
HEAD_DIM = 256
Z = 4

norm_epsilon = 1e-05
learn_rate = 0.006
beta_first = 0.9
beta_second = 0.95
adam_epsilon = 1e-08
weight_decay = 0.1

f32 = jnp.float32
bf16 = jnp.bfloat16


def layer_stats(row_data):
    center = row_data - jnp.mean(row_data, axis=-1, keepdims=True)
    inverse = lax.rsqrt(jnp.mean(center * center, axis=-1, keepdims=True) + norm_epsilon)
    return (center * inverse, inverse)


def adam_step(weight, gradient, moment_one, moment_two):
    one_new = beta_first * moment_one + (1.0 - beta_first) * gradient
    two_new = beta_second * moment_two + (1.0 - beta_second) * gradient * gradient
    corrected = (
        one_new
        / (1.0 - beta_first**ADAM_STEP)
        / (jnp.sqrt(two_new / (1.0 - beta_second**ADAM_STEP)) + adam_epsilon)
    )
    return (weight - learn_rate * (corrected + weight_decay * weight), one_new, two_new)


class Grid:
    def __init__(self, dp, tensor):
        assert tensor == 2 and dp % (2 * Z) == 0
        self.dp, self.m = dp, dp // (2 * Z)
        index = lax.axis_index("dp")
        self.index = index * 2 + lax.axis_index("tensor")
        self.z_now = index // (2 * self.m)
        self.m_now = (index // 2) % self.m
        self.c_now = index % 2
        self.t_now = lax.axis_index("tensor")
        self.diag = self.c_now == self.t_now


def prepare_kernel(rows, cotangent, attn, mlp, qk, vo, up, dn, low):
    normed, _ = layer_stats(rows[...])
    low[0] = normed.astype(bf16)
    low[1] = cotangent[...].astype(bf16)
    quarter_a = attn.shape[2] // Z
    quarter_m = mlp.shape[2] // Z
    for q in range(Z):
        for j in range(4):
            block = attn[:, j, q * quarter_a : (q + 1) * quarter_a].astype(bf16)
            (qk, qk, vo, vo)[j][q, :, (j % 2) * quarter_a : (j % 2 + 1) * quarter_a] = block
        for j in range(2):
            (up, dn)[j][q] = mlp[:, j, q * quarter_m : (q + 1) * quarter_m].astype(bf16)


def prepare(block_in, out_grad, attn_weight, mlp_weight):
    own, width = block_in.shape
    rows, _, half = attn_weight.shape
    hidden = mlp_weight.shape[2]
    step = min(rows, 16)
    steps = rows // step
    shapes = [2 * half // Z] * 2 + [hidden // Z] * 2
    by_rows = pl.BlockSpec((own // steps, width), lambda i: (i, 0))
    outs = pl.pallas_call(
        prepare_kernel,
        grid=(steps,),
        in_specs=[
            by_rows,
            by_rows,
            pl.BlockSpec((step, 4, half), lambda i: (i, 0, 0)),
            pl.BlockSpec((step, 2, hidden), lambda i: (i, 0, 0)),
        ],
        out_specs=[pl.BlockSpec((Z, step, n), lambda i: (0, i, 0)) for n in shapes]
        + [pl.BlockSpec((2, own // steps, width), lambda i: (0, i, 0))],
        out_shape=[jax.ShapeDtypeStruct((Z, rows, n), bf16) for n in shapes]
        + [jax.ShapeDtypeStruct((2, own, width), bf16)],
        name="prepare",
    )(block_in, out_grad, attn_weight, mlp_weight)
    return outs[:4], outs[4]


MESH = pl.DeviceIdType.MESH
PARTS = (1, 1, 2, 2)
CHUNKS = ((0, 0, True), (1, 0, False), (2, 0, True), (2, 1, False), (3, 0, True), (3, 1, False))
GATHER_ORDER = {
    (False, False): (
        0, 10, 500, 510, 520, 530, 540, 550, 700, 20, 1100, 600, 501, 900, 620, 511, 910, 640, 601, 1101, 801, 1110,
        521, 710, 30, 40, 50, 502, 621, 512, 602, 610, 1010, 630, 811, 1111, 920, 1030, 650, 531, 1000, 541, 551,
        1050, 1020, 641, 611, 930, 1040, 1001, 802, 1011, 522, 1120, 940, 503, 1021, 622, 513, 612, 603, 1002, 1012,
        631, 651, 812, 1121, 1041, 1031, 532, 1051, 542, 1022, 552, 642, 1003, 632, 613, 652, 803, 1042, 1032, 523,
        1013, 1200, 1052, 1130, 1201, 623, 1202, 1023, 813, 1131, 1203, 533, 1204, 543, 1205, 553, 633, 643, 653,
        1043, 1033, 1206, 1207, 1053, 1208, 1209, 1210, 1211,
    ),
    (False, True): (
        0, 10, 700, 20, 500, 510, 520, 530, 540, 550, 610, 630, 650, 501, 600, 1100, 900, 1000, 511, 620, 1020, 611,
        640, 1040, 710, 30, 40, 50, 1010, 1030, 801, 1050, 601, 1001, 521, 910, 1110, 1011, 502, 1101, 621, 1021,
        602, 1002, 811, 531, 541, 1111, 930, 631, 551, 641, 512, 612, 940, 651, 1031, 1041, 920, 1012, 802, 522,
        1120, 1051, 503, 622, 1022, 603, 1003, 812, 532, 542, 1121, 632, 552, 642, 513, 613, 652, 1032, 1042, 1013,
        1200, 1052, 1201, 803, 1202, 523, 1130, 623, 1023, 813, 533, 1131, 1203, 543, 1204, 633, 553, 1205, 643, 653,
        1043, 1033, 1206, 1207, 1208, 1053, 1209, 1210, 1211,
    ),
    (True, False): (
        0, 10, 500, 510, 520, 530, 540, 550, 900, 700, 20, 1100, 600, 200, 503, 620, 100, 300, 640, 501, 513, 603,
        210, 310, 1101, 601, 110, 511, 710, 30, 40, 50, 803, 523, 1130, 610, 801, 320, 623, 220, 400, 1110, 630,
        1010, 120, 502, 521, 410, 910, 650, 512, 1030, 1000, 602, 621, 1050, 1020, 1131, 811, 1040, 813, 230, 1111,
        533, 130, 920, 613, 330, 531, 1003, 543, 240, 1001, 1013, 340, 140, 611, 553, 643, 541, 350, 250, 1023, 150,
        1011, 551, 641, 930, 802, 612, 420, 1120, 1002, 940, 522, 1021, 1012, 1200, 633, 622, 631, 1201, 1202, 653,
        1043, 1033, 1031, 812, 651, 430, 1121, 1203, 532, 1022, 1041, 1053, 1204, 1051, 440, 1205, 542, 632, 450,
        552, 642, 1032, 1206, 652, 1207, 1042, 1208, 1052, 1209, 1210, 1211,
    ),
    (True, True): (
        0, 10, 700, 20, 500, 510, 520, 530, 540, 550, 900, 610, 630, 650, 600, 200, 503, 1100, 1000, 620, 100, 300,
        1020, 640, 501, 513, 1040, 710, 30, 613, 40, 50, 210, 310, 1010, 110, 1030, 511, 611, 1050, 603, 1003, 601,
        1001, 803, 1101, 1013, 523, 1130, 801, 320, 1011, 220, 400, 1110, 623, 1023, 120, 502, 521, 910, 602, 621,
        1002, 813, 1021, 533, 811, 330, 230, 1111, 543, 1131, 130, 633, 930, 340, 531, 643, 631, 553, 240, 350, 140,
        1033, 410, 541, 940, 653, 1043, 512, 612, 250, 1031, 150, 641, 551, 651, 920, 1053, 1041, 802, 1012, 1200,
        420, 1120, 1201, 522, 1051, 1202, 622, 1022, 812, 430, 1121, 1203, 532, 1204, 632, 440, 1205, 542, 450, 1032,
        1206, 552, 642, 1207, 652, 1042, 1208, 1209, 1052, 1210, 1211,
    ),
}
SCATTER_ORDER = {
    (False, False): (
        30, 31, 20, 21, 10, 11, 0, 1, 131, 530, 531, 520, 521, 510, 511, 500, 501, 1600, 203, 413, 223, 433, 243,
        453, 121, 1610, 202, 412, 222, 432, 242, 452, 111, 903, 1620, 201, 411, 221, 431, 241, 451, 101, 923, 943,
        1630, 200, 410, 220, 430, 240, 450, 130, 902, 1013, 1033, 303, 323, 922, 343, 120, 942, 1053, 302, 322, 342,
        110, 901, 1012, 921, 301, 321, 341, 100, 941, 300, 320, 340, 1032, 900, 920, 800, 1052, 940, 1113, 1133,
        1011, 1103, 810, 1031, 1051, 1153, 1123, 1143, 1640, 1010, 1112, 1030, 1050, 1102, 1122, 1142, 1101, 1132,
        1121, 1152, 1141, 1111, 1100, 1120, 1140, 1131, 1151, 1110, 1130, 1150,
    ),
    (False, True): (
        30, 31, 20, 21, 10, 11, 0, 1, 131, 530, 531, 520, 521, 510, 511, 500, 501, 1600, 203, 413, 223, 433, 243,
        453, 121, 1610, 903, 202, 412, 222, 432, 242, 452, 111, 923, 201, 411, 221, 431, 241, 451, 101, 943, 1620,
        200, 410, 220, 430, 240, 450, 130, 902, 1013, 922, 1033, 1630, 303, 323, 343, 120, 942, 1053, 901, 302, 322,
        342, 110, 921, 301, 321, 341, 100, 1012, 941, 300, 320, 340, 900, 920, 1032, 940, 800, 1113, 1052, 1133,
        1103, 1123, 810, 1011, 1031, 1153, 1051, 1143, 1640, 1010, 1112, 1030, 1050, 1102, 1122, 1142, 1132, 1101,
        1152, 1121, 1111, 1141, 1100, 1120, 1131, 1140, 1151, 1110, 1130, 1150,
    ),
    (True, False): (
        30, 31, 20, 21, 10, 11, 0, 1, 131, 530, 531, 520, 521, 510, 511, 500, 501, 1600, 203, 413, 223, 433, 243,
        453, 121, 1610, 202, 412, 222, 432, 242, 452, 111, 620, 903, 923, 1620, 201, 411, 221, 431, 241, 451, 101,
        943, 200, 410, 220, 430, 240, 450, 130, 902, 1013, 621, 922, 1033, 303, 323, 343, 1053, 120, 700, 901, 942,
        302, 322, 342, 110, 1012, 630, 921, 941, 301, 321, 341, 100, 710, 900, 920, 1032, 300, 320, 340, 1052, 940,
        631, 1113, 1133, 1103, 1011, 1123, 800, 1031, 1153, 1051, 1143, 810, 1630, 1310, 1112, 1010, 1330, 1300,
        1640, 1030, 1350, 1510, 1320, 1410, 1050, 1340, 1530, 1102, 1132, 1210, 1500, 1122, 1550, 1200, 1101, 1520,
        1220, 1142, 1540, 1240, 1121, 1152, 1400, 1141, 1111, 1430, 1230, 1100, 1131, 1120, 1151, 1420, 1250, 1140,
        1110, 1440, 1130, 1150, 1450,
    ),
    (True, True): (
        30, 31, 20, 21, 10, 11, 0, 1, 131, 530, 531, 520, 521, 510, 511, 500, 501, 1600, 203, 413, 223, 433, 243,
        453, 121, 1610, 903, 202, 412, 222, 432, 242, 452, 111, 620, 923, 201, 411, 221, 431, 241, 451, 101, 943,
        1620, 902, 200, 410, 220, 430, 240, 450, 130, 1013, 621, 922, 1033, 942, 1053, 303, 323, 343, 120, 700, 901,
        921, 302, 322, 342, 110, 630, 1012, 941, 900, 301, 321, 341, 100, 710, 920, 1032, 940, 300, 320, 340, 1113,
        1052, 631, 1133, 1103, 1123, 1011, 800, 1153, 1031, 1051, 1143, 810, 1630, 1112, 1102, 1310, 1330, 1010,
        1300, 1640, 1320, 1410, 1030, 1350, 1400, 1340, 1510, 1132, 1050, 1210, 1530, 1122, 1500, 1200, 1142, 1520,
        1220, 1101, 1550, 1240, 1152, 1121, 1540, 1230, 1111, 1141, 1430, 1131, 1100, 1250, 1151, 1120, 1420, 1140,
        1440, 1110, 1130, 1150, 1450,
    ),
}


class Links:
    def __init__(self, m_size):
        self.m_size = m_size
        index = lax.axis_index("dp")
        self.z, self.m, self.c = index // (2 * m_size), (index // 2) % m_size, index % 2
        self.t = lax.axis_index("tensor")
        self.sends = []

    def to(self, z=None, m=None, c=None, t=None):
        z, m, c = (own if v is None else v for v, own in ((z, self.z), (m, self.m), (c, self.c)))
        return ((z * self.m_size + m) * 2 + c, self.t if t is None else t)

    def copy(self, src, dst, send_sem, recv_sem, target):
        return pltpu.make_async_remote_copy(
            src_ref=src, dst_ref=dst, send_sem=send_sem, recv_sem=recv_sem, device_id=target, device_id_type=MESH
        )

    def send(self, src, dst, send_sem, recv_sem, target):
        one = self.copy(src, dst, send_sem, recv_sem, target)
        one.start()
        self.sends.append(one)

    def landed(self, dst, recv_sem):
        self.copy(dst, dst, recv_sem, recv_sem, self.to(c=1 - self.c)).wait_recv()

    def drain(self):
        for one in self.sends:
            one.wait_send()
        self.sends = []

    def partners(self):
        other = 1 - self.t
        out = [self.to(z=self.z ^ k) for k in range(1, Z)]
        out += [self.to(m=self.m ^ j) for j in range(1, self.m_size)]
        out += [self.to(c=1 - self.c), self.to(t=other), self.to(c=1 - self.c, t=other)]
        return out

    def doubling(self):
        high = self.z // 2
        place = ((self.m * 2 + self.c) * 2 + self.t) * 4 + lax.rem(self.z + high, 2) * 2 + high
        steps = [(1, self.to(z=self.z ^ 3)), (2, self.to(z=self.z ^ 1)), (4, self.to(t=1 - self.t))]
        steps.append((8, self.to(c=1 - self.c)))
        j = 1
        while j < self.m_size:
            steps.append((16 * j, self.to(m=self.m ^ j)))
            j *= 2
        return place, steps

    def meet(self):
        barrier = pltpu.get_barrier_semaphore()
        everyone = self.partners()
        for target in everyone:
            pl.semaphore_signal(barrier, inc=1, device_id=target, device_id_type=MESH)
        pl.semaphore_wait(barrier, len(everyone))


def gather_kernel(m_size, *refs):
    pieces, low, mine_small, base = refs[:4], refs[4], refs[5], refs[6]
    full, act_out, one_out, two_out = refs[7:11], refs[11], refs[12], refs[13]
    att, d_attn, hidden_out, d_pre, head_sums, up_sums, table = refs[14:21]
    count = len(CHUNKS)
    stage, stage_m, relay = (refs[21 + i * count : 21 + (i + 1) * count] for i in range(3))
    refs = refs[21 + 3 * count :]
    (zs, zr, gs, gr, ps, pr, ms, mr, near_s, far_s, xr, as_, ar, ws, wr, ss, sr, lin, lout, ls, os_) = refs[:21]
    bounce, refs = refs[21 : 21 + count], refs[21 + count :]
    act, w_qk, w_vo, one_v, two_v, tile_v, slope, par, bias, up_bias = refs
    net = Links(m_size)
    z, m, c, t = net.z, net.m, net.c, net.t
    rows = pieces[0].shape[1]
    half = low.shape[1]
    seq = 2 * half
    width = low.shape[2]
    n = HEAD_DIM
    role = lax.rem(c + t, 2)
    inner_z = lax.rem(z + z // 2, 2)

    def columns(ch):
        array, part, _ = CHUNKS[ch]
        wide = pieces[array].shape[2] // PARTS[array]
        return array, slice(part * wide, (part + 1) * wide)

    def piece(ch, zz):
        array, cols = columns(ch)
        return pieces[array].at[zz, :, cols]

    def whole(ch, zz, mm, cc, size=1):
        array, cols = columns(ch)
        start = ((zz * m_size + mm) * 2 + cc) * rows
        return full[array].at[pl.ds(pl.multiple_of(start, rows), size * rows), cols]

    own_place = pl.ds(pl.multiple_of(z * seq + t * half, half), half)
    place = lambda zz, h: pl.ds(pl.multiple_of(zz * seq + (t ^ h) * half, half), half)

    def load_own(ch):
        return pltpu.make_async_copy(piece(ch, z), bounce[ch], lin.at[ch])

    def store_own(ch):
        return pltpu.make_async_copy(bounce[ch], whole(ch, z, m, c), lout.at[ch])

    def low_own():
        return pltpu.make_async_copy(low.at[0], act.at[0, own_place], lin.at[count])

    @pl.when(role == 0)
    def _():
        for ch in range(count):
            load_own(ch).start()
        low_own().start()

    flat, steps = net.doubling()
    pltpu.make_async_copy(mine_small, table.at[flat], ss.at[len(steps)]).start()
    net.meet()
    pltpu.make_async_copy(mine_small, table.at[flat], ss.at[len(steps)]).wait()

    def program(inner, diag):
        state = {"small": 0}
        sent = []

        def send(parts):
            net.copy(*parts()).start()
            sent.append(parts)

        def small_send():
            i = state["small"]
            if i < len(steps):
                size, target = steps[i]

                def parts():
                    span = table.at[pl.ds(flat // size * size, size)]
                    return span, span, ss.at[i], sr.at[i], target

                send(parts)

        def small_next(*_):
            i = state["small"]
            if i < len(steps):
                size = steps[i][0]
                net.landed(table.at[pl.ds((flat // size ^ 1) * size, size)], sr.at[i])
                state["small"] += 1
                small_send()

        def small_last():
            while state["small"] < len(steps):
                small_next()

        def spot(ch, zz, j):
            if diag:
                return whole(ch, zz, m ^ j, c)
            return stage_m[ch].at[m ^ j, zz] if j else stage[ch].at[zz]

        def source(ch, k, j):
            return piece(ch, z) if k == 0 and j == 0 else spot(ch, z ^ k, j)

        def spread(ch, k, j):
            block = lambda: whole(ch, z ^ k, m ^ j, c)
            send(
                lambda: (
                    source(ch, k, j),
                    block(),
                    ps.at[ch, j, k, 1],
                    pr.at[ch, j, k, c],
                    net.to(c=t, t=1 - t),
                )
            )
            if not diag:
                send(
                    lambda: (source(ch, k, j), block(), ps.at[ch, j, k, 0], pr.at[ch, j, k, c], net.to(c=1 - c))
                )

        def spread_landed(ch, k, j):
            for cc in (1 - c,) if diag else (1 - c, c):
                net.landed(whole(ch, z ^ k, m ^ j, cc), pr.at[ch, j, k, cc])

        def swap(h, k):
            def parts():
                src = act.at[role, place(z ^ k, h)]
                return src, src, ws.at[k, h], wr.at[k, h], net.to(c=1 - c)

            send(parts)

        def rows_on(h, flip, i, hop, k):
            def parts():
                src = act.at[role, place(z ^ flip, h)]
                return src, src, as_.at[h, i], ar.at[h, k], net.to(z=z ^ hop)

            send(parts)

        def quarters(ch, _):
            for i, (k, hop, through) in enumerate(
                ((3, 3, None), (2, 3, 2), (1, 1, None)) if inner else ((3, 1, 1), (2, 1, 0), (1, 1, None))
            ):

                def parts(i=i, k=k, hop=hop, through=through):
                    if through is None:
                        dst, recv_sem = spot(ch, z, 0), zr.at[ch, k]
                    else:
                        dst, recv_sem = relay[ch].at[through], gr.at[ch, through]
                    return piece(ch, z ^ k), dst, zs.at[ch, i], recv_sem, net.to(z=z ^ hop)

                send(parts)

        def pass_on(through):
            hop, k = ((3, 2), (3, None), (1, 2), (1, 3))[through]

            def run(ch, _):
                net.landed(relay[ch].at[through], gr.at[ch, through])

                def parts():
                    if k is None:
                        dst, recv_sem = relay[ch].at[3], gr.at[ch, 3]
                    else:
                        dst, recv_sem = spot(ch, z ^ hop ^ k, 0), zr.at[ch, k]
                    return relay[ch].at[through], dst, gs.at[ch, through], recv_sem, net.to(z=z ^ hop)

                send(parts)

            return run

        def first(ch, k):
            if k:
                net.landed(spot(ch, z ^ k, 0), zr.at[ch, k])
            if CHUNKS[ch][2]:
                for j in range(1, m_size):

                    def parts(j=j):
                        dst = whole(ch, z ^ k, m, c) if diag else stage_m[ch].at[m, z ^ k]
                        return source(ch, k, 0), dst, ms.at[ch, j, k], mr.at[ch, j, k], net.to(m=m ^ j)

                    send(parts)
            spread(ch, k, 0)

        def second(ch, k):
            if CHUNKS[ch][2]:
                for j in range(1, m_size):
                    net.landed(spot(ch, z ^ k, j), mr.at[ch, j, k])
                    spread(ch, k, j)
            else:
                if diag and k == 0:
                    store_own(ch).wait()
                spread_landed(ch, k, 0)
                for j in range(1, m_size):

                    def parts(j=j):
                        both = whole(ch, z ^ k, m, 0, 2)
                        return both, both, ms.at[ch, j, k], mr.at[ch, j, k], net.to(m=m ^ j)

                    send(parts)

        def third(ch, k):
            if CHUNKS[ch][2]:
                for j in range(m_size):
                    spread_landed(ch, k, j)
                if diag and k == 0:
                    store_own(ch).wait()
            else:
                for j in range(1, m_size):
                    net.landed(whole(ch, z ^ k, m ^ j, 0, 2), mr.at[ch, j, k])

        def rows_start(h, _):
            if h:
                net.landed(act.at[0 if diag else 1, place(z, 1)], xr.at[1])
            elif diag:
                low_own().wait()
            else:
                net.landed(act.at[1, place(z, 0)], xr.at[0])
            if inner:
                rows_on(h, 0, 0, 3, 3)
            rows_on(h, 0, 1, 1, 1)
            swap(h, 0)

        def rows_next(h, k):
            net.landed(act.at[role, place(z ^ k, h)], ar.at[h, k])
            if inner:
                hop, there = {1: (3, 2), 3: (1, 2), 2: (1, 3)}[k]
                rows_on(h, k, 1 + k, hop, there)
            swap(h, k)

        def swapped(k, h):
            net.landed(act.at[1 - role, place(z ^ k, h)], wr.at[k, h])

        def begin():
            small_send()
            if diag:
                send(lambda: (low.at[1], act.at[1, own_place], near_s, xr.at[0], net.to(c=1 - c)))
                for ch in range(count):
                    load_own(ch).wait()
                    store_own(ch).start()
            else:
                send(lambda: (low.at[0], act.at[0, own_place], near_s, xr.at[1], net.to(t=1 - t)))
                send(lambda: (low.at[1], act.at[1, own_place], far_s, xr.at[1], net.to(c=1 - c, t=1 - t)))

        runs = [quarters] + [pass_on(i) for i in range(4)]
        runs += [first, second, rows_start, rows_next, small_next, third, swapped]

        def run(codes):
            for code in codes:
                runs[code // 100](code // 10 % 10, code % 10)

        def end():
            for parts in sent:
                net.copy(*parts()).wait_send()

        return begin, run, small_last, end

    programs = {key: program(*key) for key in GATHER_ORDER}
    work = len(runs_before(GATHER_ORDER[True, True]))

    def device_rows(index):
        zz, rest = index // (4 * m_size), lax.rem(index, 4 * m_size)
        return rest * 4 + lax.rem(zz + zz // 2, 2) * 2 + zz // 2

    def parameters():
        part = width // (8 * m_size * 2)
        per = 128 // part
        static = table_order(m_size)
        for b in range(width // 128):
            got = [table[static[b * per + e], 0:4, 0:part] for e in range(per)]
            par[:, b * 128 : (b + 1) * 128] = jnp.concatenate(got, axis=1)
        head = c * Z + z
        for b in range(n // 128):
            start = (head * n + b * 128) // part
            got = [table[device_rows(start + e), 4:6, 0:part] for e in range(per)]
            bias[:, b * 128 : (b + 1) * 128] = jnp.concatenate(got, axis=1)
        wide = up_bias.shape[1]
        row = 8 + head * wide // width
        for b in range(wide // 128):
            start = (lax.rem(head * wide, width) + b * 128) // part
            got = [table[device_rows(start + e), pl.ds(row, 1), 0:part] for e in range(per)]
            up_bias[:, b * 128 : (b + 1) * 128] = jnp.concatenate(got, axis=1)

    def weights_in():
        return [
            pltpu.make_async_copy(full[0], w_qk, ls.at[0]),
            pltpu.make_async_copy(full[1], w_vo, ls.at[1]),
        ]

    def rows_saved(i):
        k = i ^ (inner_z & (i // 2))
        span = pl.ds(pl.multiple_of((z ^ k) * seq, seq), seq)
        return [
            pltpu.make_async_copy(one_v.at[lax.rem(i, 2)], one_out.at[span], os_.at[0, i]),
            pltpu.make_async_copy(two_v.at[span], two_out.at[span], os_.at[1, i]),
            pltpu.make_async_copy(act.at[:, span], act_out.at[:, span], os_.at[2, i]),
        ]

    def attention(i):
        @pl.when(i == 0)
        def _():
            for one in weights_in():
                one.start()
            parameters()
            head_sums[...] = jnp.zeros_like(head_sums)
            for one in weights_in():
                one.wait()

        @pl.when(i >= 2)
        def _():
            rows_saved(i - 2)[0].wait()

        k = i ^ (inner_z & (i // 2))
        span = pl.ds(pl.multiple_of((z ^ k) * seq, seq), seq)
        x = act[0, span, :].astype(f32)
        one = (x * par[0:1, :] + par[1:2, :]).astype(bf16)
        one_v[lax.rem(i, 2)] = one
        two_v[span, :] = (x * par[2:3, :] + par[3:4, :]).astype(bf16)
        for copy in rows_saved(i):
            copy.start()
        source = device_rows((((z ^ k) * m_size + m) * 2 + t) * 2)
        across = jnp.concatenate([table[source, 12 + e : 13 + e, :] for e in range(seq // 128)], axis=1)
        spots = lax.broadcasted_iota(jnp.int32, (seq, seq), 0).astype(f32)
        hit = jnp.where(spots == across, 1.0, 0.0).astype(bf16)
        down = dot(hit, spots.astype(bf16), 0, 0)
        turns = dot(hit, base[...], 0, 0)
        tables = [sum(turns[:, (3 * a + e) * 128 : (3 * a + e + 1) * 128] for e in range(3)) for a in range(3)]
        scale = HEAD_DIM ** (-0.5)
        qk = dot(one, w_qk[...])
        q = turn(qk[:, :n] + bias[0:1, :], tables, 1.0).astype(bf16)
        k_rows = turn(qk[:, n:], tables, 1.0).astype(bf16)
        v = (dot(one, w_vo[:, :n]) + bias[1:2, :]).astype(bf16)
        d_att = dot(act[1, span, :], w_vo[:, n:]).astype(bf16)
        scores = jnp.where(across <= down, dot(q, k_rows, 1, 1) * scale, -jnp.inf)
        top = jnp.max(scores, axis=-1, keepdims=True)
        log_total = top + jnp.log(jnp.sum(jnp.exp(scores - top), axis=-1, keepdims=True))
        probs = jnp.exp(scores - log_total)
        low_probs = probs.astype(bf16)
        att[span, :] = dot(low_probs, v).astype(bf16)
        d_probs = dot(d_att, v, 1, 1)
        d_scores = (probs * (d_probs - jnp.sum(probs * d_probs, axis=-1, keepdims=True)) * scale).astype(bf16)
        d_q = turn(dot(d_scores, k_rows), tables, -1.0)
        d_k = turn(dot(d_scores, q, 0, 0), tables, -1.0)
        d_v = dot(low_probs, d_att, 0, 0)
        d_attn[span, 0:n] = d_q.astype(bf16)
        d_attn[span, n : 2 * n] = d_k.astype(bf16)
        d_attn[span, 2 * n :] = d_v.astype(bf16)
        head_sums[0:1, :] += jnp.sum(d_q, axis=0, keepdims=True)
        head_sums[1:2, :] += jnp.sum(d_v, axis=0, keepdims=True)

    wide = pieces[2].shape[2] // Z

    def tile_in(array, j):
        cols = pl.ds(pl.multiple_of(j * wide, wide), wide)
        return pltpu.make_async_copy(full[array].at[:, cols], tile_v.at[lax.rem(j, 2)], ls.at[lax.rem(j, 2)])

    def tile_ready(array, j):
        @pl.when(lax.rem(j, 2) == 0)
        def _():
            tile_in(array, j).start()
            tile_in(array, j + 1).start()

        tile_in(array, j).wait()

    def hidden(i):
        j = i - Z
        tile_ready(2, j)
        cols = pl.ds(pl.multiple_of(j * wide, wide), wide)
        pre = dot(two_v[...], tile_v[lax.rem(j, 2)]) + up_bias[:, cols]
        erf = 1.0 + lax.erf(pre * 0.7071067811865476)
        hidden_out[:, cols] = (0.5 * pre * erf).astype(bf16)
        slope[j] = 0.5 * erf + pre * jnp.exp(-0.5 * pre * pre) * 0.3989422804014327

    def hidden_back(i):
        j = i - 2 * Z
        tile_ready(3, j)
        cols = pl.ds(pl.multiple_of(j * wide, wide), wide)
        value = dot(act[1], tile_v[lax.rem(j, 2)]) * slope[j]
        d_pre[:, cols] = value.astype(bf16)
        up_sums[:, cols] = jnp.sum(value, axis=0, keepdims=True)

    def begin(inner, diag):
        start, run, small_last, _ = programs[inner, diag]
        start()
        run(runs_before(GATHER_ORDER[inner, diag])[0])
        small_last()

    def part(i, inner, diag):
        programs[inner, diag][1](runs_before(GATHER_ORDER[inner, diag])[i + 1])

    by_class(inner_z, role, begin)

    @pl.loop(0, work - 1)
    def _(i):
        pl.when(i < Z)(lambda: attention(i))
        pl.when((i >= Z) & (i < 2 * Z))(lambda: hidden(i))
        pl.when(i >= 2 * Z)(lambda: hidden_back(i))
        for e in range(work - 1):

            @pl.when(i == e)
            def _(e=e):
                by_class(inner_z, role, functools.partial(part, e))

    by_class(inner_z, role, lambda inner, diag: programs[inner, diag][3]())
    for i in range(Z):
        saved = rows_saved(i)
        for copy in saved[1:] if i < 2 else saved:
            copy.wait()


def runs_before(order):
    cuts = [i for i, code in enumerate(order) if code // 100 == 12]
    return [order[lo:hi] for lo, hi in zip([0] + [i + 1 for i in cuts], cuts + [len(order)])]


def turn_base(seq):
    terms = []
    for value in turn_tables(jnp.arange(seq).astype(f32)):
        for _ in range(3):
            low = lax.reduce_precision(value, 8, 7)
            terms.append(low.astype(bf16))
            value = value - low
    return jnp.concatenate(terms, axis=1)


def table_order(m_size):
    order = []
    for z in range(Z):
        for rest in range(4 * m_size):
            order.append(rest * 4 + (z + z // 2) % 2 * 2 + z // 2)
    return order


def by_class(inner_z, role, program):
    for inner in (False, True):
        for diag in (False, True):

            @pl.when((inner_z == int(inner)) & (role == int(not diag)))
            def _(inner=inner, diag=diag):
                program(inner, diag)


def gather(pieces, low, small, m_size):
    rows = pieces[0].shape[1]
    own, width = low.shape[1:]
    tokens = Z * 2 * own
    devices = m_size * 4 * Z
    cols = [p.shape[2] for p in pieces]
    count = len(CHUNKS)
    parts = [cols[array] // PARTS[array] for array, _, _ in CHUNKS]
    sem = pltpu.SemaphoreType.DMA
    doubling = m_size.bit_length() - 1 + 4
    in_place = pl.BlockSpec(memory_space=pl.ANY)
    in_vmem = pl.BlockSpec(memory_space=pltpu.VMEM)
    shape = lambda *dims: jax.ShapeDtypeStruct(dims, bf16)
    exact = lambda *dims: jax.ShapeDtypeStruct(dims, f32)
    hidden, n = cols[2], HEAD_DIM
    vmem = lambda *dims: pltpu.VMEM(dims, bf16)
    outs = pl.pallas_call(
        functools.partial(gather_kernel, m_size),
        out_shape=[shape(width, n) for n in cols]
        + [shape(2, tokens, width), shape(tokens, width), shape(tokens, width)]
        + [shape(tokens, n), shape(tokens, 3 * n), shape(tokens, hidden), shape(tokens, hidden)]
        + [exact(2, n), exact(1, hidden), exact(devices, *small.shape)]
        + [shape(Z, rows, n) for n in parts]
        + [shape(m_size, Z, rows, n) for n in parts]
        + [shape(4, rows, n) for n in parts],
        in_specs=[in_place] * 6 + [in_vmem],
        out_specs=[in_place] * 7 + [in_vmem] * 7 + [in_place] * (3 * count),
        scratch_shapes=[
            sem((count, 3)),
            sem((count, Z)),
            sem((count, 4)),
            sem((count, 4)),
            sem((count, m_size, Z, 2)),
            sem((count, m_size, Z, 2)),
            sem((count, m_size, Z)),
            sem((count, m_size, Z)),
            sem,
            sem,
            sem((2,)),
            sem((2, 5)),
            sem((2, Z)),
            sem((Z, 2)),
            sem((Z, 2)),
            sem((doubling + 1,)),
            sem((doubling,)),
            sem((count + 1,)),
            sem((count,)),
            sem((2,)),
            sem((3, Z)),
        ]
        + [vmem(rows, n) for n in parts]
        + [vmem(2, tokens, width), vmem(width, 2 * n), vmem(width, 2 * n), vmem(2, 2 * own, width)]
        + [vmem(tokens, width), vmem(2, width, hidden // Z), pltpu.VMEM((Z, tokens, hidden // Z), f32)]
        + [pltpu.VMEM((4, width), f32), pltpu.VMEM((2, n), f32), pltpu.VMEM((1, hidden), f32)],
        compiler_params=pltpu.CompilerParams(collective_id=0, has_side_effects=True, vmem_limit_bytes=67043328),
        name="gather_all",
    )(*pieces, low, small, turn_base(2 * own))
    return outs[:4], outs[4], outs[5:7], outs[7:11], outs[11:13], outs[13]


VMEM_BYTES = 60 * 1024 * 1024


def dot(a, b, over_a=1, over_b=0):
    return lax.dot_general(a, b, (((over_a,), (over_b,)), ((), ())), preferred_element_type=f32)


def turn(value, tables, sign):
    cos, low, high = tables
    part = value[:, :128]
    turned = part * cos + sign * (
        pltpu.roll(part, 128 - ROT // 2, 1) * low + pltpu.roll(part, ROT // 2, 1) * high
    )
    return jnp.concatenate([turned, value[:, 128:]], axis=1)


def turn_tables(places):
    half = ROT // 2
    column = jnp.arange(128)
    frequency = 10000.0 ** (-((column % half).astype(f32) * (2.0 / ROT)))
    angles = places.reshape(-1, 1) * frequency
    cos = jnp.where(column < ROT, jnp.cos(angles), 1.0)
    sin = jnp.sin(angles)
    return cos, jnp.where(column < half, -sin, 0.0), jnp.where((column >= half) & (column < ROT), sin, 0.0)


def fixed(*shape):
    return pl.BlockSpec(shape, lambda i: (0,) * len(shape))


def outs_kernel(flag, att, d_attn, act, d_pre, x, w_qk, w_vo, w_up, w_dn, par, keep, give, sums):
    diag = flag[0] == 1
    n = HEAD_DIM
    y = dot(att[...], w_vo[:, n:], 1, 1) + dot(act[...], w_dn[...], 1, 1)
    d_one = dot(d_attn[:, : 2 * n], w_qk[...], 1, 1) + dot(d_attn[:, 2 * n :], w_vo[:, :n], 1, 1)
    d_two = dot(d_pre[...], w_up[...], 1, 1)
    u = d_one * par[0:1, :] + d_two * par[2:3, :]
    keep[...] = jnp.where(diag, y, u).astype(bf16)
    give[...] = jnp.where(diag, u, y).astype(bf16)
    plain = x[...].astype(f32)
    for i, value in enumerate((d_one * plain, d_one, d_two * plain, d_two)):
        sums[i : i + 1, :] = jnp.sum(value, axis=0, keepdims=True)


def run_outs(diag, att, d_attn, act, d_pre, acts, weights, par):
    _, rows, width = acts.shape
    step = 256
    fix = lambda v: pl.BlockSpec(v.shape, lambda i, s: (0, 0), pipeline_mode=pl.Buffered(1))
    tile = lambda height: pl.BlockSpec((height, step), lambda i, s: (0, i))
    return pl.pallas_call(
        outs_kernel,
        grid_spec=pltpu.PrefetchScalarGridSpec(
            num_scalar_prefetch=1,
            grid=(width // step,),
            in_specs=[fix(v) for v in (att, d_attn, act, d_pre)]
            + [pl.BlockSpec((None, rows, step), lambda i, s: (0, 0, i))]
            + [pl.BlockSpec((step, v.shape[1]), lambda i, s: (i, 0)) for v in weights]
            + [tile(4)],
            out_specs=[tile(rows), tile(rows), tile(4)],
        ),
        out_shape=[jax.ShapeDtypeStruct((rows, width), bf16)] * 2 + [jax.ShapeDtypeStruct((4, width), f32)],
        compiler_params=pltpu.CompilerParams(vmem_limit_bytes=VMEM_BYTES),
        name="outputs",
    )(diag.astype(jnp.int32).reshape(1), att, d_attn, act, d_pre, acts, *weights, par)


def grads_kernel(one, two, g, att, d_attn, act, d_pre, qk, vo, up, dn):
    n = HEAD_DIM
    first = dot(one[...], d_attn[...], 0, 0)
    qk[...] = first[:, : 2 * n].astype(bf16)
    vo[:, :n] = first[:, 2 * n :].astype(bf16)
    vo[:, n:] = dot(g[...], att[...], 0, 0).astype(bf16)
    up[...] = dot(two[...], d_pre[...], 0, 0).astype(bf16)
    dn[...] = dot(g[...], act[...], 0, 0).astype(bf16)


def run_grads(one, two, acts, att, d_attn, act, d_pre):
    rows, width = one.shape
    step = 256
    tile = pl.BlockSpec((rows, step), lambda i: (0, i))
    fix = lambda v: pl.BlockSpec(v.shape, lambda i: (0, 0), pipeline_mode=pl.Buffered(1))
    cols = [2 * HEAD_DIM, 2 * HEAD_DIM, act.shape[1], act.shape[1]]
    return pl.pallas_call(
        grads_kernel,
        grid=(width // step,),
        in_specs=[tile, tile, pl.BlockSpec((None, rows, step), lambda i: (1, 0, i))]
        + [fix(v) for v in (att, d_attn, act, d_pre)],
        out_specs=[pl.BlockSpec((step, n), lambda i: (i, 0)) for n in cols],
        out_shape=[jax.ShapeDtypeStruct((width, n), bf16) for n in cols],
        compiler_params=pltpu.CompilerParams(vmem_limit_bytes=VMEM_BYTES),
        name="weight_grads",
    )(one, two, acts, att, d_attn, act, d_pre)


def add_rows(dst, sources):
    step = min(dst.shape[0], 32)

    @pl.loop(0, dst.shape[0] // step)
    def _(i):
        span = pl.ds(pl.multiple_of(i * step, step), step)
        total = sources[0][span, :].astype(f32)
        for one in sources[1:]:
            total = total + one[span, :].astype(f32)
        dst[span, :] = total.astype(dst.dtype)


def scatter_kernel(m_size, fused, *refs):
    if fused:
        ones, twos, acts, att, d_attn, act, d_pre = refs[:7]
        keep, give, terms = refs[7:10]
        grads, refs = refs[10:14], refs[14:]
    else:
        grads, (keep, give, terms), refs = refs[:4], refs[4:7], refs[7:]
    own, rows_out, small_out, refs = refs[:4], refs[4], refs[5], refs[6:]
    count = len(CHUNKS)
    buffers = []
    for _, _, m_first in CHUNKS:
        size = 5 if m_first else 6
        buffers.append(refs[:size])
        refs = refs[size:]
    relay, refs = refs[:count], refs[count:]
    got, kept, got_z, final, current, got_small = refs[:6]
    (gs, gr, kl, as_, ar, ys, yr, yl, ws, wr, wl, fs, fr, xs, xr, zs, zr, zl, ps, pr, ss, sr) = refs[6:28]
    if fused:
        tiles, made, tl, ml = refs[28:]
    net = Links(m_size)
    z, m, c, t = net.z, net.m, net.c, net.t
    half = rows_out.shape[1]
    role = lax.rem(c + t, 2)
    inner_z = lax.rem(z + z // 2, 2)
    flat, steps = net.doubling()
    steps = steps[::-1]

    def columns(ch):
        array, part, _ = CHUNKS[ch]
        wide = own[array].shape[2] // PARTS[array]
        return array, slice(part * wide, (part + 1) * wide)

    def rows_of(ch, k, j, cc=None):
        array, cols = columns(ch)
        if cc is None:
            return grads[array].at[z ^ k, m ^ j, :, :, cols]
        return grads[array].at[z ^ k, m ^ j, cc, :, cols]

    def owned(ch, zz):
        array, cols = columns(ch)
        return own[array].at[zz, :, cols]

    span = lambda h: pl.ds(pl.multiple_of((t ^ h) * half, half), half)
    loads_keep = [pltpu.make_async_copy(keep.at[z ^ k], kept.at[k], kl.at[k]) for k in range(Z)]
    for one in loads_keep:
        one.start()
    current[...] = terms[...]

    def tile_loads(i, slot):
        block = (z ^ (Z - 1 - lax.rem(i, Z))) * m_size + (m ^ (1 - i // Z))
        wide = tiles.shape[3]
        cols = pl.ds(pl.multiple_of(block * wide, wide), wide)
        sources = (ones.at[:, cols], twos.at[:, cols], acts.at[1, :, cols])
        return [pltpu.make_async_copy(src, tiles.at[slot, n], tl.at[slot, n]) for n, src in enumerate(sources)]

    def make(i):
        slot = lax.rem(i, 2)

        @pl.when(i < 2 * Z - 1)
        def _():
            for one in tile_loads(i + 1, 1 - slot):
                one.start()

        for one in tile_loads(i, slot):
            one.wait()
        n = HEAD_DIM
        high = made[0].shape[1]
        for array, at, left, right, lo, hi in (
            (0, 0, 0, d_attn, 0, 2 * n),
            (1, 0, 0, d_attn, 2 * n, 3 * n),
            (1, n, 2, att, 0, n),
            (2, 0, 1, d_pre, 0, d_pre.shape[1]),
            (3, 0, 2, act, 0, act.shape[1]),
        ):
            value = dot(tiles[slot, left], right[:, lo:hi], 0, 0).astype(bf16)
            for cc in range(2):
                made[array][cc, :, at : at + hi - lo] = value[cc * high : (cc + 1) * high]
        stores = [
            pltpu.make_async_copy(
                made[array], grads[array].at[z ^ (Z - 1 - lax.rem(i, Z)), m ^ (1 - i // Z)], ml.at[array]
            )
            for array in range(4)
        ]
        for one in stores:
            one.start()
        for one in stores:
            one.wait()

    if fused:
        for one in tile_loads(0, 0):
            one.start()
    net.meet()

    def program(inner, diag):
        state = {"small": 0}
        sent = []

        def send(*parts):
            (parts,) = parts
            net.copy(*parts()).start()
            sent.append(parts)

        def small_send():
            i = state["small"]
            if i < len(steps):
                size, target = steps[i]
                send(
                    lambda: (
                        current.at[pl.ds((flat // size ^ 1) * size, size)],
                        got_small.at[pl.ds(size, size)],
                        ss.at[i],
                        sr.at[i],
                        target,
                    )
                )

        def small_next(*_):
            i = state["small"]
            if i < len(steps):
                size = steps[i][0]
                net.landed(got_small.at[pl.ds(size, size)], sr.at[i])
                block = pl.ds(flat // size * size, size)
                current[block] = current[block] + got_small[pl.ds(size, size)]
                state["small"] += 1
                small_send()

        def swap(k, h):
            send(
                lambda: (give.at[z ^ k, span(h)], got.at[k, span(h)], gs.at[k, h], gr.at[k, h], net.to(c=1 - c))
            )

        def load_mine(ch, j, k):
            if CHUNKS[ch][2]:
                return pltpu.make_async_copy(rows_of(ch, k, j, c), buffers[ch][0].at[j, k], wl.at[ch, j, k])
            return pltpu.make_async_copy(rows_of(ch, k, 0), buffers[ch][0].at[k], wl.at[ch, 0, k])

        def load_made(k, own_m):
            for j in (0,) if own_m == 0 else range(1, m_size):
                for ch in range(count):
                    if (diag and CHUNKS[ch][2]) or (j == 0 and not CHUNKS[ch][2]):
                        load_mine(ch, j, k).start()

        def to_owner(source, home, far, ch, j, k):
            if diag:
                send(lambda: (source(1 - c), home(), ws.at[ch, j, k, 0], wr.at[ch, j, k, 0], net.to(c=1 - c)))
            else:
                send(lambda: (source(c), far(), ws.at[ch, j, k, 0], wr.at[ch, j, k, 1], net.to(t=1 - t)))
                send(
                    lambda: (source(1 - c), far(), ws.at[ch, j, k, 1], wr.at[ch, j, k, 1], net.to(c=1 - c, t=1 - t))
                )

        def owners_part(ch, j, k):
            home, far = buffers[ch][0], buffers[ch][1]
            to_owner(lambda cc: rows_of(ch, k, j, cc), lambda: home.at[j, k], lambda: far.at[j, k], ch, j, k)

        def others(ch, k):
            for j in range(1, m_size):
                owners_part(ch, j, k)

        def same(ch, k):
            owners_part(ch, 0, k)

        def across(ch, k):
            for j in range(1, m_size):
                send(
                    lambda j=j: (
                        rows_of(ch, k, j),
                        buffers[ch][1].at[j - 1, k],
                        fs.at[ch, j, k],
                        fr.at[ch, j, k],
                        net.to(m=m ^ j),
                    )
                )

        def collected(home, far, ch, j, k):
            if not diag:
                net.landed(home, wr.at[ch, j, k, 0])
            elif CHUNKS[ch][2]:
                load_mine(ch, j, k).wait()
            net.landed(far, wr.at[ch, j, k, 1])

        def middle(ch, k):
            home, far, mid, far_m, _ = buffers[ch]
            for j in range(1, m_size):
                collected(home.at[j, k], far.at[j, k], ch, j, k)
                add_rows(mid.at[j - 1, k], [home.at[j, k], far.at[j, k]])
                send(
                    lambda j=j: (
                        mid.at[j - 1, k],
                        far_m.at[j - 1, k],
                        xs.at[ch, j, k],
                        xr.at[ch, j, k],
                        net.to(m=m ^ j),
                    )
                )

        def summed(ch, k):
            mine, far_m, both, home, far, _ = buffers[ch]
            load_mine(ch, 0, k).wait()
            for j in range(1, m_size):
                net.landed(far_m.at[j - 1, k], fr.at[ch, j, k])
            for cc in range(2):
                add_rows(both.at[k, cc], [mine.at[k, cc]] + [far_m.at[j - 1, k, cc] for j in range(1, m_size)])
            to_owner(lambda cc: both.at[k, cc], lambda: home.at[k], lambda: far.at[k], ch, 0, k)

        def finish(ch, k):
            if CHUNKS[ch][2]:
                home, far, _, far_m, result = buffers[ch]
                collected(home.at[0, k], far.at[0, k], ch, 0, k)
                for j in range(1, m_size):
                    net.landed(far_m.at[j - 1, k], xr.at[ch, j, k])
                sources = [home.at[0, k], far.at[0, k]] + [far_m.at[j - 1, k] for j in range(1, m_size)]
            else:
                _, _, both, home, far, result = buffers[ch]
                collected(home.at[k], far.at[k], ch, 0, k)
                sources = [both.at[k, c] if diag else home.at[k], far.at[k]]
            add_rows(result.at[k], sources)
            if k == 0:
                pltpu.make_async_copy(result.at[k], owned(ch, z), zl.at[ch]).start()
                return
            hop, through = {1: (1, None), 2: (3, 2), 3: (3, None)}[k] if inner else {1: (1, None), 2: (1, 0), 3: (1, 1)}[k]
            if through is None:
                send(lambda: (result.at[k], owned(ch, z), zs.at[ch, k], zr.at[ch, k], net.to(z=z ^ hop)))
            else:
                send(
                    lambda: (
                        result.at[k],
                        relay[ch].at[through],
                        zs.at[ch, k],
                        pr.at[ch, through],
                        net.to(z=z ^ hop),
                    )
                )

        def pass_on(through):
            hop, k = ((3, 2), (3, None), (1, 2), (1, 3))[through]

            def run(ch, _):
                net.landed(relay[ch].at[through], pr.at[ch, through])

                def parts():
                    if k is None:
                        dst, recv_sem = relay[ch].at[3], pr.at[ch, 3]
                    else:
                        dst, recv_sem = owned(ch, z ^ hop ^ k), zr.at[ch, k]
                    return relay[ch].at[through], dst, ps.at[ch, through], recv_sem, net.to(z=z ^ hop)

                send(parts)

            return run

        def rows_first(k, h):
            if h == 0:
                pltpu.make_async_copy(keep.at[z ^ k], kept.at[k], kl.at[k]).wait()
            net.landed(got.at[k, span(h)], gr.at[k, h])
            add_rows(kept.at[k, span(h)], [kept.at[k, span(h)], got.at[k, span(h)]])
            if k and not inner:
                slot = {1: 0, 2: 1, 3: 2}[k]
                send(
                    lambda: (
                        kept.at[k, span(h)],
                        got_z.at[slot, span(h)],
                        as_.at[k, h],
                        ar.at[slot, h],
                        net.to(z=z ^ 1),
                    )
                )

        def rows_through(k, h, slot, there, hop):
            net.landed(got_z.at[slot, span(h)], ar.at[slot, h])
            add_rows(kept.at[k, span(h)], [kept.at[k, span(h)], got_z.at[slot, span(h)]])
            send(
                lambda: (
                    kept.at[k, span(h)],
                    got_z.at[there, span(h)],
                    as_.at[k, h],
                    ar.at[there, h],
                    net.to(z=z ^ hop),
                )
            )

        def rows_inner(k, h):
            rows_through(k, h, {3: 1, 2: 2}[k], {3: 3, 2: 4}[k], 3)

        def rows_outer(h, _):
            rows_through(1, h, 4, 0, 1)

        def rows_back(h, _):
            slots = (0, 3) if inner else (0,)
            for slot in slots:
                net.landed(got_z.at[slot, span(h)], ar.at[slot, h])
            add_rows(final.at[h], [kept.at[0, span(h)]] + [got_z.at[slot, span(h)] for slot in slots])
            if diag and h == 0:
                pltpu.make_async_copy(final.at[h], rows_out.at[0], yl).start()
            elif diag:
                send(lambda: (final.at[h], rows_out.at[0], ys.at[h], yr.at[0], net.to(t=1 - t)))
            elif h == 0:
                send(lambda: (final.at[h], rows_out.at[1], ys.at[h], yr.at[1], net.to(c=1 - c)))
            else:
                send(lambda: (final.at[h], rows_out.at[1], ys.at[h], yr.at[1], net.to(c=1 - c, t=1 - t)))

        runs = [swap, load_made, others, same, across, rows_first, rows_inner, rows_outer, rows_back]
        runs += [middle, summed, finish] + [pass_on(i) for i in range(4)] + [small_next]

        def run(codes):
            for code in codes:
                runs[code // 100](code // 10 % 10, code % 10)

        def end():
            while state["small"] < len(steps):
                small_next()
            small_out[...] = current[flat]
            for ch in range(count):
                for k in range(1, Z):
                    net.landed(owned(ch, z ^ k), zr.at[ch, k])
                pltpu.make_async_copy(owned(ch, z), owned(ch, z), zl.at[ch]).wait()
            net.landed(rows_out.at[1], yr.at[1])
            if diag:
                pltpu.make_async_copy(final.at[0], rows_out.at[0], yl).wait()
            else:
                net.landed(rows_out.at[0], yr.at[0])
            for parts in sent:
                net.copy(*parts()).wait_send()

        return small_send, run, end

    programs = {key: program(*key) for key in SCATTER_ORDER}
    cuts = {
        key: [i for i, code in enumerate(codes) if code // 100 == 1] + [len(codes)]
        for key, codes in SCATTER_ORDER.items()
    }

    def begin(inner, diag):
        small_send, run, _ = programs[inner, diag]
        small_send()
        run(SCATTER_ORDER[inner, diag][: cuts[inner, diag][0]])

    def part(i, inner, diag):
        lo, hi = cuts[inner, diag][i : i + 2]
        programs[inner, diag][1](SCATTER_ORDER[inner, diag][lo:hi])

    by_class(inner_z, role, begin)
    if fused:

        @pl.loop(0, 2 * Z)
        def _(i):
            make(i)
            for n in range(2 * Z):

                @pl.when(i == n)
                def _(n=n):
                    by_class(inner_z, role, functools.partial(part, n))

    else:
        for n in range(2 * Z):
            by_class(inner_z, role, functools.partial(part, n))
    by_class(inner_z, role, lambda inner, diag: programs[inner, diag][2]())


def scatter(factors, keep, give, terms, m_size, rows):
    one, two, acts, att, d_attn, act, d_pre = factors
    width = keep.shape[1]
    block = width // (2 * Z * m_size)
    seq = keep.shape[0] // Z
    cols = [2 * HEAD_DIM, 2 * HEAD_DIM, act.shape[1], act.shape[1]]
    parts = [cols[array] // PARTS[array] for array, _, _ in CHUNKS]
    count = len(CHUNKS)
    fused = m_size == 2 and 2 * block % 256 == 0
    sem = pltpu.SemaphoreType.DMA
    vmem = lambda *shape: pltpu.VMEM(shape, bf16)
    doubling = m_size.bit_length() - 1 + 4
    in_place = pl.BlockSpec(memory_space=pl.ANY)
    in_vmem = pl.BlockSpec(memory_space=pltpu.VMEM)
    far = m_size - 1
    term_shapes = [jax.ShapeDtypeStruct((Z, m_size, 2, block, n), bf16) for n in cols]
    out_shape = [jax.ShapeDtypeStruct((Z, block, n), bf16) for n in cols]
    out_shape += [jax.ShapeDtypeStruct((2, rows, width), bf16), jax.ShapeDtypeStruct(terms.shape[1:], f32)]
    out_specs = [in_place] * 5 + [in_vmem]
    if fused:
        inputs = [one, two, acts, att, d_attn, act, d_pre]
        in_specs = [in_place] * 3 + [in_vmem] * 4
        out_shape, out_specs = term_shapes + out_shape, [in_place] * 4 + out_specs
    else:
        inputs = [g.reshape(s.shape) for g, s in zip(run_grads(*factors), term_shapes)]
        in_specs = [in_place] * 4
    scratch = []
    for n, (_, _, m_first) in zip(parts, CHUNKS):
        if m_first:
            scratch += [vmem(m_size, Z, block, n)] * 2 + [vmem(far, Z, block, n)] * 2 + [vmem(Z, block, n)]
        else:
            scratch += [vmem(Z, 2, block, n), vmem(far, Z, 2, block, n), vmem(Z, 2, block, n)]
            scratch += [vmem(Z, block, n)] * 3
    scratch += [vmem(4, block, n) for n in parts]
    scratch += [vmem(Z, seq, width)] * 2 + [vmem(5, seq, width), vmem(2, rows, width)]
    scratch += [pltpu.VMEM(terms.shape, f32)] * 2
    scratch += [
        sem((Z, 2)),
        sem((Z, 2)),
        sem((Z,)),
        sem((Z, 2)),
        sem((5, 2)),
        sem((2,)),
        sem((2,)),
        sem,
        sem((count, m_size, Z, 2)),
        sem((count, m_size, Z, 2)),
        sem((count, m_size, Z)),
        sem((count, m_size, Z)),
        sem((count, m_size, Z)),
        sem((count, m_size, Z)),
        sem((count, m_size, Z)),
        sem((count, Z)),
        sem((count, Z)),
        sem((count,)),
        sem((count, 4)),
        sem((count, 4)),
        sem((doubling,)),
        sem((doubling,)),
    ]
    if fused:
        scratch.append(vmem(2, 3, keep.shape[0], 2 * block))
        made = [vmem(2, block, n) for n in cols]
        scratch_made = [sem((2, 3)), sem((4,))]
    outs = pl.pallas_call(
        functools.partial(scatter_entry, m_size, fused),
        out_shape=out_shape,
        in_specs=in_specs + [in_place] * 2 + [in_vmem],
        out_specs=out_specs,
        scratch_shapes=scratch + (made + scratch_made if fused else []),
        compiler_params=pltpu.CompilerParams(collective_id=1, has_side_effects=True, vmem_limit_bytes=67043328),
        name="scatter_all",
    )(*inputs, keep.reshape(Z, seq, width), give.reshape(Z, seq, width), terms)
    outs = outs[4:] if fused else outs
    return outs[:4], outs[4], outs[5]


def scatter_entry(m_size, fused, *refs):
    if fused:
        refs = refs[:-6] + (refs[-6:-2],) + refs[-2:]
    scatter_kernel(m_size, fused, *refs)


def update_kernel(*refs):
    rows, cotangent, back, bias, qk, vo, up, dn = refs[:8]
    block_out, input_grad = refs[14:16]
    normed, inverse = layer_stats(rows[...])
    block_out[...] = rows[...] + back[0].astype(f32) + bias[...]
    u = back[1].astype(f32)
    input_grad[...] = cotangent[...] + inverse * (
        u
        - jnp.mean(u, axis=-1, keepdims=True)
        - normed * jnp.mean(u * normed, axis=-1, keepdims=True)
    )
    for sources, (weight, one, two), outs in (
        ((qk, qk, vo, vo), refs[8:11], refs[16:20]),
        ((up, dn), refs[11:14], refs[20:24]),
    ):
        kinds, wide = weight.shape[1], weight.shape[2] // Z
        for j in range(kinds):
            at = j % (kinds // 2) * wide
            for q in range(Z):
                cols = slice(q * wide, (q + 1) * wide)
                g = sources[j][q, :, at : at + wide].astype(f32)
                updated = adam_step(weight[:, j, cols], g, one[:, j, cols], two[:, j, cols])
                for ref, value in zip(outs, (g, *updated)):
                    ref[:, j, cols] = value


def update(block_in, out_grad, own_rows, bias, own, attn, mlp):
    rows, width = block_in.shape
    shard = attn[0].shape[0]
    step = min(shard, 16)
    steps = shard // step
    by_rows = pl.BlockSpec((rows // steps, width), lambda i: (i, 0))
    block = lambda v: pl.BlockSpec((step,) + v.shape[1:], lambda i: (i, 0, 0))
    return pl.pallas_call(
        update_kernel,
        grid=(steps,),
        in_specs=[by_rows, by_rows, pl.BlockSpec((2, rows // steps, width), lambda i: (0, i, 0)), fixed(1, width)]
        + [pl.BlockSpec((Z, step, g.shape[2]), lambda i: (0, i, 0)) for g in own]
        + [block(v) for v in (*attn, *mlp)],
        out_specs=[by_rows, by_rows] + [block(attn[0])] * 4 + [block(mlp[0])] * 4,
        out_shape=[jax.ShapeDtypeStruct((rows, width), f32)] * 2
        + [jax.ShapeDtypeStruct(attn[0].shape, f32)] * 4
        + [jax.ShapeDtypeStruct(mlp[0].shape, f32)] * 4,
        compiler_params=pltpu.CompilerParams(vmem_limit_bytes=VMEM_BYTES),
        name="update",
    )(block_in, out_grad, own_rows, bias, *own, *attn, *mlp)


def body(
    block_in,
    positions,
    out_grad,
    attn_weight,
    mlp_weight,
    small_params,
    attn_first,
    attn_second,
    mlp_first,
    mlp_second,
    small_first,
    small_second,
):
    grid = Grid(lax.axis_size("dp"), lax.axis_size("tensor"))
    z, m, c, t, diag = grid.z_now, grid.m_now, grid.c_now, grid.t_now, grid.diag
    devices = grid.dp * 2
    rows, width = block_in.shape
    seq = 2 * rows
    part = small_params.shape[1]

    pieces, low = prepare(block_in, out_grad, attn_weight, mlp_weight)
    small_tile = jnp.concatenate(
        [jnp.pad(small_params, ((0, 0), (0, 128 - part))), positions.astype(f32).reshape(-1, 128)]
    )
    small_tile = jnp.pad(small_tile, ((0, 16 - small_tile.shape[0]), (0, 0)))
    weights, acts, norms, (attended, d_attn, activation, d_pre), (head_sums, up_sums), table = gather(
        pieces, low, small_tile, grid.m
    )
    everyone = jnp.take(table[:, :12, :part], jnp.array(table_order(grid.m)), axis=0)
    small_all = jnp.transpose(everyone, (1, 0, 2)).reshape(12, width)
    par = small_all[:4]
    head = c * Z + z
    keep, give, norm_sums = run_outs(diag, attended, d_attn, activation, d_pre, acts, weights, par)
    factors = (*norms, acts, attended, d_attn, activation, d_pre)
    spread_cols = lambda v, n: lax.dynamic_update_slice_in_dim(
        jnp.zeros((n,), f32), v, head * v.shape[0], 0
    )
    out_sum = jnp.sum(out_grad, axis=0)
    small_terms = jnp.concatenate(
        [
            norm_sums,
            spread_cols(head_sums[0], width)[None],
            spread_cols(head_sums[1], width)[None],
            out_sum[None],
            out_sum[None],
            spread_cols(up_sums[0], 4 * width).reshape(4, width),
        ],
        axis=0,
    )
    terms = jnp.transpose(small_terms.reshape(12, devices, part), (1, 0, 2)).reshape(devices, 12 * part)
    places_of = table_order(grid.m)
    terms = jnp.take(terms, jnp.array([places_of.index(i) for i in range(devices)]), axis=0)
    terms = jnp.pad(terms, ((0, 0), (0, 1024 - 12 * part))).reshape(devices, -1, 128)
    own, own_rows, own_small = scatter(factors, keep, give, terms, grid.m, rows)
    row_bias = (small_all[6] + small_all[7])[None]
    attn = (attn_weight, attn_first, attn_second)
    mlp = (mlp_weight, mlp_first, mlp_second)
    block_out, input_grad, *updated = update(block_in, out_grad, own_rows, row_bias, own, attn, mlp)
    attn_out, mlp_out = updated[:4], updated[4:]
    small_grad = own_small.reshape(-1)[: 12 * part].reshape(12, part)
    small_new, small_first_new, small_second_new = adam_step(small_params, small_grad, small_first, small_second)

    attn_grad, attn_new, attn_first_new, attn_second_new = attn_out
    mlp_grad, mlp_new, mlp_first_new, mlp_second_new = mlp_out
    return (
        block_out,
        input_grad,
        attn_grad,
        mlp_grad,
        small_grad,
        attn_new,
        attn_first_new,
        attn_second_new,
        mlp_new,
        mlp_first_new,
        mlp_second_new,
        small_new,
        small_first_new,
        small_second_new,
    )


def solution(mesh):
    rows = P(("dp", "tensor"), None)
    weights = P("dp", None, "tensor")
    small = P(None, ("dp", "tensor"))
    return jax.shard_map(
        body,
        mesh=mesh,
        in_specs=(rows, P("dp", None), rows, weights, weights, small, weights, weights, weights, weights, small, small),
        out_specs=(rows, rows) + (weights,) * 2 + (small,) + (weights,) * 6 + (small,) * 3,
        check_vma=False,
    )
```

```python
import functools
import math

import jax
import jax.numpy as jnp
from jax import lax
from jax.experimental import pallas as pl
from jax.experimental.pallas import tpu as pltpu
from jax.sharding import PartitionSpec as P

ROT = 64
ADAM_STEP = 3
HEAD_DIM = 256
Z = 4

norm_epsilon = 1e-05
learn_rate = 0.006
beta_first = 0.9
beta_second = 0.95
adam_epsilon = 1e-08
weight_decay = 0.1

f32 = jnp.float32
bf16 = jnp.bfloat16


def layer_stats(row_data):
    center = row_data - jnp.mean(row_data, axis=-1, keepdims=True)
    inverse = lax.rsqrt(jnp.mean(center * center, axis=-1, keepdims=True) + norm_epsilon)
    return (center * inverse, inverse)


def adam_step(weight, gradient, moment_one, moment_two):
    one_new = beta_first * moment_one + (1.0 - beta_first) * gradient
    two_new = beta_second * moment_two + (1.0 - beta_second) * gradient * gradient
    corrected = (
        one_new
        / (1.0 - beta_first**ADAM_STEP)
        / (jnp.sqrt(two_new / (1.0 - beta_second**ADAM_STEP)) + adam_epsilon)
    )
    return (weight - learn_rate * (corrected + weight_decay * weight), one_new, two_new)


MESH = pl.DeviceIdType.MESH
PARTS = (1, 1, 2, 2)
CHUNKS = ((0, 0, True), (1, 0, False), (2, 0, True), (2, 1, False), (3, 0, True), (3, 1, False))
GATHER_ORDER = {
    (False, False): (
        1201, 0, 10, 1200, 1202, 20, 700, 500, 501, 510, 520, 530, 540, 550, 900, 511, 1100, 521, 600, 1101, 601,
        620, 640, 710, 30, 40, 50, 801, 621, 910, 1110, 502, 512, 610, 602, 522, 630, 1010, 1111, 622, 650, 811,
        1030, 611, 531, 920, 1050, 541, 1000, 551, 1011, 1001, 641, 1020, 1040, 1021, 802, 930, 503, 1120, 513, 940,
        612, 603, 1002, 523, 1012, 623, 1022, 631, 1121, 812, 651, 1031, 532, 1041, 542, 1051, 552, 642, 1003, 613,
        632, 803, 1013, 1203, 652, 1023, 1032, 1042, 1130, 1204, 1205, 1052, 813, 533, 1131, 1206, 543, 1207, 553,
        633, 1208, 643, 653, 1033, 1043, 1209, 1210, 1053, 1211, 1212, 1213, 1214,
    ),
    (False, True): (
        1201, 0, 10, 1200, 1202, 20, 700, 500, 501, 510, 520, 530, 540, 550, 900, 511, 1100, 610, 630, 710, 30, 40,
        50, 650, 611, 521, 600, 1000, 601, 1001, 620, 1020, 640, 1040, 801, 910, 1010, 1101, 1110, 502, 1030, 1050,
        1011, 811, 621, 1021, 531, 602, 1002, 541, 551, 1111, 641, 631, 930, 512, 612, 522, 651, 1031, 940, 1041,
        1012, 622, 1022, 920, 802, 1051, 503, 1120, 603, 1003, 812, 532, 542, 552, 1121, 642, 632, 513, 613, 523,
        652, 1032, 1042, 1013, 1203, 623, 1023, 1204, 803, 1205, 1052, 1130, 813, 533, 1131, 1206, 543, 633, 1207,
        553, 1208, 643, 653, 1043, 1033, 1209, 1210, 1211, 1053, 1212, 1213, 1214,
    ),
    (True, False): (
        1201, 0, 10, 1200, 1202, 20, 700, 500, 503, 510, 520, 530, 540, 550, 200, 900, 100, 300, 1100, 501, 513, 600,
        210, 310, 1101, 603, 110, 523, 620, 511, 320, 640, 220, 710, 30, 40, 50, 601, 120, 623, 521, 803, 610, 621,
        400, 1130, 502, 630, 1010, 801, 410, 910, 602, 512, 1110, 650, 420, 613, 1030, 1131, 1000, 811, 1050, 1003,
        230, 1111, 813, 130, 1013, 533, 1020, 531, 920, 330, 611, 240, 543, 1040, 140, 340, 1001, 541, 1011, 553,
        1023, 250, 643, 350, 150, 641, 522, 1021, 551, 622, 930, 1002, 940, 802, 633, 612, 631, 1120, 1033, 1012,
        1203, 1031, 812, 1204, 653, 1041, 1043, 430, 1121, 1205, 532, 651, 1206, 542, 1022, 1053, 440, 1207, 632,
        1051, 450, 1208, 552, 642, 1032, 1209, 652, 1042, 1210, 1211, 1052, 1212, 1213, 1214,
    ),
    (True, True): (
        1201, 0, 10, 1200, 1202, 20, 700, 500, 503, 510, 520, 530, 540, 550, 200, 900, 100, 300, 1100, 610, 501, 513,
        630, 710, 30, 40, 50, 650, 600, 613, 210, 310, 1000, 603, 110, 523, 1003, 620, 511, 320, 1020, 640, 611, 220,
        1040, 120, 1101, 1010, 601, 1001, 521, 803, 1030, 400, 1130, 1050, 502, 801, 910, 1013, 1110, 623, 1023, 813,
        1011, 533, 811, 621, 1021, 330, 230, 1111, 602, 1002, 543, 130, 340, 1131, 531, 643, 633, 631, 553, 240, 930,
        350, 140, 410, 541, 1033, 512, 612, 250, 653, 420, 150, 1031, 1043, 940, 522, 551, 641, 1041, 651, 920, 1012,
        1203, 1053, 1204, 622, 1022, 802, 1205, 1051, 1120, 812, 430, 1121, 1206, 532, 1207, 440, 1208, 542, 632,
        450, 642, 552, 652, 1042, 1032, 1209, 1210, 1052, 1211, 1212, 1213, 1214,
    ),
}
SCATTER_ORDER = {
    (False, False): (
        30, 31, 20, 21, 10, 11, 0, 1, 131, 530, 531, 520, 521, 510, 511, 500, 501, 1600, 203, 413, 223, 433, 243,
        453, 121, 1610, 202, 412, 222, 432, 242, 452, 111, 903, 1620, 201, 411, 221, 431, 241, 451, 101, 923, 943,
        1630, 200, 410, 220, 430, 240, 450, 130, 902, 1013, 1033, 303, 323, 922, 343, 120, 942, 1053, 302, 322, 342,
        110, 901, 1012, 921, 301, 321, 341, 100, 941, 300, 320, 340, 1032, 900, 920, 800, 1052, 940, 1113, 1133,
        1011, 1103, 810, 1031, 1051, 1153, 1123, 1143, 1640, 1010, 1112, 1030, 1050, 1102, 1122, 1142, 1101, 1132,
        1121, 1152, 1141, 1111, 1100, 1120, 1140, 1131, 1151, 1110, 1130, 1150,
    ),
    (False, True): (
        30, 31, 20, 21, 10, 11, 0, 1, 131, 530, 531, 520, 521, 510, 511, 500, 501, 1600, 203, 413, 223, 433, 243,
        453, 121, 1610, 903, 202, 412, 222, 432, 242, 452, 111, 923, 201, 411, 221, 431, 241, 451, 101, 943, 1620,
        200, 410, 220, 430, 240, 450, 130, 902, 1013, 922, 1033, 1630, 303, 323, 343, 120, 942, 1053, 901, 302, 322,
        342, 110, 921, 301, 321, 341, 100, 1012, 941, 300, 320, 340, 900, 920, 1032, 940, 800, 1113, 1052, 1133,
        1103, 1123, 810, 1011, 1031, 1153, 1051, 1143, 1640, 1010, 1112, 1030, 1050, 1102, 1122, 1142, 1132, 1101,
        1152, 1121, 1111, 1141, 1100, 1120, 1131, 1140, 1151, 1110, 1130, 1150,
    ),
    (True, False): (
        30, 31, 20, 21, 10, 11, 0, 1, 131, 530, 531, 520, 521, 510, 511, 500, 501, 1600, 203, 413, 223, 433, 243,
        453, 121, 1610, 202, 412, 222, 432, 242, 452, 111, 620, 903, 923, 1620, 201, 411, 221, 431, 241, 451, 101,
        943, 200, 410, 220, 430, 240, 450, 130, 902, 1013, 621, 922, 1033, 303, 323, 343, 1053, 120, 700, 901, 942,
        302, 322, 342, 110, 1012, 630, 921, 941, 301, 321, 341, 100, 710, 900, 920, 1032, 300, 320, 340, 1052, 940,
        631, 1113, 1133, 1103, 1011, 1123, 800, 1031, 1153, 1051, 1143, 810, 1630, 1310, 1112, 1010, 1330, 1300,
        1640, 1030, 1350, 1510, 1320, 1410, 1050, 1340, 1530, 1102, 1132, 1210, 1500, 1122, 1550, 1200, 1101, 1520,
        1220, 1142, 1540, 1240, 1121, 1152, 1400, 1141, 1111, 1430, 1230, 1100, 1131, 1120, 1151, 1420, 1250, 1140,
        1110, 1440, 1130, 1150, 1450,
    ),
    (True, True): (
        30, 31, 20, 21, 10, 11, 0, 1, 131, 530, 531, 520, 521, 510, 511, 500, 501, 1600, 203, 413, 223, 433, 243,
        453, 121, 1610, 903, 202, 412, 222, 432, 242, 452, 111, 620, 923, 201, 411, 221, 431, 241, 451, 101, 943,
        1620, 902, 200, 410, 220, 430, 240, 450, 130, 1013, 621, 922, 1033, 942, 1053, 303, 323, 343, 120, 700, 901,
        921, 302, 322, 342, 110, 630, 1012, 941, 900, 301, 321, 341, 100, 710, 920, 1032, 940, 300, 320, 340, 1113,
        1052, 631, 1133, 1103, 1123, 1011, 800, 1153, 1031, 1051, 1143, 810, 1630, 1112, 1102, 1310, 1330, 1010,
        1300, 1640, 1320, 1410, 1030, 1350, 1400, 1340, 1510, 1132, 1050, 1210, 1530, 1122, 1500, 1200, 1142, 1520,
        1220, 1101, 1550, 1240, 1152, 1121, 1540, 1230, 1111, 1141, 1430, 1131, 1100, 1250, 1151, 1120, 1420, 1140,
        1440, 1110, 1130, 1150, 1450,
    ),
}


class Links:
    def __init__(self, m_size):
        self.m_size = m_size
        index = lax.axis_index("dp")
        self.z, self.m, self.c = index // (2 * m_size), (index // 2) % m_size, index % 2
        self.t = lax.axis_index("tensor")
        self.sends = []

    def to(self, z=None, m=None, c=None, t=None):
        z, m, c = (own if v is None else v for v, own in ((z, self.z), (m, self.m), (c, self.c)))
        return ((z * self.m_size + m) * 2 + c, self.t if t is None else t)

    def copy(self, src, dst, send_sem, recv_sem, target):
        return pltpu.make_async_remote_copy(
            src_ref=src, dst_ref=dst, send_sem=send_sem, recv_sem=recv_sem, device_id=target, device_id_type=MESH
        )

    def send(self, src, dst, send_sem, recv_sem, target):
        one = self.copy(src, dst, send_sem, recv_sem, target)
        one.start()
        self.sends.append(one)

    def landed(self, dst, recv_sem):
        self.copy(dst, dst, recv_sem, recv_sem, self.to(c=1 - self.c)).wait_recv()

    def drain(self):
        for one in self.sends:
            one.wait_send()
        self.sends = []

    def partners(self):
        other = 1 - self.t
        out = [self.to(z=self.z ^ k) for k in range(1, Z)]
        out += [self.to(m=self.m ^ j) for j in range(1, self.m_size)]
        out += [self.to(c=1 - self.c), self.to(t=other), self.to(c=1 - self.c, t=other)]
        return out

    def doubling(self):
        high = self.z // 2
        place = ((self.m * 2 + self.c) * 2 + self.t) * 4 + lax.rem(self.z + high, 2) * 2 + high
        steps = [(1, self.to(z=self.z ^ 3)), (2, self.to(z=self.z ^ 1)), (4, self.to(t=1 - self.t))]
        steps.append((8, self.to(c=1 - self.c)))
        j = 1
        while j < self.m_size:
            steps.append((16 * j, self.to(m=self.m ^ j)))
            j *= 2
        return place, steps

    def meet(self):
        barrier = pltpu.get_barrier_semaphore()
        everyone = self.partners()
        for target in everyone:
            pl.semaphore_signal(barrier, inc=1, device_id=target, device_id_type=MESH)
        pl.semaphore_wait(barrier, len(everyone))


def gather_kernel(m_size, *refs):
    weights, rows_in, small, positions = refs[:2], refs[2:4], refs[4], refs[5]
    full, act_out, one_out, two_out = refs[6:10], refs[10], refs[11], refs[12]
    att, d_attn, hidden_out, d_pre, head_sums, up_sums, par, row_bias, out_sum = refs[13:22]
    count = len(CHUNKS)
    stage, stage_m, relay = (refs[22 + i * count : 22 + (i + 1) * count] for i in range(3))
    refs = refs[22 + 3 * count :]
    (zs, zr, gs, gr, ps, pr, ms, mr, near_s, far_s, xr, as_, ar, ws, wr, ss, sr, lin, lout, ls, os_) = refs[:21]
    pieces, refs = refs[21 : 21 + count], refs[21 + count :]
    act, w_qk, w_vo, one_v, two_v, tile_v, slope, bias, up_bias, table, base, attn_v, mlp_v, rows_v, low = refs
    net = Links(m_size)
    z, m, c, t = net.z, net.m, net.c, net.t
    rows = pieces[0].shape[1]
    half = low.shape[1]
    seq = 2 * half
    width = low.shape[2]
    n = HEAD_DIM
    role = lax.rem(c + t, 2)
    inner_z = lax.rem(z + z // 2, 2)

    def columns(ch):
        array, part, _ = CHUNKS[ch]
        wide = pieces[ch].shape[2]
        return array, slice(part * wide, (part + 1) * wide)

    def piece(ch, zz):
        return pieces[ch].at[zz]

    def whole(ch, zz, mm, cc, size=1):
        array, cols = columns(ch)
        start = ((zz * m_size + mm) * 2 + cc) * rows
        return full[array].at[pl.ds(pl.multiple_of(start, rows), size * rows), cols]

    own_place = pl.ds(pl.multiple_of(z * seq + t * half, half), half)
    place = lambda zz, h: pl.ds(pl.multiple_of(zz * seq + (t ^ h) * half, half), half)

    def store_own(ch):
        return pltpu.make_async_copy(pieces[ch].at[z], whole(ch, z, m, c), lout.at[ch])

    def inputs():
        sources = (*weights, *rows_in)
        return [
            pltpu.make_async_copy(src, dst, lin.at[i])
            for i, (src, dst) in enumerate(zip(sources, (attn_v, mlp_v, rows_v.at[0], rows_v.at[1])))
        ]

    for one in inputs():
        one.start()
    flat, steps = net.doubling()
    table[flat] = jnp.zeros(table.shape[1:], f32)
    table[flat, 0:12, 0 : small.shape[1]] = small[...]
    for e in range(seq // 128):
        table[flat, 12 + e : 13 + e, :] = positions[:, e * 128 : (e + 1) * 128].astype(f32)
    net.meet()

    def program(inner, diag):
        state = {"small": 0}
        sent = []

        def send(parts):
            net.copy(*parts()).start()
            sent.append(parts)

        def small_send():
            i = state["small"]
            if i < len(steps):
                size, target = steps[i]

                def parts():
                    span = table.at[pl.ds(flat // size * size, size)]
                    return span, span, ss.at[i], sr.at[i], target

                send(parts)

        def small_next(*_):
            i = state["small"]
            if i < len(steps):
                size = steps[i][0]
                net.landed(table.at[pl.ds((flat // size ^ 1) * size, size)], sr.at[i])
                state["small"] += 1
                small_send()

        def small_last():
            while state["small"] < len(steps):
                small_next()

        def spot(ch, zz, j):
            if diag:
                return whole(ch, zz, m ^ j, c)
            return stage_m[ch].at[m ^ j, zz] if j else stage[ch].at[zz]

        def source(ch, k, j):
            return piece(ch, z) if k == 0 and j == 0 else spot(ch, z ^ k, j)

        def spread(ch, k, j):
            block = lambda: whole(ch, z ^ k, m ^ j, c)
            send(
                lambda: (
                    source(ch, k, j),
                    block(),
                    ps.at[ch, j, k, 1],
                    pr.at[ch, j, k, c],
                    net.to(c=t, t=1 - t),
                )
            )
            if not diag:
                send(
                    lambda: (source(ch, k, j), block(), ps.at[ch, j, k, 0], pr.at[ch, j, k, c], net.to(c=1 - c))
                )

        def spread_landed(ch, k, j):
            for cc in (1 - c,) if diag else (1 - c, c):
                net.landed(whole(ch, z ^ k, m ^ j, cc), pr.at[ch, j, k, cc])

        def swap(h, k):
            def parts():
                src = act.at[role, place(z ^ k, h)]
                return src, src, ws.at[k, h], wr.at[k, h], net.to(c=1 - c)

            send(parts)

        def rows_on(h, flip, i, hop, k):
            def parts():
                src = act.at[role, place(z ^ flip, h)]
                return src, src, as_.at[h, i], ar.at[h, k], net.to(z=z ^ hop)

            send(parts)

        def quarters(ch, _):
            for i, (k, hop, through) in enumerate(
                ((3, 3, None), (2, 3, 2), (1, 1, None)) if inner else ((3, 1, 1), (2, 1, 0), (1, 1, None))
            ):

                def parts(i=i, k=k, hop=hop, through=through):
                    if through is None:
                        dst, recv_sem = spot(ch, z, 0), zr.at[ch, k]
                    else:
                        dst, recv_sem = relay[ch].at[through], gr.at[ch, through]
                    return piece(ch, z ^ k), dst, zs.at[ch, i], recv_sem, net.to(z=z ^ hop)

                send(parts)

        def pass_on(through):
            hop, k = ((3, 2), (3, None), (1, 2), (1, 3))[through]

            def run(ch, _):
                net.landed(relay[ch].at[through], gr.at[ch, through])

                def parts():
                    if k is None:
                        dst, recv_sem = relay[ch].at[3], gr.at[ch, 3]
                    else:
                        dst, recv_sem = spot(ch, z ^ hop ^ k, 0), zr.at[ch, k]
                    return relay[ch].at[through], dst, gs.at[ch, through], recv_sem, net.to(z=z ^ hop)

                send(parts)

            return run

        def first(ch, k):
            if k:
                net.landed(spot(ch, z ^ k, 0), zr.at[ch, k])
            elif diag:
                store_own(ch).start()
            if CHUNKS[ch][2]:
                for j in range(1, m_size):

                    def parts(j=j):
                        dst = whole(ch, z ^ k, m, c) if diag else stage_m[ch].at[m, z ^ k]
                        return source(ch, k, 0), dst, ms.at[ch, j, k], mr.at[ch, j, k], net.to(m=m ^ j)

                    send(parts)
            spread(ch, k, 0)

        def second(ch, k):
            if CHUNKS[ch][2]:
                for j in range(1, m_size):
                    net.landed(spot(ch, z ^ k, j), mr.at[ch, j, k])
                    spread(ch, k, j)
            else:
                if diag and k == 0:
                    store_own(ch).wait()
                spread_landed(ch, k, 0)
                for j in range(1, m_size):

                    def parts(j=j):
                        both = whole(ch, z ^ k, m, 0, 2)
                        return both, both, ms.at[ch, j, k], mr.at[ch, j, k], net.to(m=m ^ j)

                    send(parts)

        def third(ch, k):
            if CHUNKS[ch][2]:
                for j in range(m_size):
                    spread_landed(ch, k, j)
                if diag and k == 0:
                    store_own(ch).wait()
            else:
                for j in range(1, m_size):
                    net.landed(whole(ch, z ^ k, m ^ j, 0, 2), mr.at[ch, j, k])

        def rows_start(h, _):
            if h:
                net.landed(act.at[0 if diag else 1, place(z, 1)], xr.at[1])
            elif not diag:
                net.landed(act.at[1, place(z, 0)], xr.at[0])
            if inner:
                rows_on(h, 0, 0, 3, 3)
            rows_on(h, 0, 1, 1, 1)
            swap(h, 0)

        def rows_next(h, k):
            net.landed(act.at[role, place(z ^ k, h)], ar.at[h, k])
            if inner:
                hop, there = {1: (3, 2), 3: (1, 2), 2: (1, 3)}[k]
                rows_on(h, k, 1 + k, hop, there)
            swap(h, k)

        def swapped(k, h):
            net.landed(act.at[1 - role, place(z ^ k, h)], wr.at[k, h])

        def rows_out():
            if diag:
                send(lambda: (low.at[1], act.at[1, own_place], near_s, xr.at[0], net.to(c=1 - c)))
            else:
                send(lambda: (low.at[0], act.at[0, own_place], near_s, xr.at[1], net.to(t=1 - t)))
                send(lambda: (low.at[1], act.at[1, own_place], far_s, xr.at[1], net.to(c=1 - c, t=1 - t)))

        runs = [quarters] + [pass_on(i) for i in range(4)]
        runs += [first, second, rows_start, rows_next, small_next, third, swapped]

        def run(codes):
            for code in codes:
                runs[code // 100](code // 10 % 10, code % 10)

        def end():
            for parts in sent:
                net.copy(*parts()).wait_send()

        return small_send, run, rows_out, small_last, end

    programs = {key: program(*key) for key in GATHER_ORDER}
    work = len(runs_before(GATHER_ORDER[True, True]))

    device_rows = functools.partial(table_place, m_size)

    def parameters():
        part = width // (8 * m_size * 2)
        per = 128 // part
        static = table_order(m_size)
        for b in range(width // 128):
            got = [table[static[b * per + e], 0:4, 0:part] for e in range(per)]
            par[:, b * 128 : (b + 1) * 128] = jnp.concatenate(got, axis=1)
        head = c * Z + z
        for b in range(n // 128):
            start = (head * n + b * 128) // part
            got = [table[device_rows(start + e), 4:6, 0:part] for e in range(per)]
            bias[:, b * 128 : (b + 1) * 128] = jnp.concatenate(got, axis=1)
        wide = up_bias.shape[1]
        for b in range(width // 128):
            got = [table[static[b * per + e], 6:8, 0:part] for e in range(per)]
            both = jnp.concatenate(got, axis=1)
            row_bias[:, b * 128 : (b + 1) * 128] = both[0:1] + both[1:2]
        row = 8 + head * wide // width
        for b in range(wide // 128):
            start = (lax.rem(head * wide, width) + b * 128) // part
            got = [table[device_rows(start + e), pl.ds(row, 1), 0:part] for e in range(per)]
            up_bias[:, b * 128 : (b + 1) * 128] = jnp.concatenate(got, axis=1)

    step = 16

    def attn_in():
        inputs()[0].wait()
        wide = attn_v.shape[2] // Z

        @pl.loop(0, rows // step)
        def _(i):
            span = pl.ds(pl.multiple_of(i * step, step), step)
            for j in range(4):
                block = attn_v[span, j, :].astype(bf16)
                for q in range(Z):
                    at = j % 2 * wide
                    pieces[j // 2][q, span, at : at + wide] = block[:, q * wide : (q + 1) * wide]

    def mlp_in():
        inputs()[1].wait()
        wide = mlp_v.shape[2] // (2 * Z)

        @pl.loop(0, rows // step)
        def _(i):
            span = pl.ds(pl.multiple_of(i * step, step), step)
            for j in range(2):
                block = mlp_v[span, j, :].astype(bf16)
                for q in range(2 * Z):
                    pieces[2 + 2 * j + q % 2][q // 2, span, :] = block[:, q * wide : (q + 1) * wide]

    def rows_low():
        for one in inputs()[2:]:
            one.wait()
        out_sum[...] = jnp.zeros_like(out_sum)

        @pl.loop(0, half // step)
        def _(i):
            start = pl.multiple_of(i * step, step)
            span = pl.ds(start, step)
            normed, _ = layer_stats(rows_v[0, span, :])
            normed = normed.astype(bf16)
            low[0, span, :] = normed
            given = rows_v[1, span, :]
            low[1, span, :] = given.astype(bf16)
            out_sum[...] += jnp.sum(given, axis=0, keepdims=True)

            @pl.when(role == 0)
            def _():
                act[0, pl.ds(pl.multiple_of(z * seq + t * half + start, step), step), :] = normed

    def turns_in():
        for a, value in enumerate(turn_tables(lax.broadcasted_iota(jnp.int32, (seq, 128), 0).astype(f32))):
            for e in range(3):
                term = value.astype(bf16)
                base[:, (3 * a + e) * 128 : (3 * a + e + 1) * 128] = term
                value = value - term.astype(f32)

    def weights_in():
        return [
            pltpu.make_async_copy(full[0], w_qk, ls.at[0]),
            pltpu.make_async_copy(full[1], w_vo, ls.at[1]),
        ]

    def rows_saved(i):
        k = i ^ (inner_z & (i // 2))
        span = pl.ds(pl.multiple_of((z ^ k) * seq, seq), seq)
        return [
            pltpu.make_async_copy(one_v.at[lax.rem(i, 2)], one_out.at[span], os_.at[0, i]),
            pltpu.make_async_copy(two_v.at[span], two_out.at[span], os_.at[1, i]),
            pltpu.make_async_copy(act.at[:, span], act_out.at[:, span], os_.at[2, i]),
        ]

    def attention(i):
        @pl.when(i == 0)
        def _():
            for one in weights_in():
                one.start()
            parameters()
            turns_in()
            head_sums[...] = jnp.zeros_like(head_sums)
            for one in weights_in():
                one.wait()

        @pl.when(i >= 2)
        def _():
            rows_saved(i - 2)[0].wait()

        k = i ^ (inner_z & (i // 2))
        span = pl.ds(pl.multiple_of((z ^ k) * seq, seq), seq)
        x = act[0, span, :].astype(f32)
        one = (x * par[0:1, :] + par[1:2, :]).astype(bf16)
        one_v[lax.rem(i, 2)] = one
        two_v[span, :] = (x * par[2:3, :] + par[3:4, :]).astype(bf16)
        for copy in rows_saved(i):
            copy.start()
        source = device_rows((((z ^ k) * m_size + m) * 2 + t) * 2)
        across = jnp.concatenate([table[source, 12 + e : 13 + e, :] for e in range(seq // 128)], axis=1)
        spots = lax.broadcasted_iota(jnp.int32, (seq, seq), 0).astype(f32)
        hit = jnp.where(spots == across, 1.0, 0.0).astype(bf16)
        down = dot(hit, spots.astype(bf16), 0, 0)
        turns = dot(hit, base[...], 0, 0)
        tables = [sum(turns[:, (3 * a + e) * 128 : (3 * a + e + 1) * 128] for e in range(3)) for a in range(3)]
        scale = HEAD_DIM ** (-0.5)
        qk = dot(one, w_qk[...])
        q = turn(qk[:, :n] + bias[0:1, :], tables, 1.0).astype(bf16)
        k_rows = turn(qk[:, n:], tables, 1.0).astype(bf16)
        v = (dot(one, w_vo[:, :n]) + bias[1:2, :]).astype(bf16)
        d_att = dot(act[1, span, :], w_vo[:, n:]).astype(bf16)
        scores = jnp.where(across <= down, dot(q, k_rows, 1, 1) * scale, -jnp.inf)
        top = jnp.max(scores, axis=-1, keepdims=True)
        log_total = top + jnp.log(jnp.sum(jnp.exp(scores - top), axis=-1, keepdims=True))
        probs = jnp.exp(scores - log_total)
        low_probs = probs.astype(bf16)
        att[span, :] = dot(low_probs, v).astype(bf16)
        d_probs = dot(d_att, v, 1, 1)
        d_scores = (probs * (d_probs - jnp.sum(probs * d_probs, axis=-1, keepdims=True)) * scale).astype(bf16)
        d_q = turn(dot(d_scores, k_rows), tables, -1.0)
        d_k = turn(dot(d_scores, q, 0, 0), tables, -1.0)
        d_v = dot(low_probs, d_att, 0, 0)
        d_attn[span, 0:n] = d_q.astype(bf16)
        d_attn[span, n : 2 * n] = d_k.astype(bf16)
        d_attn[span, 2 * n :] = d_v.astype(bf16)
        head_sums[0:1, :] += jnp.sum(d_q, axis=0, keepdims=True)
        head_sums[1:2, :] += jnp.sum(d_v, axis=0, keepdims=True)

    wide = full[2].shape[1] // Z

    def tile_in(array, j):
        cols = pl.ds(pl.multiple_of(j * wide, wide), wide)
        return pltpu.make_async_copy(full[array].at[:, cols], tile_v.at[lax.rem(j, 2)], ls.at[lax.rem(j, 2)])

    def tile_ready(array, j):
        @pl.when(lax.rem(j, 2) == 0)
        def _():
            tile_in(array, j).start()
            tile_in(array, j + 1).start()

        tile_in(array, j).wait()

    def hidden(i):
        j = i - Z
        tile_ready(2, j)
        cols = pl.ds(pl.multiple_of(j * wide, wide), wide)
        pre = dot(two_v[...], tile_v[lax.rem(j, 2)]) + up_bias[:, cols]
        erf = 1.0 + lax.erf(pre * 0.7071067811865476)
        hidden_out[:, cols] = (0.5 * pre * erf).astype(bf16)
        slope[j] = 0.5 * erf + pre * jnp.exp(-0.5 * pre * pre) * 0.3989422804014327

    def hidden_back(i):
        j = i - 2 * Z
        tile_ready(3, j)
        cols = pl.ds(pl.multiple_of(j * wide, wide), wide)
        value = dot(act[1], tile_v[lax.rem(j, 2)]) * slope[j]
        d_pre[:, cols] = value.astype(bf16)
        up_sums[:, cols] = jnp.sum(value, axis=0, keepdims=True)

    def part(i, inner, diag):
        _, run, rows_out, small_last, _ = programs[inner, diag]
        if i == 1:
            rows_out()
        run(runs_before(GATHER_ORDER[inner, diag])[i + 1])
        if i == 2:
            small_last()

    by_class(inner_z, role, lambda inner, diag: programs[inner, diag][0]())
    ahead = 3

    @pl.loop(0, work - 1)
    def _(i):
        pl.when(i == 0)(attn_in)
        pl.when(i == 1)(rows_low)
        pl.when(i == 2)(mlp_in)
        pl.when((i >= ahead) & (i < ahead + Z))(lambda: attention(i - ahead))
        pl.when((i >= ahead + Z) & (i < ahead + 2 * Z))(lambda: hidden(i - ahead))
        pl.when(i >= ahead + 2 * Z)(lambda: hidden_back(i - ahead))
        for e in range(work - 1):

            @pl.when(i == e)
            def _(e=e):
                by_class(inner_z, role, functools.partial(part, e))

    by_class(inner_z, role, lambda inner, diag: programs[inner, diag][4]())
    for i in range(Z):
        saved = rows_saved(i)
        for copy in saved[1:] if i < 2 else saved:
            copy.wait()


def runs_before(order):
    cuts = [i for i, code in enumerate(order) if code // 100 == 12]
    return [order[lo:hi] for lo, hi in zip([0] + [i + 1 for i in cuts], cuts + [len(order)])]


def table_place(m_size, index):
    z, rest = index // (4 * m_size), index % (4 * m_size)
    return rest * 4 + (z + z // 2) % 2 * 2 + z // 2


def table_order(m_size):
    return [table_place(m_size, i) for i in range(4 * m_size * Z)]


def by_class(inner_z, role, program):
    for inner in (False, True):
        for diag in (False, True):

            @pl.when((inner_z == int(inner)) & (role == int(not diag)))
            def _(inner=inner, diag=diag):
                program(inner, diag)


def gather(attn_weight, mlp_weight, block_in, out_grad, small, positions, m_size):
    rows = attn_weight.shape[0]
    own, width = block_in.shape
    tokens = Z * 2 * own
    devices = m_size * 4 * Z
    hidden, n = mlp_weight.shape[2] // Z, HEAD_DIM
    cols = [2 * n, 2 * n, hidden, hidden]
    count = len(CHUNKS)
    parts = [cols[array] // PARTS[array] for array, _, _ in CHUNKS]
    sem = pltpu.SemaphoreType.DMA
    doubling = m_size.bit_length() - 1 + 4
    in_place = pl.BlockSpec(memory_space=pl.ANY)
    in_vmem = pl.BlockSpec(memory_space=pltpu.VMEM)
    shape = lambda *dims: jax.ShapeDtypeStruct(dims, bf16)
    exact = lambda *dims: jax.ShapeDtypeStruct(dims, f32)
    vmem = lambda *dims: pltpu.VMEM(dims, bf16)
    wide = lambda *dims: pltpu.VMEM(dims, f32)
    outs = pl.pallas_call(
        functools.partial(gather_kernel, m_size),
        out_shape=[shape(width, n) for n in cols]
        + [shape(2, tokens, width), shape(tokens, width), shape(tokens, width)]
        + [shape(tokens, n), shape(tokens, 3 * n), shape(tokens, hidden), shape(tokens, hidden)]
        + [exact(2, n), exact(1, hidden), exact(4, width), exact(1, width), exact(1, width)]
        + [shape(Z, rows, n) for n in parts]
        + [shape(m_size, Z, rows, n) for n in parts]
        + [shape(4, rows, n) for n in parts],
        in_specs=[in_place] * 4 + [in_vmem] * 2,
        out_specs=[in_place] * 7 + [in_vmem] * 9 + [in_place] * (3 * count),
        scratch_shapes=[
            sem((count, 3)),
            sem((count, Z)),
            sem((count, 4)),
            sem((count, 4)),
            sem((count, m_size, Z, 2)),
            sem((count, m_size, Z, 2)),
            sem((count, m_size, Z)),
            sem((count, m_size, Z)),
            sem,
            sem,
            sem((2,)),
            sem((2, 5)),
            sem((2, Z)),
            sem((Z, 2)),
            sem((Z, 2)),
            sem((doubling,)),
            sem((doubling,)),
            sem((4,)),
            sem((count,)),
            sem((2,)),
            sem((3, Z)),
        ]
        + [vmem(Z, rows, n) for n in parts]
        + [vmem(2, tokens, width), vmem(width, 2 * n), vmem(width, 2 * n), vmem(2, 2 * own, width)]
        + [vmem(tokens, width), vmem(2, width, hidden // Z), wide(Z, tokens, hidden // Z)]
        + [wide(2, n), wide(1, hidden), wide(devices, 16, 128), vmem(2 * own, 9 * 128)]
        + [wide(*attn_weight.shape), wide(*mlp_weight.shape), wide(2, own, width), vmem(2, own, width)],
        compiler_params=pltpu.CompilerParams(collective_id=0, has_side_effects=True, vmem_limit_bytes=67043328),
        name="gather_all",
    )(attn_weight, mlp_weight, block_in, out_grad, small, positions)
    return outs[:4], outs[4], outs[5:7], outs[7:11], outs[11:13], outs[13], outs[14], outs[15]


VMEM_BYTES = 60 * 1024 * 1024


def dot(a, b, over_a=1, over_b=0):
    return lax.dot_general(a, b, (((over_a,), (over_b,)), ((), ())), preferred_element_type=f32)


def turn(value, tables, sign):
    cos, low, high = tables
    part = value[:, :128]
    turned = part * cos + sign * (
        pltpu.roll(part, 128 - ROT // 2, 1) * low + pltpu.roll(part, ROT // 2, 1) * high
    )
    return jnp.concatenate([turned, value[:, 128:]], axis=1)


def turn_tables(places):
    half = ROT // 2
    column = lax.broadcasted_iota(jnp.int32, places.shape, 1)
    frequency = jnp.exp(lax.rem(column, half).astype(f32) * (-2.0 / ROT * math.log(10000.0)))
    angles = places * frequency
    cos = jnp.where(column < ROT, jnp.cos(angles), 1.0)
    sin = jnp.sin(angles)
    return cos, jnp.where(column < half, -sin, 0.0), jnp.where((column >= half) & (column < ROT), sin, 0.0)


def fixed(*shape):
    return pl.BlockSpec(shape, lambda i: (0,) * len(shape))


def outs_kernel(flag, att, d_attn, act, d_pre, x, w_qk, w_vo, w_up, w_dn, par, keep, give, sums):
    diag = flag[0] == 1
    n = HEAD_DIM
    y = dot(att[...], w_vo[:, n:], 1, 1) + dot(act[...], w_dn[...], 1, 1)
    d_one = dot(d_attn[:, : 2 * n], w_qk[...], 1, 1) + dot(d_attn[:, 2 * n :], w_vo[:, :n], 1, 1)
    d_two = dot(d_pre[...], w_up[...], 1, 1)
    u = d_one * par[0:1, :] + d_two * par[2:3, :]
    keep[...] = jnp.where(diag, y, u).astype(bf16)
    give[...] = jnp.where(diag, u, y).astype(bf16)
    plain = x[...].astype(f32)
    for i, value in enumerate((d_one * plain, d_one, d_two * plain, d_two)):
        sums[i : i + 1, :] = jnp.sum(value, axis=0, keepdims=True)


def run_outs(diag, att, d_attn, act, d_pre, acts, weights, par):
    _, rows, width = acts.shape
    step = 256
    fix = lambda v: pl.BlockSpec(v.shape, lambda i, s: (0, 0), pipeline_mode=pl.Buffered(1))
    tile = lambda height: pl.BlockSpec((height, step), lambda i, s: (0, i))
    return pl.pallas_call(
        outs_kernel,
        grid_spec=pltpu.PrefetchScalarGridSpec(
            num_scalar_prefetch=1,
            grid=(width // step,),
            in_specs=[fix(v) for v in (att, d_attn, act, d_pre)]
            + [pl.BlockSpec((None, rows, step), lambda i, s: (0, 0, i))]
            + [pl.BlockSpec((step, v.shape[1]), lambda i, s: (i, 0)) for v in weights]
            + [tile(4)],
            out_specs=[tile(rows), tile(rows), tile(4)],
        ),
        out_shape=[jax.ShapeDtypeStruct((rows, width), bf16)] * 2 + [jax.ShapeDtypeStruct((4, width), f32)],
        compiler_params=pltpu.CompilerParams(vmem_limit_bytes=VMEM_BYTES),
        name="outputs",
    )(diag.astype(jnp.int32).reshape(1), att, d_attn, act, d_pre, acts, *weights, par)


def grads_kernel(one, two, g, att, d_attn, act, d_pre, qk, vo, up, dn):
    n = HEAD_DIM
    first = dot(one[...], d_attn[...], 0, 0)
    qk[...] = first[:, : 2 * n].astype(bf16)
    vo[:, :n] = first[:, 2 * n :].astype(bf16)
    vo[:, n:] = dot(g[...], att[...], 0, 0).astype(bf16)
    up[...] = dot(two[...], d_pre[...], 0, 0).astype(bf16)
    dn[...] = dot(g[...], act[...], 0, 0).astype(bf16)


def run_grads(one, two, acts, att, d_attn, act, d_pre):
    rows, width = one.shape
    step = 256
    tile = pl.BlockSpec((rows, step), lambda i: (0, i))
    fix = lambda v: pl.BlockSpec(v.shape, lambda i: (0, 0), pipeline_mode=pl.Buffered(1))
    cols = [2 * HEAD_DIM, 2 * HEAD_DIM, act.shape[1], act.shape[1]]
    return pl.pallas_call(
        grads_kernel,
        grid=(width // step,),
        in_specs=[tile, tile, pl.BlockSpec((None, rows, step), lambda i: (1, 0, i))]
        + [fix(v) for v in (att, d_attn, act, d_pre)],
        out_specs=[pl.BlockSpec((step, n), lambda i: (i, 0)) for n in cols],
        out_shape=[jax.ShapeDtypeStruct((width, n), bf16) for n in cols],
        compiler_params=pltpu.CompilerParams(vmem_limit_bytes=VMEM_BYTES),
        name="weight_grads",
    )(one, two, acts, att, d_attn, act, d_pre)


def add_rows(dst, sources):
    step = min(dst.shape[0], 32)

    @pl.loop(0, dst.shape[0] // step)
    def _(i):
        span = pl.ds(pl.multiple_of(i * step, step), step)
        total = sources[0][span, :].astype(f32)
        for one in sources[1:]:
            total = total + one[span, :].astype(f32)
        dst[span, :] = total.astype(dst.dtype)


def scatter_kernel(m_size, fused, *refs):
    if fused:
        ones, twos, acts, att, d_attn, act, d_pre = refs[:7]
        keep, give, *sums = refs[7:13]
        grads, refs = refs[13:17], refs[17:]
    else:
        grads, (keep, give, *sums), refs = refs[:4], refs[4:10], refs[10:]
    own, rows_out, small_out, refs = refs[:4], refs[4], refs[5], refs[6:]
    count = len(CHUNKS)
    buffers = []
    for _, _, m_first in CHUNKS:
        size = 5 if m_first else 6
        buffers.append(refs[:size])
        refs = refs[size:]
    relay, refs = refs[:count], refs[count:]
    got, kept, got_z, final, current, got_small = refs[:6]
    (gs, gr, kl, as_, ar, ys, yr, yl, ws, wr, wl, fs, fr, xs, xr, zs, zr, zl, ps, pr, ss, sr) = refs[6:28]
    if fused:
        tiles, made, tl, ml = refs[28:]
    net = Links(m_size)
    z, m, c, t = net.z, net.m, net.c, net.t
    half = rows_out.shape[1]
    role = lax.rem(c + t, 2)
    inner_z = lax.rem(z + z // 2, 2)
    flat, steps = net.doubling()
    steps = steps[::-1]

    def columns(ch):
        array, part, _ = CHUNKS[ch]
        wide = own[array].shape[2] // PARTS[array]
        return array, slice(part * wide, (part + 1) * wide)

    def rows_of(ch, k, j, cc=None):
        array, cols = columns(ch)
        if cc is None:
            return grads[array].at[z ^ k, m ^ j, :, :, cols]
        return grads[array].at[z ^ k, m ^ j, cc, :, cols]

    def owned(ch, zz):
        array, cols = columns(ch)
        return own[array].at[zz, :, cols]

    span = lambda h: pl.ds(pl.multiple_of((t ^ h) * half, half), half)
    loads_keep = [pltpu.make_async_copy(keep.at[z ^ k], kept.at[k], kl.at[k]) for k in range(Z)]
    for one in loads_keep:
        one.start()
    norm_sums, head_sums, up_sums, out_sum = sums

    def small_terms():
        current[...] = jnp.zeros_like(current)
        width, hidden, n = out_sum.shape[1], up_sums.shape[1], HEAD_DIM
        part = width // (4 * m_size * Z)
        for i, at in enumerate(table_order(m_size)):
            cols = slice(i * part, (i + 1) * part)
            current[at, 0:4, 0:part] = norm_sums[:, cols]
            current[at, 6:7, 0:part] = out_sum[:, cols]
            current[at, 7:8, 0:part] = out_sum[:, cols]
        head = c * Z + z
        for e in range(n // part):
            at = table_place(m_size, head * n // part + e)
            current[at, 4:6, 0:part] = head_sums[:, e * part : (e + 1) * part]
        row = 8 + head * hidden // width
        for e in range(hidden // part):
            at = table_place(m_size, head * hidden % width // part + e)
            current[at, pl.ds(row, 1), 0:part] = up_sums[:, e * part : (e + 1) * part]

    def tile_loads(i, slot):
        block = (z ^ (Z - 1 - lax.rem(i, Z))) * m_size + (m ^ (1 - i // Z))
        wide = tiles.shape[3]
        cols = pl.ds(pl.multiple_of(block * wide, wide), wide)
        sources = (ones.at[:, cols], twos.at[:, cols], acts.at[1, :, cols])
        return [pltpu.make_async_copy(src, tiles.at[slot, n], tl.at[slot, n]) for n, src in enumerate(sources)]

    def make(i):
        slot = lax.rem(i, 2)

        @pl.when(i < 2 * Z - 1)
        def _():
            for one in tile_loads(i + 1, 1 - slot):
                one.start()

        for one in tile_loads(i, slot):
            one.wait()
        n = HEAD_DIM
        high = made[0].shape[1]
        for array, at, left, right, lo, hi in (
            (0, 0, 0, d_attn, 0, 2 * n),
            (1, 0, 0, d_attn, 2 * n, 3 * n),
            (1, n, 2, att, 0, n),
            (2, 0, 1, d_pre, 0, d_pre.shape[1]),
            (3, 0, 2, act, 0, act.shape[1]),
        ):
            value = dot(tiles[slot, left], right[:, lo:hi], 0, 0).astype(bf16)
            for cc in range(2):
                made[array][cc, :, at : at + hi - lo] = value[cc * high : (cc + 1) * high]
        stores = [
            pltpu.make_async_copy(
                made[array], grads[array].at[z ^ (Z - 1 - lax.rem(i, Z)), m ^ (1 - i // Z)], ml.at[array]
            )
            for array in range(4)
        ]
        for one in stores:
            one.start()
        for one in stores:
            one.wait()

    if fused:
        for one in tile_loads(0, 0):
            one.start()
    net.meet()

    def program(inner, diag):
        state = {"small": 0}
        sent = []

        def send(*parts):
            (parts,) = parts
            net.copy(*parts()).start()
            sent.append(parts)

        def small_send():
            i = state["small"]
            if i < len(steps):
                size, target = steps[i]
                send(
                    lambda: (
                        current.at[pl.ds((flat // size ^ 1) * size, size)],
                        got_small.at[pl.ds(size, size)],
                        ss.at[i],
                        sr.at[i],
                        target,
                    )
                )

        def small_next(*_):
            i = state["small"]
            if i < len(steps):
                size = steps[i][0]
                net.landed(got_small.at[pl.ds(size, size)], sr.at[i])
                block = pl.ds(flat // size * size, size)
                current[block] = current[block] + got_small[pl.ds(size, size)]
                state["small"] += 1
                small_send()

        def swap(k, h):
            send(
                lambda: (give.at[z ^ k, span(h)], got.at[k, span(h)], gs.at[k, h], gr.at[k, h], net.to(c=1 - c))
            )

        def load_mine(ch, j, k):
            if CHUNKS[ch][2]:
                return pltpu.make_async_copy(rows_of(ch, k, j, c), buffers[ch][0].at[j, k], wl.at[ch, j, k])
            return pltpu.make_async_copy(rows_of(ch, k, 0), buffers[ch][0].at[k], wl.at[ch, 0, k])

        def load_made(k, own_m):
            for j in (0,) if own_m == 0 else range(1, m_size):
                for ch in range(count):
                    if (diag and CHUNKS[ch][2]) or (j == 0 and not CHUNKS[ch][2]):
                        load_mine(ch, j, k).start()

        def to_owner(source, home, far, ch, j, k):
            if diag:
                send(lambda: (source(1 - c), home(), ws.at[ch, j, k, 0], wr.at[ch, j, k, 0], net.to(c=1 - c)))
            else:
                send(lambda: (source(c), far(), ws.at[ch, j, k, 0], wr.at[ch, j, k, 1], net.to(t=1 - t)))
                send(
                    lambda: (source(1 - c), far(), ws.at[ch, j, k, 1], wr.at[ch, j, k, 1], net.to(c=1 - c, t=1 - t))
                )

        def owners_part(ch, j, k):
            home, far = buffers[ch][0], buffers[ch][1]
            to_owner(lambda cc: rows_of(ch, k, j, cc), lambda: home.at[j, k], lambda: far.at[j, k], ch, j, k)

        def others(ch, k):
            for j in range(1, m_size):
                owners_part(ch, j, k)

        def same(ch, k):
            owners_part(ch, 0, k)

        def across(ch, k):
            for j in range(1, m_size):
                send(
                    lambda j=j: (
                        rows_of(ch, k, j),
                        buffers[ch][1].at[j - 1, k],
                        fs.at[ch, j, k],
                        fr.at[ch, j, k],
                        net.to(m=m ^ j),
                    )
                )

        def collected(home, far, ch, j, k):
            if not diag:
                net.landed(home, wr.at[ch, j, k, 0])
            elif CHUNKS[ch][2]:
                load_mine(ch, j, k).wait()
            net.landed(far, wr.at[ch, j, k, 1])

        def middle(ch, k):
            home, far, mid, far_m, _ = buffers[ch]
            for j in range(1, m_size):
                collected(home.at[j, k], far.at[j, k], ch, j, k)
                add_rows(mid.at[j - 1, k], [home.at[j, k], far.at[j, k]])
                send(
                    lambda j=j: (
                        mid.at[j - 1, k],
                        far_m.at[j - 1, k],
                        xs.at[ch, j, k],
                        xr.at[ch, j, k],
                        net.to(m=m ^ j),
                    )
                )

        def summed(ch, k):
            mine, far_m, both, home, far, _ = buffers[ch]
            load_mine(ch, 0, k).wait()
            for j in range(1, m_size):
                net.landed(far_m.at[j - 1, k], fr.at[ch, j, k])
            for cc in range(2):
                add_rows(both.at[k, cc], [mine.at[k, cc]] + [far_m.at[j - 1, k, cc] for j in range(1, m_size)])
            to_owner(lambda cc: both.at[k, cc], lambda: home.at[k], lambda: far.at[k], ch, 0, k)

        def finish(ch, k):
            if CHUNKS[ch][2]:
                home, far, _, far_m, result = buffers[ch]
                collected(home.at[0, k], far.at[0, k], ch, 0, k)
                for j in range(1, m_size):
                    net.landed(far_m.at[j - 1, k], xr.at[ch, j, k])
                sources = [home.at[0, k], far.at[0, k]] + [far_m.at[j - 1, k] for j in range(1, m_size)]
            else:
                _, _, both, home, far, result = buffers[ch]
                collected(home.at[k], far.at[k], ch, 0, k)
                sources = [both.at[k, c] if diag else home.at[k], far.at[k]]
            add_rows(result.at[k], sources)
            if k == 0:
                pltpu.make_async_copy(result.at[k], owned(ch, z), zl.at[ch]).start()
                return
            hop, through = {1: (1, None), 2: (3, 2), 3: (3, None)}[k] if inner else {1: (1, None), 2: (1, 0), 3: (1, 1)}[k]
            if through is None:
                send(lambda: (result.at[k], owned(ch, z), zs.at[ch, k], zr.at[ch, k], net.to(z=z ^ hop)))
            else:
                send(
                    lambda: (
                        result.at[k],
                        relay[ch].at[through],
                        zs.at[ch, k],
                        pr.at[ch, through],
                        net.to(z=z ^ hop),
                    )
                )

        def pass_on(through):
            hop, k = ((3, 2), (3, None), (1, 2), (1, 3))[through]

            def run(ch, _):
                net.landed(relay[ch].at[through], pr.at[ch, through])

                def parts():
                    if k is None:
                        dst, recv_sem = relay[ch].at[3], pr.at[ch, 3]
                    else:
                        dst, recv_sem = owned(ch, z ^ hop ^ k), zr.at[ch, k]
                    return relay[ch].at[through], dst, ps.at[ch, through], recv_sem, net.to(z=z ^ hop)

                send(parts)

            return run

        def rows_first(k, h):
            if h == 0:
                pltpu.make_async_copy(keep.at[z ^ k], kept.at[k], kl.at[k]).wait()
            net.landed(got.at[k, span(h)], gr.at[k, h])
            add_rows(kept.at[k, span(h)], [kept.at[k, span(h)], got.at[k, span(h)]])
            if k and not inner:
                slot = {1: 0, 2: 1, 3: 2}[k]
                send(
                    lambda: (
                        kept.at[k, span(h)],
                        got_z.at[slot, span(h)],
                        as_.at[k, h],
                        ar.at[slot, h],
                        net.to(z=z ^ 1),
                    )
                )

        def rows_through(k, h, slot, there, hop):
            net.landed(got_z.at[slot, span(h)], ar.at[slot, h])
            add_rows(kept.at[k, span(h)], [kept.at[k, span(h)], got_z.at[slot, span(h)]])
            send(
                lambda: (
                    kept.at[k, span(h)],
                    got_z.at[there, span(h)],
                    as_.at[k, h],
                    ar.at[there, h],
                    net.to(z=z ^ hop),
                )
            )

        def rows_inner(k, h):
            rows_through(k, h, {3: 1, 2: 2}[k], {3: 3, 2: 4}[k], 3)

        def rows_outer(h, _):
            rows_through(1, h, 4, 0, 1)

        def rows_back(h, _):
            slots = (0, 3) if inner else (0,)
            for slot in slots:
                net.landed(got_z.at[slot, span(h)], ar.at[slot, h])
            add_rows(final.at[h], [kept.at[0, span(h)]] + [got_z.at[slot, span(h)] for slot in slots])
            if diag and h == 0:
                pltpu.make_async_copy(final.at[h], rows_out.at[0], yl).start()
            elif diag:
                send(lambda: (final.at[h], rows_out.at[0], ys.at[h], yr.at[0], net.to(t=1 - t)))
            elif h == 0:
                send(lambda: (final.at[h], rows_out.at[1], ys.at[h], yr.at[1], net.to(c=1 - c)))
            else:
                send(lambda: (final.at[h], rows_out.at[1], ys.at[h], yr.at[1], net.to(c=1 - c, t=1 - t)))

        runs = [swap, load_made, others, same, across, rows_first, rows_inner, rows_outer, rows_back]
        runs += [middle, summed, finish] + [pass_on(i) for i in range(4)] + [small_next]

        def run(codes):
            for code in codes:
                runs[code // 100](code // 10 % 10, code % 10)

        def end():
            while state["small"] < len(steps):
                small_next()
            small_out[...] = current[flat]
            for ch in range(count):
                for k in range(1, Z):
                    net.landed(owned(ch, z ^ k), zr.at[ch, k])
                pltpu.make_async_copy(owned(ch, z), owned(ch, z), zl.at[ch]).wait()
            net.landed(rows_out.at[1], yr.at[1])
            if diag:
                pltpu.make_async_copy(final.at[0], rows_out.at[0], yl).wait()
            else:
                net.landed(rows_out.at[0], yr.at[0])
            for parts in sent:
                net.copy(*parts()).wait_send()

        return small_send, run, end

    programs = {key: program(*key) for key in SCATTER_ORDER}
    cuts = {
        key: [i for i, code in enumerate(codes) if code // 100 == 1] + [len(codes)]
        for key, codes in SCATTER_ORDER.items()
    }

    def begin(inner, diag):
        _, run, _ = programs[inner, diag]
        run(SCATTER_ORDER[inner, diag][: cuts[inner, diag][0]])

    def part(i, inner, diag):
        lo, hi = cuts[inner, diag][i : i + 2]
        programs[inner, diag][1](SCATTER_ORDER[inner, diag][lo:hi])

    by_class(inner_z, role, begin)
    small_terms()
    by_class(inner_z, role, lambda inner, diag: programs[inner, diag][0]())
    if fused:

        @pl.loop(0, 2 * Z)
        def _(i):
            make(i)
            for n in range(2 * Z):

                @pl.when(i == n)
                def _(n=n):
                    by_class(inner_z, role, functools.partial(part, n))

    else:
        for n in range(2 * Z):
            by_class(inner_z, role, functools.partial(part, n))
    by_class(inner_z, role, lambda inner, diag: programs[inner, diag][2]())


def scatter(factors, keep, give, sums, m_size, rows):
    one, two, acts, att, d_attn, act, d_pre = factors
    width = keep.shape[1]
    block = width // (2 * Z * m_size)
    seq = keep.shape[0] // Z
    cols = [2 * HEAD_DIM, 2 * HEAD_DIM, act.shape[1], act.shape[1]]
    parts = [cols[array] // PARTS[array] for array, _, _ in CHUNKS]
    count = len(CHUNKS)
    fused = m_size == 2 and 2 * block % 256 == 0
    sem = pltpu.SemaphoreType.DMA
    vmem = lambda *shape: pltpu.VMEM(shape, bf16)
    doubling = m_size.bit_length() - 1 + 4
    in_place = pl.BlockSpec(memory_space=pl.ANY)
    in_vmem = pl.BlockSpec(memory_space=pltpu.VMEM)
    far = m_size - 1
    term_shapes = [jax.ShapeDtypeStruct((Z, m_size, 2, block, n), bf16) for n in cols]
    out_shape = [jax.ShapeDtypeStruct((Z, block, n), bf16) for n in cols]
    out_shape += [jax.ShapeDtypeStruct((2, rows, width), bf16), jax.ShapeDtypeStruct((16, 128), f32)]
    out_specs = [in_place] * 5 + [in_vmem]
    if fused:
        inputs = [one, two, acts, att, d_attn, act, d_pre]
        in_specs = [in_place] * 3 + [in_vmem] * 4
        out_shape, out_specs = term_shapes + out_shape, [in_place] * 4 + out_specs
    else:
        inputs = [g.reshape(s.shape) for g, s in zip(run_grads(*factors), term_shapes)]
        in_specs = [in_place] * 4
    scratch = []
    for n, (_, _, m_first) in zip(parts, CHUNKS):
        if m_first:
            scratch += [vmem(m_size, Z, block, n)] * 2 + [vmem(far, Z, block, n)] * 2 + [vmem(Z, block, n)]
        else:
            scratch += [vmem(Z, 2, block, n), vmem(far, Z, 2, block, n), vmem(Z, 2, block, n)]
            scratch += [vmem(Z, block, n)] * 3
    scratch += [vmem(4, block, n) for n in parts]
    scratch += [vmem(Z, seq, width)] * 2 + [vmem(5, seq, width), vmem(2, rows, width)]
    scratch += [pltpu.VMEM((4 * m_size * Z, 16, 128), f32)] * 2
    scratch += [
        sem((Z, 2)),
        sem((Z, 2)),
        sem((Z,)),
        sem((Z, 2)),
        sem((5, 2)),
        sem((2,)),
        sem((2,)),
        sem,
        sem((count, m_size, Z, 2)),
        sem((count, m_size, Z, 2)),
        sem((count, m_size, Z)),
        sem((count, m_size, Z)),
        sem((count, m_size, Z)),
        sem((count, m_size, Z)),
        sem((count, m_size, Z)),
        sem((count, Z)),
        sem((count, Z)),
        sem((count,)),
        sem((count, 4)),
        sem((count, 4)),
        sem((doubling,)),
        sem((doubling,)),
    ]
    if fused:
        scratch.append(vmem(2, 3, keep.shape[0], 2 * block))
        made = [vmem(2, block, n) for n in cols]
        scratch_made = [sem((2, 3)), sem((4,))]
    outs = pl.pallas_call(
        functools.partial(scatter_entry, m_size, fused),
        out_shape=out_shape,
        in_specs=in_specs + [in_place] * 2 + [in_vmem] * 4,
        out_specs=out_specs,
        scratch_shapes=scratch + (made + scratch_made if fused else []),
        compiler_params=pltpu.CompilerParams(collective_id=1, has_side_effects=True, vmem_limit_bytes=67043328),
        name="scatter_all",
    )(*inputs, keep.reshape(Z, seq, width), give.reshape(Z, seq, width), *sums)
    outs = outs[4:] if fused else outs
    return outs[:4], outs[4], outs[5]


def scatter_entry(m_size, fused, *refs):
    if fused:
        refs = refs[:-6] + (refs[-6:-2],) + refs[-2:]
    scatter_kernel(m_size, fused, *refs)


def update_kernel(*refs):
    rows, cotangent, back, bias, qk, vo, up, dn = refs[:8]
    block_out, input_grad = refs[14:16]
    normed, inverse = layer_stats(rows[...])
    block_out[...] = rows[...] + back[0].astype(f32) + bias[...]
    u = back[1].astype(f32)
    input_grad[...] = cotangent[...] + inverse * (
        u
        - jnp.mean(u, axis=-1, keepdims=True)
        - normed * jnp.mean(u * normed, axis=-1, keepdims=True)
    )
    for sources, (weight, one, two), outs in (
        ((qk, qk, vo, vo), refs[8:11], refs[16:20]),
        ((up, dn), refs[11:14], refs[20:24]),
    ):
        kinds, wide = weight.shape[1], weight.shape[2] // Z
        for j in range(kinds):
            at = j % (kinds // 2) * wide
            for q in range(Z):
                cols = slice(q * wide, (q + 1) * wide)
                g = sources[j][q, :, at : at + wide].astype(f32)
                updated = adam_step(weight[:, j, cols], g, one[:, j, cols], two[:, j, cols])
                for ref, value in zip(outs, (g, *updated)):
                    ref[:, j, cols] = value


def update(block_in, out_grad, own_rows, bias, own, attn, mlp):
    rows, width = block_in.shape
    shard = attn[0].shape[0]
    step = min(shard, 16)
    steps = shard // step
    by_rows = pl.BlockSpec((rows // steps, width), lambda i: (i, 0))
    block = lambda v: pl.BlockSpec((step,) + v.shape[1:], lambda i: (i, 0, 0))
    return pl.pallas_call(
        update_kernel,
        grid=(steps,),
        in_specs=[by_rows, by_rows, pl.BlockSpec((2, rows // steps, width), lambda i: (0, i, 0)), fixed(1, width)]
        + [pl.BlockSpec((Z, step, g.shape[2]), lambda i: (0, i, 0)) for g in own]
        + [block(v) for v in (*attn, *mlp)],
        out_specs=[by_rows, by_rows] + [block(attn[0])] * 4 + [block(mlp[0])] * 4,
        out_shape=[jax.ShapeDtypeStruct((rows, width), f32)] * 2
        + [jax.ShapeDtypeStruct(attn[0].shape, f32)] * 4
        + [jax.ShapeDtypeStruct(mlp[0].shape, f32)] * 4,
        compiler_params=pltpu.CompilerParams(vmem_limit_bytes=VMEM_BYTES),
        name="update",
    )(block_in, out_grad, own_rows, bias, *own, *attn, *mlp)


def body(
    block_in,
    positions,
    out_grad,
    attn_weight,
    mlp_weight,
    small_params,
    attn_first,
    attn_second,
    mlp_first,
    mlp_second,
    small_first,
    small_second,
):
    m_size = lax.axis_size("dp") // (2 * Z)
    diag = lax.axis_index("dp") % 2 == lax.axis_index("tensor")
    rows = block_in.shape[0]
    part = small_params.shape[1]
    weights, acts, norms, (attended, d_attn, activation, d_pre), (head_sums, up_sums), par, row_bias, out_sum = gather(
        attn_weight, mlp_weight, block_in, out_grad, small_params, positions, m_size
    )
    keep, give, norm_sums = run_outs(diag, attended, d_attn, activation, d_pre, acts, weights, par)
    factors = (*norms, acts, attended, d_attn, activation, d_pre)
    sums = (norm_sums, head_sums, up_sums, out_sum)
    own, own_rows, own_small = scatter(factors, keep, give, sums, m_size, rows)
    attn = (attn_weight, attn_first, attn_second)
    mlp = (mlp_weight, mlp_first, mlp_second)
    block_out, input_grad, *updated = update(block_in, out_grad, own_rows, row_bias, own, attn, mlp)
    attn_out, mlp_out = updated[:4], updated[4:]
    small_grad = own_small[:12, :part]
    small_new, small_first_new, small_second_new = adam_step(small_params, small_grad, small_first, small_second)

    attn_grad, attn_new, attn_first_new, attn_second_new = attn_out
    mlp_grad, mlp_new, mlp_first_new, mlp_second_new = mlp_out
    return (
        block_out,
        input_grad,
        attn_grad,
        mlp_grad,
        small_grad,
        attn_new,
        attn_first_new,
        attn_second_new,
        mlp_new,
        mlp_first_new,
        mlp_second_new,
        small_new,
        small_first_new,
        small_second_new,
    )


def solution(mesh):
    rows = P(("dp", "tensor"), None)
    weights = P("dp", None, "tensor")
    small = P(None, ("dp", "tensor"))
    return jax.shard_map(
        body,
        mesh=mesh,
        in_specs=(rows, P("dp", None), rows, weights, weights, small, weights, weights, weights, weights, small, small),
        out_specs=(rows, rows) + (weights,) * 2 + (small,) + (weights,) * 6 + (small,) * 3,
        check_vma=False,
    )
```

```python
import functools
import math

import jax
import jax.numpy as jnp
from jax import lax
from jax.experimental import pallas as pl
from jax.experimental.pallas import tpu as pltpu
from jax.sharding import PartitionSpec as P

ROT = 64
ADAM_STEP = 3
HEAD_DIM = 256
Z = 4

norm_epsilon = 1e-05
learn_rate = 0.006
beta_first = 0.9
beta_second = 0.95
adam_epsilon = 1e-08
weight_decay = 0.1

f32 = jnp.float32
bf16 = jnp.bfloat16


def layer_stats(row_data):
    center = row_data - jnp.mean(row_data, axis=-1, keepdims=True)
    inverse = lax.rsqrt(jnp.mean(center * center, axis=-1, keepdims=True) + norm_epsilon)
    return (center * inverse, inverse)


def adam_step(weight, gradient, moment_one, moment_two):
    one_new = beta_first * moment_one + (1.0 - beta_first) * gradient
    two_new = beta_second * moment_two + (1.0 - beta_second) * gradient * gradient
    corrected = (one_new * (1.0 / (1.0 - beta_first**ADAM_STEP))) / (
        jnp.sqrt(two_new * (1.0 / (1.0 - beta_second**ADAM_STEP))) + adam_epsilon
    )
    return (weight - learn_rate * (corrected + weight_decay * weight), one_new, two_new)


MESH = pl.DeviceIdType.MESH
PARTS = (1, 1, 2, 2)
CHUNKS = ((0, 0, True), (1, 0, False), (2, 0, True), (2, 1, False), (3, 0, True), (3, 1, False))
GATHER_ORDER = {
    (False, False): (
        1201, 0, 10, 1200, 500, 510, 900, 501, 700, 1202, 20, 511, 520, 530, 540, 550, 600, 601, 1100, 910, 1101,
        620, 640, 801, 1110, 710, 30, 40, 50, 521, 502, 621, 610, 512, 602, 503, 611, 1010, 603, 630, 1111, 1011,
        811, 1030, 650, 531, 920, 1000, 541, 1050, 1001, 551, 641, 930, 1020, 1040, 940, 802, 1120, 522, 1021, 513,
        612, 622, 1002, 1012, 812, 1121, 631, 1003, 532, 542, 651, 1031, 552, 1041, 642, 613, 1051, 1022, 632, 803,
        652, 1042, 1013, 1203, 523, 1032, 1130, 1204, 533, 1052, 1205, 623, 1131, 1023, 813, 1206, 543, 553, 633,
        1207, 1208, 643, 653, 1033, 1209, 1043, 1210, 1053, 1211, 1212, 1213, 1214,
    ),
    (False, True): (
        1201, 0, 10, 1200, 700, 1202, 20, 500, 501, 510, 520, 530, 540, 550, 610, 900, 511, 1100, 600, 710, 30, 40,
        50, 601, 611, 630, 650, 1000, 1001, 620, 1020, 640, 801, 1040, 1010, 521, 910, 1110, 1011, 502, 1101, 1030,
        1050, 621, 1021, 811, 602, 1002, 531, 541, 551, 1111, 641, 631, 512, 612, 930, 920, 651, 1031, 1041, 1012,
        802, 940, 522, 1051, 503, 1120, 622, 603, 1003, 1022, 812, 532, 542, 1121, 632, 552, 642, 513, 613, 652,
        1032, 1042, 1013, 1203, 803, 1204, 523, 1052, 1130, 1205, 623, 813, 533, 633, 1023, 543, 1033, 553, 643,
        1131, 1206, 653, 1207, 1208, 1043, 1209, 1053, 1210, 1211, 1212, 1213, 1214,
    ),
    (True, False): (
        1201, 0, 10, 1200, 500, 510, 900, 200, 503, 700, 1202, 20, 520, 530, 540, 550, 600, 603, 100, 300, 1100, 501,
        513, 210, 310, 1101, 620, 110, 400, 640, 511, 910, 601, 710, 30, 40, 50, 803, 1130, 610, 523, 801, 320, 1110,
        220, 1010, 502, 630, 120, 623, 410, 521, 602, 512, 650, 1000, 1030, 1003, 621, 1131, 811, 1050, 613, 813,
        230, 1111, 533, 1020, 130, 1013, 330, 1040, 531, 920, 543, 611, 240, 340, 930, 140, 1001, 643, 553, 541, 350,
        250, 1011, 150, 1023, 940, 551, 641, 1002, 802, 420, 1120, 1021, 522, 633, 612, 622, 631, 1033, 1043, 1012,
        1203, 653, 1031, 430, 812, 1121, 1204, 532, 651, 1041, 1205, 1022, 1053, 440, 1206, 542, 632, 1051, 450,
        1207, 552, 1208, 642, 1032, 1209, 652, 1210, 1042, 1211, 1052, 1212, 1213, 1214,
    ),
    (True, True): (
        1201, 0, 10, 1200, 700, 1202, 20, 500, 503, 510, 520, 530, 540, 550, 610, 200, 900, 100, 300, 1100, 600, 501,
        513, 710, 30, 40, 50, 603, 630, 650, 1000, 1003, 613, 210, 310, 620, 110, 1020, 640, 511, 1040, 611, 1010,
        601, 1001, 803, 1101, 1030, 523, 1050, 801, 320, 1130, 1013, 220, 400, 1110, 120, 502, 1011, 521, 910, 623,
        1023, 602, 1002, 621, 813, 533, 811, 1021, 330, 230, 1111, 543, 1131, 130, 633, 340, 531, 643, 631, 553, 240,
        930, 920, 1033, 350, 140, 410, 541, 1043, 1031, 653, 512, 612, 250, 940, 150, 641, 551, 651, 1053, 1041, 802,
        1012, 1203, 1051, 420, 1120, 1204, 522, 1205, 622, 1022, 812, 430, 532, 1121, 1206, 632, 440, 1207, 542,
        1208, 1032, 450, 1209, 552, 642, 1210, 652, 1042, 1211, 1212, 1052, 1213, 1214,
    ),
}
SCATTER_ORDER = {
    (False, False): (
        30, 31, 20, 21, 10, 11, 0, 1, 131, 530, 531, 520, 521, 510, 511, 500, 501, 1600, 203, 413, 223, 433, 243,
        453, 121, 1610, 202, 412, 222, 432, 242, 903, 452, 111, 923, 1620, 201, 411, 221, 431, 241, 451, 101, 943,
        1630, 200, 410, 220, 430, 240, 450, 130, 902, 1013, 922, 1033, 303, 323, 343, 120, 942, 1053, 302, 322, 342,
        110, 901, 1012, 921, 301, 321, 341, 100, 800, 1032, 900, 941, 300, 320, 340, 920, 940, 1052, 1113, 810, 1133,
        1011, 1103, 1031, 1123, 1051, 1153, 1143, 1640, 1010, 1112, 1030, 1050, 1102, 1132, 1122, 1142, 1101, 1121,
        1152, 1100, 1141, 1120, 1111, 1140, 1131, 1151, 1110, 1130, 1150,
    ),
    (False, True): (
        30, 31, 20, 21, 10, 11, 0, 1, 131, 530, 531, 520, 521, 510, 511, 500, 501, 1600, 203, 413, 223, 433, 243,
        453, 121, 903, 1610, 202, 412, 222, 432, 242, 452, 111, 923, 201, 411, 221, 431, 241, 451, 101, 943, 1620,
        902, 200, 410, 220, 430, 240, 450, 130, 1013, 922, 1033, 1630, 303, 323, 942, 343, 120, 901, 1053, 302, 322,
        342, 110, 921, 301, 321, 341, 100, 1012, 900, 800, 941, 300, 320, 340, 920, 1032, 940, 1113, 1052, 1133, 810,
        1103, 1011, 1123, 1031, 1153, 1051, 1143, 1102, 1640, 1112, 1010, 1030, 1132, 1050, 1122, 1142, 1101, 1152,
        1121, 1100, 1141, 1111, 1120, 1131, 1140, 1151, 1110, 1130, 1150,
    ),
    (True, False): (
        30, 31, 20, 21, 10, 11, 0, 1, 131, 530, 531, 520, 521, 510, 511, 500, 501, 1600, 203, 413, 223, 433, 243,
        453, 121, 1610, 202, 412, 222, 432, 242, 903, 620, 452, 111, 923, 1620, 201, 411, 221, 431, 241, 451, 101,
        943, 200, 410, 220, 430, 240, 450, 130, 621, 700, 902, 1013, 922, 1033, 942, 1053, 303, 323, 343, 120, 901,
        1012, 921, 302, 322, 342, 110, 630, 710, 900, 1032, 941, 301, 321, 341, 100, 920, 300, 320, 340, 940, 1052,
        631, 1113, 1133, 1153, 1011, 1103, 800, 1123, 1031, 1112, 1051, 1143, 810, 1630, 1310, 1010, 1330, 1410,
        1300, 1132, 1030, 1640, 1320, 1510, 1350, 1050, 1530, 1340, 1102, 1500, 1210, 1122, 1430, 1200, 1142, 1520,
        1230, 1101, 1550, 1220, 1121, 1540, 1152, 1240, 1100, 1400, 1111, 1141, 1131, 1120, 1420, 1151, 1250, 1140,
        1440, 1110, 1130, 1450, 1150,
    ),
    (True, True): (
        30, 31, 20, 21, 10, 11, 0, 1, 131, 530, 531, 520, 521, 510, 511, 500, 501, 1600, 203, 413, 223, 433, 243,
        453, 121, 903, 1610, 202, 412, 620, 222, 432, 242, 452, 111, 923, 943, 201, 411, 221, 431, 241, 451, 101,
        902, 1620, 200, 410, 220, 430, 240, 450, 130, 621, 700, 1013, 922, 1033, 942, 901, 1053, 303, 323, 343, 120,
        921, 302, 322, 342, 110, 630, 710, 900, 1012, 941, 301, 321, 341, 920, 100, 1032, 940, 300, 320, 340, 1113,
        1052, 631, 1133, 1153, 1103, 1123, 1011, 800, 1143, 1112, 1031, 1051, 810, 1630, 1102, 1310, 1330, 1132,
        1010, 1300, 1410, 1640, 1320, 1400, 1030, 1350, 1510, 1340, 1530, 1050, 1200, 1430, 1122, 1210, 1500, 1142,
        1230, 1520, 1101, 1220, 1152, 1550, 1121, 1240, 1111, 1540, 1100, 1131, 1141, 1250, 1151, 1420, 1120, 1140,
        1440, 1110, 1130, 1150, 1450,
    ),
}


class Links:
    def __init__(self, m_size):
        self.m_size = m_size
        index = lax.axis_index("dp")
        self.z, self.m, self.c = index // (2 * m_size), (index // 2) % m_size, index % 2
        self.t = lax.axis_index("tensor")
        self.sends = []

    def to(self, z=None, m=None, c=None, t=None):
        z, m, c = (own if v is None else v for v, own in ((z, self.z), (m, self.m), (c, self.c)))
        return ((z * self.m_size + m) * 2 + c, self.t if t is None else t)

    def copy(self, src, dst, send_sem, recv_sem, target):
        return pltpu.make_async_remote_copy(
            src_ref=src, dst_ref=dst, send_sem=send_sem, recv_sem=recv_sem, device_id=target, device_id_type=MESH
        )

    def send(self, src, dst, send_sem, recv_sem, target):
        one = self.copy(src, dst, send_sem, recv_sem, target)
        one.start()
        self.sends.append(one)

    def landed(self, dst, recv_sem):
        self.copy(dst, dst, recv_sem, recv_sem, self.to(c=1 - self.c)).wait_recv()

    def drain(self):
        for one in self.sends:
            one.wait_send()
        self.sends = []

    def partners(self):
        other = 1 - self.t
        out = [self.to(z=self.z ^ k) for k in range(1, Z)]
        out += [self.to(m=self.m ^ j) for j in range(1, self.m_size)]
        out += [self.to(c=1 - self.c), self.to(t=other), self.to(c=1 - self.c, t=other)]
        return out

    def doubling(self):
        high = self.z // 2
        place = ((self.m * 2 + self.c) * 2 + self.t) * 4 + lax.rem(self.z + high, 2) * 2 + high
        steps = [(1, self.to(z=self.z ^ 3)), (2, self.to(z=self.z ^ 1)), (4, self.to(t=1 - self.t))]
        steps.append((8, self.to(c=1 - self.c)))
        j = 1
        while j < self.m_size:
            steps.append((16 * j, self.to(m=self.m ^ j)))
            j *= 2
        return place, steps

    def meet(self):
        barrier = pltpu.get_barrier_semaphore()
        everyone = self.partners()
        for target in everyone:
            pl.semaphore_signal(barrier, inc=1, device_id=target, device_id_type=MESH)
        pl.semaphore_wait(barrier, len(everyone))


def gather_kernel(m_size, *refs):
    weights, rows_in, small, positions = refs[:2], refs[2:4], refs[4], refs[5]
    full, act_out, one_out, two_out = refs[6:10], refs[10], refs[11], refs[12]
    att, d_attn, hidden_out, d_pre, head_sums, up_sums, par, row_bias, out_sum = refs[13:22]
    count = len(CHUNKS)
    stage, stage_m, relay = (refs[22 + i * count : 22 + (i + 1) * count] for i in range(3))
    refs = refs[22 + 3 * count :]
    (zs, zr, gs, gr, ps, pr, ms, mr, near_s, far_s, xr, as_, ar, ws, wr, ss, sr, lin, lout, ls, os_) = refs[:21]
    pieces, refs = refs[21 : 21 + count], refs[21 + count :]
    act, w_qk, w_vo, one_v, two_v, tile_v, slope, bias, up_bias, table, base, attn_v, mlp_v, rows_v, low = refs
    net = Links(m_size)
    z, m, c, t = net.z, net.m, net.c, net.t
    rows = pieces[0].shape[1]
    half = low.shape[1]
    seq = 2 * half
    width = low.shape[2]
    n = HEAD_DIM
    role = lax.rem(c + t, 2)
    inner_z = lax.rem(z + z // 2, 2)

    def columns(ch):
        array, part, _ = CHUNKS[ch]
        wide = pieces[ch].shape[2]
        return array, slice(part * wide, (part + 1) * wide)

    def piece(ch, zz):
        return pieces[ch].at[zz]

    def whole(ch, zz, mm, cc, size=1):
        array, cols = columns(ch)
        start = ((zz * m_size + mm) * 2 + cc) * rows
        return full[array].at[pl.ds(pl.multiple_of(start, rows), size * rows), cols]

    own_place = pl.ds(pl.multiple_of(z * seq + t * half, half), half)
    place = lambda zz, h: pl.ds(pl.multiple_of(zz * seq + (t ^ h) * half, half), half)

    def store_own(ch):
        return pltpu.make_async_copy(pieces[ch].at[z], whole(ch, z, m, c), lout.at[ch])

    def inputs():
        pairs = [(weights[0].at[:, j, :], attn_v.at[j]) for j in range(4)]
        pairs += [(rows_in[i], rows_v.at[i]) for i in range(2)]
        pairs += [(weights[1].at[:, j, :], mlp_v.at[j]) for j in range(2)]
        return [pltpu.make_async_copy(src, dst, lin.at[i]) for i, (src, dst) in enumerate(pairs)]

    for one in inputs():
        one.start()
    flat, steps = net.doubling()
    table[flat] = jnp.zeros(table.shape[1:], f32)
    table[flat, 0:12, 0 : small.shape[1]] = small[...]
    for e in range(seq // 128):
        table[flat, 12 + e : 13 + e, :] = positions[:, e * 128 : (e + 1) * 128].astype(f32)
    net.meet()

    def program(inner, diag):
        state = {"small": 0}
        sent = []

        def send(parts):
            net.copy(*parts()).start()
            sent.append(parts)

        def small_send():
            i = state["small"]
            if i < len(steps):
                size, target = steps[i]

                def parts():
                    span = table.at[pl.ds(flat // size * size, size)]
                    return span, span, ss.at[i], sr.at[i], target

                send(parts)

        def small_next(*_):
            i = state["small"]
            if i < len(steps):
                size = steps[i][0]
                net.landed(table.at[pl.ds((flat // size ^ 1) * size, size)], sr.at[i])
                state["small"] += 1
                small_send()

        def small_last():
            while state["small"] < len(steps):
                small_next()

        def spot(ch, zz, j):
            if diag:
                return whole(ch, zz, m ^ j, c)
            return stage_m[ch].at[m ^ j, zz] if j else stage[ch].at[zz]

        def source(ch, k, j):
            return piece(ch, z) if k == 0 and j == 0 else spot(ch, z ^ k, j)

        def spread(ch, k, j):
            block = lambda: whole(ch, z ^ k, m ^ j, c)
            send(
                lambda: (
                    source(ch, k, j),
                    block(),
                    ps.at[ch, j, k, 1],
                    pr.at[ch, j, k, c],
                    net.to(c=t, t=1 - t),
                )
            )
            if not diag:
                send(
                    lambda: (source(ch, k, j), block(), ps.at[ch, j, k, 0], pr.at[ch, j, k, c], net.to(c=1 - c))
                )

        def spread_landed(ch, k, j):
            for cc in (1 - c,) if diag else (1 - c, c):
                net.landed(whole(ch, z ^ k, m ^ j, cc), pr.at[ch, j, k, cc])

        def swap(h, k):
            def parts():
                src = act.at[role, place(z ^ k, h)]
                return src, src, ws.at[k, h], wr.at[k, h], net.to(c=1 - c)

            send(parts)

        def rows_on(h, flip, i, hop, k):
            def parts():
                src = act.at[role, place(z ^ flip, h)]
                return src, src, as_.at[h, i], ar.at[h, k], net.to(z=z ^ hop)

            send(parts)

        def quarters(ch, _):
            for i, (k, hop, through) in enumerate(
                ((3, 3, None), (2, 3, 2), (1, 1, None)) if inner else ((3, 1, 1), (2, 1, 0), (1, 1, None))
            ):

                def parts(i=i, k=k, hop=hop, through=through):
                    if through is None:
                        dst, recv_sem = spot(ch, z, 0), zr.at[ch, k]
                    else:
                        dst, recv_sem = relay[ch].at[through], gr.at[ch, through]
                    return piece(ch, z ^ k), dst, zs.at[ch, i], recv_sem, net.to(z=z ^ hop)

                send(parts)

        def pass_on(through):
            hop, k = ((3, 2), (3, None), (1, 2), (1, 3))[through]

            def run(ch, _):
                net.landed(relay[ch].at[through], gr.at[ch, through])

                def parts():
                    if k is None:
                        dst, recv_sem = relay[ch].at[3], gr.at[ch, 3]
                    else:
                        dst, recv_sem = spot(ch, z ^ hop ^ k, 0), zr.at[ch, k]
                    return relay[ch].at[through], dst, gs.at[ch, through], recv_sem, net.to(z=z ^ hop)

                send(parts)

            return run

        def first(ch, k):
            if k:
                net.landed(spot(ch, z ^ k, 0), zr.at[ch, k])
            elif diag:
                store_own(ch).start()
            if CHUNKS[ch][2]:
                for j in range(1, m_size):

                    def parts(j=j):
                        dst = whole(ch, z ^ k, m, c) if diag else stage_m[ch].at[m, z ^ k]
                        return source(ch, k, 0), dst, ms.at[ch, j, k], mr.at[ch, j, k], net.to(m=m ^ j)

                    send(parts)
            spread(ch, k, 0)

        def second(ch, k):
            if CHUNKS[ch][2]:
                for j in range(1, m_size):
                    net.landed(spot(ch, z ^ k, j), mr.at[ch, j, k])
                    spread(ch, k, j)
            else:
                if diag and k == 0:
                    store_own(ch).wait()
                spread_landed(ch, k, 0)
                for j in range(1, m_size):

                    def parts(j=j):
                        both = whole(ch, z ^ k, m, 0, 2)
                        return both, both, ms.at[ch, j, k], mr.at[ch, j, k], net.to(m=m ^ j)

                    send(parts)

        def third(ch, k):
            if CHUNKS[ch][2]:
                for j in range(m_size):
                    spread_landed(ch, k, j)
                if diag and k == 0:
                    store_own(ch).wait()
            else:
                for j in range(1, m_size):
                    net.landed(whole(ch, z ^ k, m ^ j, 0, 2), mr.at[ch, j, k])

        def rows_start(h, _):
            if h:
                net.landed(act.at[0 if diag else 1, place(z, 1)], xr.at[1])
            elif not diag:
                net.landed(act.at[1, place(z, 0)], xr.at[0])
            if inner:
                rows_on(h, 0, 0, 3, 3)
            rows_on(h, 0, 1, 1, 1)
            swap(h, 0)

        def rows_next(h, k):
            net.landed(act.at[role, place(z ^ k, h)], ar.at[h, k])
            if inner:
                hop, there = {1: (3, 2), 3: (1, 2), 2: (1, 3)}[k]
                rows_on(h, k, 1 + k, hop, there)
            swap(h, k)

        def swapped(k, h):
            net.landed(act.at[1 - role, place(z ^ k, h)], wr.at[k, h])

        def rows_out():
            if diag:
                send(lambda: (low.at[1], act.at[1, own_place], near_s, xr.at[0], net.to(c=1 - c)))
            else:
                send(lambda: (low.at[0], act.at[0, own_place], near_s, xr.at[1], net.to(t=1 - t)))
                send(lambda: (low.at[1], act.at[1, own_place], far_s, xr.at[1], net.to(c=1 - c, t=1 - t)))

        runs = [quarters] + [pass_on(i) for i in range(4)]
        runs += [first, second, rows_start, rows_next, small_next, third, swapped]

        def run(codes):
            for code in codes:
                runs[code // 100](code // 10 % 10, code % 10)

        def end():
            for parts in sent:
                net.copy(*parts()).wait_send()

        return small_send, run, rows_out, small_last, end

    programs = {key: program(*key) for key in GATHER_ORDER}
    work = len(runs_before(GATHER_ORDER[True, True]))

    device_rows = functools.partial(table_place, m_size)

    def parameters():
        part = width // (8 * m_size * 2)
        per = 128 // part
        static = table_order(m_size)
        for b in range(width // 128):
            got = [table[static[b * per + e], 0:4, 0:part] for e in range(per)]
            par[:, b * 128 : (b + 1) * 128] = jnp.concatenate(got, axis=1)
        head = c * Z + z
        for b in range(n // 128):
            start = (head * n + b * 128) // part
            got = [table[device_rows(start + e), 4:6, 0:part] for e in range(per)]
            bias[:, b * 128 : (b + 1) * 128] = jnp.concatenate(got, axis=1)
        wide = up_bias.shape[1]
        for b in range(width // 128):
            got = [table[static[b * per + e], 6:8, 0:part] for e in range(per)]
            both = jnp.concatenate(got, axis=1)
            row_bias[:, b * 128 : (b + 1) * 128] = both[0:1] + both[1:2]
        row = 8 + head * wide // width
        for b in range(wide // 128):
            start = (lax.rem(head * wide, width) + b * 128) // part
            got = [table[device_rows(start + e), pl.ds(row, 1), 0:part] for e in range(per)]
            up_bias[:, b * 128 : (b + 1) * 128] = jnp.concatenate(got, axis=1)

    step = 16

    def attn_in():
        for one in inputs()[:4]:
            one.wait()
        wide = attn_v.shape[2] // Z

        @pl.loop(0, rows // step)
        def _(i):
            span = pl.ds(pl.multiple_of(i * step, step), step)
            for j in range(4):
                block = attn_v[j, span, :].astype(bf16)
                for q in range(Z):
                    at = j % 2 * wide
                    pieces[j // 2][q, span, at : at + wide] = block[:, q * wide : (q + 1) * wide]

    def mlp_in():
        for one in inputs()[6:]:
            one.wait()
        wide = mlp_v.shape[2] // (2 * Z)

        @pl.loop(0, rows // step)
        def _(i):
            span = pl.ds(pl.multiple_of(i * step, step), step)
            for j in range(2):
                block = mlp_v[j, span, :].astype(bf16)
                for q in range(2 * Z):
                    pieces[2 + 2 * j + q % 2][q // 2, span, :] = block[:, q * wide : (q + 1) * wide]

    def rows_low():
        for one in inputs()[4:6]:
            one.wait()
        out_sum[...] = jnp.zeros_like(out_sum)

        @pl.loop(0, half // step)
        def _(i):
            start = pl.multiple_of(i * step, step)
            span = pl.ds(start, step)
            normed, _ = layer_stats(rows_v[0, span, :])
            normed = normed.astype(bf16)
            low[0, span, :] = normed
            given = rows_v[1, span, :]
            low[1, span, :] = given.astype(bf16)
            out_sum[...] += jnp.sum(given, axis=0, keepdims=True)

            @pl.when(role == 0)
            def _():
                act[0, pl.ds(pl.multiple_of(z * seq + t * half + start, step), step), :] = normed

    def turns_in():
        for a, value in enumerate(turn_tables(lax.broadcasted_iota(jnp.int32, (seq, 128), 0).astype(f32))):
            for e in range(3):
                term = value.astype(bf16)
                base[:, (3 * a + e) * 128 : (3 * a + e + 1) * 128] = term
                value = value - term.astype(f32)

    def weights_in():
        return [
            pltpu.make_async_copy(full[0], w_qk, ls.at[0]),
            pltpu.make_async_copy(full[1], w_vo, ls.at[1]),
        ]

    def rows_saved(i):
        k = i ^ (inner_z & (i // 2))
        span = pl.ds(pl.multiple_of((z ^ k) * seq, seq), seq)
        return [
            pltpu.make_async_copy(one_v.at[lax.rem(i, 2)], one_out.at[span], os_.at[0, i]),
            pltpu.make_async_copy(two_v.at[span], two_out.at[span], os_.at[1, i]),
            pltpu.make_async_copy(act.at[:, span], act_out.at[:, span], os_.at[2, i]),
        ]

    def attention(i):
        @pl.when(i == 0)
        def _():
            for one in weights_in():
                one.start()
            parameters()
            turns_in()
            head_sums[...] = jnp.zeros_like(head_sums)
            for one in weights_in():
                one.wait()

        @pl.when(i >= 2)
        def _():
            rows_saved(i - 2)[0].wait()

        k = i ^ (inner_z & (i // 2))
        span = pl.ds(pl.multiple_of((z ^ k) * seq, seq), seq)
        x = act[0, span, :].astype(f32)
        one = (x * par[0:1, :] + par[1:2, :]).astype(bf16)
        one_v[lax.rem(i, 2)] = one
        two_v[span, :] = (x * par[2:3, :] + par[3:4, :]).astype(bf16)
        for copy in rows_saved(i):
            copy.start()
        source = device_rows((((z ^ k) * m_size + m) * 2 + t) * 2)
        across = jnp.concatenate([table[source, 12 + e : 13 + e, :] for e in range(seq // 128)], axis=1)
        spots = lax.broadcasted_iota(jnp.int32, (seq, seq), 0).astype(f32)
        hit = jnp.where(spots == across, 1.0, 0.0).astype(bf16)
        down = dot(hit, spots.astype(bf16), 0, 0)
        turns = dot(hit, base[...], 0, 0)
        tables = [sum(turns[:, (3 * a + e) * 128 : (3 * a + e + 1) * 128] for e in range(3)) for a in range(3)]
        scale = HEAD_DIM ** (-0.5)
        qk = dot(one, w_qk[...])
        q = turn(qk[:, :n] + bias[0:1, :], tables, 1.0).astype(bf16)
        k_rows = turn(qk[:, n:], tables, 1.0).astype(bf16)
        v = (dot(one, w_vo[:, :n]) + bias[1:2, :]).astype(bf16)
        d_att = dot(act[1, span, :], w_vo[:, n:]).astype(bf16)
        scores = jnp.where(across <= down, dot(q, k_rows, 1, 1) * scale, -jnp.inf)
        top = jnp.max(scores, axis=-1, keepdims=True)
        log_total = top + jnp.log(jnp.sum(jnp.exp(scores - top), axis=-1, keepdims=True))
        probs = jnp.exp(scores - log_total)
        low_probs = probs.astype(bf16)
        att[span, :] = dot(low_probs, v).astype(bf16)
        d_probs = dot(d_att, v, 1, 1)
        d_scores = (probs * (d_probs - jnp.sum(probs * d_probs, axis=-1, keepdims=True)) * scale).astype(bf16)
        d_q = turn(dot(d_scores, k_rows), tables, -1.0)
        d_k = turn(dot(d_scores, q, 0, 0), tables, -1.0)
        d_v = dot(low_probs, d_att, 0, 0)
        d_attn[span, 0:n] = d_q.astype(bf16)
        d_attn[span, n : 2 * n] = d_k.astype(bf16)
        d_attn[span, 2 * n :] = d_v.astype(bf16)
        head_sums[0:1, :] += jnp.sum(d_q, axis=0, keepdims=True)
        head_sums[1:2, :] += jnp.sum(d_v, axis=0, keepdims=True)

    wide = full[2].shape[1] // Z

    def tile_in(array, j):
        cols = pl.ds(pl.multiple_of(j * wide, wide), wide)
        return pltpu.make_async_copy(full[array].at[:, cols], tile_v.at[lax.rem(j, 2)], ls.at[lax.rem(j, 2)])

    def tile_ready(array, j):
        @pl.when(lax.rem(j, 2) == 0)
        def _():
            tile_in(array, j).start()
            tile_in(array, j + 1).start()

        tile_in(array, j).wait()

    def hidden(i):
        j = i - Z
        tile_ready(2, j)
        cols = pl.ds(pl.multiple_of(j * wide, wide), wide)
        pre = dot(two_v[...], tile_v[lax.rem(j, 2)]) + up_bias[:, cols]
        erf = 1.0 + lax.erf(pre * 0.7071067811865476)
        hidden_out[:, cols] = (0.5 * pre * erf).astype(bf16)
        slope[j] = 0.5 * erf + pre * jnp.exp(-0.5 * pre * pre) * 0.3989422804014327

    def hidden_back(i):
        j = i - 2 * Z
        tile_ready(3, j)
        cols = pl.ds(pl.multiple_of(j * wide, wide), wide)
        value = dot(act[1], tile_v[lax.rem(j, 2)]) * slope[j]
        d_pre[:, cols] = value.astype(bf16)
        up_sums[:, cols] = jnp.sum(value, axis=0, keepdims=True)

    def part(i, inner, diag):
        _, run, rows_out, small_last, _ = programs[inner, diag]
        if i == 1:
            rows_out()
        run(runs_before(GATHER_ORDER[inner, diag])[i + 1])
        if i == 2:
            small_last()

    by_class(inner_z, role, lambda inner, diag: programs[inner, diag][0]())
    ahead = 3

    @pl.loop(0, work - 1)
    def _(i):
        pl.when(i == 0)(attn_in)
        pl.when(i == 1)(rows_low)
        pl.when(i == 2)(mlp_in)
        pl.when((i >= ahead) & (i < ahead + Z))(lambda: attention(i - ahead))
        pl.when((i >= ahead + Z) & (i < ahead + 2 * Z))(lambda: hidden(i - ahead))
        pl.when(i >= ahead + 2 * Z)(lambda: hidden_back(i - ahead))
        for e in range(work - 1):

            @pl.when(i == e)
            def _(e=e):
                by_class(inner_z, role, functools.partial(part, e))

    by_class(inner_z, role, lambda inner, diag: programs[inner, diag][4]())
    for i in range(Z):
        saved = rows_saved(i)
        for copy in saved[1:] if i < 2 else saved:
            copy.wait()


def runs_before(order):
    cuts = [i for i, code in enumerate(order) if code // 100 == 12]
    return [order[lo:hi] for lo, hi in zip([0] + [i + 1 for i in cuts], cuts + [len(order)])]


def table_place(m_size, index):
    z, rest = index // (4 * m_size), index % (4 * m_size)
    return rest * 4 + (z + z // 2) % 2 * 2 + z // 2


def table_order(m_size):
    return [table_place(m_size, i) for i in range(4 * m_size * Z)]


def by_class(inner_z, role, program):
    for inner in (False, True):
        for diag in (False, True):

            @pl.when((inner_z == int(inner)) & (role == int(not diag)))
            def _(inner=inner, diag=diag):
                program(inner, diag)


def gather(attn_weight, mlp_weight, block_in, out_grad, small, positions, m_size):
    rows = attn_weight.shape[0]
    own, width = block_in.shape
    tokens = Z * 2 * own
    devices = m_size * 4 * Z
    hidden, n = mlp_weight.shape[2] // Z, HEAD_DIM
    cols = [2 * n, 2 * n, hidden, hidden]
    count = len(CHUNKS)
    parts = [cols[array] // PARTS[array] for array, _, _ in CHUNKS]
    sem = pltpu.SemaphoreType.DMA
    doubling = m_size.bit_length() - 1 + 4
    in_place = pl.BlockSpec(memory_space=pl.ANY)
    in_vmem = pl.BlockSpec(memory_space=pltpu.VMEM)
    shape = lambda *dims: jax.ShapeDtypeStruct(dims, bf16)
    exact = lambda *dims: jax.ShapeDtypeStruct(dims, f32)
    vmem = lambda *dims: pltpu.VMEM(dims, bf16)
    wide = lambda *dims: pltpu.VMEM(dims, f32)
    outs = pl.pallas_call(
        functools.partial(gather_kernel, m_size),
        out_shape=[shape(width, n) for n in cols]
        + [shape(2, tokens, width), shape(tokens, width), shape(tokens, width)]
        + [shape(tokens, n), shape(tokens, 3 * n), shape(tokens, hidden), shape(tokens, hidden)]
        + [exact(2, n), exact(1, hidden), exact(4, width), exact(1, width), exact(1, width)]
        + [shape(Z, rows, n) for n in parts]
        + [shape(m_size, Z, rows, n) for n in parts]
        + [shape(4, rows, n) for n in parts],
        in_specs=[in_place] * 4 + [in_vmem] * 2,
        out_specs=[in_place] * 7 + [in_vmem] * 9 + [in_place] * (3 * count),
        scratch_shapes=[
            sem((count, 3)),
            sem((count, Z)),
            sem((count, 4)),
            sem((count, 4)),
            sem((count, m_size, Z, 2)),
            sem((count, m_size, Z, 2)),
            sem((count, m_size, Z)),
            sem((count, m_size, Z)),
            sem,
            sem,
            sem((2,)),
            sem((2, 5)),
            sem((2, Z)),
            sem((Z, 2)),
            sem((Z, 2)),
            sem((doubling,)),
            sem((doubling,)),
            sem((8,)),
            sem((count,)),
            sem((2,)),
            sem((3, Z)),
        ]
        + [vmem(Z, rows, n) for n in parts]
        + [vmem(2, tokens, width), vmem(width, 2 * n), vmem(width, 2 * n), vmem(2, 2 * own, width)]
        + [vmem(tokens, width), vmem(2, width, hidden // Z), wide(Z, tokens, hidden // Z)]
        + [wide(2, n), wide(1, hidden), wide(devices, 16, 128), vmem(2 * own, 9 * 128)]
        + [wide(4, rows, attn_weight.shape[2]), wide(2, rows, mlp_weight.shape[2])]
        + [wide(2, own, width), vmem(2, own, width)],
        compiler_params=pltpu.CompilerParams(collective_id=0, has_side_effects=True, vmem_limit_bytes=67043328),
        name="gather_all",
    )(attn_weight, mlp_weight, block_in, out_grad, small, positions)
    return outs[:4], outs[4], outs[5:7], outs[7:11], outs[11:13], outs[13], outs[14], outs[15]


VMEM_BYTES = 60 * 1024 * 1024


def dot(a, b, over_a=1, over_b=0):
    return lax.dot_general(a, b, (((over_a,), (over_b,)), ((), ())), preferred_element_type=f32)


def turn(value, tables, sign):
    cos, low, high = tables
    part = value[:, :128]
    turned = part * cos + sign * (
        pltpu.roll(part, 128 - ROT // 2, 1) * low + pltpu.roll(part, ROT // 2, 1) * high
    )
    return jnp.concatenate([turned, value[:, 128:]], axis=1)


def turn_tables(places):
    half = ROT // 2
    column = lax.broadcasted_iota(jnp.int32, places.shape, 1)
    frequency = jnp.exp(lax.rem(column, half).astype(f32) * (-2.0 / ROT * math.log(10000.0)))
    angles = places * frequency
    cos = jnp.where(column < ROT, jnp.cos(angles), 1.0)
    sin = jnp.sin(angles)
    return cos, jnp.where(column < half, -sin, 0.0), jnp.where((column >= half) & (column < ROT), sin, 0.0)


def fixed(*shape):
    return pl.BlockSpec(shape, lambda i: (0,) * len(shape))


def outs_kernel(flag, att, d_attn, act, d_pre, x, w_qk, w_vo, w_up, w_dn, par, keep, give, sums):
    diag = flag[0] == 1
    n = HEAD_DIM
    y = dot(att[...], w_vo[:, n:], 1, 1) + dot(act[...], w_dn[...], 1, 1)
    d_one = dot(d_attn[:, : 2 * n], w_qk[...], 1, 1) + dot(d_attn[:, 2 * n :], w_vo[:, :n], 1, 1)
    d_two = dot(d_pre[...], w_up[...], 1, 1)
    u = d_one * par[0:1, :] + d_two * par[2:3, :]
    keep[...] = jnp.where(diag, y, u).astype(bf16)
    give[...] = jnp.where(diag, u, y).astype(bf16)
    plain = x[...].astype(f32)
    for i, value in enumerate((d_one * plain, d_one, d_two * plain, d_two)):
        sums[i : i + 1, :] = jnp.sum(value, axis=0, keepdims=True)


def run_outs(diag, att, d_attn, act, d_pre, acts, weights, par):
    _, rows, width = acts.shape
    step = 256
    fix = lambda v: pl.BlockSpec(v.shape, lambda i, s: (0, 0), pipeline_mode=pl.Buffered(1))
    tile = lambda height: pl.BlockSpec((height, step), lambda i, s: (0, i))
    return pl.pallas_call(
        outs_kernel,
        grid_spec=pltpu.PrefetchScalarGridSpec(
            num_scalar_prefetch=1,
            grid=(width // step,),
            in_specs=[fix(v) for v in (att, d_attn, act, d_pre)]
            + [pl.BlockSpec((None, rows, step), lambda i, s: (0, 0, i))]
            + [pl.BlockSpec((step, v.shape[1]), lambda i, s: (i, 0)) for v in weights]
            + [tile(4)],
            out_specs=[tile(rows), tile(rows), tile(4)],
        ),
        out_shape=[jax.ShapeDtypeStruct((rows, width), bf16)] * 2 + [jax.ShapeDtypeStruct((4, width), f32)],
        compiler_params=pltpu.CompilerParams(vmem_limit_bytes=VMEM_BYTES),
        name="outputs",
    )(diag.astype(jnp.int32).reshape(1), att, d_attn, act, d_pre, acts, *weights, par)


def grads_kernel(one, two, g, att, d_attn, act, d_pre, qk, vo, up, dn):
    n = HEAD_DIM
    first = dot(one[...], d_attn[...], 0, 0)
    qk[...] = first[:, : 2 * n].astype(bf16)
    vo[:, :n] = first[:, 2 * n :].astype(bf16)
    vo[:, n:] = dot(g[...], att[...], 0, 0).astype(bf16)
    up[...] = dot(two[...], d_pre[...], 0, 0).astype(bf16)
    dn[...] = dot(g[...], act[...], 0, 0).astype(bf16)


def run_grads(one, two, acts, att, d_attn, act, d_pre):
    rows, width = one.shape
    step = 256
    tile = pl.BlockSpec((rows, step), lambda i: (0, i))
    fix = lambda v: pl.BlockSpec(v.shape, lambda i: (0, 0), pipeline_mode=pl.Buffered(1))
    cols = [2 * HEAD_DIM, 2 * HEAD_DIM, act.shape[1], act.shape[1]]
    return pl.pallas_call(
        grads_kernel,
        grid=(width // step,),
        in_specs=[tile, tile, pl.BlockSpec((None, rows, step), lambda i: (1, 0, i))]
        + [fix(v) for v in (att, d_attn, act, d_pre)],
        out_specs=[pl.BlockSpec((step, n), lambda i: (i, 0)) for n in cols],
        out_shape=[jax.ShapeDtypeStruct((width, n), bf16) for n in cols],
        compiler_params=pltpu.CompilerParams(vmem_limit_bytes=VMEM_BYTES),
        name="weight_grads",
    )(one, two, acts, att, d_attn, act, d_pre)


def add_rows(dst, sources):
    step = min(dst.shape[0], 32)

    @pl.loop(0, dst.shape[0] // step)
    def _(i):
        span = pl.ds(pl.multiple_of(i * step, step), step)
        total = sources[0][span, :].astype(f32)
        for one in sources[1:]:
            total = total + one[span, :].astype(f32)
        dst[span, :] = total.astype(dst.dtype)


def scatter_kernel(m_size, fused, *refs):
    if fused:
        ones, twos, acts, att, d_attn, act, d_pre = refs[:7]
        keep, give, *sums = refs[7:13]
        grads, refs = refs[13:17], refs[17:]
    else:
        grads, (keep, give, *sums), refs = refs[:4], refs[4:10], refs[10:]
    own, rows_out, small_out, refs = refs[:4], refs[4], refs[5], refs[6:]
    count = len(CHUNKS)
    buffers = []
    for _, _, m_first in CHUNKS:
        size = 5 if m_first else 6
        buffers.append(refs[:size])
        refs = refs[size:]
    relay, refs = refs[:count], refs[count:]
    got, kept, got_z, final, current, got_small = refs[:6]
    (gs, gr, kl, as_, ar, ys, yr, yl, ws, wr, wl, fs, fr, xs, xr, zs, zr, zl, ps, pr, ss, sr) = refs[6:28]
    if fused:
        tiles, made, tl, ml = refs[28:]
    net = Links(m_size)
    z, m, c, t = net.z, net.m, net.c, net.t
    half = rows_out.shape[1]
    role = lax.rem(c + t, 2)
    inner_z = lax.rem(z + z // 2, 2)
    flat, steps = net.doubling()
    steps = steps[::-1]

    def columns(ch):
        array, part, _ = CHUNKS[ch]
        wide = own[array].shape[2] // PARTS[array]
        return array, slice(part * wide, (part + 1) * wide)

    def rows_of(ch, k, j, cc=None):
        array, cols = columns(ch)
        if cc is None:
            return grads[array].at[z ^ k, m ^ j, :, :, cols]
        return grads[array].at[z ^ k, m ^ j, cc, :, cols]

    def owned(ch, zz):
        array, cols = columns(ch)
        return own[array].at[zz, :, cols]

    span = lambda h: pl.ds(pl.multiple_of((t ^ h) * half, half), half)
    loads_keep = [pltpu.make_async_copy(keep.at[z ^ k], kept.at[k], kl.at[k]) for k in range(Z)]
    for one in loads_keep:
        one.start()
    norm_sums, head_sums, up_sums, out_sum = sums

    def small_terms():
        current[...] = jnp.zeros_like(current)
        width, hidden, n = out_sum.shape[1], up_sums.shape[1], HEAD_DIM
        part = width // (4 * m_size * Z)
        for i, at in enumerate(table_order(m_size)):
            cols = slice(i * part, (i + 1) * part)
            current[at, 0:4, 0:part] = norm_sums[:, cols]
            current[at, 6:7, 0:part] = out_sum[:, cols]
            current[at, 7:8, 0:part] = out_sum[:, cols]
        head = c * Z + z
        for e in range(n // part):
            at = table_place(m_size, head * n // part + e)
            current[at, 4:6, 0:part] = head_sums[:, e * part : (e + 1) * part]
        row = 8 + head * hidden // width
        for e in range(hidden // part):
            at = table_place(m_size, head * hidden % width // part + e)
            current[at, pl.ds(row, 1), 0:part] = up_sums[:, e * part : (e + 1) * part]

    def tile_loads(i, slot):
        block = (z ^ (Z - 1 - lax.rem(i, Z))) * m_size + (m ^ (1 - i // Z))
        wide = tiles.shape[3]
        cols = pl.ds(pl.multiple_of(block * wide, wide), wide)
        sources = (ones.at[:, cols], twos.at[:, cols], acts.at[1, :, cols])
        return [pltpu.make_async_copy(src, tiles.at[slot, n], tl.at[slot, n]) for n, src in enumerate(sources)]

    def make(i):
        slot = lax.rem(i, 2)

        @pl.when(i < 2 * Z - 1)
        def _():
            for one in tile_loads(i + 1, 1 - slot):
                one.start()

        for one in tile_loads(i, slot):
            one.wait()
        n = HEAD_DIM
        high = made[0].shape[1]
        for array, at, left, right, lo, hi in (
            (0, 0, 0, d_attn, 0, 2 * n),
            (1, 0, 0, d_attn, 2 * n, 3 * n),
            (1, n, 2, att, 0, n),
            (2, 0, 1, d_pre, 0, d_pre.shape[1]),
            (3, 0, 2, act, 0, act.shape[1]),
        ):
            value = dot(tiles[slot, left], right[:, lo:hi], 0, 0).astype(bf16)
            for cc in range(2):
                made[array][cc, :, at : at + hi - lo] = value[cc * high : (cc + 1) * high]
        stores = [
            pltpu.make_async_copy(
                made[array], grads[array].at[z ^ (Z - 1 - lax.rem(i, Z)), m ^ (1 - i // Z)], ml.at[array]
            )
            for array in range(4)
        ]
        for one in stores:
            one.start()
        for one in stores:
            one.wait()

    if fused:
        for one in tile_loads(0, 0):
            one.start()
    net.meet()

    def program(inner, diag):
        state = {"small": 0}
        sent = []

        def send(*parts):
            (parts,) = parts
            net.copy(*parts()).start()
            sent.append(parts)

        def small_send():
            i = state["small"]
            if i < len(steps):
                size, target = steps[i]
                send(
                    lambda: (
                        current.at[pl.ds((flat // size ^ 1) * size, size)],
                        got_small.at[pl.ds(size, size)],
                        ss.at[i],
                        sr.at[i],
                        target,
                    )
                )

        def small_next(*_):
            i = state["small"]
            if i < len(steps):
                size = steps[i][0]
                net.landed(got_small.at[pl.ds(size, size)], sr.at[i])
                block = pl.ds(flat // size * size, size)
                current[block] = current[block] + got_small[pl.ds(size, size)]
                state["small"] += 1
                small_send()

        def swap(k, h):
            send(
                lambda: (give.at[z ^ k, span(h)], got.at[k, span(h)], gs.at[k, h], gr.at[k, h], net.to(c=1 - c))
            )

        def load_mine(ch, j, k):
            if CHUNKS[ch][2]:
                return pltpu.make_async_copy(rows_of(ch, k, j, c), buffers[ch][0].at[j, k], wl.at[ch, j, k])
            return pltpu.make_async_copy(rows_of(ch, k, 0), buffers[ch][0].at[k], wl.at[ch, 0, k])

        def load_made(k, own_m):
            for j in (0,) if own_m == 0 else range(1, m_size):
                for ch in range(count):
                    if (diag and CHUNKS[ch][2]) or (j == 0 and not CHUNKS[ch][2]):
                        load_mine(ch, j, k).start()

        def to_owner(source, home, far, ch, j, k):
            if diag:
                send(lambda: (source(1 - c), home(), ws.at[ch, j, k, 0], wr.at[ch, j, k, 0], net.to(c=1 - c)))
            else:
                send(lambda: (source(c), far(), ws.at[ch, j, k, 0], wr.at[ch, j, k, 1], net.to(t=1 - t)))
                send(
                    lambda: (source(1 - c), far(), ws.at[ch, j, k, 1], wr.at[ch, j, k, 1], net.to(c=1 - c, t=1 - t))
                )

        def owners_part(ch, j, k):
            home, far = buffers[ch][0], buffers[ch][1]
            to_owner(lambda cc: rows_of(ch, k, j, cc), lambda: home.at[j, k], lambda: far.at[j, k], ch, j, k)

        def others(ch, k):
            for j in range(1, m_size):
                owners_part(ch, j, k)

        def same(ch, k):
            owners_part(ch, 0, k)

        def across(ch, k):
            for j in range(1, m_size):
                send(
                    lambda j=j: (
                        rows_of(ch, k, j),
                        buffers[ch][1].at[j - 1, k],
                        fs.at[ch, j, k],
                        fr.at[ch, j, k],
                        net.to(m=m ^ j),
                    )
                )

        def collected(home, far, ch, j, k):
            if not diag:
                net.landed(home, wr.at[ch, j, k, 0])
            elif CHUNKS[ch][2]:
                load_mine(ch, j, k).wait()
            net.landed(far, wr.at[ch, j, k, 1])

        def middle(ch, k):
            home, far, mid, far_m, _ = buffers[ch]
            for j in range(1, m_size):
                collected(home.at[j, k], far.at[j, k], ch, j, k)
                add_rows(mid.at[j - 1, k], [home.at[j, k], far.at[j, k]])
                send(
                    lambda j=j: (
                        mid.at[j - 1, k],
                        far_m.at[j - 1, k],
                        xs.at[ch, j, k],
                        xr.at[ch, j, k],
                        net.to(m=m ^ j),
                    )
                )

        def summed(ch, k):
            mine, far_m, both, home, far, _ = buffers[ch]
            load_mine(ch, 0, k).wait()
            for j in range(1, m_size):
                net.landed(far_m.at[j - 1, k], fr.at[ch, j, k])
            for cc in range(2):
                add_rows(both.at[k, cc], [mine.at[k, cc]] + [far_m.at[j - 1, k, cc] for j in range(1, m_size)])
            to_owner(lambda cc: both.at[k, cc], lambda: home.at[k], lambda: far.at[k], ch, 0, k)

        def finish(ch, k):
            if CHUNKS[ch][2]:
                home, far, _, far_m, result = buffers[ch]
                collected(home.at[0, k], far.at[0, k], ch, 0, k)
                for j in range(1, m_size):
                    net.landed(far_m.at[j - 1, k], xr.at[ch, j, k])
                sources = [home.at[0, k], far.at[0, k]] + [far_m.at[j - 1, k] for j in range(1, m_size)]
            else:
                _, _, both, home, far, result = buffers[ch]
                collected(home.at[k], far.at[k], ch, 0, k)
                sources = [both.at[k, c] if diag else home.at[k], far.at[k]]
            add_rows(result.at[k], sources)
            if k == 0:
                pltpu.make_async_copy(result.at[k], owned(ch, z), zl.at[ch]).start()
                return
            hop, through = {1: (1, None), 2: (3, 2), 3: (3, None)}[k] if inner else {1: (1, None), 2: (1, 0), 3: (1, 1)}[k]
            if through is None:
                send(lambda: (result.at[k], owned(ch, z), zs.at[ch, k], zr.at[ch, k], net.to(z=z ^ hop)))
            else:
                send(
                    lambda: (
                        result.at[k],
                        relay[ch].at[through],
                        zs.at[ch, k],
                        pr.at[ch, through],
                        net.to(z=z ^ hop),
                    )
                )

        def pass_on(through):
            hop, k = ((3, 2), (3, None), (1, 2), (1, 3))[through]

            def run(ch, _):
                net.landed(relay[ch].at[through], pr.at[ch, through])

                def parts():
                    if k is None:
                        dst, recv_sem = relay[ch].at[3], pr.at[ch, 3]
                    else:
                        dst, recv_sem = owned(ch, z ^ hop ^ k), zr.at[ch, k]
                    return relay[ch].at[through], dst, ps.at[ch, through], recv_sem, net.to(z=z ^ hop)

                send(parts)

            return run

        def rows_first(k, h):
            if h == 0:
                pltpu.make_async_copy(keep.at[z ^ k], kept.at[k], kl.at[k]).wait()
            net.landed(got.at[k, span(h)], gr.at[k, h])
            add_rows(kept.at[k, span(h)], [kept.at[k, span(h)], got.at[k, span(h)]])
            if k and not inner:
                slot = {1: 0, 2: 1, 3: 2}[k]
                send(
                    lambda: (
                        kept.at[k, span(h)],
                        got_z.at[slot, span(h)],
                        as_.at[k, h],
                        ar.at[slot, h],
                        net.to(z=z ^ 1),
                    )
                )

        def rows_through(k, h, slot, there, hop):
            net.landed(got_z.at[slot, span(h)], ar.at[slot, h])
            add_rows(kept.at[k, span(h)], [kept.at[k, span(h)], got_z.at[slot, span(h)]])
            send(
                lambda: (
                    kept.at[k, span(h)],
                    got_z.at[there, span(h)],
                    as_.at[k, h],
                    ar.at[there, h],
                    net.to(z=z ^ hop),
                )
            )

        def rows_inner(k, h):
            rows_through(k, h, {3: 1, 2: 2}[k], {3: 3, 2: 4}[k], 3)

        def rows_outer(h, _):
            rows_through(1, h, 4, 0, 1)

        def rows_back(h, _):
            slots = (0, 3) if inner else (0,)
            for slot in slots:
                net.landed(got_z.at[slot, span(h)], ar.at[slot, h])
            add_rows(final.at[h], [kept.at[0, span(h)]] + [got_z.at[slot, span(h)] for slot in slots])
            if diag and h == 0:
                pltpu.make_async_copy(final.at[h], rows_out.at[0], yl).start()
            elif diag:
                send(lambda: (final.at[h], rows_out.at[0], ys.at[h], yr.at[0], net.to(t=1 - t)))
            elif h == 0:
                send(lambda: (final.at[h], rows_out.at[1], ys.at[h], yr.at[1], net.to(c=1 - c)))
            else:
                send(lambda: (final.at[h], rows_out.at[1], ys.at[h], yr.at[1], net.to(c=1 - c, t=1 - t)))

        runs = [swap, load_made, others, same, across, rows_first, rows_inner, rows_outer, rows_back]
        runs += [middle, summed, finish] + [pass_on(i) for i in range(4)] + [small_next]

        def run(codes):
            for code in codes:
                runs[code // 100](code // 10 % 10, code % 10)

        def end():
            while state["small"] < len(steps):
                small_next()
            small_out[...] = current[flat]
            for ch in range(count):
                for k in range(1, Z):
                    net.landed(owned(ch, z ^ k), zr.at[ch, k])
                pltpu.make_async_copy(owned(ch, z), owned(ch, z), zl.at[ch]).wait()
            net.landed(rows_out.at[1], yr.at[1])
            if diag:
                pltpu.make_async_copy(final.at[0], rows_out.at[0], yl).wait()
            else:
                net.landed(rows_out.at[0], yr.at[0])
            for parts in sent:
                net.copy(*parts()).wait_send()

        return small_send, run, end

    programs = {key: program(*key) for key in SCATTER_ORDER}
    cuts = {
        key: [i for i, code in enumerate(codes) if code // 100 == 1] + [len(codes)]
        for key, codes in SCATTER_ORDER.items()
    }

    def begin(inner, diag):
        _, run, _ = programs[inner, diag]
        run(SCATTER_ORDER[inner, diag][: cuts[inner, diag][0]])

    def part(i, inner, diag):
        lo, hi = cuts[inner, diag][i : i + 2]
        programs[inner, diag][1](SCATTER_ORDER[inner, diag][lo:hi])

    by_class(inner_z, role, begin)
    small_terms()
    by_class(inner_z, role, lambda inner, diag: programs[inner, diag][0]())
    if fused:

        @pl.loop(0, 2 * Z)
        def _(i):
            make(i)
            for n in range(2 * Z):

                @pl.when(i == n)
                def _(n=n):
                    by_class(inner_z, role, functools.partial(part, n))

    else:
        for n in range(2 * Z):
            by_class(inner_z, role, functools.partial(part, n))
    by_class(inner_z, role, lambda inner, diag: programs[inner, diag][2]())


def scatter(factors, keep, give, sums, m_size, rows):
    one, two, acts, att, d_attn, act, d_pre = factors
    width = keep.shape[1]
    block = width // (2 * Z * m_size)
    seq = keep.shape[0] // Z
    cols = [2 * HEAD_DIM, 2 * HEAD_DIM, act.shape[1], act.shape[1]]
    parts = [cols[array] // PARTS[array] for array, _, _ in CHUNKS]
    count = len(CHUNKS)
    fused = m_size == 2 and 2 * block % 256 == 0
    sem = pltpu.SemaphoreType.DMA
    vmem = lambda *shape: pltpu.VMEM(shape, bf16)
    doubling = m_size.bit_length() - 1 + 4
    in_place = pl.BlockSpec(memory_space=pl.ANY)
    in_vmem = pl.BlockSpec(memory_space=pltpu.VMEM)
    far = m_size - 1
    term_shapes = [jax.ShapeDtypeStruct((Z, m_size, 2, block, n), bf16) for n in cols]
    out_shape = [jax.ShapeDtypeStruct((Z, block, n), bf16) for n in cols]
    out_shape += [jax.ShapeDtypeStruct((2, rows, width), bf16), jax.ShapeDtypeStruct((16, 128), f32)]
    out_specs = [in_place] * 5 + [in_vmem]
    if fused:
        inputs = [one, two, acts, att, d_attn, act, d_pre]
        in_specs = [in_place] * 3 + [in_vmem] * 4
        out_shape, out_specs = term_shapes + out_shape, [in_place] * 4 + out_specs
    else:
        inputs = [g.reshape(s.shape) for g, s in zip(run_grads(*factors), term_shapes)]
        in_specs = [in_place] * 4
    scratch = []
    for n, (_, _, m_first) in zip(parts, CHUNKS):
        if m_first:
            scratch += [vmem(m_size, Z, block, n)] * 2 + [vmem(far, Z, block, n)] * 2 + [vmem(Z, block, n)]
        else:
            scratch += [vmem(Z, 2, block, n), vmem(far, Z, 2, block, n), vmem(Z, 2, block, n)]
            scratch += [vmem(Z, block, n)] * 3
    scratch += [vmem(4, block, n) for n in parts]
    scratch += [vmem(Z, seq, width)] * 2 + [vmem(5, seq, width), vmem(2, rows, width)]
    scratch += [pltpu.VMEM((4 * m_size * Z, 16, 128), f32)] * 2
    scratch += [
        sem((Z, 2)),
        sem((Z, 2)),
        sem((Z,)),
        sem((Z, 2)),
        sem((5, 2)),
        sem((2,)),
        sem((2,)),
        sem,
        sem((count, m_size, Z, 2)),
        sem((count, m_size, Z, 2)),
        sem((count, m_size, Z)),
        sem((count, m_size, Z)),
        sem((count, m_size, Z)),
        sem((count, m_size, Z)),
        sem((count, m_size, Z)),
        sem((count, Z)),
        sem((count, Z)),
        sem((count,)),
        sem((count, 4)),
        sem((count, 4)),
        sem((doubling,)),
        sem((doubling,)),
    ]
    if fused:
        scratch.append(vmem(2, 3, keep.shape[0], 2 * block))
        made = [vmem(2, block, n) for n in cols]
        scratch_made = [sem((2, 3)), sem((4,))]
    outs = pl.pallas_call(
        functools.partial(scatter_entry, m_size, fused),
        out_shape=out_shape,
        in_specs=in_specs + [in_place] * 2 + [in_vmem] * 4,
        out_specs=out_specs,
        scratch_shapes=scratch + (made + scratch_made if fused else []),
        compiler_params=pltpu.CompilerParams(collective_id=1, has_side_effects=True, vmem_limit_bytes=67043328),
        name="scatter_all",
    )(*inputs, keep.reshape(Z, seq, width), give.reshape(Z, seq, width), *sums)
    outs = outs[4:] if fused else outs
    return outs[:4], outs[4], outs[5]


def scatter_entry(m_size, fused, *refs):
    if fused:
        refs = refs[:-6] + (refs[-6:-2],) + refs[-2:]
    scatter_kernel(m_size, fused, *refs)


def update_kernel(step, steps, *refs):
    rows, cotangent, back, bias, qk, vo, up, dn = refs[:8]
    attn, mlp, (block_out, input_grad) = refs[8:11], refs[11:14], refs[14:16]
    attn_outs, mlp_outs = refs[16:20], refs[20:24]
    attn_v, mlp_v, attn_new, mlp_new, in_sem, out_sem = refs[24:]
    i = pl.program_id(0)

    def copies(i, sources, buffer, sems, at, out):
        slot = lax.rem(i, 2)
        span = pl.ds(pl.multiple_of(i * step, step), step)
        made = []
        for n, ref in enumerate(sources):
            for j in range(ref.shape[1]):
                far, near = ref.at[span, j, :], buffer.at[slot, n, j]
                pair = (near, far) if out else (far, near)
                made.append(pltpu.make_async_copy(*pair, sems.at[slot, at + n, j]))
        return made

    loads = lambda i: copies(i, attn, attn_v, in_sem, 0, False) + copies(i, mlp, mlp_v, in_sem, 3, False)
    stores = lambda i: copies(i, attn_outs, attn_new, out_sem, 0, True) + copies(i, mlp_outs, mlp_new, out_sem, 4, True)

    @pl.when(i == 0)
    def _():
        for one in loads(0):
            one.start()

    @pl.when(i + 1 < steps)
    def _():
        for one in loads(i + 1):
            one.start()

    normed, inverse = layer_stats(rows[...])
    block_out[...] = rows[...] + back[0].astype(f32) + bias[...]
    u = back[1].astype(f32)
    input_grad[...] = cotangent[...] + inverse * (
        u
        - jnp.mean(u, axis=-1, keepdims=True)
        - normed * jnp.mean(u * normed, axis=-1, keepdims=True)
    )

    @pl.when(i >= 2)
    def _():
        for one in stores(i - 2):
            one.wait()

    for one in loads(i):
        one.wait()
    slot = lax.rem(i, 2)
    for sources, olds, news in (((qk, qk, vo, vo), attn_v, attn_new), ((up, dn), mlp_v, mlp_new)):
        kinds, wide = olds.shape[2], olds.shape[4] // Z
        for j in range(kinds):
            at = j % (kinds // 2) * wide
            for q in range(Z):
                cols = slice(q * wide, (q + 1) * wide)
                g = sources[j][q, :, at : at + wide].astype(f32)
                updated = adam_step(olds[slot, 0, j, :, cols], g, olds[slot, 1, j, :, cols], olds[slot, 2, j, :, cols])
                for n, value in enumerate((g, *updated)):
                    news[slot, n, j, :, cols] = value
    for one in stores(i):
        one.start()

    @pl.when(i == steps - 1)
    def _():
        if steps > 1:
            for one in stores(i - 1):
                one.wait()
        for one in stores(i):
            one.wait()


def update(block_in, out_grad, own_rows, bias, own, attn, mlp):
    rows, width = block_in.shape
    shard = attn[0].shape[0]
    step = min(shard, 32)
    steps = shard // step
    by_rows = pl.BlockSpec((rows // steps, width), lambda i: (i, 0))
    in_place = pl.BlockSpec(memory_space=pl.ANY)
    slots = lambda count, v: pltpu.VMEM((2, count, v.shape[1], step, v.shape[2]), f32)
    return pl.pallas_call(
        functools.partial(update_kernel, step, steps),
        grid=(steps,),
        in_specs=[by_rows, by_rows, pl.BlockSpec((2, rows // steps, width), lambda i: (0, i, 0)), fixed(1, width)]
        + [pl.BlockSpec((Z, step, g.shape[2]), lambda i: (0, i, 0)) for g in own]
        + [in_place] * 6,
        out_specs=[by_rows, by_rows] + [in_place] * 8,
        out_shape=[jax.ShapeDtypeStruct((rows, width), f32)] * 2
        + [jax.ShapeDtypeStruct(attn[0].shape, f32)] * 4
        + [jax.ShapeDtypeStruct(mlp[0].shape, f32)] * 4,
        scratch_shapes=[slots(3, attn[0]), slots(3, mlp[0]), slots(4, attn[0]), slots(4, mlp[0])]
        + [pltpu.SemaphoreType.DMA((2, 6, 4)), pltpu.SemaphoreType.DMA((2, 8, 4))],
        compiler_params=pltpu.CompilerParams(vmem_limit_bytes=VMEM_BYTES),
        name="update",
    )(block_in, out_grad, own_rows, bias, *own, *attn, *mlp)


def body(
    block_in,
    positions,
    out_grad,
    attn_weight,
    mlp_weight,
    small_params,
    attn_first,
    attn_second,
    mlp_first,
    mlp_second,
    small_first,
    small_second,
):
    m_size = lax.axis_size("dp") // (2 * Z)
    diag = lax.axis_index("dp") % 2 == lax.axis_index("tensor")
    rows = block_in.shape[0]
    part = small_params.shape[1]
    weights, acts, norms, (attended, d_attn, activation, d_pre), (head_sums, up_sums), par, row_bias, out_sum = gather(
        attn_weight, mlp_weight, block_in, out_grad, small_params, positions, m_size
    )
    keep, give, norm_sums = run_outs(diag, attended, d_attn, activation, d_pre, acts, weights, par)
    factors = (*norms, acts, attended, d_attn, activation, d_pre)
    sums = (norm_sums, head_sums, up_sums, out_sum)
    own, own_rows, own_small = scatter(factors, keep, give, sums, m_size, rows)
    attn = (attn_weight, attn_first, attn_second)
    mlp = (mlp_weight, mlp_first, mlp_second)
    block_out, input_grad, *updated = update(block_in, out_grad, own_rows, row_bias, own, attn, mlp)
    attn_out, mlp_out = updated[:4], updated[4:]
    small_grad = own_small[:12, :part]
    small_new, small_first_new, small_second_new = adam_step(small_params, small_grad, small_first, small_second)

    attn_grad, attn_new, attn_first_new, attn_second_new = attn_out
    mlp_grad, mlp_new, mlp_first_new, mlp_second_new = mlp_out
    return (
        block_out,
        input_grad,
        attn_grad,
        mlp_grad,
        small_grad,
        attn_new,
        attn_first_new,
        attn_second_new,
        mlp_new,
        mlp_first_new,
        mlp_second_new,
        small_new,
        small_first_new,
        small_second_new,
    )


def solution(mesh):
    rows = P(("dp", "tensor"), None)
    weights = P("dp", None, "tensor")
    small = P(None, ("dp", "tensor"))
    return jax.shard_map(
        body,
        mesh=mesh,
        in_specs=(rows, P("dp", None), rows, weights, weights, small, weights, weights, weights, weights, small, small),
        out_specs=(rows, rows) + (weights,) * 2 + (small,) + (weights,) * 6 + (small,) * 3,
        check_vma=False,
    )
```

```python
import functools
import math

import jax
import jax.numpy as jnp
from jax import lax
from jax.experimental import pallas as pl
from jax.experimental.pallas import tpu as pltpu
from jax.sharding import PartitionSpec as P

ROT = 64
ADAM_STEP = 3
HEAD_DIM = 256
Z = 4

norm_epsilon = 1e-05
learn_rate = 0.006
beta_first = 0.9
beta_second = 0.95
adam_epsilon = 1e-08
weight_decay = 0.1

f32 = jnp.float32
bf16 = jnp.bfloat16


def layer_stats(row_data):
    center = row_data - jnp.mean(row_data, axis=-1, keepdims=True)
    inverse = lax.rsqrt(jnp.mean(center * center, axis=-1, keepdims=True) + norm_epsilon)
    return (center * inverse, inverse)


def adam_step(weight, gradient, moment_one, moment_two):
    one_new = beta_first * moment_one + (1.0 - beta_first) * gradient
    two_new = beta_second * moment_two + (1.0 - beta_second) * gradient * gradient
    corrected = (one_new * (1.0 / (1.0 - beta_first**ADAM_STEP))) / (
        jnp.sqrt(two_new * (1.0 / (1.0 - beta_second**ADAM_STEP))) + adam_epsilon
    )
    return (weight - learn_rate * (corrected + weight_decay * weight), one_new, two_new)


MESH = pl.DeviceIdType.MESH
PARTS = (1, 1, 2, 2)
CHUNKS = ((0, 0, True), (1, 0, False), (2, 0, True), (2, 1, False), (3, 0, True), (3, 1, False))
GATHER_ORDER = {
    (False, False): (
        1201, 0, 10, 1200, 500, 510, 900, 501, 700, 1202, 20, 511, 520, 530, 540, 550, 600, 601, 1100, 910, 1101,
        620, 640, 801, 1110, 710, 30, 40, 50, 521, 502, 621, 610, 512, 602, 503, 611, 1010, 603, 630, 1111, 1011,
        811, 1030, 650, 531, 920, 1000, 541, 1050, 1001, 551, 641, 930, 1020, 1040, 940, 802, 1120, 522, 1021, 513,
        612, 622, 1002, 1012, 812, 1121, 631, 1003, 532, 542, 651, 1031, 552, 1041, 642, 613, 1051, 1022, 632, 803,
        652, 1042, 1013, 1203, 523, 1032, 1130, 1204, 533, 1052, 1205, 623, 1131, 1023, 813, 1206, 543, 553, 633,
        1207, 1208, 643, 653, 1033, 1209, 1043, 1210, 1053, 1211, 1212, 1213, 1214,
    ),
    (False, True): (
        1201, 0, 10, 1200, 700, 1202, 20, 500, 501, 510, 520, 530, 540, 550, 610, 900, 511, 1100, 600, 710, 30, 40,
        50, 601, 611, 630, 650, 1000, 1001, 620, 1020, 640, 801, 1040, 1010, 521, 910, 1110, 1011, 502, 1101, 1030,
        1050, 621, 1021, 811, 602, 1002, 531, 541, 551, 1111, 641, 631, 512, 612, 930, 920, 651, 1031, 1041, 1012,
        802, 940, 522, 1051, 503, 1120, 622, 603, 1003, 1022, 812, 532, 542, 1121, 632, 552, 642, 513, 613, 652,
        1032, 1042, 1013, 1203, 803, 1204, 523, 1052, 1130, 1205, 623, 813, 533, 633, 1023, 543, 1033, 553, 643,
        1131, 1206, 653, 1207, 1208, 1043, 1209, 1053, 1210, 1211, 1212, 1213, 1214,
    ),
    (True, False): (
        1201, 0, 10, 1200, 500, 510, 900, 200, 503, 700, 1202, 20, 520, 530, 540, 550, 600, 603, 100, 300, 1100, 501,
        513, 210, 310, 1101, 620, 110, 400, 640, 511, 910, 601, 710, 30, 40, 50, 803, 1130, 610, 523, 801, 320, 1110,
        220, 1010, 502, 630, 120, 623, 410, 521, 602, 512, 650, 1000, 1030, 1003, 621, 1131, 811, 1050, 613, 813,
        230, 1111, 533, 1020, 130, 1013, 330, 1040, 531, 920, 543, 611, 240, 340, 930, 140, 1001, 643, 553, 541, 350,
        250, 1011, 150, 1023, 940, 551, 641, 1002, 802, 420, 1120, 1021, 522, 633, 612, 622, 631, 1033, 1043, 1012,
        1203, 653, 1031, 430, 812, 1121, 1204, 532, 651, 1041, 1205, 1022, 1053, 440, 1206, 542, 632, 1051, 450,
        1207, 552, 1208, 642, 1032, 1209, 652, 1210, 1042, 1211, 1052, 1212, 1213, 1214,
    ),
    (True, True): (
        1201, 0, 10, 1200, 700, 1202, 20, 500, 503, 510, 520, 530, 540, 550, 610, 200, 900, 100, 300, 1100, 600, 501,
        513, 710, 30, 40, 50, 603, 630, 650, 1000, 1003, 613, 210, 310, 620, 110, 1020, 640, 511, 1040, 611, 1010,
        601, 1001, 803, 1101, 1030, 523, 1050, 801, 320, 1130, 1013, 220, 400, 1110, 120, 502, 1011, 521, 910, 623,
        1023, 602, 1002, 621, 813, 533, 811, 1021, 330, 230, 1111, 543, 1131, 130, 633, 340, 531, 643, 631, 553, 240,
        930, 920, 1033, 350, 140, 410, 541, 1043, 1031, 653, 512, 612, 250, 940, 150, 641, 551, 651, 1053, 1041, 802,
        1012, 1203, 1051, 420, 1120, 1204, 522, 1205, 622, 1022, 812, 430, 532, 1121, 1206, 632, 440, 1207, 542,
        1208, 1032, 450, 1209, 552, 642, 1210, 652, 1042, 1211, 1212, 1052, 1213, 1214,
    ),
}
SCATTER_ORDER = {
    (False, False): (
        30, 31, 20, 21, 10, 11, 0, 1, 131, 530, 531, 520, 521, 510, 511, 500, 501, 1600, 203, 413, 223, 433, 243,
        453, 121, 1610, 202, 412, 222, 432, 242, 903, 452, 111, 923, 1620, 201, 411, 221, 431, 241, 451, 101, 943,
        1630, 200, 410, 220, 430, 240, 450, 130, 902, 1013, 922, 1033, 303, 323, 343, 120, 942, 1053, 302, 322, 342,
        110, 901, 1012, 921, 301, 321, 341, 100, 800, 1032, 900, 941, 300, 320, 340, 920, 940, 1052, 1113, 810, 1133,
        1011, 1103, 1031, 1123, 1051, 1153, 1143, 1640, 1010, 1112, 1030, 1050, 1102, 1132, 1122, 1142, 1101, 1121,
        1152, 1100, 1141, 1120, 1111, 1140, 1131, 1151, 1110, 1130, 1150,
    ),
    (False, True): (
        30, 31, 20, 21, 10, 11, 0, 1, 131, 530, 531, 520, 521, 510, 511, 500, 501, 1600, 203, 413, 223, 433, 243,
        453, 121, 903, 1610, 202, 412, 222, 432, 242, 452, 111, 923, 201, 411, 221, 431, 241, 451, 101, 943, 1620,
        902, 200, 410, 220, 430, 240, 450, 130, 1013, 922, 1033, 1630, 303, 323, 942, 343, 120, 901, 1053, 302, 322,
        342, 110, 921, 301, 321, 341, 100, 1012, 900, 800, 941, 300, 320, 340, 920, 1032, 940, 1113, 1052, 1133, 810,
        1103, 1011, 1123, 1031, 1153, 1051, 1143, 1102, 1640, 1112, 1010, 1030, 1132, 1050, 1122, 1142, 1101, 1152,
        1121, 1100, 1141, 1111, 1120, 1131, 1140, 1151, 1110, 1130, 1150,
    ),
    (True, False): (
        30, 31, 20, 21, 10, 11, 0, 1, 131, 530, 531, 520, 521, 510, 511, 500, 501, 1600, 203, 413, 223, 433, 243,
        453, 121, 1610, 202, 412, 222, 432, 242, 903, 620, 452, 111, 923, 1620, 201, 411, 221, 431, 241, 451, 101,
        943, 200, 410, 220, 430, 240, 450, 130, 621, 700, 902, 1013, 922, 1033, 942, 1053, 303, 323, 343, 120, 901,
        1012, 921, 302, 322, 342, 110, 630, 710, 900, 1032, 941, 301, 321, 341, 100, 920, 300, 320, 340, 940, 1052,
        631, 1113, 1133, 1153, 1011, 1103, 800, 1123, 1031, 1112, 1051, 1143, 810, 1630, 1310, 1010, 1330, 1410,
        1300, 1132, 1030, 1640, 1320, 1510, 1350, 1050, 1530, 1340, 1102, 1500, 1210, 1122, 1430, 1200, 1142, 1520,
        1230, 1101, 1550, 1220, 1121, 1540, 1152, 1240, 1100, 1400, 1111, 1141, 1131, 1120, 1420, 1151, 1250, 1140,
        1440, 1110, 1130, 1450, 1150,
    ),
    (True, True): (
        30, 31, 20, 21, 10, 11, 0, 1, 131, 530, 531, 520, 521, 510, 511, 500, 501, 1600, 203, 413, 223, 433, 243,
        453, 121, 903, 1610, 202, 412, 620, 222, 432, 242, 452, 111, 923, 943, 201, 411, 221, 431, 241, 451, 101,
        902, 1620, 200, 410, 220, 430, 240, 450, 130, 621, 700, 1013, 922, 1033, 942, 901, 1053, 303, 323, 343, 120,
        921, 302, 322, 342, 110, 630, 710, 900, 1012, 941, 301, 321, 341, 920, 100, 1032, 940, 300, 320, 340, 1113,
        1052, 631, 1133, 1153, 1103, 1123, 1011, 800, 1143, 1112, 1031, 1051, 810, 1630, 1102, 1310, 1330, 1132,
        1010, 1300, 1410, 1640, 1320, 1400, 1030, 1350, 1510, 1340, 1530, 1050, 1200, 1430, 1122, 1210, 1500, 1142,
        1230, 1520, 1101, 1220, 1152, 1550, 1121, 1240, 1111, 1540, 1100, 1131, 1141, 1250, 1151, 1420, 1120, 1140,
        1440, 1110, 1130, 1150, 1450,
    ),
}


class Links:
    def __init__(self, m_size):
        self.m_size = m_size
        index = lax.axis_index("dp")
        self.z, self.m, self.c = index // (2 * m_size), (index // 2) % m_size, index % 2
        self.t = lax.axis_index("tensor")
        self.sends = []

    def to(self, z=None, m=None, c=None, t=None):
        z, m, c = (own if v is None else v for v, own in ((z, self.z), (m, self.m), (c, self.c)))
        return ((z * self.m_size + m) * 2 + c, self.t if t is None else t)

    def copy(self, src, dst, send_sem, recv_sem, target):
        return pltpu.make_async_remote_copy(
            src_ref=src, dst_ref=dst, send_sem=send_sem, recv_sem=recv_sem, device_id=target, device_id_type=MESH
        )

    def send(self, src, dst, send_sem, recv_sem, target):
        one = self.copy(src, dst, send_sem, recv_sem, target)
        one.start()
        self.sends.append(one)

    def landed(self, dst, recv_sem):
        self.copy(dst, dst, recv_sem, recv_sem, self.to(c=1 - self.c)).wait_recv()

    def drain(self):
        for one in self.sends:
            one.wait_send()
        self.sends = []

    def partners(self):
        other = 1 - self.t
        out = [self.to(z=self.z ^ k) for k in range(1, Z)]
        out += [self.to(m=self.m ^ j) for j in range(1, self.m_size)]
        out += [self.to(c=1 - self.c), self.to(t=other), self.to(c=1 - self.c, t=other)]
        return out

    def doubling(self):
        high = self.z // 2
        place = ((self.m * 2 + self.c) * 2 + self.t) * 4 + lax.rem(self.z + high, 2) * 2 + high
        steps = [(1, self.to(z=self.z ^ 3)), (2, self.to(z=self.z ^ 1)), (4, self.to(t=1 - self.t))]
        steps.append((8, self.to(c=1 - self.c)))
        j = 1
        while j < self.m_size:
            steps.append((16 * j, self.to(m=self.m ^ j)))
            j *= 2
        return place, steps

    def meet(self):
        barrier = pltpu.get_barrier_semaphore()
        everyone = self.partners()
        for target in everyone:
            pl.semaphore_signal(barrier, inc=1, device_id=target, device_id_type=MESH)
        pl.semaphore_wait(barrier, len(everyone))


def gather_kernel(m_size, *refs):
    weights, rows_in, small, positions = refs[:2], refs[2:4], refs[4], refs[5]
    full, act_out, one_out, two_out = refs[6:10], refs[10], refs[11], refs[12]
    made_out, rows_made = refs[13:17], refs[17:19]
    head_sums, up_sums, norm_sums, row_bias, out_sum = refs[19:24]
    count = len(CHUNKS)
    stage, stage_m, relay = (refs[24 + i * count : 24 + (i + 1) * count] for i in range(3))
    refs = refs[24 + 3 * count :]
    (zs, zr, gs, gr, ps, pr, ms, mr, near_s, far_s, xr, as_, ar, ws, wr, ss, sr, lin, lout, ls, os_, made_s, tile_s, rows_s) = refs[:24]
    pieces, refs = refs[24 : 24 + count], refs[24 + count :]
    act, w_qk, w_vo, one_v, two_v, tile_v, slope, bias, up_bias, table, base, attn_v, mlp_v, rows_v, low = refs[:15]
    par, att, d_attn, hidden_out, d_pre = refs[15:20]
    tiles, both_v = refs[20:24], refs[24]
    net = Links(m_size)
    z, m, c, t = net.z, net.m, net.c, net.t
    rows = pieces[0].shape[1]
    half = low.shape[1]
    seq = 2 * half
    width = low.shape[2]
    n = HEAD_DIM
    role = lax.rem(c + t, 2)
    inner_z = lax.rem(z + z // 2, 2)

    def columns(ch):
        array, part, _ = CHUNKS[ch]
        wide = pieces[ch].shape[2]
        return array, slice(part * wide, (part + 1) * wide)

    def piece(ch, zz):
        return pieces[ch].at[zz]

    def whole(ch, zz, mm, cc, size=1):
        array, cols = columns(ch)
        start = ((zz * m_size + mm) * 2 + cc) * rows
        return full[array].at[pl.ds(pl.multiple_of(start, rows), size * rows), cols]

    own_place = pl.ds(pl.multiple_of(z * seq + t * half, half), half)
    place = lambda zz, h: pl.ds(pl.multiple_of(zz * seq + (t ^ h) * half, half), half)

    def store_own(ch):
        return pltpu.make_async_copy(pieces[ch].at[z], whole(ch, z, m, c), lout.at[ch])

    def inputs():
        pairs = [(weights[0].at[:, j, :], attn_v.at[j]) for j in range(4)]
        pairs += [(rows_in[i], rows_v.at[i]) for i in range(2)]
        pairs += [(weights[1].at[:, j, :], mlp_v.at[j]) for j in range(2)]
        return [pltpu.make_async_copy(src, dst, lin.at[i]) for i, (src, dst) in enumerate(pairs)]

    for one in inputs():
        one.start()
    flat, steps = net.doubling()
    table[flat] = jnp.zeros(table.shape[1:], f32)
    table[flat, 0:12, 0 : small.shape[1]] = small[...]
    for e in range(seq // 128):
        table[flat, 12 + e : 13 + e, :] = positions[:, e * 128 : (e + 1) * 128].astype(f32)
    net.meet()

    def program(inner, diag):
        state = {"small": 0}
        sent = []

        def send(parts):
            net.copy(*parts()).start()
            sent.append(parts)

        def small_send():
            i = state["small"]
            if i < len(steps):
                size, target = steps[i]

                def parts():
                    span = table.at[pl.ds(flat // size * size, size)]
                    return span, span, ss.at[i], sr.at[i], target

                send(parts)

        def small_next(*_):
            i = state["small"]
            if i < len(steps):
                size = steps[i][0]
                net.landed(table.at[pl.ds((flat // size ^ 1) * size, size)], sr.at[i])
                state["small"] += 1
                small_send()

        def small_last():
            while state["small"] < len(steps):
                small_next()

        def spot(ch, zz, j):
            if diag:
                return whole(ch, zz, m ^ j, c)
            return stage_m[ch].at[m ^ j, zz] if j else stage[ch].at[zz]

        def source(ch, k, j):
            return piece(ch, z) if k == 0 and j == 0 else spot(ch, z ^ k, j)

        def spread(ch, k, j):
            block = lambda: whole(ch, z ^ k, m ^ j, c)
            send(
                lambda: (
                    source(ch, k, j),
                    block(),
                    ps.at[ch, j, k, 1],
                    pr.at[ch, j, k, c],
                    net.to(c=t, t=1 - t),
                )
            )
            if not diag:
                send(
                    lambda: (source(ch, k, j), block(), ps.at[ch, j, k, 0], pr.at[ch, j, k, c], net.to(c=1 - c))
                )

        def spread_landed(ch, k, j):
            for cc in (1 - c,) if diag else (1 - c, c):
                net.landed(whole(ch, z ^ k, m ^ j, cc), pr.at[ch, j, k, cc])

        def swap(h, k):
            def parts():
                src = act.at[role, place(z ^ k, h)]
                return src, src, ws.at[k, h], wr.at[k, h], net.to(c=1 - c)

            send(parts)

        def rows_on(h, flip, i, hop, k):
            def parts():
                src = act.at[role, place(z ^ flip, h)]
                return src, src, as_.at[h, i], ar.at[h, k], net.to(z=z ^ hop)

            send(parts)

        def quarters(ch, _):
            for i, (k, hop, through) in enumerate(
                ((3, 3, None), (2, 3, 2), (1, 1, None)) if inner else ((3, 1, 1), (2, 1, 0), (1, 1, None))
            ):

                def parts(i=i, k=k, hop=hop, through=through):
                    if through is None:
                        dst, recv_sem = spot(ch, z, 0), zr.at[ch, k]
                    else:
                        dst, recv_sem = relay[ch].at[through], gr.at[ch, through]
                    return piece(ch, z ^ k), dst, zs.at[ch, i], recv_sem, net.to(z=z ^ hop)

                send(parts)

        def pass_on(through):
            hop, k = ((3, 2), (3, None), (1, 2), (1, 3))[through]

            def run(ch, _):
                net.landed(relay[ch].at[through], gr.at[ch, through])

                def parts():
                    if k is None:
                        dst, recv_sem = relay[ch].at[3], gr.at[ch, 3]
                    else:
                        dst, recv_sem = spot(ch, z ^ hop ^ k, 0), zr.at[ch, k]
                    return relay[ch].at[through], dst, gs.at[ch, through], recv_sem, net.to(z=z ^ hop)

                send(parts)

            return run

        def first(ch, k):
            if k:
                net.landed(spot(ch, z ^ k, 0), zr.at[ch, k])
            elif diag:
                store_own(ch).start()
            if CHUNKS[ch][2]:
                for j in range(1, m_size):

                    def parts(j=j):
                        dst = whole(ch, z ^ k, m, c) if diag else stage_m[ch].at[m, z ^ k]
                        return source(ch, k, 0), dst, ms.at[ch, j, k], mr.at[ch, j, k], net.to(m=m ^ j)

                    send(parts)
            spread(ch, k, 0)

        def second(ch, k):
            if CHUNKS[ch][2]:
                for j in range(1, m_size):
                    net.landed(spot(ch, z ^ k, j), mr.at[ch, j, k])
                    spread(ch, k, j)
            else:
                if diag and k == 0:
                    store_own(ch).wait()
                spread_landed(ch, k, 0)
                for j in range(1, m_size):

                    def parts(j=j):
                        both = whole(ch, z ^ k, m, 0, 2)
                        return both, both, ms.at[ch, j, k], mr.at[ch, j, k], net.to(m=m ^ j)

                    send(parts)

        def third(ch, k):
            if CHUNKS[ch][2]:
                for j in range(m_size):
                    spread_landed(ch, k, j)
                if diag and k == 0:
                    store_own(ch).wait()
            else:
                for j in range(1, m_size):
                    net.landed(whole(ch, z ^ k, m ^ j, 0, 2), mr.at[ch, j, k])

        def rows_start(h, _):
            if h:
                net.landed(act.at[0 if diag else 1, place(z, 1)], xr.at[1])
            elif not diag:
                net.landed(act.at[1, place(z, 0)], xr.at[0])
            if inner:
                rows_on(h, 0, 0, 3, 3)
            rows_on(h, 0, 1, 1, 1)
            swap(h, 0)

        def rows_next(h, k):
            net.landed(act.at[role, place(z ^ k, h)], ar.at[h, k])
            if inner:
                hop, there = {1: (3, 2), 3: (1, 2), 2: (1, 3)}[k]
                rows_on(h, k, 1 + k, hop, there)
            swap(h, k)

        def swapped(k, h):
            net.landed(act.at[1 - role, place(z ^ k, h)], wr.at[k, h])

        def rows_out():
            if diag:
                send(lambda: (low.at[1], act.at[1, own_place], near_s, xr.at[0], net.to(c=1 - c)))
            else:
                send(lambda: (low.at[0], act.at[0, own_place], near_s, xr.at[1], net.to(t=1 - t)))
                send(lambda: (low.at[1], act.at[1, own_place], far_s, xr.at[1], net.to(c=1 - c, t=1 - t)))

        runs = [quarters] + [pass_on(i) for i in range(4)]
        runs += [first, second, rows_start, rows_next, small_next, third, swapped]

        def run(codes):
            for code in codes:
                runs[code // 100](code // 10 % 10, code % 10)

        def end():
            for parts in sent:
                net.copy(*parts()).wait_send()

        return small_send, run, rows_out, small_last, end

    programs = {key: program(*key) for key in GATHER_ORDER}
    work = len(runs_before(GATHER_ORDER[True, True]))

    device_rows = functools.partial(table_place, m_size)

    def parameters():
        part = width // (8 * m_size * 2)
        per = 128 // part
        static = table_order(m_size)
        for b in range(width // 128):
            got = [table[static[b * per + e], 0:4, 0:part] for e in range(per)]
            par[:, b * 128 : (b + 1) * 128] = jnp.concatenate(got, axis=1)
        head = c * Z + z
        for b in range(n // 128):
            start = (head * n + b * 128) // part
            got = [table[device_rows(start + e), 4:6, 0:part] for e in range(per)]
            bias[:, b * 128 : (b + 1) * 128] = jnp.concatenate(got, axis=1)
        wide = up_bias.shape[1]
        for b in range(width // 128):
            got = [table[static[b * per + e], 6:8, 0:part] for e in range(per)]
            both = jnp.concatenate(got, axis=1)
            row_bias[:, b * 128 : (b + 1) * 128] = both[0:1] + both[1:2]
        row = 8 + head * wide // width
        for b in range(wide // 128):
            start = (lax.rem(head * wide, width) + b * 128) // part
            got = [table[device_rows(start + e), pl.ds(row, 1), 0:part] for e in range(per)]
            up_bias[:, b * 128 : (b + 1) * 128] = jnp.concatenate(got, axis=1)

    step = 16

    def attn_in():
        for one in inputs()[:4]:
            one.wait()
        wide = attn_v.shape[2] // Z

        @pl.loop(0, rows // step)
        def _(i):
            span = pl.ds(pl.multiple_of(i * step, step), step)
            for j in range(4):
                block = attn_v[j, span, :].astype(bf16)
                for q in range(Z):
                    at = j % 2 * wide
                    pieces[j // 2][q, span, at : at + wide] = block[:, q * wide : (q + 1) * wide]

    def mlp_in():
        for one in inputs()[6:]:
            one.wait()
        wide = mlp_v.shape[2] // (2 * Z)

        @pl.loop(0, rows // step)
        def _(i):
            span = pl.ds(pl.multiple_of(i * step, step), step)
            for j in range(2):
                block = mlp_v[j, span, :].astype(bf16)
                for q in range(2 * Z):
                    pieces[2 + 2 * j + q % 2][q // 2, span, :] = block[:, q * wide : (q + 1) * wide]

    def rows_low():
        for one in inputs()[4:6]:
            one.wait()
        out_sum[...] = jnp.zeros_like(out_sum)

        @pl.loop(0, half // step)
        def _(i):
            start = pl.multiple_of(i * step, step)
            span = pl.ds(start, step)
            normed, _ = layer_stats(rows_v[0, span, :])
            normed = normed.astype(bf16)
            low[0, span, :] = normed
            given = rows_v[1, span, :]
            low[1, span, :] = given.astype(bf16)
            out_sum[...] += jnp.sum(given, axis=0, keepdims=True)

            @pl.when(role == 0)
            def _():
                act[0, pl.ds(pl.multiple_of(z * seq + t * half + start, step), step), :] = normed

    def turns_in():
        for a, value in enumerate(turn_tables(lax.broadcasted_iota(jnp.int32, (seq, 128), 0).astype(f32))):
            for e in range(3):
                term = value.astype(bf16)
                base[:, (3 * a + e) * 128 : (3 * a + e + 1) * 128] = term
                value = value - term.astype(f32)

    def weights_in():
        return [
            pltpu.make_async_copy(full[0], w_qk, ls.at[0]),
            pltpu.make_async_copy(full[1], w_vo, ls.at[1]),
        ]

    def rows_saved(i):
        k = i ^ (inner_z & (i // 2))
        span = pl.ds(pl.multiple_of((z ^ k) * seq, seq), seq)
        return [
            pltpu.make_async_copy(one_v.at[lax.rem(i, 2)], one_out.at[span], os_.at[0, i]),
            pltpu.make_async_copy(two_v.at[span], two_out.at[span], os_.at[1, i]),
            pltpu.make_async_copy(act.at[:, span], act_out.at[:, span], os_.at[2, i]),
        ]

    def attention(i):
        @pl.when(i == 0)
        def _():
            for one in weights_in():
                one.start()
            parameters()
            turns_in()
            head_sums[...] = jnp.zeros_like(head_sums)
            for one in weights_in():
                one.wait()

        @pl.when(i >= 2)
        def _():
            rows_saved(i - 2)[0].wait()

        k = i ^ (inner_z & (i // 2))
        span = pl.ds(pl.multiple_of((z ^ k) * seq, seq), seq)
        x = act[0, span, :].astype(f32)
        one = (x * par[0:1, :] + par[1:2, :]).astype(bf16)
        one_v[lax.rem(i, 2)] = one
        two_v[span, :] = (x * par[2:3, :] + par[3:4, :]).astype(bf16)
        for copy in rows_saved(i):
            copy.start()
        source = device_rows((((z ^ k) * m_size + m) * 2 + t) * 2)
        across = jnp.concatenate([table[source, 12 + e : 13 + e, :] for e in range(seq // 128)], axis=1)
        spots = lax.broadcasted_iota(jnp.int32, (seq, seq), 0).astype(f32)
        hit = jnp.where(spots == across, 1.0, 0.0).astype(bf16)
        down = dot(hit, spots.astype(bf16), 0, 0)
        turns = dot(hit, base[...], 0, 0)
        tables = [sum(turns[:, (3 * a + e) * 128 : (3 * a + e + 1) * 128] for e in range(3)) for a in range(3)]
        scale = HEAD_DIM ** (-0.5)
        qk = dot(one, w_qk[...])
        q = turn(qk[:, :n] + bias[0:1, :], tables, 1.0).astype(bf16)
        k_rows = turn(qk[:, n:], tables, 1.0).astype(bf16)
        v = (dot(one, w_vo[:, :n]) + bias[1:2, :]).astype(bf16)
        d_att = dot(act[1, span, :], w_vo[:, n:]).astype(bf16)
        scores = jnp.where(across <= down, dot(q, k_rows, 1, 1) * scale, -jnp.inf)
        top = jnp.max(scores, axis=-1, keepdims=True)
        log_total = top + jnp.log(jnp.sum(jnp.exp(scores - top), axis=-1, keepdims=True))
        probs = jnp.exp(scores - log_total)
        low_probs = probs.astype(bf16)
        att[span, :] = dot(low_probs, v).astype(bf16)
        d_probs = dot(d_att, v, 1, 1)
        d_scores = (probs * (d_probs - jnp.sum(probs * d_probs, axis=-1, keepdims=True)) * scale).astype(bf16)
        d_q = turn(dot(d_scores, k_rows), tables, -1.0)
        d_k = turn(dot(d_scores, q, 0, 0), tables, -1.0)
        d_v = dot(low_probs, d_att, 0, 0)
        d_attn[span, 0:n] = d_q.astype(bf16)
        d_attn[span, n : 2 * n] = d_k.astype(bf16)
        d_attn[span, 2 * n :] = d_v.astype(bf16)
        head_sums[0:1, :] += jnp.sum(d_q, axis=0, keepdims=True)
        head_sums[1:2, :] += jnp.sum(d_v, axis=0, keepdims=True)

    wide = full[2].shape[1] // Z

    def tile_in(array, j):
        cols = pl.ds(pl.multiple_of(j * wide, wide), wide)
        return pltpu.make_async_copy(full[array].at[:, cols], tile_v.at[lax.rem(j, 2)], ls.at[lax.rem(j, 2)])

    def tile_ready(array, j):
        @pl.when(lax.rem(j, 2) == 0)
        def _():
            tile_in(array, j).start()
            tile_in(array, j + 1).start()

        tile_in(array, j).wait()

    def hidden(i):
        j = i - Z
        tile_ready(2, j)
        cols = pl.ds(pl.multiple_of(j * wide, wide), wide)
        pre = dot(two_v[...], tile_v[lax.rem(j, 2)]) + up_bias[:, cols]
        erf = 1.0 + lax.erf(pre * 0.7071067811865476)
        hidden_out[:, cols] = (0.5 * pre * erf).astype(bf16)
        slope[j] = 0.5 * erf + pre * jnp.exp(-0.5 * pre * pre) * 0.3989422804014327

    def hidden_back(i):
        j = i - 2 * Z
        tile_ready(3, j)
        cols = pl.ds(pl.multiple_of(j * wide, wide), wide)
        value = dot(act[1], tile_v[lax.rem(j, 2)]) * slope[j]
        d_pre[:, cols] = value.astype(bf16)
        up_sums[:, cols] = jnp.sum(value, axis=0, keepdims=True)

        @pl.when(j == Z - 1)
        def _():
            for one in tile_rows(0) + made_saved():
                one.start()

    def made_saved():
        pairs = zip((att, d_attn, hidden_out, d_pre), made_out)
        return [pltpu.make_async_copy(src, dst, made_s.at[i]) for i, (src, dst) in enumerate(pairs)]

    tall = 256
    last = width // tall

    def tile_rows(p):
        span = pl.ds(pl.multiple_of(p * tall, tall), tall)
        slot = lax.rem(p, 2)
        return [
            pltpu.make_async_copy(src.at[span], dst.at[slot], tile_s.at[slot, i])
            for i, (src, dst) in enumerate(zip(full, tiles))
        ]

    def rows_stored(p):
        cols = pl.ds(pl.multiple_of(p * tall, tall), tall)
        slot = lax.rem(p, 2)
        return [
            pltpu.make_async_copy(both_v.at[slot, i], ref.at[:, cols], rows_s.at[slot, i])
            for i, ref in enumerate(rows_made)
        ]

    def outputs(p):
        slot = lax.rem(p, 2)

        @pl.when(p + 1 < last)
        def _():
            for one in tile_rows(p + 1):
                one.start()

        @pl.when(p >= 2)
        def _():
            for one in rows_stored(p - 2):
                one.wait()

        for one in tile_rows(p):
            one.wait()
        cols = pl.ds(pl.multiple_of(p * tall, tall), tall)
        t_qk, t_vo, t_up, t_dn = (tile[slot] for tile in tiles)
        y = dot(att[...], t_vo[:, n:], 1, 1) + dot(hidden_out[...], t_dn, 1, 1)
        d_one = dot(d_attn[:, 0 : 2 * n], t_qk, 1, 1) + dot(d_attn[:, 2 * n :], t_vo[:, :n], 1, 1)
        d_two = dot(d_pre[...], t_up, 1, 1)
        u = d_one * par[0:1, cols] + d_two * par[2:3, cols]
        both_v[slot, 0] = jnp.where(role == 0, y, u).astype(bf16)
        both_v[slot, 1] = jnp.where(role == 0, u, y).astype(bf16)
        plain = act[0, :, cols].astype(f32)
        for i, value in enumerate((d_one * plain, d_one, d_two * plain, d_two)):
            norm_sums[i : i + 1, cols] = jnp.sum(value, axis=0, keepdims=True)
        for one in rows_stored(p):
            one.start()

    def part(i, inner, diag):
        _, run, rows_out, small_last, _ = programs[inner, diag]
        if i == 1:
            rows_out()
        run(runs_before(GATHER_ORDER[inner, diag])[i + 1])
        if i == 2:
            small_last()

    by_class(inner_z, role, lambda inner, diag: programs[inner, diag][0]())
    ahead = 3

    @pl.loop(0, work - 1 + last)
    def _(i):
        pl.when(i == 0)(attn_in)
        pl.when(i == 1)(rows_low)
        pl.when(i == 2)(mlp_in)
        pl.when((i >= ahead) & (i < ahead + Z))(lambda: attention(i - ahead))
        pl.when((i >= ahead + Z) & (i < ahead + 2 * Z))(lambda: hidden(i - ahead))
        pl.when((i >= ahead + 2 * Z) & (i < ahead + 3 * Z))(lambda: hidden_back(i - ahead))
        pl.when(i >= ahead + 3 * Z)(lambda: outputs(i - ahead - 3 * Z))
        for e in range(work - 1):

            @pl.when(i == e)
            def _(e=e):
                by_class(inner_z, role, functools.partial(part, e))

    by_class(inner_z, role, lambda inner, diag: programs[inner, diag][4]())
    for i in range(Z):
        saved = rows_saved(i)
        for copy in saved[1:] if i < 2 else saved:
            copy.wait()
    for copy in made_saved() + rows_stored(last - 2) + rows_stored(last - 1):
        copy.wait()


def runs_before(order):
    cuts = [i for i, code in enumerate(order) if code // 100 == 12]
    return [order[lo:hi] for lo, hi in zip([0] + [i + 1 for i in cuts], cuts + [len(order)])]


def table_place(m_size, index):
    z, rest = index // (4 * m_size), index % (4 * m_size)
    return rest * 4 + (z + z // 2) % 2 * 2 + z // 2


def table_order(m_size):
    return [table_place(m_size, i) for i in range(4 * m_size * Z)]


def by_class(inner_z, role, program):
    for inner in (False, True):
        for diag in (False, True):

            @pl.when((inner_z == int(inner)) & (role == int(not diag)))
            def _(inner=inner, diag=diag):
                program(inner, diag)


def gather(attn_weight, mlp_weight, block_in, out_grad, small, positions, m_size):
    rows = attn_weight.shape[0]
    own, width = block_in.shape
    tokens = Z * 2 * own
    devices = m_size * 4 * Z
    hidden, n = mlp_weight.shape[2] // Z, HEAD_DIM
    cols = [2 * n, 2 * n, hidden, hidden]
    count = len(CHUNKS)
    parts = [cols[array] // PARTS[array] for array, _, _ in CHUNKS]
    sem = pltpu.SemaphoreType.DMA
    doubling = m_size.bit_length() - 1 + 4
    in_place = pl.BlockSpec(memory_space=pl.ANY)
    in_vmem = pl.BlockSpec(memory_space=pltpu.VMEM)
    shape = lambda *dims: jax.ShapeDtypeStruct(dims, bf16)
    exact = lambda *dims: jax.ShapeDtypeStruct(dims, f32)
    vmem = lambda *dims: pltpu.VMEM(dims, bf16)
    wide = lambda *dims: pltpu.VMEM(dims, f32)
    outs = pl.pallas_call(
        functools.partial(gather_kernel, m_size),
        out_shape=[shape(width, n) for n in cols]
        + [shape(2, tokens, width), shape(tokens, width), shape(tokens, width)]
        + [shape(tokens, n), shape(tokens, 3 * n), shape(tokens, hidden), shape(tokens, hidden)]
        + [shape(tokens, width)] * 2
        + [exact(2, n), exact(1, hidden), exact(4, width), exact(1, width), exact(1, width)]
        + [shape(Z, rows, n) for n in parts]
        + [shape(m_size, Z, rows, n) for n in parts]
        + [shape(4, rows, n) for n in parts],
        in_specs=[in_place] * 4 + [in_vmem] * 2,
        out_specs=[in_place] * 13 + [in_vmem] * 5 + [in_place] * (3 * count),
        scratch_shapes=[
            sem((count, 3)),
            sem((count, Z)),
            sem((count, 4)),
            sem((count, 4)),
            sem((count, m_size, Z, 2)),
            sem((count, m_size, Z, 2)),
            sem((count, m_size, Z)),
            sem((count, m_size, Z)),
            sem,
            sem,
            sem((2,)),
            sem((2, 5)),
            sem((2, Z)),
            sem((Z, 2)),
            sem((Z, 2)),
            sem((doubling,)),
            sem((doubling,)),
            sem((8,)),
            sem((count,)),
            sem((2,)),
            sem((3, Z)),
            sem((4,)),
            sem((2, 4)),
            sem((2, 2)),
        ]
        + [vmem(Z, rows, n) for n in parts]
        + [vmem(2, tokens, width), vmem(width, 2 * n), vmem(width, 2 * n), vmem(2, 2 * own, width)]
        + [vmem(tokens, width), vmem(2, width, hidden // Z), wide(Z, tokens, hidden // Z)]
        + [wide(2, n), wide(1, hidden), wide(devices, 16, 128), vmem(2 * own, 9 * 128)]
        + [wide(4, rows, attn_weight.shape[2]), wide(2, rows, mlp_weight.shape[2])]
        + [wide(2, own, width), vmem(2, own, width), wide(4, width)]
        + [vmem(tokens, n), vmem(tokens, 3 * n), vmem(tokens, hidden), vmem(tokens, hidden)]
        + [vmem(2, 256, cols) for cols in cols]
        + [vmem(2, 2, tokens, 256)],
        compiler_params=pltpu.CompilerParams(collective_id=0, has_side_effects=True, vmem_limit_bytes=67043328),
        name="gather_all",
    )(attn_weight, mlp_weight, block_in, out_grad, small, positions)
    return (*outs[5:7], outs[4], *outs[7:11]), outs[11:13], outs[13:18]


VMEM_BYTES = 60 * 1024 * 1024


def dot(a, b, over_a=1, over_b=0):
    return lax.dot_general(a, b, (((over_a,), (over_b,)), ((), ())), preferred_element_type=f32)


def turn(value, tables, sign):
    cos, low, high = tables
    part = value[:, :128]
    turned = part * cos + sign * (
        pltpu.roll(part, 128 - ROT // 2, 1) * low + pltpu.roll(part, ROT // 2, 1) * high
    )
    return jnp.concatenate([turned, value[:, 128:]], axis=1)


def turn_tables(places):
    half = ROT // 2
    column = lax.broadcasted_iota(jnp.int32, places.shape, 1)
    frequency = jnp.exp(lax.rem(column, half).astype(f32) * (-2.0 / ROT * math.log(10000.0)))
    angles = places * frequency
    cos = jnp.where(column < ROT, jnp.cos(angles), 1.0)
    sin = jnp.sin(angles)
    return cos, jnp.where(column < half, -sin, 0.0), jnp.where((column >= half) & (column < ROT), sin, 0.0)


def fixed(*shape):
    return pl.BlockSpec(shape, lambda i: (0,) * len(shape))


def grads_kernel(one, two, g, att, d_attn, act, d_pre, qk, vo, up, dn):
    n = HEAD_DIM
    first = dot(one[...], d_attn[...], 0, 0)
    qk[...] = first[:, : 2 * n].astype(bf16)
    vo[:, :n] = first[:, 2 * n :].astype(bf16)
    vo[:, n:] = dot(g[...], att[...], 0, 0).astype(bf16)
    up[...] = dot(two[...], d_pre[...], 0, 0).astype(bf16)
    dn[...] = dot(g[...], act[...], 0, 0).astype(bf16)


def run_grads(one, two, acts, att, d_attn, act, d_pre):
    rows, width = one.shape
    step = 256
    tile = pl.BlockSpec((rows, step), lambda i: (0, i))
    fix = lambda v: pl.BlockSpec(v.shape, lambda i: (0, 0), pipeline_mode=pl.Buffered(1))
    cols = [2 * HEAD_DIM, 2 * HEAD_DIM, act.shape[1], act.shape[1]]
    return pl.pallas_call(
        grads_kernel,
        grid=(width // step,),
        in_specs=[tile, tile, pl.BlockSpec((None, rows, step), lambda i: (1, 0, i))]
        + [fix(v) for v in (att, d_attn, act, d_pre)],
        out_specs=[pl.BlockSpec((step, n), lambda i: (i, 0)) for n in cols],
        out_shape=[jax.ShapeDtypeStruct((width, n), bf16) for n in cols],
        compiler_params=pltpu.CompilerParams(vmem_limit_bytes=VMEM_BYTES),
        name="weight_grads",
    )(one, two, acts, att, d_attn, act, d_pre)


def add_rows(dst, sources):
    step = min(dst.shape[0], 32)

    @pl.loop(0, dst.shape[0] // step)
    def _(i):
        span = pl.ds(pl.multiple_of(i * step, step), step)
        total = sources[0][span, :].astype(f32)
        for one in sources[1:]:
            total = total + one[span, :].astype(f32)
        dst[span, :] = total.astype(dst.dtype)


def scatter_kernel(m_size, fused, *refs):
    if fused:
        ones, twos, acts, *factors_in = refs[:7]
        keep, give, *sums = refs[7:13]
        grads, refs = refs[13:17], refs[17:]
    else:
        grads, (keep, give, *sums), refs = refs[:4], refs[4:10], refs[10:]
    own, rows_out, small_out, refs = refs[:4], refs[4], refs[5], refs[6:]
    count = len(CHUNKS)
    buffers = []
    for _, _, m_first in CHUNKS:
        size = 5 if m_first else 6
        buffers.append(refs[:size])
        refs = refs[size:]
    relay, refs = refs[:count], refs[count:]
    got, kept, got_z, final, current, got_small = refs[:6]
    (gs, gr, kl, as_, ar, ys, yr, yl, ws, wr, wl, fs, fr, xs, xr, zs, zr, zl, ps, pr, ss, sr) = refs[6:28]
    if fused:
        tiles, made, tl, ml, factors, fl = refs[28:]
        att, d_attn, act, d_pre = factors
    net = Links(m_size)
    z, m, c, t = net.z, net.m, net.c, net.t
    half = rows_out.shape[1]
    role = lax.rem(c + t, 2)
    inner_z = lax.rem(z + z // 2, 2)
    flat, steps = net.doubling()
    steps = steps[::-1]

    def columns(ch):
        array, part, _ = CHUNKS[ch]
        wide = own[array].shape[2] // PARTS[array]
        return array, slice(part * wide, (part + 1) * wide)

    def rows_of(ch, k, j, cc=None):
        array, cols = columns(ch)
        if cc is None:
            return grads[array].at[z ^ k, m ^ j, :, :, cols]
        return grads[array].at[z ^ k, m ^ j, cc, :, cols]

    def owned(ch, zz):
        array, cols = columns(ch)
        return own[array].at[zz, :, cols]

    span = lambda h: pl.ds(pl.multiple_of((t ^ h) * half, half), half)
    loads_keep = [pltpu.make_async_copy(keep.at[z ^ k], kept.at[k], kl.at[k]) for k in range(Z)]
    for one in loads_keep:
        one.start()
    norm_sums, head_sums, up_sums, out_sum = sums

    def small_terms():
        current[...] = jnp.zeros_like(current)
        width, hidden, n = out_sum.shape[1], up_sums.shape[1], HEAD_DIM
        part = width // (4 * m_size * Z)
        for i, at in enumerate(table_order(m_size)):
            cols = slice(i * part, (i + 1) * part)
            current[at, 0:4, 0:part] = norm_sums[:, cols]
            current[at, 6:7, 0:part] = out_sum[:, cols]
            current[at, 7:8, 0:part] = out_sum[:, cols]
        head = c * Z + z
        for e in range(n // part):
            at = table_place(m_size, head * n // part + e)
            current[at, 4:6, 0:part] = head_sums[:, e * part : (e + 1) * part]
        row = 8 + head * hidden // width
        for e in range(hidden // part):
            at = table_place(m_size, head * hidden % width // part + e)
            current[at, pl.ds(row, 1), 0:part] = up_sums[:, e * part : (e + 1) * part]

    def tile_loads(i, slot):
        block = (z ^ (Z - 1 - lax.rem(i, Z))) * m_size + (m ^ (1 - i // Z))
        wide = tiles.shape[3]
        cols = pl.ds(pl.multiple_of(block * wide, wide), wide)
        sources = (ones.at[:, cols], twos.at[:, cols], acts.at[1, :, cols])
        return [pltpu.make_async_copy(src, tiles.at[slot, n], tl.at[slot, n]) for n, src in enumerate(sources)]

    def make(i):
        slot = lax.rem(i, 2)

        @pl.when(i < 2 * Z - 1)
        def _():
            for one in tile_loads(i + 1, 1 - slot):
                one.start()

        for one in tile_loads(i, slot):
            one.wait()

        @pl.when(i == 0)
        def _():
            for one in factor_loads():
                one.wait()

        n = HEAD_DIM
        high = made[0].shape[1]
        for array, at, left, right, lo, hi in (
            (0, 0, 0, d_attn, 0, 2 * n),
            (1, 0, 0, d_attn, 2 * n, 3 * n),
            (1, n, 2, att, 0, n),
            (2, 0, 1, d_pre, 0, d_pre.shape[1]),
            (3, 0, 2, act, 0, act.shape[1]),
        ):
            value = dot(tiles[slot, left], right[:, lo:hi], 0, 0).astype(bf16)
            for cc in range(2):
                made[array][cc, :, at : at + hi - lo] = value[cc * high : (cc + 1) * high]
        stores = [
            pltpu.make_async_copy(
                made[array], grads[array].at[z ^ (Z - 1 - lax.rem(i, Z)), m ^ (1 - i // Z)], ml.at[array]
            )
            for array in range(4)
        ]
        for one in stores:
            one.start()
        for one in stores:
            one.wait()

    def factor_loads():
        return [pltpu.make_async_copy(src, dst, fl.at[n]) for n, (src, dst) in enumerate(zip(factors_in, factors))]

    if fused:
        for one in tile_loads(0, 0) + factor_loads():
            one.start()
    net.meet()

    def program(inner, diag):
        state = {"small": 0}
        sent = []

        def send(*parts):
            (parts,) = parts
            net.copy(*parts()).start()
            sent.append(parts)

        def small_send():
            i = state["small"]
            if i < len(steps):
                size, target = steps[i]
                send(
                    lambda: (
                        current.at[pl.ds((flat // size ^ 1) * size, size)],
                        got_small.at[pl.ds(size, size)],
                        ss.at[i],
                        sr.at[i],
                        target,
                    )
                )

        def small_next(*_):
            i = state["small"]
            if i < len(steps):
                size = steps[i][0]
                net.landed(got_small.at[pl.ds(size, size)], sr.at[i])
                block = pl.ds(flat // size * size, size)
                current[block] = current[block] + got_small[pl.ds(size, size)]
                state["small"] += 1
                small_send()

        def swap(k, h):
            send(
                lambda: (give.at[z ^ k, span(h)], got.at[k, span(h)], gs.at[k, h], gr.at[k, h], net.to(c=1 - c))
            )

        def load_mine(ch, j, k):
            if CHUNKS[ch][2]:
                return pltpu.make_async_copy(rows_of(ch, k, j, c), buffers[ch][0].at[j, k], wl.at[ch, j, k])
            return pltpu.make_async_copy(rows_of(ch, k, 0), buffers[ch][0].at[k], wl.at[ch, 0, k])

        def load_made(k, own_m):
            for j in (0,) if own_m == 0 else range(1, m_size):
                for ch in range(count):
                    if (diag and CHUNKS[ch][2]) or (j == 0 and not CHUNKS[ch][2]):
                        load_mine(ch, j, k).start()

        def to_owner(source, home, far, ch, j, k):
            if diag:
                send(lambda: (source(1 - c), home(), ws.at[ch, j, k, 0], wr.at[ch, j, k, 0], net.to(c=1 - c)))
            else:
                send(lambda: (source(c), far(), ws.at[ch, j, k, 0], wr.at[ch, j, k, 1], net.to(t=1 - t)))
                send(
                    lambda: (source(1 - c), far(), ws.at[ch, j, k, 1], wr.at[ch, j, k, 1], net.to(c=1 - c, t=1 - t))
                )

        def owners_part(ch, j, k):
            home, far = buffers[ch][0], buffers[ch][1]
            to_owner(lambda cc: rows_of(ch, k, j, cc), lambda: home.at[j, k], lambda: far.at[j, k], ch, j, k)

        def others(ch, k):
            for j in range(1, m_size):
                owners_part(ch, j, k)

        def same(ch, k):
            owners_part(ch, 0, k)

        def across(ch, k):
            for j in range(1, m_size):
                send(
                    lambda j=j: (
                        rows_of(ch, k, j),
                        buffers[ch][1].at[j - 1, k],
                        fs.at[ch, j, k],
                        fr.at[ch, j, k],
                        net.to(m=m ^ j),
                    )
                )

        def collected(home, far, ch, j, k):
            if not diag:
                net.landed(home, wr.at[ch, j, k, 0])
            elif CHUNKS[ch][2]:
                load_mine(ch, j, k).wait()
            net.landed(far, wr.at[ch, j, k, 1])

        def middle(ch, k):
            home, far, mid, far_m, _ = buffers[ch]
            for j in range(1, m_size):
                collected(home.at[j, k], far.at[j, k], ch, j, k)
                add_rows(mid.at[j - 1, k], [home.at[j, k], far.at[j, k]])
                send(
                    lambda j=j: (
                        mid.at[j - 1, k],
                        far_m.at[j - 1, k],
                        xs.at[ch, j, k],
                        xr.at[ch, j, k],
                        net.to(m=m ^ j),
                    )
                )

        def summed(ch, k):
            mine, far_m, both, home, far, _ = buffers[ch]
            load_mine(ch, 0, k).wait()
            for j in range(1, m_size):
                net.landed(far_m.at[j - 1, k], fr.at[ch, j, k])
            for cc in range(2):
                add_rows(both.at[k, cc], [mine.at[k, cc]] + [far_m.at[j - 1, k, cc] for j in range(1, m_size)])
            to_owner(lambda cc: both.at[k, cc], lambda: home.at[k], lambda: far.at[k], ch, 0, k)

        def finish(ch, k):
            if CHUNKS[ch][2]:
                home, far, _, far_m, result = buffers[ch]
                collected(home.at[0, k], far.at[0, k], ch, 0, k)
                for j in range(1, m_size):
                    net.landed(far_m.at[j - 1, k], xr.at[ch, j, k])
                sources = [home.at[0, k], far.at[0, k]] + [far_m.at[j - 1, k] for j in range(1, m_size)]
            else:
                _, _, both, home, far, result = buffers[ch]
                collected(home.at[k], far.at[k], ch, 0, k)
                sources = [both.at[k, c] if diag else home.at[k], far.at[k]]
            add_rows(result.at[k], sources)
            if k == 0:
                pltpu.make_async_copy(result.at[k], owned(ch, z), zl.at[ch]).start()
                return
            hop, through = {1: (1, None), 2: (3, 2), 3: (3, None)}[k] if inner else {1: (1, None), 2: (1, 0), 3: (1, 1)}[k]
            if through is None:
                send(lambda: (result.at[k], owned(ch, z), zs.at[ch, k], zr.at[ch, k], net.to(z=z ^ hop)))
            else:
                send(
                    lambda: (
                        result.at[k],
                        relay[ch].at[through],
                        zs.at[ch, k],
                        pr.at[ch, through],
                        net.to(z=z ^ hop),
                    )
                )

        def pass_on(through):
            hop, k = ((3, 2), (3, None), (1, 2), (1, 3))[through]

            def run(ch, _):
                net.landed(relay[ch].at[through], pr.at[ch, through])

                def parts():
                    if k is None:
                        dst, recv_sem = relay[ch].at[3], pr.at[ch, 3]
                    else:
                        dst, recv_sem = owned(ch, z ^ hop ^ k), zr.at[ch, k]
                    return relay[ch].at[through], dst, ps.at[ch, through], recv_sem, net.to(z=z ^ hop)

                send(parts)

            return run

        def rows_first(k, h):
            if h == 0:
                pltpu.make_async_copy(keep.at[z ^ k], kept.at[k], kl.at[k]).wait()
            net.landed(got.at[k, span(h)], gr.at[k, h])
            add_rows(kept.at[k, span(h)], [kept.at[k, span(h)], got.at[k, span(h)]])
            if k and not inner:
                slot = {1: 0, 2: 1, 3: 2}[k]
                send(
                    lambda: (
                        kept.at[k, span(h)],
                        got_z.at[slot, span(h)],
                        as_.at[k, h],
                        ar.at[slot, h],
                        net.to(z=z ^ 1),
                    )
                )

        def rows_through(k, h, slot, there, hop):
            net.landed(got_z.at[slot, span(h)], ar.at[slot, h])
            add_rows(kept.at[k, span(h)], [kept.at[k, span(h)], got_z.at[slot, span(h)]])
            send(
                lambda: (
                    kept.at[k, span(h)],
                    got_z.at[there, span(h)],
                    as_.at[k, h],
                    ar.at[there, h],
                    net.to(z=z ^ hop),
                )
            )

        def rows_inner(k, h):
            rows_through(k, h, {3: 1, 2: 2}[k], {3: 3, 2: 4}[k], 3)

        def rows_outer(h, _):
            rows_through(1, h, 4, 0, 1)

        def rows_back(h, _):
            slots = (0, 3) if inner else (0,)
            for slot in slots:
                net.landed(got_z.at[slot, span(h)], ar.at[slot, h])
            add_rows(final.at[h], [kept.at[0, span(h)]] + [got_z.at[slot, span(h)] for slot in slots])
            if diag and h == 0:
                pltpu.make_async_copy(final.at[h], rows_out.at[0], yl).start()
            elif diag:
                send(lambda: (final.at[h], rows_out.at[0], ys.at[h], yr.at[0], net.to(t=1 - t)))
            elif h == 0:
                send(lambda: (final.at[h], rows_out.at[1], ys.at[h], yr.at[1], net.to(c=1 - c)))
            else:
                send(lambda: (final.at[h], rows_out.at[1], ys.at[h], yr.at[1], net.to(c=1 - c, t=1 - t)))

        runs = [swap, load_made, others, same, across, rows_first, rows_inner, rows_outer, rows_back]
        runs += [middle, summed, finish] + [pass_on(i) for i in range(4)] + [small_next]

        def run(codes):
            for code in codes:
                runs[code // 100](code // 10 % 10, code % 10)

        def end():
            while state["small"] < len(steps):
                small_next()
            small_out[...] = current[flat]
            for ch in range(count):
                for k in range(1, Z):
                    net.landed(owned(ch, z ^ k), zr.at[ch, k])
                pltpu.make_async_copy(owned(ch, z), owned(ch, z), zl.at[ch]).wait()
            net.landed(rows_out.at[1], yr.at[1])
            if diag:
                pltpu.make_async_copy(final.at[0], rows_out.at[0], yl).wait()
            else:
                net.landed(rows_out.at[0], yr.at[0])
            for parts in sent:
                net.copy(*parts()).wait_send()

        return small_send, run, end

    programs = {key: program(*key) for key in SCATTER_ORDER}
    cuts = {
        key: [i for i, code in enumerate(codes) if code // 100 == 1] + [len(codes)]
        for key, codes in SCATTER_ORDER.items()
    }

    def begin(inner, diag):
        _, run, _ = programs[inner, diag]
        run(SCATTER_ORDER[inner, diag][: cuts[inner, diag][0]])

    def part(i, inner, diag):
        lo, hi = cuts[inner, diag][i : i + 2]
        programs[inner, diag][1](SCATTER_ORDER[inner, diag][lo:hi])

    by_class(inner_z, role, begin)
    small_terms()
    by_class(inner_z, role, lambda inner, diag: programs[inner, diag][0]())
    if fused:

        @pl.loop(0, 2 * Z)
        def _(i):
            make(i)
            for n in range(2 * Z):

                @pl.when(i == n)
                def _(n=n):
                    by_class(inner_z, role, functools.partial(part, n))

    else:
        for n in range(2 * Z):
            by_class(inner_z, role, functools.partial(part, n))
    by_class(inner_z, role, lambda inner, diag: programs[inner, diag][2]())


def scatter(factors, keep, give, sums, m_size, rows):
    one, two, acts, att, d_attn, act, d_pre = factors
    width = keep.shape[1]
    block = width // (2 * Z * m_size)
    seq = keep.shape[0] // Z
    cols = [2 * HEAD_DIM, 2 * HEAD_DIM, act.shape[1], act.shape[1]]
    parts = [cols[array] // PARTS[array] for array, _, _ in CHUNKS]
    count = len(CHUNKS)
    fused = m_size == 2 and 2 * block % 256 == 0
    sem = pltpu.SemaphoreType.DMA
    vmem = lambda *shape: pltpu.VMEM(shape, bf16)
    doubling = m_size.bit_length() - 1 + 4
    in_place = pl.BlockSpec(memory_space=pl.ANY)
    in_vmem = pl.BlockSpec(memory_space=pltpu.VMEM)
    far = m_size - 1
    term_shapes = [jax.ShapeDtypeStruct((Z, m_size, 2, block, n), bf16) for n in cols]
    out_shape = [jax.ShapeDtypeStruct((Z, block, n), bf16) for n in cols]
    out_shape += [jax.ShapeDtypeStruct((2, rows, width), bf16), jax.ShapeDtypeStruct((16, 128), f32)]
    out_specs = [in_place] * 5 + [in_vmem]
    if fused:
        inputs = [one, two, acts, att, d_attn, act, d_pre]
        in_specs = [in_place] * 7
        out_shape, out_specs = term_shapes + out_shape, [in_place] * 4 + out_specs
    else:
        inputs = [g.reshape(s.shape) for g, s in zip(run_grads(*factors), term_shapes)]
        in_specs = [in_place] * 4
    scratch = []
    for n, (_, _, m_first) in zip(parts, CHUNKS):
        if m_first:
            scratch += [vmem(m_size, Z, block, n)] * 2 + [vmem(far, Z, block, n)] * 2 + [vmem(Z, block, n)]
        else:
            scratch += [vmem(Z, 2, block, n), vmem(far, Z, 2, block, n), vmem(Z, 2, block, n)]
            scratch += [vmem(Z, block, n)] * 3
    scratch += [vmem(4, block, n) for n in parts]
    scratch += [vmem(Z, seq, width)] * 2 + [vmem(5, seq, width), vmem(2, rows, width)]
    scratch += [pltpu.VMEM((4 * m_size * Z, 16, 128), f32)] * 2
    scratch += [
        sem((Z, 2)),
        sem((Z, 2)),
        sem((Z,)),
        sem((Z, 2)),
        sem((5, 2)),
        sem((2,)),
        sem((2,)),
        sem,
        sem((count, m_size, Z, 2)),
        sem((count, m_size, Z, 2)),
        sem((count, m_size, Z)),
        sem((count, m_size, Z)),
        sem((count, m_size, Z)),
        sem((count, m_size, Z)),
        sem((count, m_size, Z)),
        sem((count, Z)),
        sem((count, Z)),
        sem((count,)),
        sem((count, 4)),
        sem((count, 4)),
        sem((doubling,)),
        sem((doubling,)),
    ]
    if fused:
        scratch.append(vmem(2, 3, keep.shape[0], 2 * block))
        made = [vmem(2, block, n) for n in cols]
        scratch_made = [sem((2, 3)), sem((4,))]
        loaded = [pltpu.VMEM(v.shape, bf16) for v in (att, d_attn, act, d_pre)] + [sem((4,))]
    outs = pl.pallas_call(
        functools.partial(scatter_entry, m_size, fused),
        out_shape=out_shape,
        in_specs=in_specs + [in_place] * 2 + [in_vmem] * 4,
        out_specs=out_specs,
        scratch_shapes=scratch + (made + scratch_made + loaded if fused else []),
        compiler_params=pltpu.CompilerParams(collective_id=1, has_side_effects=True, vmem_limit_bytes=67043328),
        name="scatter_all",
    )(*inputs, keep.reshape(Z, seq, width), give.reshape(Z, seq, width), *sums)
    outs = outs[4:] if fused else outs
    return outs[:4], outs[4], outs[5]


def scatter_entry(m_size, fused, *refs):
    if fused:
        refs = refs[:-11] + (refs[-11:-7],) + refs[-7:-5] + (refs[-5:-1],) + refs[-1:]
    scatter_kernel(m_size, fused, *refs)


def update_kernel(step, steps, *refs):
    rows, cotangent, back, bias, qk, vo, up, dn = refs[:8]
    attn, mlp, small_sums, small, refs = refs[8:11], refs[11:14], refs[14], refs[15:18], refs[18:]
    (block_out, input_grad), attn_outs, mlp_outs, small_outs = refs[:2], refs[2:6], refs[6:10], refs[10:14]
    attn_v, mlp_v, attn_new, mlp_new, in_sem, out_sem = refs[14:]
    i = pl.program_id(0)

    def copies(i, sources, buffer, sems, at, out):
        slot = lax.rem(i, 2)
        span = pl.ds(pl.multiple_of(i * step, step), step)
        made = []
        for n, ref in enumerate(sources):
            for j in range(ref.shape[1]):
                far, near = ref.at[span, j, :], buffer.at[slot, n, j]
                pair = (near, far) if out else (far, near)
                made.append(pltpu.make_async_copy(*pair, sems.at[slot, at + n, j]))
        return made

    loads = lambda i: copies(i, attn, attn_v, in_sem, 0, False) + copies(i, mlp, mlp_v, in_sem, 3, False)
    stores = lambda i: copies(i, attn_outs, attn_new, out_sem, 0, True) + copies(i, mlp_outs, mlp_new, out_sem, 4, True)

    @pl.when(i == 0)
    def _():
        for one in loads(0):
            one.start()
        g = small_sums[0 : small[0].shape[0], 0 : small[0].shape[1]]
        for ref, value in zip(small_outs, (g, *adam_step(small[0][...], g, small[1][...], small[2][...]))):
            ref[...] = value

    @pl.when(i + 1 < steps)
    def _():
        for one in loads(i + 1):
            one.start()

    normed, inverse = layer_stats(rows[...])
    block_out[...] = rows[...] + back[0].astype(f32) + bias[...]
    u = back[1].astype(f32)
    input_grad[...] = cotangent[...] + inverse * (
        u
        - jnp.mean(u, axis=-1, keepdims=True)
        - normed * jnp.mean(u * normed, axis=-1, keepdims=True)
    )

    @pl.when(i >= 2)
    def _():
        for one in stores(i - 2):
            one.wait()

    for one in loads(i):
        one.wait()
    slot = lax.rem(i, 2)
    for sources, olds, news in (((qk, qk, vo, vo), attn_v, attn_new), ((up, dn), mlp_v, mlp_new)):
        kinds, wide = olds.shape[2], olds.shape[4] // Z
        for j in range(kinds):
            at = j % (kinds // 2) * wide
            for q in range(Z):
                cols = slice(q * wide, (q + 1) * wide)
                g = sources[j][q, :, at : at + wide].astype(f32)
                updated = adam_step(olds[slot, 0, j, :, cols], g, olds[slot, 1, j, :, cols], olds[slot, 2, j, :, cols])
                for n, value in enumerate((g, *updated)):
                    news[slot, n, j, :, cols] = value
    for one in stores(i):
        one.start()

    @pl.when(i == steps - 1)
    def _():
        if steps > 1:
            for one in stores(i - 1):
                one.wait()
        for one in stores(i):
            one.wait()


def update(block_in, out_grad, own_rows, bias, own, attn, mlp, small_sums, small):
    rows, width = block_in.shape
    shard = attn[0].shape[0]
    step = min(shard, 32)
    steps = shard // step
    by_rows = pl.BlockSpec((rows // steps, width), lambda i: (i, 0))
    in_place = pl.BlockSpec(memory_space=pl.ANY)
    slots = lambda count, v: pltpu.VMEM((2, count, v.shape[1], step, v.shape[2]), f32)
    return pl.pallas_call(
        functools.partial(update_kernel, step, steps),
        grid=(steps,),
        in_specs=[by_rows, by_rows, pl.BlockSpec((2, rows // steps, width), lambda i: (0, i, 0)), fixed(1, width)]
        + [pl.BlockSpec((Z, step, g.shape[2]), lambda i: (0, i, 0)) for g in own]
        + [in_place] * 6
        + [fixed(*v.shape) for v in (small_sums, *small)],
        out_specs=[by_rows, by_rows] + [in_place] * 8 + [fixed(*small[0].shape)] * 4,
        out_shape=[jax.ShapeDtypeStruct((rows, width), f32)] * 2
        + [jax.ShapeDtypeStruct(attn[0].shape, f32)] * 4
        + [jax.ShapeDtypeStruct(mlp[0].shape, f32)] * 4
        + [jax.ShapeDtypeStruct(small[0].shape, f32)] * 4,
        scratch_shapes=[slots(3, attn[0]), slots(3, mlp[0]), slots(4, attn[0]), slots(4, mlp[0])]
        + [pltpu.SemaphoreType.DMA((2, 6, 4)), pltpu.SemaphoreType.DMA((2, 8, 4))],
        compiler_params=pltpu.CompilerParams(vmem_limit_bytes=VMEM_BYTES),
        name="update",
    )(block_in, out_grad, own_rows, bias, *own, *attn, *mlp, small_sums, *small)


def body(
    block_in,
    positions,
    out_grad,
    attn_weight,
    mlp_weight,
    small_params,
    attn_first,
    attn_second,
    mlp_first,
    mlp_second,
    small_first,
    small_second,
):
    m_size = lax.axis_size("dp") // (2 * Z)
    rows = block_in.shape[0]
    factors, (keep, give), sums = gather(
        attn_weight, mlp_weight, block_in, out_grad, small_params, positions, m_size
    )
    head_sums, up_sums, norm_sums, row_bias, out_sum = sums
    own, own_rows, own_small = scatter(
        factors, keep, give, (norm_sums, head_sums, up_sums, out_sum), m_size, rows
    )
    attn = (attn_weight, attn_first, attn_second)
    mlp = (mlp_weight, mlp_first, mlp_second)
    small = (small_params, small_first, small_second)
    block_out, input_grad, *updated = update(
        block_in, out_grad, own_rows, row_bias, own, attn, mlp, own_small, small
    )
    attn_out, mlp_out = updated[:4], updated[4:8]
    small_grad, small_new, small_first_new, small_second_new = updated[8:]

    attn_grad, attn_new, attn_first_new, attn_second_new = attn_out
    mlp_grad, mlp_new, mlp_first_new, mlp_second_new = mlp_out
    return (
        block_out,
        input_grad,
        attn_grad,
        mlp_grad,
        small_grad,
        attn_new,
        attn_first_new,
        attn_second_new,
        mlp_new,
        mlp_first_new,
        mlp_second_new,
        small_new,
        small_first_new,
        small_second_new,
    )


def solution(mesh):
    rows = P(("dp", "tensor"), None)
    weights = P("dp", None, "tensor")
    small = P(None, ("dp", "tensor"))
    return jax.shard_map(
        body,
        mesh=mesh,
        in_specs=(rows, P("dp", None), rows, weights, weights, small, weights, weights, weights, weights, small, small),
        out_specs=(rows, rows) + (weights,) * 2 + (small,) + (weights,) * 6 + (small,) * 3,
        check_vma=False,
    )
```

```python
import functools
import math

import jax
import jax.numpy as jnp
from jax import lax
from jax.experimental import pallas as pl
from jax.experimental.pallas import tpu as pltpu
from jax.sharding import PartitionSpec as P

ROT = 64
ADAM_STEP = 3
HEAD_DIM = 256
Z = 4

norm_epsilon = 1e-05
learn_rate = 0.006
beta_first = 0.9
beta_second = 0.95
adam_epsilon = 1e-08
weight_decay = 0.1

f32 = jnp.float32
bf16 = jnp.bfloat16


def layer_stats(row_data):
    center = row_data - jnp.mean(row_data, axis=-1, keepdims=True)
    inverse = lax.rsqrt(jnp.mean(center * center, axis=-1, keepdims=True) + norm_epsilon)
    return (center * inverse, inverse)


def adam_step(weight, gradient, moment_one, moment_two):
    one_new = beta_first * moment_one + (1.0 - beta_first) * gradient
    two_new = beta_second * moment_two + (1.0 - beta_second) * gradient * gradient
    corrected = (one_new * (1.0 / (1.0 - beta_first**ADAM_STEP))) / (
        jnp.sqrt(two_new * (1.0 / (1.0 - beta_second**ADAM_STEP))) + adam_epsilon
    )
    return (weight - learn_rate * (corrected + weight_decay * weight), one_new, two_new)


MESH = pl.DeviceIdType.MESH
PARTS = (1, 1, 2, 2)
CHUNKS = ((0, 0, True), (1, 0, False), (2, 0, True), (2, 1, False), (3, 0, True), (3, 1, False))
GATHER_ORDER = {
    (False, False): (
        1201, 0, 10, 1200, 500, 510, 900, 501, 700, 1202, 20, 511, 520, 530, 540, 550, 600, 601, 1100, 910, 1101,
        620, 640, 801, 1110, 710, 30, 40, 50, 521, 502, 621, 610, 512, 602, 503, 611, 1010, 603, 630, 1111, 1011,
        811, 1030, 650, 531, 920, 1000, 541, 1050, 1001, 551, 641, 930, 1020, 1040, 940, 802, 1120, 522, 1021, 513,
        612, 622, 1002, 1012, 812, 1121, 631, 1003, 532, 542, 651, 1031, 552, 1041, 642, 613, 1051, 1022, 632, 803,
        652, 1042, 1013, 1203, 523, 1032, 1130, 1204, 533, 1052, 1205, 623, 1131, 1023, 813, 1206, 543, 553, 633,
        1207, 1208, 643, 653, 1033, 1209, 1043, 1210, 1053, 1211, 1212, 1213, 1214,
    ),
    (False, True): (
        1201, 0, 10, 1200, 700, 1202, 20, 500, 501, 510, 520, 530, 540, 550, 610, 900, 511, 1100, 600, 710, 30, 40,
        50, 601, 611, 630, 650, 1000, 1001, 620, 1020, 640, 801, 1040, 1010, 521, 910, 1110, 1011, 502, 1101, 1030,
        1050, 621, 1021, 811, 602, 1002, 531, 541, 551, 1111, 641, 631, 512, 612, 930, 920, 651, 1031, 1041, 1012,
        802, 940, 522, 1051, 503, 1120, 622, 603, 1003, 1022, 812, 532, 542, 1121, 632, 552, 642, 513, 613, 652,
        1032, 1042, 1013, 1203, 803, 1204, 523, 1052, 1130, 1205, 623, 813, 533, 633, 1023, 543, 1033, 553, 643,
        1131, 1206, 653, 1207, 1208, 1043, 1209, 1053, 1210, 1211, 1212, 1213, 1214,
    ),
    (True, False): (
        1201, 0, 10, 1200, 500, 510, 900, 200, 503, 700, 1202, 20, 520, 530, 540, 550, 600, 603, 100, 300, 1100, 501,
        513, 210, 310, 1101, 620, 110, 400, 640, 511, 910, 601, 710, 30, 40, 50, 803, 1130, 610, 523, 801, 320, 1110,
        220, 1010, 502, 630, 120, 623, 410, 521, 602, 512, 650, 1000, 1030, 1003, 621, 1131, 811, 1050, 613, 813,
        230, 1111, 533, 1020, 130, 1013, 330, 1040, 531, 920, 543, 611, 240, 340, 930, 140, 1001, 643, 553, 541, 350,
        250, 1011, 150, 1023, 940, 551, 641, 1002, 802, 420, 1120, 1021, 522, 633, 612, 622, 631, 1033, 1043, 1012,
        1203, 653, 1031, 430, 812, 1121, 1204, 532, 651, 1041, 1205, 1022, 1053, 440, 1206, 542, 632, 1051, 450,
        1207, 552, 1208, 642, 1032, 1209, 652, 1210, 1042, 1211, 1052, 1212, 1213, 1214,
    ),
    (True, True): (
        1201, 0, 10, 1200, 700, 1202, 20, 500, 503, 510, 520, 530, 540, 550, 610, 200, 900, 100, 300, 1100, 600, 501,
        513, 710, 30, 40, 50, 603, 630, 650, 1000, 1003, 613, 210, 310, 620, 110, 1020, 640, 511, 1040, 611, 1010,
        601, 1001, 803, 1101, 1030, 523, 1050, 801, 320, 1130, 1013, 220, 400, 1110, 120, 502, 1011, 521, 910, 623,
        1023, 602, 1002, 621, 813, 533, 811, 1021, 330, 230, 1111, 543, 1131, 130, 633, 340, 531, 643, 631, 553, 240,
        930, 920, 1033, 350, 140, 410, 541, 1043, 1031, 653, 512, 612, 250, 940, 150, 641, 551, 651, 1053, 1041, 802,
        1012, 1203, 1051, 420, 1120, 1204, 522, 1205, 622, 1022, 812, 430, 532, 1121, 1206, 632, 440, 1207, 542,
        1208, 1032, 450, 1209, 552, 642, 1210, 652, 1042, 1211, 1212, 1052, 1213, 1214,
    ),
}
SCATTER_ORDER = {
    (False, False): (
        30, 31, 20, 21, 10, 11, 0, 1, 131, 530, 531, 520, 521, 510, 511, 500, 501, 1600, 203, 413, 223, 433, 243,
        453, 121, 1610, 202, 412, 222, 432, 242, 903, 452, 111, 923, 1620, 201, 411, 221, 431, 241, 451, 101, 943,
        1630, 200, 410, 220, 430, 240, 450, 130, 902, 1013, 922, 1033, 303, 323, 343, 120, 942, 1053, 302, 322, 342,
        110, 901, 1012, 921, 301, 321, 341, 100, 800, 1032, 900, 941, 300, 320, 340, 920, 940, 1052, 1113, 810, 1133,
        1011, 1103, 1031, 1123, 1051, 1153, 1143, 1640, 1010, 1112, 1030, 1050, 1102, 1132, 1122, 1142, 1101, 1121,
        1152, 1100, 1141, 1120, 1111, 1140, 1131, 1151, 1110, 1130, 1150,
    ),
    (False, True): (
        30, 31, 20, 21, 10, 11, 0, 1, 131, 530, 531, 520, 521, 510, 511, 500, 501, 1600, 203, 413, 223, 433, 243,
        453, 121, 903, 1610, 202, 412, 222, 432, 242, 452, 111, 923, 201, 411, 221, 431, 241, 451, 101, 943, 1620,
        902, 200, 410, 220, 430, 240, 450, 130, 1013, 922, 1033, 1630, 303, 323, 942, 343, 120, 901, 1053, 302, 322,
        342, 110, 921, 301, 321, 341, 100, 1012, 900, 800, 941, 300, 320, 340, 920, 1032, 940, 1113, 1052, 1133, 810,
        1103, 1011, 1123, 1031, 1153, 1051, 1143, 1102, 1640, 1112, 1010, 1030, 1132, 1050, 1122, 1142, 1101, 1152,
        1121, 1100, 1141, 1111, 1120, 1131, 1140, 1151, 1110, 1130, 1150,
    ),
    (True, False): (
        30, 31, 20, 21, 10, 11, 0, 1, 131, 530, 531, 520, 521, 510, 511, 500, 501, 1600, 203, 413, 223, 433, 243,
        453, 121, 1610, 202, 412, 222, 432, 242, 903, 620, 452, 111, 923, 1620, 201, 411, 221, 431, 241, 451, 101,
        943, 200, 410, 220, 430, 240, 450, 130, 621, 700, 902, 1013, 922, 1033, 942, 1053, 303, 323, 343, 120, 901,
        1012, 921, 302, 322, 342, 110, 630, 710, 900, 1032, 941, 301, 321, 341, 100, 920, 300, 320, 340, 940, 1052,
        631, 1113, 1133, 1153, 1011, 1103, 800, 1123, 1031, 1112, 1051, 1143, 810, 1630, 1310, 1010, 1330, 1410,
        1300, 1132, 1030, 1640, 1320, 1510, 1350, 1050, 1530, 1340, 1102, 1500, 1210, 1122, 1430, 1200, 1142, 1520,
        1230, 1101, 1550, 1220, 1121, 1540, 1152, 1240, 1100, 1400, 1111, 1141, 1131, 1120, 1420, 1151, 1250, 1140,
        1440, 1110, 1130, 1450, 1150,
    ),
    (True, True): (
        30, 31, 20, 21, 10, 11, 0, 1, 131, 530, 531, 520, 521, 510, 511, 500, 501, 1600, 203, 413, 223, 433, 243,
        453, 121, 903, 1610, 202, 412, 620, 222, 432, 242, 452, 111, 923, 943, 201, 411, 221, 431, 241, 451, 101,
        902, 1620, 200, 410, 220, 430, 240, 450, 130, 621, 700, 1013, 922, 1033, 942, 901, 1053, 303, 323, 343, 120,
        921, 302, 322, 342, 110, 630, 710, 900, 1012, 941, 301, 321, 341, 920, 100, 1032, 940, 300, 320, 340, 1113,
        1052, 631, 1133, 1153, 1103, 1123, 1011, 800, 1143, 1112, 1031, 1051, 810, 1630, 1102, 1310, 1330, 1132,
        1010, 1300, 1410, 1640, 1320, 1400, 1030, 1350, 1510, 1340, 1530, 1050, 1200, 1430, 1122, 1210, 1500, 1142,
        1230, 1520, 1101, 1220, 1152, 1550, 1121, 1240, 1111, 1540, 1100, 1131, 1141, 1250, 1151, 1420, 1120, 1140,
        1440, 1110, 1130, 1150, 1450,
    ),
}


class Links:
    def __init__(self, m_size):
        self.m_size = m_size
        index = lax.axis_index("dp")
        self.z, self.m, self.c = index // (2 * m_size), (index // 2) % m_size, index % 2
        self.t = lax.axis_index("tensor")
        self.sends = []

    def to(self, z=None, m=None, c=None, t=None):
        z, m, c = (own if v is None else v for v, own in ((z, self.z), (m, self.m), (c, self.c)))
        return ((z * self.m_size + m) * 2 + c, self.t if t is None else t)

    def copy(self, src, dst, send_sem, recv_sem, target):
        return pltpu.make_async_remote_copy(
            src_ref=src, dst_ref=dst, send_sem=send_sem, recv_sem=recv_sem, device_id=target, device_id_type=MESH
        )

    def send(self, src, dst, send_sem, recv_sem, target):
        one = self.copy(src, dst, send_sem, recv_sem, target)
        one.start()
        self.sends.append(one)

    def landed(self, dst, recv_sem):
        self.copy(dst, dst, recv_sem, recv_sem, self.to(c=1 - self.c)).wait_recv()

    def drain(self):
        for one in self.sends:
            one.wait_send()
        self.sends = []

    def partners(self):
        other = 1 - self.t
        out = [self.to(z=self.z ^ k) for k in range(1, Z)]
        out += [self.to(m=self.m ^ j) for j in range(1, self.m_size)]
        out += [self.to(c=1 - self.c), self.to(t=other), self.to(c=1 - self.c, t=other)]
        return out

    def doubling(self):
        high = self.z // 2
        place = ((self.m * 2 + self.c) * 2 + self.t) * 4 + lax.rem(self.z + high, 2) * 2 + high
        steps = [(1, self.to(z=self.z ^ 3)), (2, self.to(z=self.z ^ 1)), (4, self.to(t=1 - self.t))]
        steps.append((8, self.to(c=1 - self.c)))
        j = 1
        while j < self.m_size:
            steps.append((16 * j, self.to(m=self.m ^ j)))
            j *= 2
        return place, steps

    def greet(self):
        for target in self.partners():
            pl.semaphore_signal(pltpu.get_barrier_semaphore(), inc=1, device_id=target, device_id_type=MESH)

    def meet(self):
        pl.semaphore_wait(pltpu.get_barrier_semaphore(), len(self.partners()))


def gather_kernel(m_size, *refs):
    weights, rows_in, small, positions = refs[:2], refs[2:4], refs[4], refs[5]
    full, act_out, one_out, two_out = refs[6:10], refs[10], refs[11], refs[12]
    made_out, rows_made = refs[13:17], refs[17:19]
    head_sums, up_sums, norm_sums, row_bias, out_sum = refs[19:24]
    count = len(CHUNKS)
    stage, stage_m, relay = (refs[24 + i * count : 24 + (i + 1) * count] for i in range(3))
    refs = refs[24 + 3 * count :]
    (zs, zr, gs, gr, ps, pr, ms, mr, near_s, far_s, xr, as_, ar, ws, wr, ss, sr, lin, lout, ls, os_, made_s, tile_s, rows_s) = refs[:24]
    pieces, refs = refs[24 : 24 + count], refs[24 + count :]
    act, w_qk, w_vo, one_v, two_v, tile_v, slope, bias, up_bias, table, base, attn_v, mlp_v, rows_v, low = refs[:15]
    par, att, d_attn, hidden_out, d_pre = refs[15:20]
    tiles, both_v = refs[20:24], refs[24]
    net = Links(m_size)
    z, m, c, t = net.z, net.m, net.c, net.t
    rows = pieces[0].shape[1]
    half = low.shape[1]
    seq = 2 * half
    width = low.shape[2]
    n = HEAD_DIM
    role = lax.rem(c + t, 2)
    inner_z = lax.rem(z + z // 2, 2)

    def columns(ch):
        array, part, _ = CHUNKS[ch]
        wide = pieces[ch].shape[2]
        return array, slice(part * wide, (part + 1) * wide)

    def piece(ch, zz):
        return pieces[ch].at[zz]

    def whole(ch, zz, mm, cc, size=1):
        array, cols = columns(ch)
        start = ((zz * m_size + mm) * 2 + cc) * rows
        return full[array].at[pl.ds(pl.multiple_of(start, rows), size * rows), cols]

    own_place = pl.ds(pl.multiple_of(z * seq + t * half, half), half)
    place = lambda zz, h: pl.ds(pl.multiple_of(zz * seq + (t ^ h) * half, half), half)

    def store_own(ch):
        return pltpu.make_async_copy(pieces[ch].at[z], whole(ch, z, m, c), lout.at[ch])

    def inputs():
        pairs = [(weights[0].at[:, j, :], attn_v.at[j]) for j in range(4)]
        pairs += [(rows_in[i], rows_v.at[i]) for i in range(2)]
        pairs += [(weights[1].at[:, j, :], mlp_v.at[j]) for j in range(2)]
        return [pltpu.make_async_copy(src, dst, lin.at[i]) for i, (src, dst) in enumerate(pairs)]

    net.greet()
    for one in inputs():
        one.start()
    flat, steps = net.doubling()
    table[flat] = jnp.zeros(table.shape[1:], f32)
    table[flat, 0:12, 0 : small.shape[1]] = small[...]
    for e in range(seq // 128):
        table[flat, 12 + e : 13 + e, :] = positions[:, e * 128 : (e + 1) * 128].astype(f32)

    def program(inner, diag):
        state = {"small": 0}
        sent = []

        def send(parts):
            net.copy(*parts()).start()
            sent.append(parts)

        def small_send():
            i = state["small"]
            if i < len(steps):
                size, target = steps[i]

                def parts():
                    span = table.at[pl.ds(flat // size * size, size)]
                    return span, span, ss.at[i], sr.at[i], target

                send(parts)

        def small_next(*_):
            i = state["small"]
            if i < len(steps):
                size = steps[i][0]
                net.landed(table.at[pl.ds((flat // size ^ 1) * size, size)], sr.at[i])
                state["small"] += 1
                small_send()

        def small_last():
            while state["small"] < len(steps):
                small_next()

        def spot(ch, zz, j):
            if diag:
                return whole(ch, zz, m ^ j, c)
            return stage_m[ch].at[m ^ j, zz] if j else stage[ch].at[zz]

        def source(ch, k, j):
            return piece(ch, z) if k == 0 and j == 0 else spot(ch, z ^ k, j)

        def spread(ch, k, j):
            block = lambda: whole(ch, z ^ k, m ^ j, c)
            send(
                lambda: (
                    source(ch, k, j),
                    block(),
                    ps.at[ch, j, k, 1],
                    pr.at[ch, j, k, c],
                    net.to(c=t, t=1 - t),
                )
            )
            if not diag:
                send(
                    lambda: (source(ch, k, j), block(), ps.at[ch, j, k, 0], pr.at[ch, j, k, c], net.to(c=1 - c))
                )

        def spread_landed(ch, k, j):
            for cc in (1 - c,) if diag else (1 - c, c):
                net.landed(whole(ch, z ^ k, m ^ j, cc), pr.at[ch, j, k, cc])

        def swap(h, k):
            def parts():
                src = act.at[role, place(z ^ k, h)]
                return src, src, ws.at[k, h], wr.at[k, h], net.to(c=1 - c)

            send(parts)

        def rows_on(h, flip, i, hop, k):
            def parts():
                src = act.at[role, place(z ^ flip, h)]
                return src, src, as_.at[h, i], ar.at[h, k], net.to(z=z ^ hop)

            send(parts)

        def quarters(ch, _):
            for i, (k, hop, through) in enumerate(
                ((3, 3, None), (2, 3, 2), (1, 1, None)) if inner else ((3, 1, 1), (2, 1, 0), (1, 1, None))
            ):

                def parts(i=i, k=k, hop=hop, through=through):
                    if through is None:
                        dst, recv_sem = spot(ch, z, 0), zr.at[ch, k]
                    else:
                        dst, recv_sem = relay[ch].at[through], gr.at[ch, through]
                    return piece(ch, z ^ k), dst, zs.at[ch, i], recv_sem, net.to(z=z ^ hop)

                send(parts)

        def pass_on(through):
            hop, k = ((3, 2), (3, None), (1, 2), (1, 3))[through]

            def run(ch, _):
                net.landed(relay[ch].at[through], gr.at[ch, through])

                def parts():
                    if k is None:
                        dst, recv_sem = relay[ch].at[3], gr.at[ch, 3]
                    else:
                        dst, recv_sem = spot(ch, z ^ hop ^ k, 0), zr.at[ch, k]
                    return relay[ch].at[through], dst, gs.at[ch, through], recv_sem, net.to(z=z ^ hop)

                send(parts)

            return run

        def first(ch, k):
            if k:
                net.landed(spot(ch, z ^ k, 0), zr.at[ch, k])
            elif diag:
                store_own(ch).start()
            if CHUNKS[ch][2]:
                for j in range(1, m_size):

                    def parts(j=j):
                        dst = whole(ch, z ^ k, m, c) if diag else stage_m[ch].at[m, z ^ k]
                        return source(ch, k, 0), dst, ms.at[ch, j, k], mr.at[ch, j, k], net.to(m=m ^ j)

                    send(parts)
            spread(ch, k, 0)

        def second(ch, k):
            if CHUNKS[ch][2]:
                for j in range(1, m_size):
                    net.landed(spot(ch, z ^ k, j), mr.at[ch, j, k])
                    spread(ch, k, j)
            else:
                if diag and k == 0:
                    store_own(ch).wait()
                spread_landed(ch, k, 0)
                for j in range(1, m_size):

                    def parts(j=j):
                        both = whole(ch, z ^ k, m, 0, 2)
                        return both, both, ms.at[ch, j, k], mr.at[ch, j, k], net.to(m=m ^ j)

                    send(parts)

        def third(ch, k):
            if CHUNKS[ch][2]:
                for j in range(m_size):
                    spread_landed(ch, k, j)
                if diag and k == 0:
                    store_own(ch).wait()
            else:
                for j in range(1, m_size):
                    net.landed(whole(ch, z ^ k, m ^ j, 0, 2), mr.at[ch, j, k])

        def rows_start(h, _):
            if h:
                net.landed(act.at[0 if diag else 1, place(z, 1)], xr.at[1])
            elif not diag:
                net.landed(act.at[1, place(z, 0)], xr.at[0])
            if inner:
                rows_on(h, 0, 0, 3, 3)
            rows_on(h, 0, 1, 1, 1)
            swap(h, 0)

        def rows_next(h, k):
            net.landed(act.at[role, place(z ^ k, h)], ar.at[h, k])
            if inner:
                hop, there = {1: (3, 2), 3: (1, 2), 2: (1, 3)}[k]
                rows_on(h, k, 1 + k, hop, there)
            swap(h, k)

        def swapped(k, h):
            net.landed(act.at[1 - role, place(z ^ k, h)], wr.at[k, h])

        def rows_out():
            if diag:
                send(lambda: (low.at[1], act.at[1, own_place], near_s, xr.at[0], net.to(c=1 - c)))
            else:
                send(lambda: (low.at[0], act.at[0, own_place], near_s, xr.at[1], net.to(t=1 - t)))
                send(lambda: (low.at[1], act.at[1, own_place], far_s, xr.at[1], net.to(c=1 - c, t=1 - t)))

        runs = [quarters] + [pass_on(i) for i in range(4)]
        runs += [first, second, rows_start, rows_next, small_next, third, swapped]

        def run(codes):
            for code in codes:
                runs[code // 100](code // 10 % 10, code % 10)

        def end():
            for parts in sent:
                net.copy(*parts()).wait_send()

        return small_send, run, rows_out, small_last, end

    programs = {key: program(*key) for key in GATHER_ORDER}
    work = len(runs_before(GATHER_ORDER[True, True]))

    device_rows = functools.partial(table_place, m_size)

    def parameters():
        part = width // (8 * m_size * 2)
        per = 128 // part
        static = table_order(m_size)
        for b in range(width // 128):
            got = [table[static[b * per + e], 0:4, 0:part] for e in range(per)]
            par[:, b * 128 : (b + 1) * 128] = jnp.concatenate(got, axis=1)
        head = c * Z + z
        for b in range(n // 128):
            start = (head * n + b * 128) // part
            got = [table[device_rows(start + e), 4:6, 0:part] for e in range(per)]
            bias[:, b * 128 : (b + 1) * 128] = jnp.concatenate(got, axis=1)
        wide = up_bias.shape[1]
        for b in range(width // 128):
            got = [table[static[b * per + e], 6:8, 0:part] for e in range(per)]
            both = jnp.concatenate(got, axis=1)
            row_bias[:, b * 128 : (b + 1) * 128] = both[0:1] + both[1:2]
        row = 8 + head * wide // width
        for b in range(wide // 128):
            start = (lax.rem(head * wide, width) + b * 128) // part
            got = [table[device_rows(start + e), pl.ds(row, 1), 0:part] for e in range(per)]
            up_bias[:, b * 128 : (b + 1) * 128] = jnp.concatenate(got, axis=1)

    step = 16

    def attn_in():
        for one in inputs()[:4]:
            one.wait()
        wide = attn_v.shape[2] // Z

        @pl.loop(0, rows // step)
        def _(i):
            span = pl.ds(pl.multiple_of(i * step, step), step)
            for j in range(4):
                block = attn_v[j, span, :].astype(bf16)
                for q in range(Z):
                    at = j % 2 * wide
                    pieces[j // 2][q, span, at : at + wide] = block[:, q * wide : (q + 1) * wide]

    def mlp_in():
        for one in inputs()[6:]:
            one.wait()
        wide = mlp_v.shape[2] // (2 * Z)

        @pl.loop(0, rows // step)
        def _(i):
            span = pl.ds(pl.multiple_of(i * step, step), step)
            for j in range(2):
                block = mlp_v[j, span, :].astype(bf16)
                for q in range(2 * Z):
                    pieces[2 + 2 * j + q % 2][q // 2, span, :] = block[:, q * wide : (q + 1) * wide]

    def rows_low():
        for one in inputs()[4:6]:
            one.wait()
        out_sum[...] = jnp.zeros_like(out_sum)

        @pl.loop(0, half // step)
        def _(i):
            start = pl.multiple_of(i * step, step)
            span = pl.ds(start, step)
            normed, _ = layer_stats(rows_v[0, span, :])
            normed = normed.astype(bf16)
            low[0, span, :] = normed
            given = rows_v[1, span, :]
            low[1, span, :] = given.astype(bf16)
            out_sum[...] += jnp.sum(given, axis=0, keepdims=True)

            @pl.when(role == 0)
            def _():
                act[0, pl.ds(pl.multiple_of(z * seq + t * half + start, step), step), :] = normed

    def turns_in():
        for a, value in enumerate(turn_tables(lax.broadcasted_iota(jnp.int32, (seq, 128), 0).astype(f32))):
            for e in range(3):
                term = value.astype(bf16)
                base[:, (3 * a + e) * 128 : (3 * a + e + 1) * 128] = term
                value = value - term.astype(f32)

    def weights_in():
        return [
            pltpu.make_async_copy(full[0], w_qk, ls.at[0]),
            pltpu.make_async_copy(full[1], w_vo, ls.at[1]),
        ]

    def rows_saved(i):
        k = i ^ (inner_z & (i // 2))
        span = pl.ds(pl.multiple_of((z ^ k) * seq, seq), seq)
        return [
            pltpu.make_async_copy(one_v.at[lax.rem(i, 2)], one_out.at[span], os_.at[0, i]),
            pltpu.make_async_copy(two_v.at[span], two_out.at[span], os_.at[1, i]),
            pltpu.make_async_copy(act.at[:, span], act_out.at[:, span], os_.at[2, i]),
        ]

    def attention(i):
        @pl.when(i == 0)
        def _():
            for one in weights_in():
                one.start()
            parameters()
            turns_in()
            head_sums[...] = jnp.zeros_like(head_sums)
            for one in weights_in():
                one.wait()

        @pl.when(i >= 2)
        def _():
            rows_saved(i - 2)[0].wait()

        k = i ^ (inner_z & (i // 2))
        span = pl.ds(pl.multiple_of((z ^ k) * seq, seq), seq)
        x = act[0, span, :].astype(f32)
        one = (x * par[0:1, :] + par[1:2, :]).astype(bf16)
        one_v[lax.rem(i, 2)] = one
        two_v[span, :] = (x * par[2:3, :] + par[3:4, :]).astype(bf16)
        for copy in rows_saved(i):
            copy.start()
        source = device_rows((((z ^ k) * m_size + m) * 2 + t) * 2)
        across = jnp.concatenate([table[source, 12 + e : 13 + e, :] for e in range(seq // 128)], axis=1)
        spots = lax.broadcasted_iota(jnp.int32, (seq, seq), 0).astype(f32)
        hit = jnp.where(spots == across, 1.0, 0.0).astype(bf16)
        down = dot(hit, spots.astype(bf16), 0, 0)
        turns = dot(hit, base[...], 0, 0)
        tables = [sum(turns[:, (3 * a + e) * 128 : (3 * a + e + 1) * 128] for e in range(3)) for a in range(3)]
        scale = HEAD_DIM ** (-0.5)
        qk = dot(one, w_qk[...])
        q = turn(qk[:, :n] + bias[0:1, :], tables, 1.0).astype(bf16)
        k_rows = turn(qk[:, n:], tables, 1.0).astype(bf16)
        v = (dot(one, w_vo[:, :n]) + bias[1:2, :]).astype(bf16)
        d_att = dot(act[1, span, :], w_vo[:, n:]).astype(bf16)
        scores = jnp.where(across <= down, dot(q, k_rows, 1, 1) * scale, -jnp.inf)
        top = jnp.max(scores, axis=-1, keepdims=True)
        log_total = top + jnp.log(jnp.sum(jnp.exp(scores - top), axis=-1, keepdims=True))
        probs = jnp.exp(scores - log_total)
        low_probs = probs.astype(bf16)
        att[span, :] = dot(low_probs, v).astype(bf16)
        d_probs = dot(d_att, v, 1, 1)
        d_scores = (probs * (d_probs - jnp.sum(probs * d_probs, axis=-1, keepdims=True)) * scale).astype(bf16)
        d_q = turn(dot(d_scores, k_rows), tables, -1.0)
        d_k = turn(dot(d_scores, q, 0, 0), tables, -1.0)
        d_v = dot(low_probs, d_att, 0, 0)
        d_attn[span, 0:n] = d_q.astype(bf16)
        d_attn[span, n : 2 * n] = d_k.astype(bf16)
        d_attn[span, 2 * n :] = d_v.astype(bf16)
        head_sums[0:1, :] += jnp.sum(d_q, axis=0, keepdims=True)
        head_sums[1:2, :] += jnp.sum(d_v, axis=0, keepdims=True)

    wide = full[2].shape[1] // Z

    def tile_in(array, j):
        cols = pl.ds(pl.multiple_of(j * wide, wide), wide)
        return pltpu.make_async_copy(full[array].at[:, cols], tile_v.at[lax.rem(j, 2)], ls.at[lax.rem(j, 2)])

    def tile_ready(array, j):
        @pl.when(lax.rem(j, 2) == 0)
        def _():
            tile_in(array, j).start()
            tile_in(array, j + 1).start()

        tile_in(array, j).wait()

    def hidden(i):
        j = i - Z
        tile_ready(2, j)
        cols = pl.ds(pl.multiple_of(j * wide, wide), wide)
        pre = dot(two_v[...], tile_v[lax.rem(j, 2)]) + up_bias[:, cols]
        erf = 1.0 + lax.erf(pre * 0.7071067811865476)
        hidden_out[:, cols] = (0.5 * pre * erf).astype(bf16)
        slope[j] = 0.5 * erf + pre * jnp.exp(-0.5 * pre * pre) * 0.3989422804014327

    def hidden_back(i):
        j = i - 2 * Z
        tile_ready(3, j)
        cols = pl.ds(pl.multiple_of(j * wide, wide), wide)
        value = dot(act[1], tile_v[lax.rem(j, 2)]) * slope[j]
        d_pre[:, cols] = value.astype(bf16)
        up_sums[:, cols] = jnp.sum(value, axis=0, keepdims=True)

        @pl.when(j == Z - 1)
        def _():
            for one in tile_rows(0) + made_saved():
                one.start()

    def made_saved():
        pairs = zip((att, d_attn, hidden_out, d_pre), made_out)
        return [pltpu.make_async_copy(src, dst, made_s.at[i]) for i, (src, dst) in enumerate(pairs)]

    tall = 256
    last = width // tall

    def tile_rows(p):
        span = pl.ds(pl.multiple_of(p * tall, tall), tall)
        slot = lax.rem(p, 2)
        return [
            pltpu.make_async_copy(src.at[span], dst.at[slot], tile_s.at[slot, i])
            for i, (src, dst) in enumerate(zip(full, tiles))
        ]

    def rows_stored(p):
        cols = pl.ds(pl.multiple_of(p * tall, tall), tall)
        slot = lax.rem(p, 2)
        return [
            pltpu.make_async_copy(both_v.at[slot, i], ref.at[:, cols], rows_s.at[slot, i])
            for i, ref in enumerate(rows_made)
        ]

    def outputs(p):
        slot = lax.rem(p, 2)

        @pl.when(p + 1 < last)
        def _():
            for one in tile_rows(p + 1):
                one.start()

        @pl.when(p >= 2)
        def _():
            for one in rows_stored(p - 2):
                one.wait()

        for one in tile_rows(p):
            one.wait()
        cols = pl.ds(pl.multiple_of(p * tall, tall), tall)
        t_qk, t_vo, t_up, t_dn = (tile[slot] for tile in tiles)
        y = dot(att[...], t_vo[:, n:], 1, 1) + dot(hidden_out[...], t_dn, 1, 1)
        d_one = dot(d_attn[:, 0 : 2 * n], t_qk, 1, 1) + dot(d_attn[:, 2 * n :], t_vo[:, :n], 1, 1)
        d_two = dot(d_pre[...], t_up, 1, 1)
        u = d_one * par[0:1, cols] + d_two * par[2:3, cols]
        both_v[slot, 0] = jnp.where(role == 0, y, u).astype(bf16)
        both_v[slot, 1] = jnp.where(role == 0, u, y).astype(bf16)
        plain = act[0, :, cols].astype(f32)
        for i, value in enumerate((d_one * plain, d_one, d_two * plain, d_two)):
            norm_sums[i : i + 1, cols] = jnp.sum(value, axis=0, keepdims=True)
        for one in rows_stored(p):
            one.start()

    def part(i, inner, diag):
        _, run, rows_out, small_last, _ = programs[inner, diag]
        if i == 1:
            rows_out()
        run(runs_before(GATHER_ORDER[inner, diag])[i + 1])
        if i == 2:
            small_last()

    attn_in()
    net.meet()
    by_class(inner_z, role, lambda inner, diag: programs[inner, diag][0]())
    by_class(inner_z, role, functools.partial(part, 0))
    ahead = 3

    @pl.loop(1, work - 1 + last)
    def _(i):
        pl.when(i == 1)(rows_low)
        pl.when(i == 2)(mlp_in)
        pl.when((i >= ahead) & (i < ahead + Z))(lambda: attention(i - ahead))
        pl.when((i >= ahead + Z) & (i < ahead + 2 * Z))(lambda: hidden(i - ahead))
        pl.when((i >= ahead + 2 * Z) & (i < ahead + 3 * Z))(lambda: hidden_back(i - ahead))
        pl.when(i >= ahead + 3 * Z)(lambda: outputs(i - ahead - 3 * Z))
        for e in range(1, work - 1):

            @pl.when(i == e)
            def _(e=e):
                by_class(inner_z, role, functools.partial(part, e))

    by_class(inner_z, role, lambda inner, diag: programs[inner, diag][4]())
    for i in range(Z):
        saved = rows_saved(i)
        for copy in saved[1:] if i < 2 else saved:
            copy.wait()
    for copy in made_saved() + rows_stored(last - 2) + rows_stored(last - 1):
        copy.wait()


def runs_before(order):
    cuts = [i for i, code in enumerate(order) if code // 100 == 12]
    return [order[lo:hi] for lo, hi in zip([0] + [i + 1 for i in cuts], cuts + [len(order)])]


def table_place(m_size, index):
    z, rest = index // (4 * m_size), index % (4 * m_size)
    return rest * 4 + (z + z // 2) % 2 * 2 + z // 2


def table_order(m_size):
    return [table_place(m_size, i) for i in range(4 * m_size * Z)]


def by_class(inner_z, role, program):
    for inner in (False, True):
        for diag in (False, True):

            @pl.when((inner_z == int(inner)) & (role == int(not diag)))
            def _(inner=inner, diag=diag):
                program(inner, diag)


def gather(attn_weight, mlp_weight, block_in, out_grad, small, positions, m_size):
    rows = attn_weight.shape[0]
    own, width = block_in.shape
    tokens = Z * 2 * own
    devices = m_size * 4 * Z
    hidden, n = mlp_weight.shape[2] // Z, HEAD_DIM
    cols = [2 * n, 2 * n, hidden, hidden]
    count = len(CHUNKS)
    parts = [cols[array] // PARTS[array] for array, _, _ in CHUNKS]
    sem = pltpu.SemaphoreType.DMA
    doubling = m_size.bit_length() - 1 + 4
    in_place = pl.BlockSpec(memory_space=pl.ANY)
    in_vmem = pl.BlockSpec(memory_space=pltpu.VMEM)
    shape = lambda *dims: jax.ShapeDtypeStruct(dims, bf16)
    exact = lambda *dims: jax.ShapeDtypeStruct(dims, f32)
    vmem = lambda *dims: pltpu.VMEM(dims, bf16)
    wide = lambda *dims: pltpu.VMEM(dims, f32)
    outs = pl.pallas_call(
        functools.partial(gather_kernel, m_size),
        out_shape=[shape(width, n) for n in cols]
        + [shape(2, tokens, width), shape(tokens, width), shape(tokens, width)]
        + [shape(tokens, n), shape(tokens, 3 * n), shape(tokens, hidden), shape(tokens, hidden)]
        + [shape(tokens, width)] * 2
        + [exact(2, n), exact(1, hidden), exact(4, width), exact(1, width), exact(1, width)]
        + [shape(Z, rows, n) for n in parts]
        + [shape(m_size, Z, rows, n) for n in parts]
        + [shape(4, rows, n) for n in parts],
        in_specs=[in_place] * 4 + [in_vmem] * 2,
        out_specs=[in_place] * 13 + [in_vmem] * 5 + [in_place] * (3 * count),
        scratch_shapes=[
            sem((count, 3)),
            sem((count, Z)),
            sem((count, 4)),
            sem((count, 4)),
            sem((count, m_size, Z, 2)),
            sem((count, m_size, Z, 2)),
            sem((count, m_size, Z)),
            sem((count, m_size, Z)),
            sem,
            sem,
            sem((2,)),
            sem((2, 5)),
            sem((2, Z)),
            sem((Z, 2)),
            sem((Z, 2)),
            sem((doubling,)),
            sem((doubling,)),
            sem((8,)),
            sem((count,)),
            sem((2,)),
            sem((3, Z)),
            sem((4,)),
            sem((2, 4)),
            sem((2, 2)),
        ]
        + [vmem(Z, rows, n) for n in parts]
        + [vmem(2, tokens, width), vmem(width, 2 * n), vmem(width, 2 * n), vmem(2, 2 * own, width)]
        + [vmem(tokens, width), vmem(2, width, hidden // Z), wide(Z, tokens, hidden // Z)]
        + [wide(2, n), wide(1, hidden), wide(devices, 16, 128), vmem(2 * own, 9 * 128)]
        + [wide(4, rows, attn_weight.shape[2]), wide(2, rows, mlp_weight.shape[2])]
        + [wide(2, own, width), vmem(2, own, width), wide(4, width)]
        + [vmem(tokens, n), vmem(tokens, 3 * n), vmem(tokens, hidden), vmem(tokens, hidden)]
        + [vmem(2, 256, cols) for cols in cols]
        + [vmem(2, 2, tokens, 256)],
        compiler_params=pltpu.CompilerParams(collective_id=0, has_side_effects=True, vmem_limit_bytes=67043328),
        name="gather_all",
    )(attn_weight, mlp_weight, block_in, out_grad, small, positions)
    return (*outs[5:7], outs[4], *outs[7:11]), outs[11:13], outs[13:18]


VMEM_BYTES = 60 * 1024 * 1024


def dot(a, b, over_a=1, over_b=0):
    return lax.dot_general(a, b, (((over_a,), (over_b,)), ((), ())), preferred_element_type=f32)


def turn(value, tables, sign):
    cos, low, high = tables
    part = value[:, :128]
    turned = part * cos + sign * (
        pltpu.roll(part, 128 - ROT // 2, 1) * low + pltpu.roll(part, ROT // 2, 1) * high
    )
    return jnp.concatenate([turned, value[:, 128:]], axis=1)


def turn_tables(places):
    half = ROT // 2
    column = lax.broadcasted_iota(jnp.int32, places.shape, 1)
    frequency = jnp.exp(lax.rem(column, half).astype(f32) * (-2.0 / ROT * math.log(10000.0)))
    angles = places * frequency
    cos = jnp.where(column < ROT, jnp.cos(angles), 1.0)
    sin = jnp.sin(angles)
    return cos, jnp.where(column < half, -sin, 0.0), jnp.where((column >= half) & (column < ROT), sin, 0.0)


def fixed(*shape):
    return pl.BlockSpec(shape, lambda i: (0,) * len(shape))


def grads_kernel(one, two, g, att, d_attn, act, d_pre, qk, vo, up, dn):
    n = HEAD_DIM
    first = dot(one[...], d_attn[...], 0, 0)
    qk[...] = first[:, : 2 * n].astype(bf16)
    vo[:, :n] = first[:, 2 * n :].astype(bf16)
    vo[:, n:] = dot(g[...], att[...], 0, 0).astype(bf16)
    up[...] = dot(two[...], d_pre[...], 0, 0).astype(bf16)
    dn[...] = dot(g[...], act[...], 0, 0).astype(bf16)


def run_grads(one, two, acts, att, d_attn, act, d_pre):
    rows, width = one.shape
    step = 256
    tile = pl.BlockSpec((rows, step), lambda i: (0, i))
    fix = lambda v: pl.BlockSpec(v.shape, lambda i: (0, 0), pipeline_mode=pl.Buffered(1))
    cols = [2 * HEAD_DIM, 2 * HEAD_DIM, act.shape[1], act.shape[1]]
    return pl.pallas_call(
        grads_kernel,
        grid=(width // step,),
        in_specs=[tile, tile, pl.BlockSpec((None, rows, step), lambda i: (1, 0, i))]
        + [fix(v) for v in (att, d_attn, act, d_pre)],
        out_specs=[pl.BlockSpec((step, n), lambda i: (i, 0)) for n in cols],
        out_shape=[jax.ShapeDtypeStruct((width, n), bf16) for n in cols],
        compiler_params=pltpu.CompilerParams(vmem_limit_bytes=VMEM_BYTES),
        name="weight_grads",
    )(one, two, acts, att, d_attn, act, d_pre)


def add_rows(dst, sources):
    step = min(dst.shape[0], 32)

    @pl.loop(0, dst.shape[0] // step)
    def _(i):
        span = pl.ds(pl.multiple_of(i * step, step), step)
        total = sources[0][span, :].astype(f32)
        for one in sources[1:]:
            total = total + one[span, :].astype(f32)
        dst[span, :] = total.astype(dst.dtype)


def scatter_kernel(m_size, fused, *refs):
    if fused:
        ones, twos, acts, *factors_in = refs[:7]
        keep, give, *sums = refs[7:13]
        grads, refs = refs[13:17], refs[17:]
    else:
        grads, (keep, give, *sums), refs = refs[:4], refs[4:10], refs[10:]
    own, rows_out, small_out, refs = refs[:4], refs[4], refs[5], refs[6:]
    count = len(CHUNKS)
    buffers = []
    for _, _, m_first in CHUNKS:
        size = 5 if m_first else 6
        buffers.append(refs[:size])
        refs = refs[size:]
    relay, refs = refs[:count], refs[count:]
    got, kept, got_z, final, current, got_small = refs[:6]
    (gs, gr, kl, as_, ar, ys, yr, yl, ws, wr, wl, fs, fr, xs, xr, zs, zr, zl, ps, pr, ss, sr) = refs[6:28]
    if fused:
        tiles, made, tl, ml, factors, fl = refs[28:]
        att, d_attn, act, d_pre = factors
    net = Links(m_size)
    z, m, c, t = net.z, net.m, net.c, net.t
    half = rows_out.shape[1]
    role = lax.rem(c + t, 2)
    inner_z = lax.rem(z + z // 2, 2)
    flat, steps = net.doubling()
    steps = steps[::-1]

    def columns(ch):
        array, part, _ = CHUNKS[ch]
        wide = own[array].shape[2] // PARTS[array]
        return array, slice(part * wide, (part + 1) * wide)

    def rows_of(ch, k, j, cc=None):
        array, cols = columns(ch)
        if cc is None:
            return grads[array].at[z ^ k, m ^ j, :, :, cols]
        return grads[array].at[z ^ k, m ^ j, cc, :, cols]

    def owned(ch, zz):
        array, cols = columns(ch)
        return own[array].at[zz, :, cols]

    span = lambda h: pl.ds(pl.multiple_of((t ^ h) * half, half), half)
    loads_keep = [pltpu.make_async_copy(keep.at[z ^ k], kept.at[k], kl.at[k]) for k in range(Z)]
    for one in loads_keep:
        one.start()
    norm_sums, head_sums, up_sums, out_sum = sums

    def small_terms():
        current[...] = jnp.zeros_like(current)
        width, hidden, n = out_sum.shape[1], up_sums.shape[1], HEAD_DIM
        part = width // (4 * m_size * Z)
        for i, at in enumerate(table_order(m_size)):
            cols = slice(i * part, (i + 1) * part)
            current[at, 0:4, 0:part] = norm_sums[:, cols]
            current[at, 6:7, 0:part] = out_sum[:, cols]
            current[at, 7:8, 0:part] = out_sum[:, cols]
        head = c * Z + z
        for e in range(n // part):
            at = table_place(m_size, head * n // part + e)
            current[at, 4:6, 0:part] = head_sums[:, e * part : (e + 1) * part]
        row = 8 + head * hidden // width
        for e in range(hidden // part):
            at = table_place(m_size, head * hidden % width // part + e)
            current[at, pl.ds(row, 1), 0:part] = up_sums[:, e * part : (e + 1) * part]

    def tile_loads(i, slot):
        block = (z ^ (Z - 1 - lax.rem(i, Z))) * m_size + (m ^ (1 - i // Z))
        wide = tiles.shape[3]
        cols = pl.ds(pl.multiple_of(block * wide, wide), wide)
        sources = (ones.at[:, cols], twos.at[:, cols], acts.at[1, :, cols])
        return [pltpu.make_async_copy(src, tiles.at[slot, n], tl.at[slot, n]) for n, src in enumerate(sources)]

    def make(i):
        slot = lax.rem(i, 2)

        @pl.when(i < 2 * Z - 1)
        def _():
            for one in tile_loads(i + 1, 1 - slot):
                one.start()

        for one in tile_loads(i, slot):
            one.wait()

        @pl.when(i == 0)
        def _():
            for one in factor_loads():
                one.wait()

        n = HEAD_DIM
        high = made[0].shape[1]

        def stored(array):
            there = grads[array].at[z ^ (Z - 1 - lax.rem(i, Z)), m ^ (1 - i // Z)]
            return pltpu.make_async_copy(made[array], there, ml.at[array])

        for array, at, left, right, lo, hi in (
            (0, 0, 0, d_attn, 0, 2 * n),
            (1, 0, 0, d_attn, 2 * n, 3 * n),
            (1, n, 2, att, 0, n),
            (2, 0, 1, d_pre, 0, d_pre.shape[1]),
            (3, 0, 2, act, 0, act.shape[1]),
        ):
            value = dot(tiles[slot, left], right[:, lo:hi], 0, 0).astype(bf16)
            for cc in range(2):
                made[array][cc, :, at : at + hi - lo] = value[cc * high : (cc + 1) * high]
            if array != 1 or at:
                stored(array).start()
        for array in range(4):
            stored(array).wait()

    def factor_loads():
        return [pltpu.make_async_copy(src, dst, fl.at[n]) for n, (src, dst) in enumerate(zip(factors_in, factors))]

    net.greet()
    if fused:
        for one in tile_loads(0, 0) + factor_loads():
            one.start()
    small_terms()
    net.meet()

    def program(inner, diag):
        state = {"small": 0}
        sent = []

        def send(*parts):
            (parts,) = parts
            net.copy(*parts()).start()
            sent.append(parts)

        def small_send():
            i = state["small"]
            if i < len(steps):
                size, target = steps[i]
                send(
                    lambda: (
                        current.at[pl.ds((flat // size ^ 1) * size, size)],
                        got_small.at[pl.ds(size, size)],
                        ss.at[i],
                        sr.at[i],
                        target,
                    )
                )

        def small_next(*_):
            i = state["small"]
            if i < len(steps):
                size = steps[i][0]
                net.landed(got_small.at[pl.ds(size, size)], sr.at[i])
                block = pl.ds(flat // size * size, size)
                current[block] = current[block] + got_small[pl.ds(size, size)]
                state["small"] += 1
                small_send()

        def swap(k, h):
            send(
                lambda: (give.at[z ^ k, span(h)], got.at[k, span(h)], gs.at[k, h], gr.at[k, h], net.to(c=1 - c))
            )

        def load_mine(ch, j, k):
            if CHUNKS[ch][2]:
                return pltpu.make_async_copy(rows_of(ch, k, j, c), buffers[ch][0].at[j, k], wl.at[ch, j, k])
            return pltpu.make_async_copy(rows_of(ch, k, 0), buffers[ch][0].at[k], wl.at[ch, 0, k])

        def load_made(k, own_m):
            for j in (0,) if own_m == 0 else range(1, m_size):
                for ch in range(count):
                    if (diag and CHUNKS[ch][2]) or (j == 0 and not CHUNKS[ch][2]):
                        load_mine(ch, j, k).start()

        def to_owner(source, home, far, ch, j, k):
            if diag:
                send(lambda: (source(1 - c), home(), ws.at[ch, j, k, 0], wr.at[ch, j, k, 0], net.to(c=1 - c)))
            else:
                send(lambda: (source(c), far(), ws.at[ch, j, k, 0], wr.at[ch, j, k, 1], net.to(t=1 - t)))
                send(
                    lambda: (source(1 - c), far(), ws.at[ch, j, k, 1], wr.at[ch, j, k, 1], net.to(c=1 - c, t=1 - t))
                )

        def owners_part(ch, j, k):
            home, far = buffers[ch][0], buffers[ch][1]
            to_owner(lambda cc: rows_of(ch, k, j, cc), lambda: home.at[j, k], lambda: far.at[j, k], ch, j, k)

        def others(ch, k):
            for j in range(1, m_size):
                owners_part(ch, j, k)

        def same(ch, k):
            owners_part(ch, 0, k)

        def across(ch, k):
            for j in range(1, m_size):
                send(
                    lambda j=j: (
                        rows_of(ch, k, j),
                        buffers[ch][1].at[j - 1, k],
                        fs.at[ch, j, k],
                        fr.at[ch, j, k],
                        net.to(m=m ^ j),
                    )
                )

        def collected(home, far, ch, j, k):
            if not diag:
                net.landed(home, wr.at[ch, j, k, 0])
            elif CHUNKS[ch][2]:
                load_mine(ch, j, k).wait()
            net.landed(far, wr.at[ch, j, k, 1])

        def middle(ch, k):
            home, far, mid, far_m, _ = buffers[ch]
            for j in range(1, m_size):
                collected(home.at[j, k], far.at[j, k], ch, j, k)
                add_rows(mid.at[j - 1, k], [home.at[j, k], far.at[j, k]])
                send(
                    lambda j=j: (
                        mid.at[j - 1, k],
                        far_m.at[j - 1, k],
                        xs.at[ch, j, k],
                        xr.at[ch, j, k],
                        net.to(m=m ^ j),
                    )
                )

        def summed(ch, k):
            mine, far_m, both, home, far, _ = buffers[ch]
            load_mine(ch, 0, k).wait()
            for j in range(1, m_size):
                net.landed(far_m.at[j - 1, k], fr.at[ch, j, k])
            for cc in range(2):
                add_rows(both.at[k, cc], [mine.at[k, cc]] + [far_m.at[j - 1, k, cc] for j in range(1, m_size)])
            to_owner(lambda cc: both.at[k, cc], lambda: home.at[k], lambda: far.at[k], ch, 0, k)

        def finish(ch, k):
            if CHUNKS[ch][2]:
                home, far, _, far_m, result = buffers[ch]
                collected(home.at[0, k], far.at[0, k], ch, 0, k)
                for j in range(1, m_size):
                    net.landed(far_m.at[j - 1, k], xr.at[ch, j, k])
                sources = [home.at[0, k], far.at[0, k]] + [far_m.at[j - 1, k] for j in range(1, m_size)]
            else:
                _, _, both, home, far, result = buffers[ch]
                collected(home.at[k], far.at[k], ch, 0, k)
                sources = [both.at[k, c] if diag else home.at[k], far.at[k]]
            add_rows(result.at[k], sources)
            if k == 0:
                pltpu.make_async_copy(result.at[k], owned(ch, z), zl.at[ch]).start()
                return
            hop, through = {1: (1, None), 2: (3, 2), 3: (3, None)}[k] if inner else {1: (1, None), 2: (1, 0), 3: (1, 1)}[k]
            if through is None:
                send(lambda: (result.at[k], owned(ch, z), zs.at[ch, k], zr.at[ch, k], net.to(z=z ^ hop)))
            else:
                send(
                    lambda: (
                        result.at[k],
                        relay[ch].at[through],
                        zs.at[ch, k],
                        pr.at[ch, through],
                        net.to(z=z ^ hop),
                    )
                )

        def pass_on(through):
            hop, k = ((3, 2), (3, None), (1, 2), (1, 3))[through]

            def run(ch, _):
                net.landed(relay[ch].at[through], pr.at[ch, through])

                def parts():
                    if k is None:
                        dst, recv_sem = relay[ch].at[3], pr.at[ch, 3]
                    else:
                        dst, recv_sem = owned(ch, z ^ hop ^ k), zr.at[ch, k]
                    return relay[ch].at[through], dst, ps.at[ch, through], recv_sem, net.to(z=z ^ hop)

                send(parts)

            return run

        def rows_first(k, h):
            if h == 0:
                pltpu.make_async_copy(keep.at[z ^ k], kept.at[k], kl.at[k]).wait()
            net.landed(got.at[k, span(h)], gr.at[k, h])
            add_rows(kept.at[k, span(h)], [kept.at[k, span(h)], got.at[k, span(h)]])
            if k and not inner:
                slot = {1: 0, 2: 1, 3: 2}[k]
                send(
                    lambda: (
                        kept.at[k, span(h)],
                        got_z.at[slot, span(h)],
                        as_.at[k, h],
                        ar.at[slot, h],
                        net.to(z=z ^ 1),
                    )
                )

        def rows_through(k, h, slot, there, hop):
            net.landed(got_z.at[slot, span(h)], ar.at[slot, h])
            add_rows(kept.at[k, span(h)], [kept.at[k, span(h)], got_z.at[slot, span(h)]])
            send(
                lambda: (
                    kept.at[k, span(h)],
                    got_z.at[there, span(h)],
                    as_.at[k, h],
                    ar.at[there, h],
                    net.to(z=z ^ hop),
                )
            )

        def rows_inner(k, h):
            rows_through(k, h, {3: 1, 2: 2}[k], {3: 3, 2: 4}[k], 3)

        def rows_outer(h, _):
            rows_through(1, h, 4, 0, 1)

        def rows_back(h, _):
            slots = (0, 3) if inner else (0,)
            for slot in slots:
                net.landed(got_z.at[slot, span(h)], ar.at[slot, h])
            add_rows(final.at[h], [kept.at[0, span(h)]] + [got_z.at[slot, span(h)] for slot in slots])
            if diag and h == 0:
                pltpu.make_async_copy(final.at[h], rows_out.at[0], yl).start()
            elif diag:
                send(lambda: (final.at[h], rows_out.at[0], ys.at[h], yr.at[0], net.to(t=1 - t)))
            elif h == 0:
                send(lambda: (final.at[h], rows_out.at[1], ys.at[h], yr.at[1], net.to(c=1 - c)))
            else:
                send(lambda: (final.at[h], rows_out.at[1], ys.at[h], yr.at[1], net.to(c=1 - c, t=1 - t)))

        runs = [swap, load_made, others, same, across, rows_first, rows_inner, rows_outer, rows_back]
        runs += [middle, summed, finish] + [pass_on(i) for i in range(4)] + [small_next]

        def run(codes):
            for code in codes:
                runs[code // 100](code // 10 % 10, code % 10)

        def end():
            while state["small"] < len(steps):
                small_next()
            small_out[...] = current[flat]
            for ch in range(count):
                for k in range(1, Z):
                    net.landed(owned(ch, z ^ k), zr.at[ch, k])
                pltpu.make_async_copy(owned(ch, z), owned(ch, z), zl.at[ch]).wait()
            net.landed(rows_out.at[1], yr.at[1])
            if diag:
                pltpu.make_async_copy(final.at[0], rows_out.at[0], yl).wait()
            else:
                net.landed(rows_out.at[0], yr.at[0])
            for parts in sent:
                net.copy(*parts()).wait_send()

        return small_send, run, end

    programs = {key: program(*key) for key in SCATTER_ORDER}
    cuts = {
        key: [i for i, code in enumerate(codes) if code // 100 == 1] + [len(codes)]
        for key, codes in SCATTER_ORDER.items()
    }

    def begin(inner, diag):
        _, run, _ = programs[inner, diag]
        run(SCATTER_ORDER[inner, diag][: cuts[inner, diag][0]])

    def part(i, inner, diag):
        lo, hi = cuts[inner, diag][i : i + 2]
        programs[inner, diag][1](SCATTER_ORDER[inner, diag][lo:hi])

    by_class(inner_z, role, begin)
    by_class(inner_z, role, lambda inner, diag: programs[inner, diag][0]())
    if fused:

        @pl.loop(0, 2 * Z)
        def _(i):
            make(i)
            for n in range(2 * Z):

                @pl.when(i == n)
                def _(n=n):
                    by_class(inner_z, role, functools.partial(part, n))

    else:
        for n in range(2 * Z):
            by_class(inner_z, role, functools.partial(part, n))
    by_class(inner_z, role, lambda inner, diag: programs[inner, diag][2]())


def scatter(factors, keep, give, sums, m_size, rows):
    one, two, acts, att, d_attn, act, d_pre = factors
    width = keep.shape[1]
    block = width // (2 * Z * m_size)
    seq = keep.shape[0] // Z
    cols = [2 * HEAD_DIM, 2 * HEAD_DIM, act.shape[1], act.shape[1]]
    parts = [cols[array] // PARTS[array] for array, _, _ in CHUNKS]
    count = len(CHUNKS)
    fused = m_size == 2 and 2 * block % 256 == 0
    sem = pltpu.SemaphoreType.DMA
    vmem = lambda *shape: pltpu.VMEM(shape, bf16)
    doubling = m_size.bit_length() - 1 + 4
    in_place = pl.BlockSpec(memory_space=pl.ANY)
    in_vmem = pl.BlockSpec(memory_space=pltpu.VMEM)
    far = m_size - 1
    term_shapes = [jax.ShapeDtypeStruct((Z, m_size, 2, block, n), bf16) for n in cols]
    out_shape = [jax.ShapeDtypeStruct((Z, block, n), bf16) for n in cols]
    out_shape += [jax.ShapeDtypeStruct((2, rows, width), bf16), jax.ShapeDtypeStruct((16, 128), f32)]
    out_specs = [in_place] * 5 + [in_vmem]
    if fused:
        inputs = [one, two, acts, att, d_attn, act, d_pre]
        in_specs = [in_place] * 7
        out_shape, out_specs = term_shapes + out_shape, [in_place] * 4 + out_specs
    else:
        inputs = [g.reshape(s.shape) for g, s in zip(run_grads(*factors), term_shapes)]
        in_specs = [in_place] * 4
    scratch = []
    for n, (_, _, m_first) in zip(parts, CHUNKS):
        if m_first:
            scratch += [vmem(m_size, Z, block, n)] * 2 + [vmem(far, Z, block, n)] * 2 + [vmem(Z, block, n)]
        else:
            scratch += [vmem(Z, 2, block, n), vmem(far, Z, 2, block, n), vmem(Z, 2, block, n)]
            scratch += [vmem(Z, block, n)] * 3
    scratch += [vmem(4, block, n) for n in parts]
    scratch += [vmem(Z, seq, width)] * 2 + [vmem(5, seq, width), vmem(2, rows, width)]
    scratch += [pltpu.VMEM((4 * m_size * Z, 16, 128), f32)] * 2
    scratch += [
        sem((Z, 2)),
        sem((Z, 2)),
        sem((Z,)),
        sem((Z, 2)),
        sem((5, 2)),
        sem((2,)),
        sem((2,)),
        sem,
        sem((count, m_size, Z, 2)),
        sem((count, m_size, Z, 2)),
        sem((count, m_size, Z)),
        sem((count, m_size, Z)),
        sem((count, m_size, Z)),
        sem((count, m_size, Z)),
        sem((count, m_size, Z)),
        sem((count, Z)),
        sem((count, Z)),
        sem((count,)),
        sem((count, 4)),
        sem((count, 4)),
        sem((doubling,)),
        sem((doubling,)),
    ]
    if fused:
        scratch.append(vmem(2, 3, keep.shape[0], 2 * block))
        made = [vmem(2, block, n) for n in cols]
        scratch_made = [sem((2, 3)), sem((4,))]
        loaded = [pltpu.VMEM(v.shape, bf16) for v in (att, d_attn, act, d_pre)] + [sem((4,))]
    outs = pl.pallas_call(
        functools.partial(scatter_entry, m_size, fused),
        out_shape=out_shape,
        in_specs=in_specs + [in_place] * 2 + [in_vmem] * 4,
        out_specs=out_specs,
        scratch_shapes=scratch + (made + scratch_made + loaded if fused else []),
        compiler_params=pltpu.CompilerParams(collective_id=1, has_side_effects=True, vmem_limit_bytes=67043328),
        name="scatter_all",
    )(*inputs, keep.reshape(Z, seq, width), give.reshape(Z, seq, width), *sums)
    outs = outs[4:] if fused else outs
    return outs[:4], outs[4], outs[5]


def scatter_entry(m_size, fused, *refs):
    if fused:
        refs = refs[:-11] + (refs[-11:-7],) + refs[-7:-5] + (refs[-5:-1],) + refs[-1:]
    scatter_kernel(m_size, fused, *refs)


def update_kernel(step, steps, *refs):
    rows, cotangent, back, bias, qk, vo, up, dn = refs[:8]
    attn, mlp, small_sums, small, refs = refs[8:11], refs[11:14], refs[14], refs[15:18], refs[18:]
    (block_out, input_grad), attn_outs, mlp_outs, small_outs = refs[:2], refs[2:6], refs[6:10], refs[10:14]
    attn_v, mlp_v, attn_new, mlp_new, in_sem, out_sem = refs[14:]
    i = pl.program_id(0)

    def copies(i, sources, buffer, sems, at, out):
        slot = lax.rem(i, 2)
        span = pl.ds(pl.multiple_of(i * step, step), step)
        made = []
        for n, ref in enumerate(sources):
            for j in range(ref.shape[1]):
                far, near = ref.at[span, j, :], buffer.at[slot, n, j]
                pair = (near, far) if out else (far, near)
                made.append(pltpu.make_async_copy(*pair, sems.at[slot, at + n, j]))
        return made

    loads = lambda i: copies(i, attn, attn_v, in_sem, 0, False) + copies(i, mlp, mlp_v, in_sem, 3, False)
    stores = lambda i: copies(i, attn_outs, attn_new, out_sem, 0, True) + copies(i, mlp_outs, mlp_new, out_sem, 4, True)

    @pl.when(i == 0)
    def _():
        for one in loads(0):
            one.start()
        g = small_sums[0 : small[0].shape[0], 0 : small[0].shape[1]]
        for ref, value in zip(small_outs, (g, *adam_step(small[0][...], g, small[1][...], small[2][...]))):
            ref[...] = value

    @pl.when(i + 1 < steps)
    def _():
        for one in loads(i + 1):
            one.start()

    normed, inverse = layer_stats(rows[...])
    block_out[...] = rows[...] + back[0].astype(f32) + bias[...]
    u = back[1].astype(f32)
    input_grad[...] = cotangent[...] + inverse * (
        u
        - jnp.mean(u, axis=-1, keepdims=True)
        - normed * jnp.mean(u * normed, axis=-1, keepdims=True)
    )

    @pl.when(i >= 2)
    def _():
        for one in stores(i - 2):
            one.wait()

    for one in loads(i):
        one.wait()
    slot = lax.rem(i, 2)
    for sources, olds, news in (((qk, qk, vo, vo), attn_v, attn_new), ((up, dn), mlp_v, mlp_new)):
        kinds, wide = olds.shape[2], olds.shape[4] // Z
        for j in range(kinds):
            at = j % (kinds // 2) * wide
            for q in range(Z):
                cols = slice(q * wide, (q + 1) * wide)
                g = sources[j][q, :, at : at + wide].astype(f32)
                updated = adam_step(olds[slot, 0, j, :, cols], g, olds[slot, 1, j, :, cols], olds[slot, 2, j, :, cols])
                for n, value in enumerate((g, *updated)):
                    news[slot, n, j, :, cols] = value
    for one in stores(i):
        one.start()

    @pl.when(i == steps - 1)
    def _():
        if steps > 1:
            for one in stores(i - 1):
                one.wait()
        for one in stores(i):
            one.wait()


def update(block_in, out_grad, own_rows, bias, own, attn, mlp, small_sums, small):
    rows, width = block_in.shape
    shard = attn[0].shape[0]
    step = min(shard, 32)
    steps = shard // step
    by_rows = pl.BlockSpec((rows // steps, width), lambda i: (i, 0))
    in_place = pl.BlockSpec(memory_space=pl.ANY)
    slots = lambda count, v: pltpu.VMEM((2, count, v.shape[1], step, v.shape[2]), f32)
    return pl.pallas_call(
        functools.partial(update_kernel, step, steps),
        grid=(steps,),
        in_specs=[by_rows, by_rows, pl.BlockSpec((2, rows // steps, width), lambda i: (0, i, 0)), fixed(1, width)]
        + [pl.BlockSpec((Z, step, g.shape[2]), lambda i: (0, i, 0)) for g in own]
        + [in_place] * 6
        + [fixed(*v.shape) for v in (small_sums, *small)],
        out_specs=[by_rows, by_rows] + [in_place] * 8 + [fixed(*small[0].shape)] * 4,
        out_shape=[jax.ShapeDtypeStruct((rows, width), f32)] * 2
        + [jax.ShapeDtypeStruct(attn[0].shape, f32)] * 4
        + [jax.ShapeDtypeStruct(mlp[0].shape, f32)] * 4
        + [jax.ShapeDtypeStruct(small[0].shape, f32)] * 4,
        scratch_shapes=[slots(3, attn[0]), slots(3, mlp[0]), slots(4, attn[0]), slots(4, mlp[0])]
        + [pltpu.SemaphoreType.DMA((2, 6, 4)), pltpu.SemaphoreType.DMA((2, 8, 4))],
        compiler_params=pltpu.CompilerParams(vmem_limit_bytes=VMEM_BYTES),
        name="update",
    )(block_in, out_grad, own_rows, bias, *own, *attn, *mlp, small_sums, *small)


def body(
    block_in,
    positions,
    out_grad,
    attn_weight,
    mlp_weight,
    small_params,
    attn_first,
    attn_second,
    mlp_first,
    mlp_second,
    small_first,
    small_second,
):
    m_size = lax.axis_size("dp") // (2 * Z)
    rows = block_in.shape[0]
    factors, (keep, give), sums = gather(
        attn_weight, mlp_weight, block_in, out_grad, small_params, positions, m_size
    )
    head_sums, up_sums, norm_sums, row_bias, out_sum = sums
    own, own_rows, own_small = scatter(
        factors, keep, give, (norm_sums, head_sums, up_sums, out_sum), m_size, rows
    )
    attn = (attn_weight, attn_first, attn_second)
    mlp = (mlp_weight, mlp_first, mlp_second)
    small = (small_params, small_first, small_second)
    block_out, input_grad, *updated = update(
        block_in, out_grad, own_rows, row_bias, own, attn, mlp, own_small, small
    )
    attn_out, mlp_out = updated[:4], updated[4:8]
    small_grad, small_new, small_first_new, small_second_new = updated[8:]

    attn_grad, attn_new, attn_first_new, attn_second_new = attn_out
    mlp_grad, mlp_new, mlp_first_new, mlp_second_new = mlp_out
    return (
        block_out,
        input_grad,
        attn_grad,
        mlp_grad,
        small_grad,
        attn_new,
        attn_first_new,
        attn_second_new,
        mlp_new,
        mlp_first_new,
        mlp_second_new,
        small_new,
        small_first_new,
        small_second_new,
    )


def solution(mesh):
    rows = P(("dp", "tensor"), None)
    weights = P("dp", None, "tensor")
    small = P(None, ("dp", "tensor"))
    return jax.shard_map(
        body,
        mesh=mesh,
        in_specs=(rows, P("dp", None), rows, weights, weights, small, weights, weights, weights, weights, small, small),
        out_specs=(rows, rows) + (weights,) * 2 + (small,) + (weights,) * 6 + (small,) * 3,
        check_vma=False,
    )
```
